32 devices in a mesh: band: 4 (over z), ga: 8 (over y, x, core).
Axes of the slice: x: 2, y: 2, z: 4, core: 2. Of those that a mesh axis runs over, the one named last changes fastest.
Arguments:
- coeffs: float32 [2, 4, 18432], P(None, 'band', 'ga'), may hold values from -8 to 8
- cell_map: int32 [18432], P('ga'), may hold values from 0 to 110591, as said below
- potential: float32 [96, 96, 96], P(None, 'ga'), may hold values from -2 to 1
- projectors: float32 [2, 64, 18432], P(None, None, 'ga'), may hold values from -6 to 6
- strengths: float32 [8, 8, 8], replicated, may hold values from -2 to 2
- proj_atom: int32 [64], replicated, may hold values from 0 to 7, as said below
- proj_chan: int32 [64], replicated, may hold values from 0 to 7, as said below
Outputs:
- new_bands: float32 [2, 4, 18432], P(None, 'band', 'ga')
- energy: float32 [4], P('band')
- residual_norm: float32 [4], P('band')
- correlation: float32 [2, 4, 4], P(None, 'band')
- subspace: float32 [2, 4, 4], P(None, 'band')
The draws below stay inside these ranges and needn't reach their ends.
Inputs may be any that keep to these rules, and one draw needn't show every extreme that they name: `cell_map`: in block d (entries d * 2304 to (d + 1) * 2304 - 1) the entries are distinct cells (i * 96 + y) * 96 + z of grid planes x = d + 8 * i. `proj_atom`: each pair of atom and channel belongs to exactly one projector. `proj_chan`: each pair of atom and channel belongs to exactly one projector.
All inputs are finite; a program needn't handle non-finite values.
Results may differ from the reference program's by a relative error of at most 0.0002.
Values sent between devices are 32-bit elements; how exact they have to be, the bound alone decides.
A program may use at most 64 MiB of HBM per device.

```python
import jax
import jax.numpy as jnp
from jax import lax

NG = 96
PW_DEV = 2304
NATOM = 8
NCH = 8
NPROJ = 64
PW_BLOCKS = 8
NPW = 18432
NBANDS = 4


kin_unit = 0.02


def signed_freq_drawn(index_arr):
    return jnp.where(index_arr < NG // 2, index_arr, index_arr - NG)


def sphere_cells(key):
    block_count = NPW // PW_DEV
    planes = NG // block_count
    slab_cells = planes * NG * NG
    cell_ids = jnp.arange(slab_cells, dtype=jnp.int32)
    plane_num = cell_ids // (NG * NG)
    freq_y = signed_freq_drawn(cell_ids // NG % NG)
    freq_z = signed_freq_drawn(cell_ids % NG)

    def pick_cells(block_key, block_num):
        freq_x = signed_freq_drawn(block_num + block_count * plane_num)
        radius_sq = freq_x * freq_x + freq_y * freq_y + freq_z * freq_z
        jitter_key, order_key = jax.random.split(block_key)
        jitter_score = radius_sq * 8 + jax.random.randint(jitter_key, (slab_cells,), 0, 192, dtype=jnp.int32)
        chosen = jnp.argsort(jitter_score, stable=True)[:PW_DEV]
        shuffle = jax.random.permutation(order_key, PW_DEV)
        return chosen[shuffle].astype(jnp.int32)
    block_keys = jax.random.split(key, block_count)
    block_nums = jnp.arange(block_count, dtype=jnp.int32)
    return jax.vmap(pick_cells)(block_keys, block_nums).reshape(NPW)


def cell_energy(cells):
    block_count = NPW // PW_DEV
    owner = jnp.arange(NPW, dtype=jnp.int32) // PW_DEV
    freq_x = signed_freq_drawn(owner + block_count * (cells // (NG * NG)))
    freq_y = signed_freq_drawn(cells // NG % NG)
    freq_z = signed_freq_drawn(cells % NG)
    return kin_unit * (freq_x * freq_x + freq_y * freq_y + freq_z * freq_z).astype(jnp.float32)


def projector_values(key):
    cells = sphere_cells(jax.random.fold_in(key, 11))
    energy = cell_energy(cells)
    shape_key, scale_key = jax.random.split(jax.random.fold_in(key, 23))
    raw_values = jax.random.truncated_normal(shape_key, -6.0, 6.0, (2, NPROJ, NPW), jnp.float32)
    row_scale = jnp.exp(jax.random.uniform(scale_key, (NPROJ,), jnp.float32, -0.7, 0.7))
    shaped = raw_values * row_scale[None, :, None] / (1.0 + energy / 8.0)[None, None, :]
    return (jnp.clip(shaped, -6.0, 6.0), energy)


def draw_cell_map(key, part):
    return sphere_cells(jax.random.fold_in(key, 11))


def draw_projectors(key, part):
    return projector_values(key)[0]


def draw_coeffs(key, part):
    projectors, energy = projector_values(key)
    noise_key, mix_key, common_key, scale_key = jax.random.split(jax.random.fold_in(key, 37), 4)
    envelope = 1.0 / (1.0 + energy / 4.0)
    noise = jax.random.truncated_normal(noise_key, -6.0, 6.0, (2, NBANDS, NPW), jnp.float32)
    mixing = jax.random.truncated_normal(mix_key, -4.0, 4.0, (2, NBANDS, NPROJ), jnp.float32) * (0.5 / NPROJ ** 0.5)
    along_re = jnp.einsum('bp,pg->bg', mixing[0], projectors[0]) - jnp.einsum('bp,pg->bg', mixing[1], projectors[1])
    along_im = jnp.einsum('bp,pg->bg', mixing[0], projectors[1]) + jnp.einsum('bp,pg->bg', mixing[1], projectors[0])
    values = noise * envelope[None, None, :] + jnp.stack([along_re, along_im])
    return jnp.clip(values, -8.0, 8.0)


def projector_slots(key):
    ordering = jax.random.permutation(jax.random.fold_in(key, 51), NPROJ).astype(jnp.int32)
    return (ordering // NCH, ordering % NCH)


def draw_proj_atom(key, part):
    return projector_slots(key)[0]


def draw_proj_chan(key, part):
    return projector_slots(key)[1]


def shard_levels(key, extent, cuts, low, top_value):
    loudness = 1.0
    for axis_at, shards_of in cuts:
        heights = jax.random.uniform(jax.random.fold_in(jax.random.fold_in(key, 6), axis_at), (shards_of,), jnp.float32, low / len(cuts), top_value / len(cuts))
        loudness = loudness * jnp.repeat(jnp.exp(heights), extent[axis_at] // shards_of).reshape((-1,) + (1,) * (len(extent) - 1 - axis_at))
    return loudness


def setup_inputs(seed: int = 0) -> dict:
    arg_keys = jax.random.split(jax.random.key(seed), 8)
    coeffs = draw_coeffs(jax.random.fold_in(arg_keys[7], 71), 0)
    cell_map = draw_cell_map(jax.random.fold_in(arg_keys[7], 71), 0)
    potential = jnp.clip(-2.0 + 3.0 * jax.random.uniform(arg_keys[2], (NG, NG, NG), jnp.float32) ** shard_levels(arg_keys[2], (NG, NG, NG), ((1, 8),), -0.2, 0.2), -2.0, 1.0)
    projectors = draw_projectors(jax.random.fold_in(arg_keys[7], 71), 0)
    strengths = jnp.clip(jax.random.uniform(arg_keys[4], (NATOM, NCH, NCH), jnp.float32, -2.0, 2.0), -2.0, 2.0)
    proj_atom = draw_proj_atom(jax.random.fold_in(arg_keys[7], 71), 0)
    proj_chan = draw_proj_chan(jax.random.fold_in(arg_keys[7], 71), 0)
    return dict(coeffs=coeffs, cell_map=cell_map, potential=potential, projectors=projectors, strengths=strengths, proj_atom=proj_atom, proj_chan=proj_chan)


top_precision = lax.Precision.HIGHEST
kin_unit = 0.02
small_eps = 1e-6


def signed_freq(index_arr):
    return jnp.where(index_arr < NG // 2, index_arr, index_arr - NG)


def coupling_matrix(proj_atom, proj_chan, strengths):
    symmetric = 0.5 * (strengths + jnp.swapaxes(strengths, 1, 2))
    atom_hot = (proj_atom[:, None] == jnp.arange(NATOM, dtype=jnp.int32)[None, :]).astype(jnp.float32)
    chan_hot = (proj_chan[:, None] == jnp.arange(NCH, dtype=jnp.int32)[None, :]).astype(jnp.float32)
    rows_d = jnp.einsum("pa,pc,acd->pd", atom_hot, chan_hot, symmetric, precision=top_precision)
    same_atom = jnp.dot(atom_hot, atom_hot.T, precision=top_precision, preferred_element_type=jnp.float32)
    return same_atom * jnp.dot(rows_d, chan_hot.T, precision=top_precision, preferred_element_type=jnp.float32)


def band_dot(left_vec, right_vec, weight):
    return jnp.sum(left_vec * right_vec * weight, axis=(0, 2)) / NPW


def per_band(values):
    return values[None, :, None]


def precondition(residual, kinetic, kin_level):
    x_ratio = kinetic[None, :] / (1.5 * kin_level[:, None] + 1.0)
    numer_poly = 27.0 + x_ratio * (18.0 + x_ratio * (12.0 + 8.0 * x_ratio))
    square = x_ratio * x_ratio
    return residual * (numer_poly / (numer_poly + 16.0 * square * square))[None]


def pair_products(left_vec, right_vec):
    def contract(first_part, second_part):
        return jnp.einsum("bg,cg->bc", first_part, second_part, precision=top_precision)
    real_part = contract(left_vec[0], right_vec[0]) + contract(left_vec[1], right_vec[1])
    imag_part = contract(left_vec[0], right_vec[1]) - contract(left_vec[1], right_vec[0])
    return jnp.stack([real_part, imag_part])


def local_one(vector, flat_cells, potential):
    values = vector[0] + 1j * vector[1]
    grid_g = jnp.zeros((NG * NG * NG,), values.dtype).at[flat_cells].set(values)
    space = jnp.fft.ifftn(grid_g.reshape(NG, NG, NG)) * potential
    back = jnp.fft.fftn(space).reshape(NG * NG * NG)[flat_cells]
    return jnp.stack([jnp.real(back), jnp.imag(back)])


def reference(coeffs, cell_map, potential, projectors, strengths, proj_atom, proj_chan):
    owner = jnp.arange(NPW, dtype=jnp.int32) // PW_DEV
    x_index = owner + PW_BLOCKS * (cell_map // (NG * NG))
    y_index = (cell_map // NG) % NG
    z_index = cell_map % NG
    flat_cells = (x_index * NG + y_index) * NG + z_index
    freq_x = signed_freq(x_index)
    freq_y = signed_freq(y_index)
    freq_z = signed_freq(z_index)
    kinetic = kin_unit * (freq_x * freq_x + freq_y * freq_y + freq_z * freq_z).astype(jnp.float32)
    kin_weight = kinetic[None, None, :]
    coupling = coupling_matrix(proj_atom, proj_chan, strengths)

    def contract(first_part, second_part):
        return jnp.einsum("pg,bg->pb", first_part, second_part, precision=top_precision)

    def spread(weights, proj_table):
        return jnp.einsum("pb,pg->bg", weights, proj_table, precision=top_precision)

    def apply_h(vectors):
        local_term = lax.map(lambda vector: local_one(vector, flat_cells, potential), jnp.swapaxes(vectors, 0, 1))
        local_term = jnp.swapaxes(local_term, 0, 1)
        proj_re = (contract(projectors[0], vectors[0]) + contract(projectors[1], vectors[1])) / NPW
        proj_im = (contract(projectors[0], vectors[1]) - contract(projectors[1], vectors[0])) / NPW
        mixed_re = jnp.dot(coupling, proj_re, precision=top_precision, preferred_element_type=jnp.float32)
        mixed_im = jnp.dot(coupling, proj_im, precision=top_precision, preferred_element_type=jnp.float32)
        out_re = spread(mixed_re, projectors[0]) - spread(mixed_im, projectors[1])
        out_im = spread(mixed_re, projectors[1]) + spread(mixed_im, projectors[0])
        return kin_weight * vectors + local_term + jnp.stack([out_re, out_im])

    h_zero = apply_h(coeffs)
    eps_zero = band_dot(coeffs, h_zero, 1.0) / (band_dot(coeffs, coeffs, 1.0) + small_eps)
    r_zero = h_zero - per_band(eps_zero) * coeffs
    level_zero = band_dot(r_zero, r_zero, kin_weight) / (band_dot(r_zero, r_zero, 1.0) + small_eps)
    p_zero = precondition(r_zero, kinetic, level_zero)
    g_zero = apply_h(p_zero)
    q_zero = g_zero - per_band(eps_zero) * p_zero
    lam_zero = -band_dot(r_zero, q_zero, 1.0) / (band_dot(q_zero, q_zero, 1.0) + small_eps)
    psi_one = coeffs + per_band(lam_zero) * p_zero
    h_one = h_zero + per_band(lam_zero) * g_zero
    eps_one = band_dot(psi_one, h_one, 1.0) / (band_dot(psi_one, psi_one, 1.0) + small_eps)
    r_one = h_one - per_band(eps_one) * psi_one
    change = r_zero - r_one
    weight_one = band_dot(r_zero, change, 1.0) / (band_dot(change, change, 1.0) + small_eps)
    step_mid = weight_one * lam_zero
    psi_mid = coeffs + per_band(step_mid) * p_zero
    h_mid = h_zero + per_band(step_mid) * g_zero
    r_mid = r_zero - per_band(weight_one) * change
    eps_mid = band_dot(psi_mid, h_mid, 1.0) / (band_dot(psi_mid, psi_mid, 1.0) + small_eps)
    level_mid = band_dot(r_mid, r_mid, kin_weight) / (band_dot(r_mid, r_mid, 1.0) + small_eps)
    p_one = precondition(r_mid, kinetic, level_mid)
    g_one = apply_h(p_one)
    q_one = g_one - per_band(eps_mid) * p_one
    lam_one = -band_dot(r_mid, q_one, 1.0) / (band_dot(q_one, q_one, 1.0) + small_eps)
    new_bands = psi_mid + per_band(lam_one) * p_one
    new_ham = h_mid + per_band(lam_one) * g_one
    norm_new = band_dot(new_bands, new_bands, 1.0) + small_eps
    energy = band_dot(new_bands, new_ham, 1.0) / norm_new
    residual = new_ham - per_band(energy) * new_bands
    residual_norm = band_dot(residual, residual, 1.0) / norm_new
    correlation = pair_products(new_bands, new_bands) / NPW
    subspace = pair_products(new_bands, new_ham) / NPW
    return new_bands, energy, residual_norm, correlation, subspace
```

```python
import functools

import jax
import jax.numpy as jnp
import numpy as np
from jax import lax
from jax.experimental import pallas as pl
from jax.experimental.pallas import tpu as pltpu
from jax.sharding import PartitionSpec as P

top_precision = lax.Precision.HIGHEST
kin_unit = 0.02
small_eps = 1e-06


def signed_freq(index_arr, grid_len):
    return jnp.where(index_arr < grid_len // 2, index_arr, index_arr - grid_len)


def wave_tables(grid_len, row_freq, col_freq, sign_val, factor):
    phase = row_freq[:, None] * col_freq[None, :] % grid_len
    angle = 2.0 * jnp.pi / grid_len * phase.astype(jnp.float32)
    return (jnp.cos(angle) * factor, jnp.sin(angle) * (sign_val * factor))


def block_table(cos_table, sin_table):
    upper = jnp.concatenate([cos_table, sin_table], axis=1)
    lower = jnp.concatenate([-sin_table, cos_table], axis=1)
    return jnp.concatenate([upper, lower], axis=0)


def quarter_turn(grid_vals):
    half_len = grid_vals.shape[-1] // 2
    return jnp.concatenate([-grid_vals[..., half_len:], grid_vals[..., :half_len]], axis=-1)


def mix_dim(grid_vals, cos_table, sin_table, pattern):
    direct = jnp.einsum(pattern, cos_table, grid_vals, precision=top_precision)
    turned = jnp.einsum(pattern, sin_table, quarter_turn(grid_vals), precision=top_precision)
    return direct + turned


def mix_last(grid_vals, table_full):
    row_width = grid_vals.shape[-1]
    product = jnp.dot(
        grid_vals.reshape(-1, row_width),
        table_full,
        precision=top_precision,
        preferred_element_type=jnp.float32,
    )
    return product.reshape(grid_vals.shape)


def band_dot(left_vec, right_vec, weight):
    return jnp.sum(left_vec * right_vec * weight, axis=(0, 2))


def per_band(values):
    return values[None, :, None]


def pair_products(left_vec, right_vec):

    def contract(first_part, second_part):
        return jnp.einsum("bg,cg->bc", first_part, second_part, precision=top_precision)

    real_part = contract(left_vec[0], right_vec[0]) + contract(left_vec[1], right_vec[1])
    imag_part = contract(left_vec[0], right_vec[1]) - contract(left_vec[1], right_vec[0])
    return jnp.stack([real_part, imag_part])


def precondition(residual, kinetic, kin_level):
    x_ratio = kinetic[None, :] / (1.5 * kin_level[:, None] + 1.0)
    numer_poly = 27.0 + x_ratio * (18.0 + x_ratio * (12.0 + 8.0 * x_ratio))
    square = x_ratio * x_ratio
    return residual * (numer_poly / (numer_poly + 16.0 * square * square))[None]


def coupling_matrix(proj_atom, proj_chan, strengths):
    atom_count = strengths.shape[0]
    chan_count = strengths.shape[1]
    symmetric = 0.5 * (strengths + jnp.swapaxes(strengths, 1, 2))
    atom_hot = (proj_atom[:, None] == jnp.arange(atom_count, dtype=jnp.int32)[None, :]).astype(
        jnp.float32
    )
    chan_hot = (proj_chan[:, None] == jnp.arange(chan_count, dtype=jnp.int32)[None, :]).astype(
        jnp.float32
    )
    rows_d = jnp.einsum("pa,pc,acd->pd", atom_hot, chan_hot, symmetric, precision=top_precision)
    same_atom = jnp.dot(
        atom_hot, atom_hot.T, precision=top_precision, preferred_element_type=jnp.float32
    )
    return same_atom * jnp.dot(
        rows_d, chan_hot.T, precision=top_precision, preferred_element_type=jnp.float32
    )


def combine(term_list):
    merged = {}
    for scalar, coef_map in term_list:
        for index_one, coef_a in coef_map.items():
            merged[index_one] = merged.get(index_one, 0.0) + scalar * coef_a
    return merged


def gram_form(gram_table, left_map, right_map, use_kin):
    running = 0.0
    for index_one, coef_a in left_map.items():
        for index_two, coef_b in right_map.items():
            running = running + coef_a * coef_b * gram_table[use_kin, index_one, index_two]
    return running


def new_pairs(first_new, last_new, kinds):
    pair_list = []
    for use_kin in kinds:
        for index_two in range(first_new, last_new):
            for index_one in range(index_two + 1):
                pair_list.append((index_one, index_two, use_kin))
    return pair_list


def plain_body(coeffs, cell_map, potential, projectors, strengths, proj_atom, proj_chan):
    ga_count = lax.axis_size("ga")
    grid_len = potential.shape[0]
    planes = grid_len // ga_count
    band_local = coeffs.shape[1]
    total_pw = coeffs.shape[2] * ga_count
    device = lax.axis_index("ga")
    plane_num = cell_map // (grid_len * grid_len)
    y_index = cell_map // grid_len % grid_len
    z_index = cell_map % grid_len
    freq_x = signed_freq(device + ga_count * plane_num, grid_len)
    freq_y = signed_freq(y_index, grid_len)
    freq_z = signed_freq(z_index, grid_len)
    kinetic = kin_unit * (freq_x * freq_x + freq_y * freq_y + freq_z * freq_z).astype(jnp.float32)
    kin_weight = kinetic[None, None, :]
    slot_re = (plane_num * grid_len + y_index) * (2 * grid_len) + z_index
    slot_im = slot_re + grid_len
    cell_count = planes * grid_len * 2 * grid_len
    natural = jnp.arange(grid_len, dtype=jnp.int32)
    cyclic = natural % planes * ga_count + natural // planes
    cos_fwd, sin_fwd = wave_tables(grid_len, natural, natural, 1.0, 1.0)
    cos_back, sin_back = wave_tables(grid_len, natural, natural, -1.0, 1.0 / grid_len)
    z_forward = block_table(cos_fwd, sin_fwd)
    z_backward = block_table(cos_back, sin_back)
    xcos_fwd, xsin_fwd = wave_tables(grid_len, natural, cyclic, 1.0, 1.0)
    xcos_back, xsin_back = wave_tables(grid_len, cyclic, natural, -1.0, 1.0 / grid_len)
    doubled = jnp.concatenate([potential, potential], axis=-1)
    coupling = coupling_matrix(proj_atom, proj_chan, strengths)

    def real_space(grid_vals):
        grid_vals = mix_dim(grid_vals, xcos_fwd, xsin_fwd, "kj,bjyw->bkyw")
        grid_vals = grid_vals * doubled[None]
        grid_vals = mix_dim(grid_vals, xcos_back, xsin_back, "jk,bkyw->bjyw")
        return lax.all_to_all(grid_vals, "ga", split_axis=1, concat_axis=2, tiled=True)

    def local_part(vectors):
        item_count = vectors.shape[1]
        flat_grid = jnp.zeros((item_count, cell_count), jnp.float32)
        flat_grid = flat_grid.at[:, slot_re].set(vectors[0]).at[:, slot_im].set(vectors[1])
        grid_vals = mix_last(
            flat_grid.reshape(item_count, planes, grid_len, 2 * grid_len), z_forward
        )
        grid_vals = mix_dim(grid_vals, cos_fwd, sin_fwd, "ky,bpyw->bpkw")
        grid_vals = real_space(
            lax.all_to_all(grid_vals, "ga", split_axis=2, concat_axis=1, tiled=True)
        )
        grid_vals = mix_dim(grid_vals, cos_back, sin_back, "ky,bpyw->bpkw")
        flat_grid = mix_last(grid_vals, z_backward).reshape(item_count, cell_count)
        return jnp.stack([flat_grid[:, slot_re], flat_grid[:, slot_im]])

    def contract(first_part, second_part):
        return jnp.einsum("pg,bg->pb", first_part, second_part, precision=top_precision)

    def spread(weights, proj_table):
        return jnp.einsum("pb,pg->bg", weights, proj_table, precision=top_precision)

    def projected_part(vectors):
        proj_re = contract(projectors[0], vectors[0]) + contract(projectors[1], vectors[1])
        proj_im = contract(projectors[0], vectors[1]) - contract(projectors[1], vectors[0])
        proj_re, proj_im = lax.psum((proj_re, proj_im), "ga")
        mixed_re = jnp.dot(
            coupling,
            proj_re / total_pw,
            precision=top_precision,
            preferred_element_type=jnp.float32,
        )
        mixed_im = jnp.dot(
            coupling,
            proj_im / total_pw,
            precision=top_precision,
            preferred_element_type=jnp.float32,
        )
        out_re = spread(mixed_re, projectors[0]) - spread(mixed_im, projectors[1])
        out_im = spread(mixed_re, projectors[1]) + spread(mixed_im, projectors[0])
        return jnp.stack([out_re, out_im])

    def apply_h(vectors):
        return kin_weight * vectors + local_part(vectors) + projected_part(vectors)

    def gram_sums(basis, pair_list):
        stacked = []
        for index_one, index_two, use_kin in pair_list:
            stacked.append(
                band_dot(basis[index_one], basis[index_two], kin_weight if use_kin else 1.0)
            )
        summed = lax.psum(jnp.stack(stacked), "ga") / total_pw
        found = {}
        for slot_num, entry in enumerate(pair_list):
            index_one, index_two, use_kin = entry
            found[use_kin, index_one, index_two] = summed[slot_num]
            found[use_kin, index_two, index_one] = summed[slot_num]
        return found

    def realize(coef_map, basis):
        running = jnp.zeros_like(basis[0])
        for index_one, coef_a in coef_map.items():
            running = (
                running
                + per_band(jnp.zeros((band_local,), jnp.float32) + coef_a) * basis[index_one]
            )
        return running

    h_zero = apply_h(coeffs)
    basis = [coeffs, h_zero]
    gram_table = gram_sums(basis, new_pairs(0, 2, (False, True)))
    psi_map = {0: 1.0}
    ham_map = {1: 1.0}
    eps_zero = gram_form(gram_table, psi_map, ham_map, False) / (
        gram_form(gram_table, psi_map, psi_map, False) + small_eps
    )
    r_map = combine([(1.0, ham_map), (-eps_zero, psi_map)])
    level_zero = gram_form(gram_table, r_map, r_map, True) / (
        gram_form(gram_table, r_map, r_map, False) + small_eps
    )
    p_zero = precondition(realize(r_map, basis), kinetic, level_zero)
    g_zero = apply_h(p_zero)
    basis = [coeffs, h_zero, p_zero, g_zero]
    gram_table.update(gram_sums(basis, new_pairs(2, 4, (False, True))))
    q_map = combine([(1.0, {3: 1.0}), (-eps_zero, {2: 1.0})])
    lam_zero = -gram_form(gram_table, r_map, q_map, False) / (
        gram_form(gram_table, q_map, q_map, False) + small_eps
    )
    psi_one_map = combine([(1.0, psi_map), (lam_zero, {2: 1.0})])
    h_one_map = combine([(1.0, ham_map), (lam_zero, {3: 1.0})])
    eps_one = gram_form(gram_table, psi_one_map, h_one_map, False) / (
        gram_form(gram_table, psi_one_map, psi_one_map, False) + small_eps
    )
    r_one_map = combine([(1.0, h_one_map), (-eps_one, psi_one_map)])
    change_map = combine([(1.0, r_map), (-1.0, r_one_map)])
    weight_one = gram_form(gram_table, r_map, change_map, False) / (
        gram_form(gram_table, change_map, change_map, False) + small_eps
    )
    step_mid = weight_one * lam_zero
    psi_mid_map = combine([(1.0, psi_map), (step_mid, {2: 1.0})])
    h_mid_map = combine([(1.0, ham_map), (step_mid, {3: 1.0})])
    r_mid_map = combine([(1.0, r_map), (-weight_one, change_map)])
    eps_mid = gram_form(gram_table, psi_mid_map, h_mid_map, False) / (
        gram_form(gram_table, psi_mid_map, psi_mid_map, False) + small_eps
    )
    level_mid = gram_form(gram_table, r_mid_map, r_mid_map, True) / (
        gram_form(gram_table, r_mid_map, r_mid_map, False) + small_eps
    )
    p_one = precondition(realize(r_mid_map, basis), kinetic, level_mid)
    g_one = apply_h(p_one)
    basis = [coeffs, h_zero, p_zero, g_zero, p_one, g_one]
    gram_table.update(gram_sums(basis, new_pairs(4, 6, (False,))))
    q_one_map = combine([(1.0, {5: 1.0}), (-eps_mid, {4: 1.0})])
    lam_one = -gram_form(gram_table, r_mid_map, q_one_map, False) / (
        gram_form(gram_table, q_one_map, q_one_map, False) + small_eps
    )
    new_map = combine([(1.0, psi_mid_map), (lam_one, {4: 1.0})])
    ham_new_map = combine([(1.0, h_mid_map), (lam_one, {5: 1.0})])
    norm_new = gram_form(gram_table, new_map, new_map, False) + small_eps
    energy = gram_form(gram_table, new_map, ham_new_map, False) / norm_new
    resid_map = combine([(1.0, ham_new_map), (-energy, new_map)])
    residual_norm = gram_form(gram_table, resid_map, resid_map, False) / norm_new
    new_bands = realize(new_map, basis)
    new_ham = realize(ham_new_map, basis)
    blank_rows = jnp.zeros((2, band_local, band_local * lax.axis_size("band")), jnp.float32)
    first_row = jnp.int32(0)
    over_rows = blank_rows
    ham_rows = blank_rows
    piece_bands = lax.all_gather(new_bands, "band", axis=1, tiled=True)
    piece_ham = lax.all_gather(new_ham, "band", axis=1, tiled=True)
    over_rows = lax.dynamic_update_slice_in_dim(
        over_rows, pair_products(new_bands, piece_bands), first_row, 2
    )
    ham_rows = lax.dynamic_update_slice_in_dim(
        ham_rows, pair_products(new_bands, piece_ham), first_row, 2
    )
    over_rows, ham_rows = (over_rows, ham_rows)
    over_rows, ham_rows = lax.psum((over_rows, ham_rows), "ga")
    correlation = over_rows / total_pw
    subspace = ham_rows / total_pw
    return (new_bands, energy, residual_norm, correlation, subspace)


QUAD = 4
TRIPLE = 3
WIDE = 256
MESH = pl.DeviceIdType.MESH


def split_const(values):
    high = np.asarray(values, np.float32).astype(jnp.bfloat16)
    low = (values - high.astype(np.float64)).astype(np.float32).astype(jnp.bfloat16)
    return np.stack([high, low])


def const_tables(grid_len, group):
    planes = grid_len // group
    chunks = planes // QUAD
    unit = 2.0 * np.pi / grid_len
    quarter = grid_len / 4.0
    dev = np.arange(group)[:, None, None, None]
    chunk = np.arange(chunks)[None, :, None, None]
    part = np.arange(2)[None, None, :, None]
    inner = np.arange(QUAD)[None, None, None, :]
    y_real = (dev * planes + chunk * QUAD + inner + 0 * part).reshape(group, -1)
    part_row = (part + 0 * (dev + chunk + inner)).reshape(group, -1)
    freq = np.arange(grid_len)
    phase = (y_real[..., None] * freq) % grid_len
    tab_a = np.cos(unit * (phase - quarter * part_row[..., None]))
    tab_b = np.cos(unit * (phase + quarter * (1 - part_row[..., None])))
    high, low = split_const(np.concatenate([tab_a, tab_b], axis=1))
    wave = np.concatenate([high, low], axis=2)
    four = np.repeat(np.arange(4), grid_len)
    zed = np.tile(freq, 4)
    theta = 2.0 * np.pi * ((four[:, None] * four[None, :] % 4) / 4.0
                           + (zed[:, None] * zed[None, :] % grid_len) / grid_len)
    fourz = split_const(np.concatenate([np.cos(theta), np.sin(theta)], axis=1))
    dft = 2.0 * np.pi * np.outer(np.arange(group), np.arange(group)) / group
    real_mix = np.zeros((group, 2, QUAD, group, 2, QUAD))
    for row in range(QUAD):
        real_mix[:, 0, row, :, 0, row] = np.cos(dft)
        real_mix[:, 1, row, :, 1, row] = np.cos(dft)
        real_mix[:, 0, row, :, 1, row] = -np.sin(dft)
        real_mix[:, 1, row, :, 0, row] = np.sin(dft)
    size = group * 2 * QUAD
    real_mix = real_mix.reshape(size, size)

    def stacked(mat):
        high, low = split_const(mat)
        return np.concatenate([high, high, low], axis=1)

    across = np.stack([stacked(real_mix), stacked(real_mix.T)])
    b_lane = np.repeat(np.arange(TRIPLE), 4 * grid_len)
    a_lane = np.tile(np.repeat(np.arange(4), grid_len), TRIPLE)
    one = 2.0 * np.pi * (a_lane * b_lane) / planes
    two = unit * np.outer(np.arange(group), TRIPLE * a_lane + b_lane)
    lane_tw = np.stack([np.cos(one), np.sin(one)]).astype(np.float32)[:, None, :]
    dev_tw = np.stack([np.cos(two), np.sin(two)]).astype(np.float32)[:, :, None, :]
    return wave, fourz, across, lane_tw, dev_tw


def two_parts(values):
    high = values.astype(jnp.bfloat16)
    low = (values - high.astype(jnp.float32)).astype(jnp.bfloat16)
    return high, low


def split_rows(values):
    high = values.astype(jnp.bfloat16).astype(jnp.float32)
    return jnp.concatenate([high, values - high], axis=0).astype(jnp.bfloat16)


def bdot(left, right):
    return jnp.dot(left, right, preferred_element_type=jnp.float32)


def bdot_t(left, right):
    return lax.dot_general(left, right, (((1,), (1,)), ((), ())), preferred_element_type=jnp.float32)


def total_of(values):
    return jnp.sum(jnp.sum(values, axis=0, keepdims=True), axis=1, keepdims=True)


def sweep_kernel(
    dims,
    coeffs_ref, cell_ref, potential_hbm, proj_hbm, strength_ref, atom_ref, chan_ref,
    wave_ref, fourz_hbm, across_ref, lane_ref, dev_ref,
    new_ref, scal_ref,
    hot_ref, mask_ref, group_ref, ta_ref, tb_ref, kin_ref, field_ref, back_ref,
    pot_ref, potential_ref, proj_ref, fourz_ref, couple_ref, in_vec, out_vec, save_ref, in_sem,
    ksend, krecv, xsend, xrecv, rsend, rrecv, hsend, hrecv, psend, precv,
    gsend, grecv, nsend, nrecv, isend, irecv, lsend, lrecv, csend, crecv,
    ks_sem, kr_sem, xs_sem, xr_sem, rs_sem, rr_sem, hs_sem, hr_sem, ps_sem, pr_sem,
    gs_sem, gr_sem, ns_sem, nr_sem, cs_sem, cr_sem,
):
    group, bands, chunks, grid_len, total_pw, pw = dims
    rows = group * 2 * QUAD
    slab = chunks * 2 * QUAD
    lanes = TRIPLE * 4 * grid_len
    quad_lanes = 4 * grid_len
    folds = -(-lanes // WIDE)
    tiles = pw // 128
    me = lax.axis_index("ga")
    band = lax.axis_index("band")
    sides = [1 - 2 * lax.rem(me // (1 << bit), 2) for bit in range(3)]

    def peer_of(mask):
        return me + sum((sides[bit] << bit) if mask >> bit & 1 else 0 for bit in range(3))

    loads = [
        pltpu.make_async_copy(source, target, in_sem.at[k])
        for k, (source, target) in enumerate(
            ((proj_hbm, proj_ref), (potential_hbm, potential_ref), (fourz_hbm, fourz_ref)))
    ]
    for load in loads:
        load.start()
    barrier = pltpu.get_barrier_semaphore()
    for mask in range(1, group):
        pl.semaphore_signal(barrier, inc=1, device_id={"ga": peer_of(mask)}, device_id_type=MESH)
    for off in range(1, bands):
        pl.semaphore_signal(barrier, inc=1, device_id={"band": lax.rem(band + off, bands)}, device_id_type=MESH)

    cell = cell_ref[...].astype(jnp.float32)
    for k in range(tiles):
        ksend[:, k * 128:(k + 1) * 128] = cell[k:k + 1]
    xsend[...] = coeffs_ref[:, 0, :]

    far_first = (6, 7, 4, 5, 2, 3, 1)

    def spread_copy(mask, send, recv, send_sem, recv_sem, incoming):
        peer = peer_of(mask)
        return pltpu.make_async_remote_copy(
            src_ref=send, dst_ref=recv.at[peer if incoming else me],
            send_sem=send_sem.at[mask - 1], recv_sem=recv_sem.at[mask - 1],
            device_id={"ga": peer}, device_id_type=MESH)

    def spread_start(send, recv, send_sem, recv_sem):
        for mask in far_first:
            spread_copy(mask, send, recv, send_sem, recv_sem, False).start()

    def spread_wait(send, recv, send_sem, recv_sem):
        for mask in range(1, group):
            spread_copy(mask, send, recv, send_sem, recv_sem, True).wait()

    keys = (ksend, krecv, ks_sem, kr_sem)
    firsts = (xsend, xrecv, xs_sem, xr_sem)
    pl.semaphore_wait(barrier, group + bands - 2)
    spread_start(*keys)
    spread_start(*firsts)
    krecv[me] = ksend[...]
    xrecv[me] = xsend[...]

    def whole(values):
        return jnp.floor(values)

    def signed(values):
        return jnp.where(2.0 * values < grid_len, values, values - grid_len)

    def numbers(cells):
        plane = whole((cells + 0.5) * (1.0 / (grid_len * grid_len)))
        in_plane = cells - plane * (grid_len * grid_len)
        y_num = whole((in_plane + 0.5) * (1.0 / grid_len))
        return plane, y_num, in_plane - y_num * grid_len

    def kinetic(plane, y_num, z_num, device):
        f_x = signed(plane * group + device)
        f_y, f_z = signed(y_num), signed(z_num)
        return kin_unit * (f_x * f_x + f_y * f_y + f_z * f_z)

    def marks(numbers_row, count):
        wide_row = jnp.broadcast_to(numbers_row, (16, pw)).astype(jnp.bfloat16)
        row_id = lax.broadcasted_iota(jnp.int32, (16, pw), 0).astype(jnp.float32).astype(jnp.bfloat16)
        one, zero = jnp.ones((16, pw), jnp.bfloat16), jnp.zeros((16, pw), jnp.bfloat16)
        return [jnp.where(row_id + 16.0 * k == wide_row, one, zero) for k in range(count)]

    def build_source(src):
        plane, y_num, z_num = numbers(krecv[src])
        key = plane * grid_len + z_num
        fold = whole((key + 0.5) * (1.0 / WIDE))
        group_ref[src] = fold
        for k, piece in enumerate(marks(key - fold * WIDE, WIDE // 16)):
            hot_ref[src, 16 * k:16 * (k + 1), :] = piece
        wide_fold = jnp.broadcast_to(fold, (16, pw)).astype(jnp.bfloat16)
        one, zero = jnp.ones((16, pw), jnp.bfloat16), jnp.zeros((16, pw), jnp.bfloat16)
        for k in range(folds):
            mask_ref[src, k] = jnp.where(wide_fold == float(k), one, zero)
        y_hot = marks(y_num, grid_len // 16)
        table = bdot(wave_ref[me], jnp.concatenate(y_hot + y_hot, axis=0))
        ta_ref[src] = table[:slab]
        tb_ref[src] = table[slab:]

    def build_potential():
        for part in range(chunks):
            for b in range(TRIPLE):
                for a in range(4):
                    at = (b * 4 + a) * grid_len
                    for dev in range(group):
                        row = dev * lanes // grid_len + TRIPLE * a + b
                        block = potential_ref[part * QUAD:(part + 1) * QUAD, row, :] * (1.0 / grid_len**3)
                        pot_ref[part, dev, :QUAD, at:at + grid_len] = block
                        pot_ref[part, dev, QUAD:, at:at + grid_len] = block

    def build_coupling():
        atoms, chans = strength_ref.shape[0] // strength_ref.shape[1], strength_ref.shape[1]
        size = atoms * chans
        ident = atom_ref[...] * chans + chan_ref[...]
        hot = (lax.broadcasted_iota(jnp.int32, (size, ident.shape[1]), 0) == ident).astype(jnp.float32)
        row_at = lax.broadcasted_iota(jnp.int32, (size, size), 0)
        col_at = lax.broadcasted_iota(jnp.int32, (size, size), 1)
        tiled = jnp.concatenate([strength_ref[...]] * atoms, axis=1)
        same = (row_at // chans == col_at // chans).astype(jnp.float32)
        block = tiled * same
        block = 0.5 * (block + jnp.transpose(block))
        half = lax.dot_general(hot, block, (((0,), (0,)), ((), ())), precision=top_precision, preferred_element_type=jnp.float32)
        couple_ref[...] = jnp.dot(half, hot, precision=top_precision, preferred_element_type=jnp.float32)

    build_coupling()
    for load in loads:
        load.wait()
    build_potential()
    spread_wait(*keys)

    def build_step(src, carry):
        build_source(src)
        return carry

    lax.fori_loop(0, group, build_step, 0)

    def stack_rows(pieces):
        return jnp.concatenate(pieces, axis=0)

    cells = stack_rows([krecv[s] for s in range(group)])
    owner = lax.broadcasted_iota(jnp.int32, (group, pw), 0).astype(jnp.float32)
    kin_ref[...] = kinetic(*numbers(cells), owner)
    spread_wait(*firsts)
    for part in range(2):
        in_vec[0, part] = stack_rows([xrecv[s, part:part + 1] for s in range(group)])

    sign = jnp.where(lax.broadcasted_iota(jnp.int32, (1, 2 * QUAD, 1), 1) < QUAD, -1.0, 1.0).astype(jnp.float32)

    def times_i(values):
        return pltpu.roll(values, QUAD, 1) * sign

    def lane_split(values):
        return [values[..., k * quad_lanes:(k + 1) * quad_lanes] for k in range(TRIPLE)]

    def mix_fourz(triple, direction):
        stacked = jnp.concatenate([t.reshape(rows, quad_lanes) for t in triple], axis=0)
        high, low = two_parts(stacked)
        out = bdot(high, fourz_ref[0]) + bdot(low, fourz_ref[0]) + bdot(high, fourz_ref[1])
        out = out.reshape(TRIPLE * group, 2 * QUAD, 2 * quad_lanes)
        mixed = out[..., :quad_lanes] + direction * times_i(out[..., quad_lanes:])
        return [mixed[k * group:(k + 1) * group] for k in range(TRIPLE)]

    def turn_lane(triple, direction):
        done = [triple[0]]
        for k in range(1, TRIPLE):
            at = slice(k * quad_lanes, (k + 1) * quad_lanes)
            done.append(triple[k] * lane_ref[0, :, at][None] + direction * times_i(triple[k]) * lane_ref[1, :, at][None])
        return done

    def three(triple, direction):
        total = triple[1] + triple[2]
        diff = times_i(triple[1] - triple[2]) * (direction * 0.8660254037844386)
        base = triple[0] - 0.5 * total
        return [triple[0] + total, base + diff, base - diff]

    def turn_dev(values, direction):
        return values * dev_ref[0] + direction * times_i(values) * dev_ref[1]

    def mix_devices(values, which):
        high, low = two_parts(values.reshape(rows, lanes))
        return bdot(across_ref[which], jnp.concatenate([high, low, high], axis=0))

    def own_row(ref, turn, part):
        return ref[turn, part, pl.ds(me, 1), :]

    def put(turn):
        for src in range(group):
            v_re, v_im = in_vec[turn, 0, src:src + 1, :], in_vec[turn, 1, src:src + 1, :]
            both = split_rows(ta_ref[src] * v_re + tb_ref[src] * v_im)
            pieces = []
            for k in range(folds):
                for at in range(0, 2 * slab, 16):
                    pieces.append(both[at:at + 16] * mask_ref[src, k])
            out = bdot_t(jnp.concatenate(pieces, axis=0), hot_ref[src])
            for k in range(folds):
                width = min(WIDE, lanes - k * WIDE)
                base = k * 2 * slab
                for part in range(chunks):
                    at = base + part * 2 * QUAD
                    block = out[at:at + 2 * QUAD] + out[at + slab:at + slab + 2 * QUAD]
                    field_ref[part, src, :, k * WIDE:k * WIDE + width] = block[:, :width]

    def middle(part, carry):
        triple = turn_lane(three(lane_split(field_ref[part]), 1.0), 1.0)
        values = turn_dev(jnp.concatenate(mix_fourz(triple, 1.0), axis=-1), 1.0)
        values = mix_devices(values, 0) * pot_ref[part].reshape(rows, lanes)
        values = mix_devices(values, 1).reshape(group, 2 * QUAD, lanes)
        triple = mix_fourz(lane_split(turn_dev(values, -1.0)), -1.0)
        triple = three(turn_lane(triple, -1.0), -1.0)
        back_ref[part] = jnp.concatenate(triple, axis=-1)
        return carry

    def partial_copy(turn, mask):
        return pltpu.make_async_remote_copy(
            src_ref=rsend.at[turn, mask], dst_ref=rrecv.at[turn, mask],
            send_sem=rs_sem.at[turn, mask - 1], recv_sem=rr_sem.at[turn, mask - 1],
            device_id={"ga": peer_of(mask)}, device_id_type=MESH)

    def take(turn, mask):
        dest = peer_of(mask)
        both = split_rows(jnp.concatenate([back_ref[part, dest] for part in range(chunks)], axis=0))
        if folds * WIDE > lanes:
            both = jnp.concatenate([both, jnp.zeros((2 * slab, folds * WIDE - lanes), jnp.bfloat16)], axis=1)
        stacked = jnp.concatenate([both[:, k * WIDE:(k + 1) * WIDE] for k in range(folds)], axis=0)
        for at in range(0, pw, WIDE):
            span = slice(at, at + WIDE)
            out = bdot(stacked, hot_ref[dest, :, span])
            fold = group_ref[dest, :, span]
            chosen = out[:2 * slab]
            for k in range(1, folds):
                chosen = jnp.where(fold == float(k), out[k * 2 * slab:(k + 1) * 2 * slab], chosen)
            value = chosen[:slab] + chosen[slab:]
            for part, table in enumerate((ta_ref, tb_ref)):
                rsend[turn, mask, part:part + 1, span] = jnp.sum(table[dest, :, span] * value, axis=0, keepdims=True)
        if mask:
            partial_copy(turn, mask).start()

    def sum_copy(off, send, recv, send_sem, recv_sem, incoming):
        source = lax.rem(me + group - off, group) if incoming else me
        return pltpu.make_async_remote_copy(
            src_ref=send, dst_ref=recv.at[source],
            send_sem=send_sem.at[off - 1], recv_sem=recv_sem.at[off - 1],
            device_id={"ga": lax.rem(me + off, group)}, device_id_type=MESH)

    def all_sum(local, send, recv, send_sem, recv_sem):
        send[...] = local
        recv[me] = local
        for off in range(1, group):
            sum_copy(off, send, recv, send_sem, recv_sem, False).start()

    def all_sum_end(send, recv, send_sem, recv_sem):
        for off in range(1, group):
            sum_copy(off, send, recv, send_sem, recv_sem, True).wait()
        running = recv[0]
        for dev in range(1, group):
            running = running + recv[dev]
        return running

    def project(turn):
        found = []
        for part in range(2):
            row = own_row(in_vec, turn, part)
            running = proj_ref[:, :128] * row[:, :128]
            for at in range(128, pw, 128):
                running = running + proj_ref[:, at:at + 128] * row[:, at:at + 128]
            found.append(jnp.sum(jnp.transpose(running), axis=0, keepdims=True))
        return jnp.concatenate(found, axis=0)

    def nonlocal_rows(sums):
        half = sums.shape[1] // 2
        pair = jnp.concatenate([
            sums[0:1, :half] + sums[1:2, half:], sums[1:2, :half] - sums[0:1, half:]], axis=0)
        mixed = jnp.dot(pair, couple_ref[...], precision=top_precision, preferred_element_type=jnp.float32)
        m_re, m_im = mixed[0:1], mixed[1:2]
        found = []
        for row in (jnp.concatenate([m_re, -m_im], axis=1), jnp.concatenate([m_im, m_re], axis=1)):
            column = jnp.transpose(jnp.broadcast_to(row, (2 * half, 128)))
            found.append(jnp.concatenate([
                jnp.sum(proj_ref[:, at:at + 128] * column, axis=0, keepdims=True) for at in range(0, pw, 128)], axis=1))
        return jnp.concatenate(found, axis=0)

    def apply_h(turn):
        sums = (psend.at[turn], precv.at[turn], ps_sem.at[turn], pr_sem.at[turn])
        all_sum(project(turn), *sums)
        put(turn)
        lax.fori_loop(0, chunks, middle, 0)
        start = nonlocal_rows(all_sum_end(*sums) * (1.0 / total_pw))
        own_kin = kin_ref[pl.ds(me, 1), :]
        start = start + own_kin * jnp.concatenate([own_row(in_vec, turn, 0), own_row(in_vec, turn, 1)], axis=0)
        for mask in (6, 7, 4, 5, 2, 3, 1, 0):
            take(turn, mask)
        running = start + rsend[turn, 0]
        for mask in range(1, group):
            partial_copy(turn, mask).wait()
            running = running + rrecv[turn, mask]
        hsend[turn] = running
        return running

    def share_h(turn):
        out = (hsend.at[turn], hrecv.at[turn], hs_sem.at[turn], hr_sem.at[turn])
        spread_start(*out)
        hrecv[turn, me] = hsend[turn]
        spread_wait(*out)
        for part in range(2):
            out_vec[turn, part] = stack_rows([hrecv[turn, s, part:part + 1] for s in range(group)])

    def vector(index):
        ref = out_vec if index % 2 else in_vec
        return ref[index // 2]

    def gram_sums(pair_list):
        found = {}
        for one, two, use_kin in pair_list:
            left, right = vector(one), vector(two)
            product = left[0] * right[0] + left[1] * right[1]
            value = total_of(product * kin_ref[...] if use_kin else product) * (1.0 / total_pw)
            found[use_kin, one, two] = value
            found[use_kin, two, one] = value
        return found

    def realize(coef_map, basis):
        running = 0.0
        for index, coef in coef_map.items():
            running = running + (basis(index) if isinstance(coef, float) and coef == 1.0 else coef * basis(index))
        return running

    def smooth(residual, level):
        kin = kin_ref[...]
        ratio = kin / (1.5 * level + 1.0)
        poly = 27.0 + ratio * (18.0 + ratio * (12.0 + 8.0 * ratio))
        square = ratio * ratio
        return residual * (poly / (poly + 16.0 * square * square))

    def save(names, slot):
        for k, value in enumerate(names):
            save_ref[slot + k:slot + k + 1, :] = jnp.broadcast_to(value, (1, 128))

    def load_saved(slot):
        return save_ref[slot:slot + 1, 0:1]

    def first_step(gram):
        psi, ham = {0: 1.0}, {1: 1.0}
        eps_zero = gram_form(gram, psi, ham, False) / (gram_form(gram, psi, psi, False) + small_eps)
        return psi, ham, eps_zero, combine([(1.0, ham), (-eps_zero, psi)])

    def second_step(gram):
        psi, ham, eps_zero, r_map = first_step(gram)
        q_map = combine([(1.0, {3: 1.0}), (-eps_zero, {2: 1.0})])
        lam_zero = -gram_form(gram, r_map, q_map, False) / (gram_form(gram, q_map, q_map, False) + small_eps)
        psi_one = combine([(1.0, psi), (lam_zero, {2: 1.0})])
        h_one = combine([(1.0, ham), (lam_zero, {3: 1.0})])
        eps_one = gram_form(gram, psi_one, h_one, False) / (gram_form(gram, psi_one, psi_one, False) + small_eps)
        r_one = combine([(1.0, h_one), (-eps_one, psi_one)])
        change = combine([(1.0, r_map), (-1.0, r_one)])
        weight = gram_form(gram, r_map, change, False) / (gram_form(gram, change, change, False) + small_eps)
        step = weight * lam_zero
        psi_mid = combine([(1.0, psi), (step, {2: 1.0})])
        h_mid = combine([(1.0, ham), (step, {3: 1.0})])
        r_mid = combine([(1.0, r_map), (-weight, change)])
        eps_mid = gram_form(gram, psi_mid, h_mid, False) / (gram_form(gram, psi_mid, psi_mid, False) + small_eps)
        return psi_mid, h_mid, r_mid, eps_mid, step

    first_pairs = new_pairs(0, 2, (False, True))
    second_pairs = new_pairs(2, 4, (False, True))
    gram_pairs = first_pairs + second_pairs

    def swap(which, send, recv, off, incoming):
        source = lax.rem(band + bands - off, bands) if incoming else band
        return pltpu.make_async_remote_copy(
            src_ref=send, dst_ref=recv.at[source],
            send_sem=ns_sem.at[which, off - 1], recv_sem=nr_sem.at[which, off - 1],
            device_id={"band": lax.rem(band + off, bands)}, device_id_type=MESH)

    def share(which, send, recv, values):
        send[...] = values
        recv[band] = values
        for off in range(1, bands):
            swap(which, send, recv, off, False).start()

    def share_end(which, send, recv):
        for off in range(1, bands):
            swap(which, send, recv, off, True).wait()

    def own(index):
        ref = out_vec if index % 2 else in_vec
        return jnp.concatenate([own_row(ref, index // 2, 0), own_row(ref, index // 2, 1)], axis=0)

    def turn_step(turn, carry):
        apply_h(turn)

        @pl.when(turn == 0)
        def _():
            share_h(0)
            gram = gram_sums(first_pairs)
            save([gram[kind, one, two] for one, two, kind in first_pairs], 0)
            r_map = first_step(gram)[3]
            level = gram_form(gram, r_map, r_map, True) / (gram_form(gram, r_map, r_map, False) + small_eps)
            p_zero = smooth(realize(r_map, vector), level)
            in_vec[1] = p_zero

        @pl.when(turn == 1)
        def _():
            share_h(1)
            gram = gram_sums(second_pairs)
            save([gram[kind, one, two] for one, two, kind in second_pairs], len(first_pairs))
            for k, (one, two, kind) in enumerate(first_pairs):
                gram[kind, one, two] = gram[kind, two, one] = load_saved(k)
            psi_mid, h_mid, r_mid, eps_mid, step = second_step(gram)
            level = gram_form(gram, r_mid, r_mid, True) / (gram_form(gram, r_mid, r_mid, False) + small_eps)
            p_one = smooth(realize(r_mid, vector), level)
            in_vec[2] = p_one
            share(0, nsend, nrecv, jnp.stack([realize(psi_mid, own), own(4), realize(h_mid, own)]))

        return carry

    lax.fori_loop(0, 3, turn_step, 0)

    g_own = hsend[2]
    share(1, isend, irecv, g_own)
    last_pairs = new_pairs(4, 6, (False,))

    def own_last(index):
        return g_own if index == 5 else own(index)

    lane_id = lax.broadcasted_iota(jnp.int32, (1, 128), 1)
    local = jnp.zeros((1, 128), jnp.float32)
    held = [own_last(index) for index in range(6)]
    for k, (one, two, kind) in enumerate(last_pairs):
        local = jnp.where(lane_id == k, total_of(held[one] * held[two]), local)
    sums = (gsend, grecv, gs_sem, gr_sem)
    all_sum(local, *sums)
    gram = {}
    for k, (one, two, kind) in enumerate(gram_pairs):
        gram[kind, one, two] = gram[kind, two, one] = load_saved(k)
    psi_mid, h_mid, r_mid, eps_mid, step = second_step(gram)
    summed = all_sum_end(*sums) * (1.0 / total_pw)
    for k, (one, two, kind) in enumerate(last_pairs):
        gram[kind, one, two] = gram[kind, two, one] = summed[:, k:k + 1]
    q_one = combine([(1.0, {5: 1.0}), (-eps_mid, {4: 1.0})])
    lam_one = -gram_form(gram, r_mid, q_one, False) / (gram_form(gram, q_one, q_one, False) + small_eps)
    share(2, lsend, lrecv, jnp.broadcast_to(lam_one, (1, 128)))
    share_end(0, nsend, nrecv)
    share_end(1, isend, irecv)

    pairs = [
        [stack_rows([nrecv[o, 0, part:part + 1] for o in range(bands)] + [nrecv[o, 1, part:part + 1] for o in range(bands)]) for part in range(2)],
        [stack_rows([nrecv[o, 2, part:part + 1] for o in range(bands)] + [irecv[o, part:part + 1] for o in range(bands)]) for part in range(2)],
    ]
    column_id = lax.broadcasted_iota(jnp.int32, (2 * bands, 128), 1)
    local = jnp.zeros((2 * bands, 128), jnp.float32)
    slot = 0
    for o_re, o_im in pairs:
        for mine in (0, 1):
            m_re, m_im = nsend[mine, 0:1], nsend[mine, 1:2]
            for product in (m_re * o_re + m_im * o_im, m_re * o_im - m_im * o_re):
                local = jnp.where(column_id == slot, jnp.sum(product, axis=1, keepdims=True), local)
                slot += 1
    crossed = (csend, crecv, cs_sem, cr_sem)
    all_sum(local, *crossed)

    new_map = combine([(1.0, psi_mid), (lam_one, {4: 1.0})])
    ham_new = combine([(1.0, h_mid), (lam_one, {5: 1.0})])
    norm_new = gram_form(gram, new_map, new_map, False) + small_eps
    energy = gram_form(gram, new_map, ham_new, False) / norm_new
    resid = combine([(1.0, ham_new), (-energy, new_map)])
    resid_norm = gram_form(gram, resid, resid, False) / norm_new
    new_ref[...] = nsend[0] + lam_one * nsend[1]
    share_end(2, lsend, lrecv)
    summed = all_sum_end(*crossed) * (1.0 / total_pw)
    lam_rows = stack_rows([lrecv[o] for o in range(bands)])
    mixed = summed[:bands] + lam_rows * summed[bands:]
    result = mixed + lam_one * pltpu.roll(mixed, 126, 1)
    scal_ref[...] = jnp.concatenate([
        result, jnp.broadcast_to(energy, (1, 128)), jnp.broadcast_to(resid_norm, (1, 128)),
        jnp.zeros((scal_ref.shape[0] - bands - 2, 128), jnp.float32)], axis=0)


def finish_kernel(bands, new_ref, scal_ref, bands_ref, energy_ref, norm_ref, corr_ref, sub_ref):
    bands_ref[:, 0, :] = new_ref[...]
    lane = lax.broadcasted_iota(jnp.int32, (1, bands), 1)
    for ref, base in ((corr_ref, 0), (sub_ref, 4)):
        for part in range(2):
            row = jnp.zeros((1, bands), jnp.float32)
            for other in range(bands):
                at = base + part
                row = jnp.where(lane == other, scal_ref[other:other + 1, at:at + 1], row)
            ref[part] = row
    energy_ref[0] = scal_ref[bands, 0]
    norm_ref[0] = scal_ref[bands + 1, 0]


def kernel_body(coeffs, cell_map, potential, projectors, strengths, proj_atom, proj_chan):
    group = lax.axis_size("ga")
    bands = lax.axis_size("band")
    grid_len = potential.shape[0]
    planes = grid_len // group
    chunks = planes // QUAD
    pw = coeffs.shape[2]
    total_pw = pw * group
    rows = group * 2 * QUAD
    slab = chunks * 2 * QUAD
    lanes = planes * grid_len
    folds = -(-lanes // WIDE)
    proj_rows = 2 * projectors.shape[1]
    tables = [jnp.asarray(t) for t in const_tables(grid_len, group)]
    dma = pltpu.SemaphoreType.DMA
    vmem = pl.BlockSpec(memory_space=pltpu.VMEM)
    far = pl.BlockSpec(memory_space=pl.ANY)
    f32, b16 = jnp.float32, jnp.bfloat16
    scal_rows = 8 * (-(-(bands + 2) // 8))
    peers = group - 1
    new, scal = pl.pallas_call(
        functools.partial(sweep_kernel, (group, bands, chunks, grid_len, total_pw, pw)),
        out_shape=(
            jax.ShapeDtypeStruct((2, pw), f32),
            jax.ShapeDtypeStruct((scal_rows, 128), f32),
        ),
        in_specs=[vmem, vmem, far, far] + [vmem] * 4 + [far] + [vmem] * 3,
        out_specs=(vmem, vmem),
        scratch_shapes=[
            pltpu.VMEM((group, WIDE, pw), b16),
            pltpu.VMEM((group, folds, 16, pw), b16),
            pltpu.VMEM((group, 1, pw), f32),
            pltpu.VMEM((group, slab, pw), f32),
            pltpu.VMEM((group, slab, pw), f32),
            pltpu.VMEM((group, pw), f32),
            pltpu.VMEM((chunks, group, 2 * QUAD, lanes), f32),
            pltpu.VMEM((chunks, group, 2 * QUAD, lanes), f32),
            pltpu.VMEM((chunks, group, 2 * QUAD, lanes), f32),
            pltpu.VMEM((planes, grid_len, grid_len), f32),
            pltpu.VMEM((proj_rows, pw), f32),
            pltpu.VMEM(tables[1].shape, b16),
            pltpu.VMEM((proj_rows // 2, proj_rows // 2), f32),
            pltpu.VMEM((3, 2, group, pw), f32),
            pltpu.VMEM((2, 2, group, pw), f32),
            pltpu.VMEM((24, 128), f32),
            dma((3,)),
            pltpu.VMEM((1, pw), f32), pltpu.VMEM((group, 1, pw), f32),
            pltpu.VMEM((2, pw), f32), pltpu.VMEM((group, 2, pw), f32),
            pltpu.VMEM((3, group, 2, pw), f32), pltpu.VMEM((3, group, 2, pw), f32),
            pltpu.VMEM((3, 2, pw), f32), pltpu.VMEM((2, group, 2, pw), f32),
            pltpu.VMEM((3, 2, proj_rows), f32), pltpu.VMEM((3, group, 2, proj_rows), f32),
            pltpu.VMEM((1, 128), f32), pltpu.VMEM((group, 1, 128), f32),
            pltpu.VMEM((3, 2, pw), f32), pltpu.VMEM((bands, 3, 2, pw), f32),
            pltpu.VMEM((2, pw), f32), pltpu.VMEM((bands, 2, pw), f32),
            pltpu.VMEM((1, 128), f32), pltpu.VMEM((bands, 1, 128), f32),
            pltpu.VMEM((2 * bands, 128), f32), pltpu.VMEM((group, 2 * bands, 128), f32),
            dma((peers,)), dma((peers,)), dma((peers,)), dma((peers,)),
            dma((3, peers)), dma((3, peers)), dma((2, peers)), dma((2, peers)),
            dma((3, peers)), dma((3, peers)), dma((peers,)), dma((peers,)),
            dma((3, bands - 1)), dma((3, bands - 1)), dma((peers,)), dma((peers,)),
        ],
        compiler_params=pltpu.CompilerParams(
            collective_id=0, has_side_effects=True, vmem_limit_bytes=60 * 1024 * 1024
        ),
        name="sweeps",
    )(
        coeffs, cell_map.reshape(-1, 128), jnp.swapaxes(potential, 0, 1),
        projectors.reshape(proj_rows, pw), strengths.reshape(-1, strengths.shape[2]),
        proj_atom.reshape(1, -1), proj_chan.reshape(1, -1), *tables,
    )

    smem = pl.BlockSpec(memory_space=pltpu.SMEM)
    return pl.pallas_call(
        functools.partial(finish_kernel, bands),
        out_shape=(
            jax.ShapeDtypeStruct((2, 1, pw), f32),
            jax.ShapeDtypeStruct((1,), f32),
            jax.ShapeDtypeStruct((1,), f32),
            jax.ShapeDtypeStruct((2, 1, bands), f32),
            jax.ShapeDtypeStruct((2, 1, bands), f32),
        ),
        in_specs=[vmem, vmem],
        out_specs=(vmem, smem, smem, vmem, vmem),
        name="finish",
    )(new, scal)


def body(coeffs, cell_map, potential, projectors, strengths, proj_atom, proj_chan):
    group = lax.axis_size("ga")
    grid_len = potential.shape[0]
    planes = grid_len // group
    fits = (
        group == 8
        and planes == 4 * TRIPLE
        and 4 * grid_len % 128 == 0
        and grid_len % 16 == 0
        and coeffs.shape[1] == 1
        and coeffs.shape[2] % 256 == 0
        and 2 * projectors.shape[1] == 128
    )
    chosen = kernel_body if fits else plain_body
    return chosen(coeffs, cell_map, potential, projectors, strengths, proj_atom, proj_chan)


def solution(mesh):
    placed = (
        P(None, "band", "ga"),
        P("ga"),
        P(None, "ga", None),
        P(None, None, "ga"),
        P(),
        P(),
        P(),
    )
    return jax.shard_map(
        body,
        mesh=mesh,
        in_specs=placed,
        out_specs=(
            P(None, "band", "ga"),
            P("band"),
            P("band"),
            P(None, "band", None),
            P(None, "band", None),
        ),
        check_vma=False,
    )
```

```python
import functools

import jax
import jax.numpy as jnp
import numpy as np
from jax import lax
from jax.experimental import pallas as pl
from jax.experimental.pallas import tpu as pltpu
from jax.sharding import PartitionSpec as P

top_precision = lax.Precision.HIGHEST
kin_unit = 0.02
small_eps = 1e-06


def signed_freq(index_arr, grid_len):
    return jnp.where(index_arr < grid_len // 2, index_arr, index_arr - grid_len)


def wave_tables(grid_len, row_freq, col_freq, sign_val, factor):
    phase = row_freq[:, None] * col_freq[None, :] % grid_len
    angle = 2.0 * jnp.pi / grid_len * phase.astype(jnp.float32)
    return (jnp.cos(angle) * factor, jnp.sin(angle) * (sign_val * factor))


def block_table(cos_table, sin_table):
    upper = jnp.concatenate([cos_table, sin_table], axis=1)
    lower = jnp.concatenate([-sin_table, cos_table], axis=1)
    return jnp.concatenate([upper, lower], axis=0)


def quarter_turn(grid_vals):
    half_len = grid_vals.shape[-1] // 2
    return jnp.concatenate([-grid_vals[..., half_len:], grid_vals[..., :half_len]], axis=-1)


def mix_dim(grid_vals, cos_table, sin_table, pattern):
    direct = jnp.einsum(pattern, cos_table, grid_vals, precision=top_precision)
    turned = jnp.einsum(pattern, sin_table, quarter_turn(grid_vals), precision=top_precision)
    return direct + turned


def mix_last(grid_vals, table_full):
    row_width = grid_vals.shape[-1]
    product = jnp.dot(
        grid_vals.reshape(-1, row_width),
        table_full,
        precision=top_precision,
        preferred_element_type=jnp.float32,
    )
    return product.reshape(grid_vals.shape)


def band_dot(left_vec, right_vec, weight):
    return jnp.sum(left_vec * right_vec * weight, axis=(0, 2))


def per_band(values):
    return values[None, :, None]


def pair_products(left_vec, right_vec):

    def contract(first_part, second_part):
        return jnp.einsum("bg,cg->bc", first_part, second_part, precision=top_precision)

    real_part = contract(left_vec[0], right_vec[0]) + contract(left_vec[1], right_vec[1])
    imag_part = contract(left_vec[0], right_vec[1]) - contract(left_vec[1], right_vec[0])
    return jnp.stack([real_part, imag_part])


def precondition(residual, kinetic, kin_level):
    x_ratio = kinetic[None, :] / (1.5 * kin_level[:, None] + 1.0)
    numer_poly = 27.0 + x_ratio * (18.0 + x_ratio * (12.0 + 8.0 * x_ratio))
    square = x_ratio * x_ratio
    return residual * (numer_poly / (numer_poly + 16.0 * square * square))[None]


def coupling_matrix(proj_atom, proj_chan, strengths):
    atom_count = strengths.shape[0]
    chan_count = strengths.shape[1]
    symmetric = 0.5 * (strengths + jnp.swapaxes(strengths, 1, 2))
    atom_hot = (proj_atom[:, None] == jnp.arange(atom_count, dtype=jnp.int32)[None, :]).astype(
        jnp.float32
    )
    chan_hot = (proj_chan[:, None] == jnp.arange(chan_count, dtype=jnp.int32)[None, :]).astype(
        jnp.float32
    )
    rows_d = jnp.einsum("pa,pc,acd->pd", atom_hot, chan_hot, symmetric, precision=top_precision)
    same_atom = jnp.dot(
        atom_hot, atom_hot.T, precision=top_precision, preferred_element_type=jnp.float32
    )
    return same_atom * jnp.dot(
        rows_d, chan_hot.T, precision=top_precision, preferred_element_type=jnp.float32
    )


def combine(term_list):
    merged = {}
    for scalar, coef_map in term_list:
        for index_one, coef_a in coef_map.items():
            merged[index_one] = merged.get(index_one, 0.0) + scalar * coef_a
    return merged


def gram_form(gram_table, left_map, right_map, use_kin):
    running = 0.0
    for index_one, coef_a in left_map.items():
        for index_two, coef_b in right_map.items():
            running = running + coef_a * coef_b * gram_table[use_kin, index_one, index_two]
    return running


def new_pairs(first_new, last_new, kinds):
    pair_list = []
    for use_kin in kinds:
        for index_two in range(first_new, last_new):
            for index_one in range(index_two + 1):
                pair_list.append((index_one, index_two, use_kin))
    return pair_list


def plain_body(coeffs, cell_map, potential, projectors, strengths, proj_atom, proj_chan):
    ga_count = lax.axis_size("ga")
    grid_len = potential.shape[0]
    planes = grid_len // ga_count
    band_local = coeffs.shape[1]
    total_pw = coeffs.shape[2] * ga_count
    device = lax.axis_index("ga")
    plane_num = cell_map // (grid_len * grid_len)
    y_index = cell_map // grid_len % grid_len
    z_index = cell_map % grid_len
    freq_x = signed_freq(device + ga_count * plane_num, grid_len)
    freq_y = signed_freq(y_index, grid_len)
    freq_z = signed_freq(z_index, grid_len)
    kinetic = kin_unit * (freq_x * freq_x + freq_y * freq_y + freq_z * freq_z).astype(jnp.float32)
    kin_weight = kinetic[None, None, :]
    slot_re = (plane_num * grid_len + y_index) * (2 * grid_len) + z_index
    slot_im = slot_re + grid_len
    cell_count = planes * grid_len * 2 * grid_len
    natural = jnp.arange(grid_len, dtype=jnp.int32)
    cyclic = natural % planes * ga_count + natural // planes
    cos_fwd, sin_fwd = wave_tables(grid_len, natural, natural, 1.0, 1.0)
    cos_back, sin_back = wave_tables(grid_len, natural, natural, -1.0, 1.0 / grid_len)
    z_forward = block_table(cos_fwd, sin_fwd)
    z_backward = block_table(cos_back, sin_back)
    xcos_fwd, xsin_fwd = wave_tables(grid_len, natural, cyclic, 1.0, 1.0)
    xcos_back, xsin_back = wave_tables(grid_len, cyclic, natural, -1.0, 1.0 / grid_len)
    doubled = jnp.concatenate([potential, potential], axis=-1)
    coupling = coupling_matrix(proj_atom, proj_chan, strengths)

    def real_space(grid_vals):
        grid_vals = mix_dim(grid_vals, xcos_fwd, xsin_fwd, "kj,bjyw->bkyw")
        grid_vals = grid_vals * doubled[None]
        grid_vals = mix_dim(grid_vals, xcos_back, xsin_back, "jk,bkyw->bjyw")
        return lax.all_to_all(grid_vals, "ga", split_axis=1, concat_axis=2, tiled=True)

    def local_part(vectors):
        item_count = vectors.shape[1]
        flat_grid = jnp.zeros((item_count, cell_count), jnp.float32)
        flat_grid = flat_grid.at[:, slot_re].set(vectors[0]).at[:, slot_im].set(vectors[1])
        grid_vals = mix_last(
            flat_grid.reshape(item_count, planes, grid_len, 2 * grid_len), z_forward
        )
        grid_vals = mix_dim(grid_vals, cos_fwd, sin_fwd, "ky,bpyw->bpkw")
        grid_vals = real_space(
            lax.all_to_all(grid_vals, "ga", split_axis=2, concat_axis=1, tiled=True)
        )
        grid_vals = mix_dim(grid_vals, cos_back, sin_back, "ky,bpyw->bpkw")
        flat_grid = mix_last(grid_vals, z_backward).reshape(item_count, cell_count)
        return jnp.stack([flat_grid[:, slot_re], flat_grid[:, slot_im]])

    def contract(first_part, second_part):
        return jnp.einsum("pg,bg->pb", first_part, second_part, precision=top_precision)

    def spread(weights, proj_table):
        return jnp.einsum("pb,pg->bg", weights, proj_table, precision=top_precision)

    def projected_part(vectors):
        proj_re = contract(projectors[0], vectors[0]) + contract(projectors[1], vectors[1])
        proj_im = contract(projectors[0], vectors[1]) - contract(projectors[1], vectors[0])
        proj_re, proj_im = lax.psum((proj_re, proj_im), "ga")
        mixed_re = jnp.dot(
            coupling,
            proj_re / total_pw,
            precision=top_precision,
            preferred_element_type=jnp.float32,
        )
        mixed_im = jnp.dot(
            coupling,
            proj_im / total_pw,
            precision=top_precision,
            preferred_element_type=jnp.float32,
        )
        out_re = spread(mixed_re, projectors[0]) - spread(mixed_im, projectors[1])
        out_im = spread(mixed_re, projectors[1]) + spread(mixed_im, projectors[0])
        return jnp.stack([out_re, out_im])

    def apply_h(vectors):
        return kin_weight * vectors + local_part(vectors) + projected_part(vectors)

    def gram_sums(basis, pair_list):
        stacked = []
        for index_one, index_two, use_kin in pair_list:
            stacked.append(
                band_dot(basis[index_one], basis[index_two], kin_weight if use_kin else 1.0)
            )
        summed = lax.psum(jnp.stack(stacked), "ga") / total_pw
        found = {}
        for slot_num, entry in enumerate(pair_list):
            index_one, index_two, use_kin = entry
            found[use_kin, index_one, index_two] = summed[slot_num]
            found[use_kin, index_two, index_one] = summed[slot_num]
        return found

    def realize(coef_map, basis):
        running = jnp.zeros_like(basis[0])
        for index_one, coef_a in coef_map.items():
            running = (
                running
                + per_band(jnp.zeros((band_local,), jnp.float32) + coef_a) * basis[index_one]
            )
        return running

    h_zero = apply_h(coeffs)
    basis = [coeffs, h_zero]
    gram_table = gram_sums(basis, new_pairs(0, 2, (False, True)))
    psi_map = {0: 1.0}
    ham_map = {1: 1.0}
    eps_zero = gram_form(gram_table, psi_map, ham_map, False) / (
        gram_form(gram_table, psi_map, psi_map, False) + small_eps
    )
    r_map = combine([(1.0, ham_map), (-eps_zero, psi_map)])
    level_zero = gram_form(gram_table, r_map, r_map, True) / (
        gram_form(gram_table, r_map, r_map, False) + small_eps
    )
    p_zero = precondition(realize(r_map, basis), kinetic, level_zero)
    g_zero = apply_h(p_zero)
    basis = [coeffs, h_zero, p_zero, g_zero]
    gram_table.update(gram_sums(basis, new_pairs(2, 4, (False, True))))
    q_map = combine([(1.0, {3: 1.0}), (-eps_zero, {2: 1.0})])
    lam_zero = -gram_form(gram_table, r_map, q_map, False) / (
        gram_form(gram_table, q_map, q_map, False) + small_eps
    )
    psi_one_map = combine([(1.0, psi_map), (lam_zero, {2: 1.0})])
    h_one_map = combine([(1.0, ham_map), (lam_zero, {3: 1.0})])
    eps_one = gram_form(gram_table, psi_one_map, h_one_map, False) / (
        gram_form(gram_table, psi_one_map, psi_one_map, False) + small_eps
    )
    r_one_map = combine([(1.0, h_one_map), (-eps_one, psi_one_map)])
    change_map = combine([(1.0, r_map), (-1.0, r_one_map)])
    weight_one = gram_form(gram_table, r_map, change_map, False) / (
        gram_form(gram_table, change_map, change_map, False) + small_eps
    )
    step_mid = weight_one * lam_zero
    psi_mid_map = combine([(1.0, psi_map), (step_mid, {2: 1.0})])
    h_mid_map = combine([(1.0, ham_map), (step_mid, {3: 1.0})])
    r_mid_map = combine([(1.0, r_map), (-weight_one, change_map)])
    eps_mid = gram_form(gram_table, psi_mid_map, h_mid_map, False) / (
        gram_form(gram_table, psi_mid_map, psi_mid_map, False) + small_eps
    )
    level_mid = gram_form(gram_table, r_mid_map, r_mid_map, True) / (
        gram_form(gram_table, r_mid_map, r_mid_map, False) + small_eps
    )
    p_one = precondition(realize(r_mid_map, basis), kinetic, level_mid)
    g_one = apply_h(p_one)
    basis = [coeffs, h_zero, p_zero, g_zero, p_one, g_one]
    gram_table.update(gram_sums(basis, new_pairs(4, 6, (False,))))
    q_one_map = combine([(1.0, {5: 1.0}), (-eps_mid, {4: 1.0})])
    lam_one = -gram_form(gram_table, r_mid_map, q_one_map, False) / (
        gram_form(gram_table, q_one_map, q_one_map, False) + small_eps
    )
    new_map = combine([(1.0, psi_mid_map), (lam_one, {4: 1.0})])
    ham_new_map = combine([(1.0, h_mid_map), (lam_one, {5: 1.0})])
    norm_new = gram_form(gram_table, new_map, new_map, False) + small_eps
    energy = gram_form(gram_table, new_map, ham_new_map, False) / norm_new
    resid_map = combine([(1.0, ham_new_map), (-energy, new_map)])
    residual_norm = gram_form(gram_table, resid_map, resid_map, False) / norm_new
    new_bands = realize(new_map, basis)
    new_ham = realize(ham_new_map, basis)
    blank_rows = jnp.zeros((2, band_local, band_local * lax.axis_size("band")), jnp.float32)
    first_row = jnp.int32(0)
    over_rows = blank_rows
    ham_rows = blank_rows
    piece_bands = lax.all_gather(new_bands, "band", axis=1, tiled=True)
    piece_ham = lax.all_gather(new_ham, "band", axis=1, tiled=True)
    over_rows = lax.dynamic_update_slice_in_dim(
        over_rows, pair_products(new_bands, piece_bands), first_row, 2
    )
    ham_rows = lax.dynamic_update_slice_in_dim(
        ham_rows, pair_products(new_bands, piece_ham), first_row, 2
    )
    over_rows, ham_rows = (over_rows, ham_rows)
    over_rows, ham_rows = lax.psum((over_rows, ham_rows), "ga")
    correlation = over_rows / total_pw
    subspace = ham_rows / total_pw
    return (new_bands, energy, residual_norm, correlation, subspace)


WIDE = 256
MESH = pl.DeviceIdType.MESH


def split_const(values):
    high = np.asarray(values, np.float32).astype(jnp.bfloat16)
    low = (values - high.astype(np.float64)).astype(np.float32).astype(jnp.bfloat16)
    return np.stack([high, low])


def const_tables(grid_len, group):
    planes = grid_len // group
    unit = 2.0 * np.pi / grid_len
    quarter = grid_len / 4.0
    main = list(range(8))
    rest = list(range(8, planes))
    y_in = np.array(main + rest + rest + main)
    part_row = np.array([0] * planes + [1] * planes)
    y_real = np.arange(group)[:, None] * planes + y_in[None, :]
    freq = np.arange(grid_len)
    phase = (y_real[..., None] * freq) % grid_len
    tab_a = np.cos(unit * (phase - quarter * part_row[:, None]))
    tab_b = np.cos(unit * (phase + quarter * (1 - part_row[:, None])))
    high, low = split_const(np.concatenate([tab_a, tab_b], axis=1))
    wave = np.concatenate([high, low], axis=2)
    theta = unit * (np.outer(freq, freq) % grid_len)
    turn = np.zeros((2, 128, 2, 128))
    turn[0, :grid_len, 0, :grid_len] = np.cos(theta)
    turn[0, :grid_len, 1, :grid_len] = np.sin(theta)
    turn[1, :grid_len, 0, :grid_len] = -np.sin(theta)
    turn[1, :grid_len, 1, :grid_len] = np.cos(theta)
    turn = turn.reshape(256, 256)
    zed = np.concatenate([split_const(turn), split_const(turn.T)], axis=0)
    return wave, zed


def two_parts(values):
    high = values.astype(jnp.bfloat16)
    low = (values - high.astype(jnp.float32)).astype(jnp.bfloat16)
    return high, low


def split_rows(values):
    high = values.astype(jnp.bfloat16).astype(jnp.float32)
    return jnp.concatenate([high, values - high], axis=0).astype(jnp.bfloat16)


def bdot(left, right):
    return jnp.dot(left, right, preferred_element_type=jnp.float32)


def bdot_t(left, right):
    return lax.dot_general(left, right, (((1,), (1,)), ((), ())), preferred_element_type=jnp.float32)


def total_of(values):
    return jnp.sum(jnp.sum(values, axis=0, keepdims=True), axis=1, keepdims=True)


def c_add(one, two):
    return one[0] + two[0], one[1] + two[1]


def c_sub(one, two):
    return one[0] - two[0], one[1] - two[1]


def c_turn(one, direction):
    return (-one[1], one[0]) if direction > 0 else (one[1], -one[0])


def c_mul(one, cos_val, sin_val):
    return one[0] * cos_val - one[1] * sin_val, one[0] * sin_val + one[1] * cos_val


def c_scale(one, factor):
    return one[0] * factor, one[1] * factor


def three_point(items, direction):
    total = c_add(items[1], items[2])
    side = c_scale(c_turn(c_sub(items[1], items[2]), direction), 0.8660254037844386)
    base = c_sub(items[0], c_scale(total, 0.5))
    return [c_add(items[0], total), c_add(base, side), c_sub(base, side)]


def four_point(items, direction):
    even, odd = c_add(items[0], items[2]), c_add(items[1], items[3])
    low, high = c_sub(items[0], items[2]), c_turn(c_sub(items[1], items[3]), direction)
    return [c_add(even, odd), c_add(low, high), c_sub(even, odd), c_sub(low, high)]


def eight_point(items, direction):
    even = four_point(items[0::2], direction)
    odd = four_point(items[1::2], direction)
    root = 0.7071067811865476
    turned = [
        odd[0],
        c_scale(c_add(odd[1], c_turn(odd[1], direction)), root),
        c_turn(odd[2], direction),
        c_scale(c_sub(c_turn(odd[3], direction), odd[3]), root),
    ]
    return [c_add(e, o) for e, o in zip(even, turned)] + [c_sub(e, o) for e, o in zip(even, turned)]


def twelve_point(items, direction):
    fours = [four_point([items[(4 * a + 3 * b) % 12] for b in range(4)], direction) for a in range(3)]
    threes = [three_point([fours[a][v] for a in range(3)], direction) for v in range(4)]
    return [threes[v % 4][v % 3] for v in range(12)]


def sweep_kernel(
    dims,
    coeffs_ref, cell_ref, potential_hbm, proj_hbm, strength_ref, atom_ref, chan_ref,
    wave_ref, zed_ref,
    new_ref, scal_ref,
    hot_ref, mask_ref, group_ref, ta_ref, tb_ref, kin_ref, work_ref, left_ref,
    pot_ref, potential_ref, proj_ref, couple_ref, in_vec, out_vec, save_ref, in_sem,
    ksend, krecv, xsend, xrecv, rsend, rrecv, hsend, hrecv, psend, precv,
    gsend, grecv, nsend, nrecv, isend, irecv, lsend, lrecv, csend, crecv,
    ks_sem, kr_sem, xs_sem, xr_sem, rs_sem, rr_sem, hs_sem, hr_sem, ps_sem, pr_sem,
    gs_sem, gr_sem, ns_sem, nr_sem, cs_sem, cr_sem,
):
    group, bands, planes, grid_len, total_pw, pw = dims
    slab = 2 * planes
    folds = planes // 2
    half = group // 2
    tiles = pw // 128
    me = lax.axis_index("ga")
    band = lax.axis_index("band")
    sides = [1 - 2 * lax.rem(me // (1 << bit), 2) for bit in range(3)]

    def peer_of(mask):
        return me + sum(sides[bit] * ((mask // (1 << bit)) % 2) * (1 << bit) for bit in range(3))

    loads = [
        pltpu.make_async_copy(source, target, in_sem.at[k])
        for k, (source, target) in enumerate(
            ((proj_hbm, proj_ref), (potential_hbm, potential_ref)))
    ]
    for load in loads:
        load.start()
    barrier = pltpu.get_barrier_semaphore()
    for mask in range(1, group):
        pl.semaphore_signal(barrier, inc=1, device_id={"ga": peer_of(mask)}, device_id_type=MESH)
    for off in range(1, bands):
        pl.semaphore_signal(barrier, inc=1, device_id={"band": lax.rem(band + off, bands)}, device_id_type=MESH)

    cell = cell_ref[...].astype(jnp.float32)
    for k in range(tiles):
        ksend[:, k * 128:(k + 1) * 128] = cell[k:k + 1]
    xsend[...] = coeffs_ref[:, 0, :]

    far_first = (6, 7, 4, 5, 2, 3, 1)

    def spread_copy(mask, send, recv, send_sem, recv_sem, incoming):
        peer = peer_of(mask)
        return pltpu.make_async_remote_copy(
            src_ref=send, dst_ref=recv.at[peer if incoming else me],
            send_sem=send_sem.at[mask - 1], recv_sem=recv_sem.at[mask - 1],
            device_id={"ga": peer}, device_id_type=MESH)

    def spread_start(send, recv, send_sem, recv_sem):
        for mask in far_first:
            spread_copy(mask, send, recv, send_sem, recv_sem, False).start()

    def spread_wait(send, recv, send_sem, recv_sem):
        for mask in range(1, group):
            spread_copy(mask, send, recv, send_sem, recv_sem, True).wait()

    keys = (ksend, krecv, ks_sem, kr_sem)
    firsts = (xsend, xrecv, xs_sem, xr_sem)
    pl.semaphore_wait(barrier, group + bands - 2)
    spread_start(*keys)
    spread_start(*firsts)
    krecv[me] = ksend[...]
    xrecv[me] = xsend[...]

    def whole(values):
        return jnp.floor(values)

    def signed(values):
        return jnp.where(2.0 * values < grid_len, values, values - grid_len)

    def numbers(cells):
        plane = whole((cells + 0.5) * (1.0 / (grid_len * grid_len)))
        in_plane = cells - plane * (grid_len * grid_len)
        y_num = whole((in_plane + 0.5) * (1.0 / grid_len))
        return plane, y_num, in_plane - y_num * grid_len

    def kinetic(plane, y_num, z_num, device):
        f_x = signed(plane * group + device)
        f_y, f_z = signed(y_num), signed(z_num)
        return kin_unit * (f_x * f_x + f_y * f_y + f_z * f_z)

    def marks(numbers_row, count):
        wide_row = jnp.broadcast_to(numbers_row, (16, pw)).astype(jnp.bfloat16)
        row_id = lax.broadcasted_iota(jnp.int32, (16, pw), 0).astype(jnp.float32).astype(jnp.bfloat16)
        one, zero = jnp.ones((16, pw), jnp.bfloat16), jnp.zeros((16, pw), jnp.bfloat16)
        return [jnp.where(row_id + 16.0 * k == wide_row, one, zero) for k in range(count)]

    def build_source(src):
        plane, y_num, z_num = numbers(krecv[src])
        fold = whole((plane + 0.5) * 0.5)
        group_ref[src] = fold
        for k, piece in enumerate(marks((plane - 2.0 * fold) * 128.0 + z_num, WIDE // 16)):
            hot_ref[src, 16 * k:16 * (k + 1), :] = piece
        wide_fold = jnp.broadcast_to(fold, (16, pw)).astype(jnp.bfloat16)
        one, zero = jnp.ones((16, pw), jnp.bfloat16), jnp.zeros((16, pw), jnp.bfloat16)
        for k in range(folds):
            mask_ref[src, k] = jnp.where(wide_fold == float(k), one, zero)
        y_hot = marks(y_num, grid_len // 16)
        table = bdot(wave_ref[me], jnp.concatenate(y_hot + y_hot, axis=0))
        ta_ref[src] = table[:slab]
        tb_ref[src] = table[slab:]

    def build_potential():
        pad = jnp.zeros((8, 128 - grid_len), jnp.float32)

        def put_tile(v, slot, block):
            pot_ref[v, slot] = jnp.concatenate([block * (1.0 / grid_len**3), pad], axis=1)

        def lines(x_real, first, count):
            return potential_ref[pl.ds(first * grid_len + x_real, count, stride=grid_len), :]

        for v in range(planes):
            for u in range(group):
                put_tile(v, u, lines(v + planes * u, 0, 8))
            for t in range(half):
                put_tile(v, group + t, jnp.concatenate([
                    lines(v + planes * 2 * t, 8, planes - 8), lines(v + planes * (2 * t + 1), 8, planes - 8)], axis=0))

    def build_coupling():
        atoms, chans = strength_ref.shape[0] // strength_ref.shape[1], strength_ref.shape[1]
        size = atoms * chans
        ident = atom_ref[...] * chans + chan_ref[...]
        hot = (lax.broadcasted_iota(jnp.int32, (size, ident.shape[1]), 0) == ident).astype(jnp.float32)
        row_at = lax.broadcasted_iota(jnp.int32, (size, size), 0)
        col_at = lax.broadcasted_iota(jnp.int32, (size, size), 1)
        tiled = jnp.concatenate([strength_ref[...]] * atoms, axis=1)
        same = (row_at // chans == col_at // chans).astype(jnp.float32)
        block = tiled * same
        block = 0.5 * (block + jnp.transpose(block))
        half = lax.dot_general(hot, block, (((0,), (0,)), ((), ())), precision=top_precision, preferred_element_type=jnp.float32)
        couple_ref[...] = jnp.dot(half, hot, precision=top_precision, preferred_element_type=jnp.float32)

    build_source(me)
    build_coupling()
    for load in loads:
        load.wait()
    build_potential()

    def build_step(mask, carry):
        spread_copy(mask, *keys, True).wait()
        build_source(peer_of(mask))
        return carry

    lax.fori_loop(1, group, build_step, 0)

    def stack_rows(pieces):
        return jnp.concatenate(pieces, axis=0)

    cells = stack_rows([krecv[s] for s in range(group)])
    owner = lax.broadcasted_iota(jnp.int32, (group, pw), 0).astype(jnp.float32)
    kin_ref[...] = kinetic(*numbers(cells), owner)
    spread_wait(*firsts)
    for part in range(2):
        in_vec[0, part] = stack_rows([xrecv[s, part:part + 1] for s in range(group)])

    upper = lax.broadcasted_iota(jnp.int32, (8, 128), 0) < 4
    flip = jnp.where(upper, 1.0, -1.0).astype(jnp.float32)

    def swap_half(values):
        return pltpu.roll(values, 4, 0)

    def halves(low, high):
        return low if low == high else jnp.where(upper, low, high)

    def lane_turn(s, v, paired):
        angle = [2.0 * np.pi * ((k * v) % grid_len) / grid_len for k in (s, s + half)]
        cos_val, sin_val = [float(np.cos(a)) for a in angle], [float(np.sin(a)) for a in angle]
        if paired:
            return halves(*cos_val), halves(*sin_val)
        return cos_val[0], sin_val[0]

    def twist(item, s, v, paired, direction):
        if v == 0 or (s == 0 and not paired):
            return item
        cos_val, sin_val = lane_turn(s, v, paired)
        return c_mul(item, cos_val, sin_val if direction > 0 else -sin_val)

    def z_turn(tiles, which):
        stacked = jnp.concatenate([jnp.concatenate(list(t), axis=1) for t in tiles], axis=0)
        high, low = two_parts(stacked)
        out = bdot(high, zed_ref[which]) + bdot(low, zed_ref[which]) + bdot(high, zed_ref[which + 1])
        return [(out[8 * k:8 * k + 8, :128], out[8 * k:8 * k + 8, 128:]) for k in range(len(tiles))]

    def keep(slot, v, item):
        work_ref[0, v, slot] = item[0]
        work_ref[1, v, slot] = item[1]

    def kept(slot, v):
        return work_ref[0, v, slot], work_ref[1, v, slot]

    def own_row(ref, turn, part):
        return ref[turn, part, pl.ds(me, 1), :]

    def put(turn, src):
        v_re, v_im = in_vec[turn, 0, src:src + 1, :], in_vec[turn, 1, src:src + 1, :]
        both = split_rows(ta_ref[src] * v_re + tb_ref[src] * v_im)
        pieces = []
        for k in range(folds):
            for at in range(0, 2 * slab, 16):
                pieces.append(both[at:at + 16] * mask_ref[src, k])
        out = bdot_t(jnp.concatenate(pieces, axis=0), hot_ref[src])
        tiles = []
        for k in range(folds):
            base = k * 2 * slab
            block = out[base:base + slab] + out[base + slab:base + 2 * slab]
            for at in (0, 128):
                tiles.append([block[8 * t:8 * t + 8, at:at + 128] for t in range(3)])
        return tiles

    def forward_pair(turn, s):
        low, high = put(turn, s), put(turn, s + half)
        rest = [(
            jnp.where(upper, a[1], swap_half(b[1])), jnp.where(upper, swap_half(a[1]), b[1]),
        ) for a, b in zip(low, high)]
        turned = z_turn([(a[0], a[2]) for a in low] + [(b[0], b[2]) for b in high] + rest, 0)
        for k, (slot, first, paired) in enumerate(((s, s, False), (s + half, s + half, False), (group + s, s, True))):
            for v, item in enumerate(twelve_point(turned[k * planes:(k + 1) * planes], 1)):
                keep(slot, v, twist(item, first, v, paired, 1))

    def cross(item):
        return tuple(swap_half(x) + x * flip for x in item)

    def half_turn(item, s, direction):
        if s == 0:
            return item
        angle = 2.0 * np.pi * s / group
        return c_mul(item, halves(1.0, float(np.cos(angle))), direction * halves(0.0, float(np.sin(angle))))

    def middle(v):
        items = eight_point([kept(s, v) for s in range(group)], 1)
        items = [c_scale(item, pot_ref[v, u]) for u, item in enumerate(items)]
        for s, item in enumerate(eight_point(items, -1)):
            keep(s, v, twist(item, s, v, False, -1))
        items = four_point([half_turn(cross(kept(group + s, v)), s, 1) for s in range(half)], 1)
        items = [c_scale(item, pot_ref[v, group + t]) for t, item in enumerate(items)]
        for s, item in enumerate(four_point(items, -1)):
            keep(group + s, v, twist(cross(half_turn(item, s, -1)), s, v, True, -1))

    def backward_pair(s):
        spread = []
        for slot in (s, s + half, group + s):
            spread += twelve_point([kept(slot, v) for v in range(planes)], -1)
        turned = z_turn(spread, 2)
        low, high, rest = [turned[k * planes:(k + 1) * planes] for k in range(3)]
        low = [(a[0], jnp.where(upper, r[0], swap_half(r[1])), a[1]) for a, r in zip(low, rest)]
        high = [(b[0], jnp.where(upper, swap_half(r[0]), r[1]), b[1]) for b, r in zip(high, rest)]
        for dest, tiles in ((s, low), (s + half, high)):
            for k in range(folds):
                block = jnp.concatenate([jnp.concatenate(tiles[2 * k + m], axis=0) for m in range(2)], axis=1)
                left_ref[dest, k * 2 * slab:(k + 1) * 2 * slab, :] = split_rows(block)

    def partial_copy(turn, mask):
        return pltpu.make_async_remote_copy(
            src_ref=rsend.at[turn, mask], dst_ref=rrecv.at[turn, mask],
            send_sem=rs_sem.at[turn, mask - 1], recv_sem=rr_sem.at[turn, mask - 1],
            device_id={"ga": peer_of(mask)}, device_id_type=MESH)

    def take(turn, mask):
        dest = peer_of(mask)
        stacked = left_ref[dest]
        for at in range(0, pw, WIDE):
            span = slice(at, at + WIDE)
            out = bdot(stacked, hot_ref[dest, :, span])
            fold = group_ref[dest, :, span]
            chosen = out[:2 * slab]
            for k in range(1, folds):
                chosen = jnp.where(fold == float(k), out[k * 2 * slab:(k + 1) * 2 * slab], chosen)
            value = chosen[:slab] + chosen[slab:]
            for part, table in enumerate((ta_ref, tb_ref)):
                rsend[turn, mask, part:part + 1, span] = jnp.sum(table[dest, :, span] * value, axis=0, keepdims=True)
        if mask:
            partial_copy(turn, mask).start()

    def sum_copy(off, send, recv, send_sem, recv_sem, incoming):
        source = lax.rem(me + group - off, group) if incoming else me
        return pltpu.make_async_remote_copy(
            src_ref=send, dst_ref=recv.at[source],
            send_sem=send_sem.at[off - 1], recv_sem=recv_sem.at[off - 1],
            device_id={"ga": lax.rem(me + off, group)}, device_id_type=MESH)

    def all_sum(local, send, recv, send_sem, recv_sem):
        send[...] = local
        recv[me] = local
        for off in range(1, group):
            sum_copy(off, send, recv, send_sem, recv_sem, False).start()

    def all_sum_end(send, recv, send_sem, recv_sem):
        for off in range(1, group):
            sum_copy(off, send, recv, send_sem, recv_sem, True).wait()
        running = recv[0]
        for dev in range(1, group):
            running = running + recv[dev]
        return running

    def project(turn):
        found = []
        for part in range(2):
            row = own_row(in_vec, turn, part)
            running = proj_ref[:, :128] * row[:, :128]
            for at in range(128, pw, 128):
                running = running + proj_ref[:, at:at + 128] * row[:, at:at + 128]
            found.append(jnp.sum(jnp.transpose(running), axis=0, keepdims=True))
        return jnp.concatenate(found, axis=0)

    def nonlocal_rows(sums):
        half = sums.shape[1] // 2
        pair = jnp.concatenate([
            sums[0:1, :half] + sums[1:2, half:], sums[1:2, :half] - sums[0:1, half:]], axis=0)
        mixed = jnp.dot(pair, couple_ref[...], precision=top_precision, preferred_element_type=jnp.float32)
        m_re, m_im = mixed[0:1], mixed[1:2]
        found = []
        for row in (jnp.concatenate([m_re, -m_im], axis=1), jnp.concatenate([m_im, m_re], axis=1)):
            column = jnp.transpose(jnp.broadcast_to(row, (2 * half, 128)))
            found.append(jnp.concatenate([
                jnp.sum(proj_ref[:, at:at + 128] * column, axis=0, keepdims=True) for at in range(0, pw, 128)], axis=1))
        return jnp.concatenate(found, axis=0)

    def apply_h(turn):
        sums = (psend.at[turn], precv.at[turn], ps_sem.at[turn], pr_sem.at[turn])
        all_sum(project(turn), *sums)
        for s in range(half):
            forward_pair(turn, s)
        for v in range(planes):
            middle(v)
        for masks in ((6, 7, 2, 3), (4, 5, 1, 0)):
            for mask in masks[:2]:
                backward_pair(lax.rem(peer_of(mask), half))
            for mask in masks:
                take(turn, mask)
        start = nonlocal_rows(all_sum_end(*sums) * (1.0 / total_pw))
        own_kin = kin_ref[pl.ds(me, 1), :]
        start = start + own_kin * jnp.concatenate([own_row(in_vec, turn, 0), own_row(in_vec, turn, 1)], axis=0)
        running = start + rsend[turn, 0]
        for mask in range(1, group):
            partial_copy(turn, mask).wait()
            running = running + rrecv[turn, mask]
        hsend[turn] = running
        return running

    def share_h(turn):
        out = (hsend.at[turn], hrecv.at[turn], hs_sem.at[turn], hr_sem.at[turn])
        spread_start(*out)
        hrecv[turn, me] = hsend[turn]
        spread_wait(*out)
        for part in range(2):
            out_vec[turn, part] = stack_rows([hrecv[turn, s, part:part + 1] for s in range(group)])

    def vector(index):
        ref = out_vec if index % 2 else in_vec
        return ref[index // 2]

    def gram_sums(pair_list):
        found = {}
        for one, two, use_kin in pair_list:
            left, right = vector(one), vector(two)
            product = left[0] * right[0] + left[1] * right[1]
            value = total_of(product * kin_ref[...] if use_kin else product) * (1.0 / total_pw)
            found[use_kin, one, two] = value
            found[use_kin, two, one] = value
        return found

    def realize(coef_map, basis):
        running = 0.0
        for index, coef in coef_map.items():
            running = running + (basis(index) if isinstance(coef, float) and coef == 1.0 else coef * basis(index))
        return running

    def smooth(residual, level):
        kin = kin_ref[...]
        ratio = kin / (1.5 * level + 1.0)
        poly = 27.0 + ratio * (18.0 + ratio * (12.0 + 8.0 * ratio))
        square = ratio * ratio
        return residual * (poly / (poly + 16.0 * square * square))

    def save(names, slot):
        for k, value in enumerate(names):
            save_ref[slot + k:slot + k + 1, :] = jnp.broadcast_to(value, (1, 128))

    def load_saved(slot):
        return save_ref[slot:slot + 1, 0:1]

    def first_step(gram):
        psi, ham = {0: 1.0}, {1: 1.0}
        eps_zero = gram_form(gram, psi, ham, False) / (gram_form(gram, psi, psi, False) + small_eps)
        return psi, ham, eps_zero, combine([(1.0, ham), (-eps_zero, psi)])

    def second_step(gram):
        psi, ham, eps_zero, r_map = first_step(gram)
        q_map = combine([(1.0, {3: 1.0}), (-eps_zero, {2: 1.0})])
        lam_zero = -gram_form(gram, r_map, q_map, False) / (gram_form(gram, q_map, q_map, False) + small_eps)
        psi_one = combine([(1.0, psi), (lam_zero, {2: 1.0})])
        h_one = combine([(1.0, ham), (lam_zero, {3: 1.0})])
        eps_one = gram_form(gram, psi_one, h_one, False) / (gram_form(gram, psi_one, psi_one, False) + small_eps)
        r_one = combine([(1.0, h_one), (-eps_one, psi_one)])
        change = combine([(1.0, r_map), (-1.0, r_one)])
        weight = gram_form(gram, r_map, change, False) / (gram_form(gram, change, change, False) + small_eps)
        step = weight * lam_zero
        psi_mid = combine([(1.0, psi), (step, {2: 1.0})])
        h_mid = combine([(1.0, ham), (step, {3: 1.0})])
        r_mid = combine([(1.0, r_map), (-weight, change)])
        eps_mid = gram_form(gram, psi_mid, h_mid, False) / (gram_form(gram, psi_mid, psi_mid, False) + small_eps)
        return psi_mid, h_mid, r_mid, eps_mid, step

    first_pairs = new_pairs(0, 2, (False, True))
    second_pairs = new_pairs(2, 4, (False, True))
    gram_pairs = first_pairs + second_pairs

    def swap(which, send, recv, off, incoming):
        source = lax.rem(band + bands - off, bands) if incoming else band
        return pltpu.make_async_remote_copy(
            src_ref=send, dst_ref=recv.at[source],
            send_sem=ns_sem.at[which, off - 1], recv_sem=nr_sem.at[which, off - 1],
            device_id={"band": lax.rem(band + off, bands)}, device_id_type=MESH)

    def share(which, send, recv, values):
        send[...] = values
        recv[band] = values
        for off in range(1, bands):
            swap(which, send, recv, off, False).start()

    def share_end(which, send, recv):
        for off in range(1, bands):
            swap(which, send, recv, off, True).wait()

    def own(index):
        ref = out_vec if index % 2 else in_vec
        return jnp.concatenate([own_row(ref, index // 2, 0), own_row(ref, index // 2, 1)], axis=0)

    def turn_step(turn, carry):
        apply_h(turn)

        @pl.when(turn == 0)
        def _():
            share_h(0)
            gram = gram_sums(first_pairs)
            save([gram[kind, one, two] for one, two, kind in first_pairs], 0)
            r_map = first_step(gram)[3]
            level = gram_form(gram, r_map, r_map, True) / (gram_form(gram, r_map, r_map, False) + small_eps)
            p_zero = smooth(realize(r_map, vector), level)
            in_vec[1] = p_zero

        @pl.when(turn == 1)
        def _():
            share_h(1)
            gram = gram_sums(second_pairs)
            save([gram[kind, one, two] for one, two, kind in second_pairs], len(first_pairs))
            for k, (one, two, kind) in enumerate(first_pairs):
                gram[kind, one, two] = gram[kind, two, one] = load_saved(k)
            psi_mid, h_mid, r_mid, eps_mid, step = second_step(gram)
            level = gram_form(gram, r_mid, r_mid, True) / (gram_form(gram, r_mid, r_mid, False) + small_eps)
            p_one = smooth(realize(r_mid, vector), level)
            in_vec[2] = p_one
            share(0, nsend, nrecv, jnp.stack([realize(psi_mid, own), own(4), realize(h_mid, own)]))

        return carry

    lax.fori_loop(0, 3, turn_step, 0)

    g_own = hsend[2]
    share(1, isend, irecv, g_own)
    last_pairs = new_pairs(4, 6, (False,))

    def own_last(index):
        return g_own if index == 5 else own(index)

    lane_id = lax.broadcasted_iota(jnp.int32, (1, 128), 1)
    local = jnp.zeros((1, 128), jnp.float32)
    held = [own_last(index) for index in range(6)]
    for k, (one, two, kind) in enumerate(last_pairs):
        local = jnp.where(lane_id == k, total_of(held[one] * held[two]), local)
    sums = (gsend, grecv, gs_sem, gr_sem)
    all_sum(local, *sums)
    gram = {}
    for k, (one, two, kind) in enumerate(gram_pairs):
        gram[kind, one, two] = gram[kind, two, one] = load_saved(k)
    psi_mid, h_mid, r_mid, eps_mid, step = second_step(gram)
    summed = all_sum_end(*sums) * (1.0 / total_pw)
    for k, (one, two, kind) in enumerate(last_pairs):
        gram[kind, one, two] = gram[kind, two, one] = summed[:, k:k + 1]
    q_one = combine([(1.0, {5: 1.0}), (-eps_mid, {4: 1.0})])
    lam_one = -gram_form(gram, r_mid, q_one, False) / (gram_form(gram, q_one, q_one, False) + small_eps)
    share(2, lsend, lrecv, jnp.broadcast_to(lam_one, (1, 128)))
    share_end(0, nsend, nrecv)
    share_end(1, isend, irecv)

    pairs = [
        [stack_rows([nrecv[o, 0, part:part + 1] for o in range(bands)] + [nrecv[o, 1, part:part + 1] for o in range(bands)]) for part in range(2)],
        [stack_rows([nrecv[o, 2, part:part + 1] for o in range(bands)] + [irecv[o, part:part + 1] for o in range(bands)]) for part in range(2)],
    ]
    column_id = lax.broadcasted_iota(jnp.int32, (2 * bands, 128), 1)
    local = jnp.zeros((2 * bands, 128), jnp.float32)
    slot = 0
    for o_re, o_im in pairs:
        for mine in (0, 1):
            m_re, m_im = nsend[mine, 0:1], nsend[mine, 1:2]
            for product in (m_re * o_re + m_im * o_im, m_re * o_im - m_im * o_re):
                local = jnp.where(column_id == slot, jnp.sum(product, axis=1, keepdims=True), local)
                slot += 1
    crossed = (csend, crecv, cs_sem, cr_sem)
    all_sum(local, *crossed)

    new_map = combine([(1.0, psi_mid), (lam_one, {4: 1.0})])
    ham_new = combine([(1.0, h_mid), (lam_one, {5: 1.0})])
    norm_new = gram_form(gram, new_map, new_map, False) + small_eps
    energy = gram_form(gram, new_map, ham_new, False) / norm_new
    resid = combine([(1.0, ham_new), (-energy, new_map)])
    resid_norm = gram_form(gram, resid, resid, False) / norm_new
    new_ref[...] = nsend[0] + lam_one * nsend[1]
    share_end(2, lsend, lrecv)
    summed = all_sum_end(*crossed) * (1.0 / total_pw)
    lam_rows = stack_rows([lrecv[o] for o in range(bands)])
    mixed = summed[:bands] + lam_rows * summed[bands:]
    result = mixed + lam_one * pltpu.roll(mixed, 126, 1)
    scal_ref[...] = jnp.concatenate([
        result, jnp.broadcast_to(energy, (1, 128)), jnp.broadcast_to(resid_norm, (1, 128)),
        jnp.zeros((scal_ref.shape[0] - bands - 2, 128), jnp.float32)], axis=0)


def finish_kernel(bands, new_ref, scal_ref, bands_ref, energy_ref, norm_ref, corr_ref, sub_ref):
    bands_ref[:, 0, :] = new_ref[...]
    lane = lax.broadcasted_iota(jnp.int32, (1, bands), 1)
    for ref, base in ((corr_ref, 0), (sub_ref, 4)):
        for part in range(2):
            row = jnp.zeros((1, bands), jnp.float32)
            for other in range(bands):
                at = base + part
                row = jnp.where(lane == other, scal_ref[other:other + 1, at:at + 1], row)
            ref[part] = row
    energy_ref[0] = scal_ref[bands, 0]
    norm_ref[0] = scal_ref[bands + 1, 0]


def kernel_body(coeffs, cell_map, potential, projectors, strengths, proj_atom, proj_chan):
    group = lax.axis_size("ga")
    bands = lax.axis_size("band")
    grid_len = potential.shape[0]
    planes = grid_len // group
    pw = coeffs.shape[2]
    total_pw = pw * group
    slab = 2 * planes
    folds = planes // 2
    tile_count = group + group // 2
    proj_rows = 2 * projectors.shape[1]
    tables = [jnp.asarray(t) for t in const_tables(grid_len, group)]
    dma = pltpu.SemaphoreType.DMA
    vmem = pl.BlockSpec(memory_space=pltpu.VMEM)
    far = pl.BlockSpec(memory_space=pl.ANY)
    f32, b16 = jnp.float32, jnp.bfloat16
    scal_rows = 8 * (-(-(bands + 2) // 8))
    peers = group - 1
    new, scal = pl.pallas_call(
        functools.partial(sweep_kernel, (group, bands, planes, grid_len, total_pw, pw)),
        out_shape=(
            jax.ShapeDtypeStruct((2, pw), f32),
            jax.ShapeDtypeStruct((scal_rows, 128), f32),
        ),
        in_specs=[vmem, vmem, far, far] + [vmem] * 5,
        out_specs=(vmem, vmem),
        scratch_shapes=[
            pltpu.VMEM((group, WIDE, pw), b16),
            pltpu.VMEM((group, folds, 16, pw), b16),
            pltpu.VMEM((group, 1, pw), f32),
            pltpu.VMEM((group, slab, pw), f32),
            pltpu.VMEM((group, slab, pw), f32),
            pltpu.VMEM((group, pw), f32),
            pltpu.VMEM((2, planes, tile_count, 8, 128), f32),
            pltpu.VMEM((group, folds * 2 * slab, WIDE), b16),
            pltpu.VMEM((planes, tile_count, 8, 128), f32),
            pltpu.VMEM((planes * grid_len, grid_len), f32),
            pltpu.VMEM((proj_rows, pw), f32),
            pltpu.VMEM((proj_rows // 2, proj_rows // 2), f32),
            pltpu.VMEM((3, 2, group, pw), f32),
            pltpu.VMEM((2, 2, group, pw), f32),
            pltpu.VMEM((24, 128), f32),
            dma((2,)),
            pltpu.VMEM((1, pw), f32), pltpu.VMEM((group, 1, pw), f32),
            pltpu.VMEM((2, pw), f32), pltpu.VMEM((group, 2, pw), f32),
            pltpu.VMEM((3, group, 2, pw), f32), pltpu.VMEM((3, group, 2, pw), f32),
            pltpu.VMEM((3, 2, pw), f32), pltpu.VMEM((2, group, 2, pw), f32),
            pltpu.VMEM((3, 2, proj_rows), f32), pltpu.VMEM((3, group, 2, proj_rows), f32),
            pltpu.VMEM((1, 128), f32), pltpu.VMEM((group, 1, 128), f32),
            pltpu.VMEM((3, 2, pw), f32), pltpu.VMEM((bands, 3, 2, pw), f32),
            pltpu.VMEM((2, pw), f32), pltpu.VMEM((bands, 2, pw), f32),
            pltpu.VMEM((1, 128), f32), pltpu.VMEM((bands, 1, 128), f32),
            pltpu.VMEM((2 * bands, 128), f32), pltpu.VMEM((group, 2 * bands, 128), f32),
            dma((peers,)), dma((peers,)), dma((peers,)), dma((peers,)),
            dma((3, peers)), dma((3, peers)), dma((2, peers)), dma((2, peers)),
            dma((3, peers)), dma((3, peers)), dma((peers,)), dma((peers,)),
            dma((3, bands - 1)), dma((3, bands - 1)), dma((peers,)), dma((peers,)),
        ],
        compiler_params=pltpu.CompilerParams(
            collective_id=0, has_side_effects=True, vmem_limit_bytes=60 * 1024 * 1024
        ),
        name="sweeps",
    )(
        coeffs, cell_map.reshape(-1, 128), jnp.swapaxes(potential, 0, 1).reshape(planes * grid_len, grid_len),
        projectors.reshape(proj_rows, pw), strengths.reshape(-1, strengths.shape[2]),
        proj_atom.reshape(1, -1), proj_chan.reshape(1, -1), *tables,
    )

    smem = pl.BlockSpec(memory_space=pltpu.SMEM)
    return pl.pallas_call(
        functools.partial(finish_kernel, bands),
        out_shape=(
            jax.ShapeDtypeStruct((2, 1, pw), f32),
            jax.ShapeDtypeStruct((1,), f32),
            jax.ShapeDtypeStruct((1,), f32),
            jax.ShapeDtypeStruct((2, 1, bands), f32),
            jax.ShapeDtypeStruct((2, 1, bands), f32),
        ),
        in_specs=[vmem, vmem],
        out_specs=(vmem, smem, smem, vmem, vmem),
        name="finish",
    )(new, scal)


def body(coeffs, cell_map, potential, projectors, strengths, proj_atom, proj_chan):
    group = lax.axis_size("ga")
    grid_len = potential.shape[0]
    planes = grid_len // group
    fits = (
        group == 8
        and planes == 12
        and coeffs.shape[1] == 1
        and coeffs.shape[2] % 256 == 0
        and 2 * projectors.shape[1] == 128
    )
    chosen = kernel_body if fits else plain_body
    return chosen(coeffs, cell_map, potential, projectors, strengths, proj_atom, proj_chan)


def solution(mesh):
    placed = (
        P(None, "band", "ga"),
        P("ga"),
        P(None, "ga", None),
        P(None, None, "ga"),
        P(),
        P(),
        P(),
    )
    return jax.shard_map(
        body,
        mesh=mesh,
        in_specs=placed,
        out_specs=(
            P(None, "band", "ga"),
            P("band"),
            P("band"),
            P(None, "band", None),
            P(None, "band", None),
        ),
        check_vma=False,
    )
```

```python
import functools

import jax
import jax.numpy as jnp
import numpy as np
from jax import lax
from jax.experimental import pallas as pl
from jax.experimental.pallas import tpu as pltpu
from jax.sharding import PartitionSpec as P

top_precision = lax.Precision.HIGHEST
kin_unit = 0.02
small_eps = 1e-06


def signed_freq(index_arr, grid_len):
    return jnp.where(index_arr < grid_len // 2, index_arr, index_arr - grid_len)


def wave_tables(grid_len, row_freq, col_freq, sign_val, factor):
    phase = row_freq[:, None] * col_freq[None, :] % grid_len
    angle = 2.0 * jnp.pi / grid_len * phase.astype(jnp.float32)
    return (jnp.cos(angle) * factor, jnp.sin(angle) * (sign_val * factor))


def block_table(cos_table, sin_table):
    upper = jnp.concatenate([cos_table, sin_table], axis=1)
    lower = jnp.concatenate([-sin_table, cos_table], axis=1)
    return jnp.concatenate([upper, lower], axis=0)


def quarter_turn(grid_vals):
    half_len = grid_vals.shape[-1] // 2
    return jnp.concatenate([-grid_vals[..., half_len:], grid_vals[..., :half_len]], axis=-1)


def mix_dim(grid_vals, cos_table, sin_table, pattern):
    direct = jnp.einsum(pattern, cos_table, grid_vals, precision=top_precision)
    turned = jnp.einsum(pattern, sin_table, quarter_turn(grid_vals), precision=top_precision)
    return direct + turned


def mix_last(grid_vals, table_full):
    row_width = grid_vals.shape[-1]
    product = jnp.dot(
        grid_vals.reshape(-1, row_width),
        table_full,
        precision=top_precision,
        preferred_element_type=jnp.float32,
    )
    return product.reshape(grid_vals.shape)


def band_dot(left_vec, right_vec, weight):
    return jnp.sum(left_vec * right_vec * weight, axis=(0, 2))


def per_band(values):
    return values[None, :, None]


def pair_products(left_vec, right_vec):

    def contract(first_part, second_part):
        return jnp.einsum("bg,cg->bc", first_part, second_part, precision=top_precision)

    real_part = contract(left_vec[0], right_vec[0]) + contract(left_vec[1], right_vec[1])
    imag_part = contract(left_vec[0], right_vec[1]) - contract(left_vec[1], right_vec[0])
    return jnp.stack([real_part, imag_part])


def precondition(residual, kinetic, kin_level):
    x_ratio = kinetic[None, :] / (1.5 * kin_level[:, None] + 1.0)
    numer_poly = 27.0 + x_ratio * (18.0 + x_ratio * (12.0 + 8.0 * x_ratio))
    square = x_ratio * x_ratio
    return residual * (numer_poly / (numer_poly + 16.0 * square * square))[None]


def coupling_matrix(proj_atom, proj_chan, strengths):
    atom_count = strengths.shape[0]
    chan_count = strengths.shape[1]
    symmetric = 0.5 * (strengths + jnp.swapaxes(strengths, 1, 2))
    atom_hot = (proj_atom[:, None] == jnp.arange(atom_count, dtype=jnp.int32)[None, :]).astype(
        jnp.float32
    )
    chan_hot = (proj_chan[:, None] == jnp.arange(chan_count, dtype=jnp.int32)[None, :]).astype(
        jnp.float32
    )
    rows_d = jnp.einsum("pa,pc,acd->pd", atom_hot, chan_hot, symmetric, precision=top_precision)
    same_atom = jnp.dot(
        atom_hot, atom_hot.T, precision=top_precision, preferred_element_type=jnp.float32
    )
    return same_atom * jnp.dot(
        rows_d, chan_hot.T, precision=top_precision, preferred_element_type=jnp.float32
    )


def combine(term_list):
    merged = {}
    for scalar, coef_map in term_list:
        for index_one, coef_a in coef_map.items():
            merged[index_one] = merged.get(index_one, 0.0) + scalar * coef_a
    return merged


def gram_form(gram_table, left_map, right_map, use_kin):
    running = 0.0
    for index_one, coef_a in left_map.items():
        for index_two, coef_b in right_map.items():
            running = running + coef_a * coef_b * gram_table[use_kin, index_one, index_two]
    return running


def new_pairs(first_new, last_new, kinds):
    pair_list = []
    for use_kin in kinds:
        for index_two in range(first_new, last_new):
            for index_one in range(index_two + 1):
                pair_list.append((index_one, index_two, use_kin))
    return pair_list


def plain_body(coeffs, cell_map, potential, projectors, strengths, proj_atom, proj_chan):
    ga_count = lax.axis_size("ga")
    grid_len = potential.shape[0]
    planes = grid_len // ga_count
    band_local = coeffs.shape[1]
    total_pw = coeffs.shape[2] * ga_count
    device = lax.axis_index("ga")
    plane_num = cell_map // (grid_len * grid_len)
    y_index = cell_map // grid_len % grid_len
    z_index = cell_map % grid_len
    freq_x = signed_freq(device + ga_count * plane_num, grid_len)
    freq_y = signed_freq(y_index, grid_len)
    freq_z = signed_freq(z_index, grid_len)
    kinetic = kin_unit * (freq_x * freq_x + freq_y * freq_y + freq_z * freq_z).astype(jnp.float32)
    kin_weight = kinetic[None, None, :]
    slot_re = (plane_num * grid_len + y_index) * (2 * grid_len) + z_index
    slot_im = slot_re + grid_len
    cell_count = planes * grid_len * 2 * grid_len
    natural = jnp.arange(grid_len, dtype=jnp.int32)
    cyclic = natural % planes * ga_count + natural // planes
    cos_fwd, sin_fwd = wave_tables(grid_len, natural, natural, 1.0, 1.0)
    cos_back, sin_back = wave_tables(grid_len, natural, natural, -1.0, 1.0 / grid_len)
    z_forward = block_table(cos_fwd, sin_fwd)
    z_backward = block_table(cos_back, sin_back)
    xcos_fwd, xsin_fwd = wave_tables(grid_len, natural, cyclic, 1.0, 1.0)
    xcos_back, xsin_back = wave_tables(grid_len, cyclic, natural, -1.0, 1.0 / grid_len)
    doubled = jnp.concatenate([potential, potential], axis=-1)
    coupling = coupling_matrix(proj_atom, proj_chan, strengths)

    def real_space(grid_vals):
        grid_vals = mix_dim(grid_vals, xcos_fwd, xsin_fwd, "kj,bjyw->bkyw")
        grid_vals = grid_vals * doubled[None]
        grid_vals = mix_dim(grid_vals, xcos_back, xsin_back, "jk,bkyw->bjyw")
        return lax.all_to_all(grid_vals, "ga", split_axis=1, concat_axis=2, tiled=True)

    def local_part(vectors):
        item_count = vectors.shape[1]
        flat_grid = jnp.zeros((item_count, cell_count), jnp.float32)
        flat_grid = flat_grid.at[:, slot_re].set(vectors[0]).at[:, slot_im].set(vectors[1])
        grid_vals = mix_last(
            flat_grid.reshape(item_count, planes, grid_len, 2 * grid_len), z_forward
        )
        grid_vals = mix_dim(grid_vals, cos_fwd, sin_fwd, "ky,bpyw->bpkw")
        grid_vals = real_space(
            lax.all_to_all(grid_vals, "ga", split_axis=2, concat_axis=1, tiled=True)
        )
        grid_vals = mix_dim(grid_vals, cos_back, sin_back, "ky,bpyw->bpkw")
        flat_grid = mix_last(grid_vals, z_backward).reshape(item_count, cell_count)
        return jnp.stack([flat_grid[:, slot_re], flat_grid[:, slot_im]])

    def contract(first_part, second_part):
        return jnp.einsum("pg,bg->pb", first_part, second_part, precision=top_precision)

    def spread(weights, proj_table):
        return jnp.einsum("pb,pg->bg", weights, proj_table, precision=top_precision)

    def projected_part(vectors):
        proj_re = contract(projectors[0], vectors[0]) + contract(projectors[1], vectors[1])
        proj_im = contract(projectors[0], vectors[1]) - contract(projectors[1], vectors[0])
        proj_re, proj_im = lax.psum((proj_re, proj_im), "ga")
        mixed_re = jnp.dot(
            coupling,
            proj_re / total_pw,
            precision=top_precision,
            preferred_element_type=jnp.float32,
        )
        mixed_im = jnp.dot(
            coupling,
            proj_im / total_pw,
            precision=top_precision,
            preferred_element_type=jnp.float32,
        )
        out_re = spread(mixed_re, projectors[0]) - spread(mixed_im, projectors[1])
        out_im = spread(mixed_re, projectors[1]) + spread(mixed_im, projectors[0])
        return jnp.stack([out_re, out_im])

    def apply_h(vectors):
        return kin_weight * vectors + local_part(vectors) + projected_part(vectors)

    def gram_sums(basis, pair_list):
        stacked = []
        for index_one, index_two, use_kin in pair_list:
            stacked.append(
                band_dot(basis[index_one], basis[index_two], kin_weight if use_kin else 1.0)
            )
        summed = lax.psum(jnp.stack(stacked), "ga") / total_pw
        found = {}
        for slot_num, entry in enumerate(pair_list):
            index_one, index_two, use_kin = entry
            found[use_kin, index_one, index_two] = summed[slot_num]
            found[use_kin, index_two, index_one] = summed[slot_num]
        return found

    def realize(coef_map, basis):
        running = jnp.zeros_like(basis[0])
        for index_one, coef_a in coef_map.items():
            running = (
                running
                + per_band(jnp.zeros((band_local,), jnp.float32) + coef_a) * basis[index_one]
            )
        return running

    h_zero = apply_h(coeffs)
    basis = [coeffs, h_zero]
    gram_table = gram_sums(basis, new_pairs(0, 2, (False, True)))
    psi_map = {0: 1.0}
    ham_map = {1: 1.0}
    eps_zero = gram_form(gram_table, psi_map, ham_map, False) / (
        gram_form(gram_table, psi_map, psi_map, False) + small_eps
    )
    r_map = combine([(1.0, ham_map), (-eps_zero, psi_map)])
    level_zero = gram_form(gram_table, r_map, r_map, True) / (
        gram_form(gram_table, r_map, r_map, False) + small_eps
    )
    p_zero = precondition(realize(r_map, basis), kinetic, level_zero)
    g_zero = apply_h(p_zero)
    basis = [coeffs, h_zero, p_zero, g_zero]
    gram_table.update(gram_sums(basis, new_pairs(2, 4, (False, True))))
    q_map = combine([(1.0, {3: 1.0}), (-eps_zero, {2: 1.0})])
    lam_zero = -gram_form(gram_table, r_map, q_map, False) / (
        gram_form(gram_table, q_map, q_map, False) + small_eps
    )
    psi_one_map = combine([(1.0, psi_map), (lam_zero, {2: 1.0})])
    h_one_map = combine([(1.0, ham_map), (lam_zero, {3: 1.0})])
    eps_one = gram_form(gram_table, psi_one_map, h_one_map, False) / (
        gram_form(gram_table, psi_one_map, psi_one_map, False) + small_eps
    )
    r_one_map = combine([(1.0, h_one_map), (-eps_one, psi_one_map)])
    change_map = combine([(1.0, r_map), (-1.0, r_one_map)])
    weight_one = gram_form(gram_table, r_map, change_map, False) / (
        gram_form(gram_table, change_map, change_map, False) + small_eps
    )
    step_mid = weight_one * lam_zero
    psi_mid_map = combine([(1.0, psi_map), (step_mid, {2: 1.0})])
    h_mid_map = combine([(1.0, ham_map), (step_mid, {3: 1.0})])
    r_mid_map = combine([(1.0, r_map), (-weight_one, change_map)])
    eps_mid = gram_form(gram_table, psi_mid_map, h_mid_map, False) / (
        gram_form(gram_table, psi_mid_map, psi_mid_map, False) + small_eps
    )
    level_mid = gram_form(gram_table, r_mid_map, r_mid_map, True) / (
        gram_form(gram_table, r_mid_map, r_mid_map, False) + small_eps
    )
    p_one = precondition(realize(r_mid_map, basis), kinetic, level_mid)
    g_one = apply_h(p_one)
    basis = [coeffs, h_zero, p_zero, g_zero, p_one, g_one]
    gram_table.update(gram_sums(basis, new_pairs(4, 6, (False,))))
    q_one_map = combine([(1.0, {5: 1.0}), (-eps_mid, {4: 1.0})])
    lam_one = -gram_form(gram_table, r_mid_map, q_one_map, False) / (
        gram_form(gram_table, q_one_map, q_one_map, False) + small_eps
    )
    new_map = combine([(1.0, psi_mid_map), (lam_one, {4: 1.0})])
    ham_new_map = combine([(1.0, h_mid_map), (lam_one, {5: 1.0})])
    norm_new = gram_form(gram_table, new_map, new_map, False) + small_eps
    energy = gram_form(gram_table, new_map, ham_new_map, False) / norm_new
    resid_map = combine([(1.0, ham_new_map), (-energy, new_map)])
    residual_norm = gram_form(gram_table, resid_map, resid_map, False) / norm_new
    new_bands = realize(new_map, basis)
    new_ham = realize(ham_new_map, basis)
    blank_rows = jnp.zeros((2, band_local, band_local * lax.axis_size("band")), jnp.float32)
    first_row = jnp.int32(0)
    over_rows = blank_rows
    ham_rows = blank_rows
    piece_bands = lax.all_gather(new_bands, "band", axis=1, tiled=True)
    piece_ham = lax.all_gather(new_ham, "band", axis=1, tiled=True)
    over_rows = lax.dynamic_update_slice_in_dim(
        over_rows, pair_products(new_bands, piece_bands), first_row, 2
    )
    ham_rows = lax.dynamic_update_slice_in_dim(
        ham_rows, pair_products(new_bands, piece_ham), first_row, 2
    )
    over_rows, ham_rows = (over_rows, ham_rows)
    over_rows, ham_rows = lax.psum((over_rows, ham_rows), "ga")
    correlation = over_rows / total_pw
    subspace = ham_rows / total_pw
    return (new_bands, energy, residual_norm, correlation, subspace)


WIDE = 256
MESH = pl.DeviceIdType.MESH


def split_const(values):
    high = np.asarray(values, np.float32).astype(jnp.bfloat16)
    low = (values - high.astype(np.float64)).astype(np.float32).astype(jnp.bfloat16)
    return np.stack([high, low])


def const_tables(grid_len, group):
    planes = grid_len // group
    unit = 2.0 * np.pi / grid_len
    quarter = grid_len / 4.0
    main = list(range(8))
    rest = list(range(8, planes))
    y_in = np.array(main + rest + rest + main)
    part_row = np.array([0] * planes + [1] * planes)
    y_real = np.arange(group)[:, None] * planes + y_in[None, :]
    freq = np.arange(grid_len)
    phase = (y_real[..., None] * freq) % grid_len
    tab_a = np.cos(unit * (phase - quarter * part_row[:, None]))
    tab_b = np.cos(unit * (phase + quarter * (1 - part_row[:, None])))
    high, low = split_const(np.concatenate([tab_a, tab_b], axis=1))
    wave = np.concatenate([high, low], axis=2)
    theta = unit * (np.outer(freq, freq) % grid_len)
    turn = np.zeros((2, 128, 2, 128))
    turn[0, :grid_len, 0, :grid_len] = np.cos(theta)
    turn[0, :grid_len, 1, :grid_len] = np.sin(theta)
    turn[1, :grid_len, 0, :grid_len] = -np.sin(theta)
    turn[1, :grid_len, 1, :grid_len] = np.cos(theta)
    turn = turn.reshape(256, 256)
    zed = np.concatenate([split_const(turn), split_const(turn.T)], axis=0)
    return wave, zed


def two_parts(values):
    high = values.astype(jnp.bfloat16)
    low = (values - high.astype(jnp.float32)).astype(jnp.bfloat16)
    return high, low


def split_rows(values):
    high = values.astype(jnp.bfloat16).astype(jnp.float32)
    return jnp.concatenate([high, values - high], axis=0).astype(jnp.bfloat16)


def bdot(left, right):
    return jnp.dot(left, right, preferred_element_type=jnp.float32)


def bdot_t(left, right):
    return lax.dot_general(left, right, (((1,), (1,)), ((), ())), preferred_element_type=jnp.float32)


def total_of(values):
    return jnp.sum(jnp.sum(values, axis=0, keepdims=True), axis=1, keepdims=True)


def c_add(one, two):
    return one[0] + two[0], one[1] + two[1]


def c_sub(one, two):
    return one[0] - two[0], one[1] - two[1]


def c_turn(one, direction):
    return (-one[1], one[0]) if direction > 0 else (one[1], -one[0])


def c_mul(one, cos_val, sin_val):
    return one[0] * cos_val - one[1] * sin_val, one[0] * sin_val + one[1] * cos_val


def c_scale(one, factor):
    return one[0] * factor, one[1] * factor


def three_point(items, direction):
    total = c_add(items[1], items[2])
    side = c_scale(c_turn(c_sub(items[1], items[2]), direction), 0.8660254037844386)
    base = c_sub(items[0], c_scale(total, 0.5))
    return [c_add(items[0], total), c_add(base, side), c_sub(base, side)]


def four_point(items, direction):
    even, odd = c_add(items[0], items[2]), c_add(items[1], items[3])
    low, high = c_sub(items[0], items[2]), c_turn(c_sub(items[1], items[3]), direction)
    return [c_add(even, odd), c_add(low, high), c_sub(even, odd), c_sub(low, high)]


def eight_point(items, direction):
    even = four_point(items[0::2], direction)
    odd = four_point(items[1::2], direction)
    root = 0.7071067811865476
    turned = [
        odd[0],
        c_scale(c_add(odd[1], c_turn(odd[1], direction)), root),
        c_turn(odd[2], direction),
        c_scale(c_sub(c_turn(odd[3], direction), odd[3]), root),
    ]
    return [c_add(e, o) for e, o in zip(even, turned)] + [c_sub(e, o) for e, o in zip(even, turned)]


def twelve_point(items, direction):
    fours = [four_point([items[(4 * a + 3 * b) % 12] for b in range(4)], direction) for a in range(3)]
    threes = [three_point([fours[a][v] for a in range(3)], direction) for v in range(4)]
    return [threes[v % 4][v % 3] for v in range(12)]


def sweep_kernel(
    dims,
    coeffs_hbm, cell_hbm, potential_hbm, proj_hbm, strength_hbm, atom_hbm, chan_hbm,
    wave_hbm, zed_hbm,
    new_hbm, scal_hbm,
    hot_ref, mask_ref, group_ref, ta_ref, tb_ref, kin_ref, work_ref, left_ref,
    pot_ref, potential_ref, proj_ref, couple_ref, in_vec, out_vec, save_ref,
    strength_ref, atom_ref, chan_ref, wave_ref, zed_ref, new_ref, scal_ref, in_sem,
    ksend, krecv, xsend, xrecv, rsend, rrecv, hsend, hrecv, psend, precv,
    gsend, grecv, nsend, nrecv, isend, irecv, lsend, lrecv, csend, crecv,
    ks_sem, kr_sem, xs_sem, xr_sem, rs_sem, rr_sem, hs_sem, hr_sem, ps_sem, pr_sem,
    gs_sem, gr_sem, ns_sem, nr_sem, cs_sem, cr_sem,
):
    group, bands, planes, grid_len, total_pw, pw = dims
    slab = 2 * planes
    folds = planes // 2
    half = group // 2
    tiles = pw // 128
    me = lax.axis_index("ga")
    band = lax.axis_index("band")
    sides = [1 - 2 * lax.rem(me // (1 << bit), 2) for bit in range(3)]

    def peer_of(mask):
        return me + sum(sides[bit] * ((mask // (1 << bit)) % 2) * (1 << bit) for bit in range(3))

    loads = [
        pltpu.make_async_copy(source, target, in_sem.at[k])
        for k, (source, target) in enumerate((
            (cell_hbm, ksend), (coeffs_hbm, xsend), (wave_hbm.at[me], wave_ref), (strength_hbm, strength_ref),
            (atom_hbm, atom_ref), (chan_hbm, chan_ref), (potential_hbm, potential_ref), (proj_hbm, proj_ref),
            (zed_hbm, zed_ref)))
    ]
    barrier = pltpu.get_barrier_semaphore()
    for mask in range(1, group):
        pl.semaphore_signal(barrier, inc=1, device_id={"ga": peer_of(mask)}, device_id_type=MESH)
    for off in range(1, bands):
        pl.semaphore_signal(barrier, inc=1, device_id={"band": lax.rem(band + off, bands)}, device_id_type=MESH)
    for load in loads:
        load.start()
    for load in loads[:2]:
        load.wait()

    far_first = (6, 7, 4, 5, 2, 3, 1)

    def spread_copy(mask, send, recv, send_sem, recv_sem, incoming):
        peer = peer_of(mask)
        return pltpu.make_async_remote_copy(
            src_ref=send, dst_ref=recv.at[peer if incoming else me],
            send_sem=send_sem.at[mask - 1], recv_sem=recv_sem.at[mask - 1],
            device_id={"ga": peer}, device_id_type=MESH)

    def spread_start(send, recv, send_sem, recv_sem):
        for mask in far_first:
            spread_copy(mask, send, recv, send_sem, recv_sem, False).start()

    def spread_wait(send, recv, send_sem, recv_sem):
        for mask in range(1, group):
            spread_copy(mask, send, recv, send_sem, recv_sem, True).wait()

    keys = (ksend, krecv, ks_sem, kr_sem)
    firsts = (xsend, xrecv, xs_sem, xr_sem)
    pl.semaphore_wait(barrier, group + bands - 2)
    spread_start(*keys)
    spread_start(*firsts)
    krecv[me] = ksend[...]
    xrecv[me] = xsend[...]

    def whole(values):
        return jnp.floor(values)

    def signed(values):
        return jnp.where(2.0 * values < grid_len, values, values - grid_len)

    def numbers(cells):
        plane = whole((cells + 0.5) * (1.0 / (grid_len * grid_len)))
        in_plane = cells - plane * (grid_len * grid_len)
        y_num = whole((in_plane + 0.5) * (1.0 / grid_len))
        return plane, y_num, in_plane - y_num * grid_len

    def cell_row(src):
        cell = krecv[src].astype(jnp.float32)
        return jnp.concatenate([cell[k:k + 1] for k in range(tiles)], axis=1)

    def kinetic(plane, y_num, z_num, device):
        f_x = signed(plane * group + device)
        f_y, f_z = signed(y_num), signed(z_num)
        return kin_unit * (f_x * f_x + f_y * f_y + f_z * f_z)

    def marks(numbers_row, count):
        wide_row = jnp.broadcast_to(numbers_row, (16, pw)).astype(jnp.bfloat16)
        row_id = lax.broadcasted_iota(jnp.int32, (16, pw), 0).astype(jnp.float32).astype(jnp.bfloat16)
        one, zero = jnp.ones((16, pw), jnp.bfloat16), jnp.zeros((16, pw), jnp.bfloat16)
        return [jnp.where(row_id + 16.0 * k == wide_row, one, zero) for k in range(count)]

    def build_source(src):
        plane, y_num, z_num = numbers(cell_row(src))
        fold = whole((plane + 0.5) * 0.5)
        group_ref[src] = fold
        for k, piece in enumerate(marks((plane - 2.0 * fold) * 128.0 + z_num, WIDE // 16)):
            hot_ref[src, 16 * k:16 * (k + 1), :] = piece
        wide_fold = jnp.broadcast_to(fold, (16, pw)).astype(jnp.bfloat16)
        one, zero = jnp.ones((16, pw), jnp.bfloat16), jnp.zeros((16, pw), jnp.bfloat16)
        for k in range(folds):
            mask_ref[src, k] = jnp.where(wide_fold == float(k), one, zero)
        y_hot = marks(y_num, grid_len // 16)
        table = bdot(wave_ref[...], jnp.concatenate(y_hot + y_hot, axis=0))
        ta_ref[src] = table[:slab]
        tb_ref[src] = table[slab:]

    def build_potential():
        pad = jnp.zeros((8, 128 - grid_len), jnp.float32)

        def put_tile(v, slot, block):
            pot_ref[v, slot] = jnp.concatenate([block * (1.0 / grid_len**3), pad], axis=1)

        def lines(x_real, first, count):
            return potential_ref[pl.ds(first * grid_len + x_real, count, stride=grid_len), :]

        for v in range(planes):
            for u in range(group):
                put_tile(v, u, lines(v + planes * u, 0, 8))
            for t in range(half):
                put_tile(v, group + t, jnp.concatenate([
                    lines(v + planes * 2 * t, 8, planes - 8), lines(v + planes * (2 * t + 1), 8, planes - 8)], axis=0))

    def build_coupling():
        atoms, chans = strength_ref.shape[0] // strength_ref.shape[1], strength_ref.shape[1]
        size = atoms * chans
        ident = atom_ref[...] * chans + chan_ref[...]
        hot = (lax.broadcasted_iota(jnp.int32, (size, ident.shape[1]), 0) == ident).astype(jnp.float32)
        row_at = lax.broadcasted_iota(jnp.int32, (size, size), 0)
        col_at = lax.broadcasted_iota(jnp.int32, (size, size), 1)
        tiled = jnp.concatenate([strength_ref[...]] * atoms, axis=1)
        same = (row_at // chans == col_at // chans).astype(jnp.float32)
        block = tiled * same
        block = 0.5 * (block + jnp.transpose(block))
        half = lax.dot_general(hot, block, (((0,), (0,)), ((), ())), precision=top_precision, preferred_element_type=jnp.float32)
        couple_ref[...] = jnp.dot(half, hot, precision=top_precision, preferred_element_type=jnp.float32)

    loads[2].wait()
    build_source(me)
    for load in loads[3:]:
        load.wait()
    build_coupling()
    build_potential()
    for mask in range(1, group):
        spread_copy(mask, *keys, True).wait()
        build_source(peer_of(mask))

    def stack_rows(pieces):
        return jnp.concatenate(pieces, axis=0)

    cells = stack_rows([cell_row(s) for s in range(group)])
    owner = lax.broadcasted_iota(jnp.int32, (group, pw), 0).astype(jnp.float32)
    kin_ref[...] = kinetic(*numbers(cells), owner)
    spread_wait(*firsts)
    for part in range(2):
        in_vec[0, part] = stack_rows([xrecv[s, part] for s in range(group)])

    upper = lax.broadcasted_iota(jnp.int32, (8, 128), 0) < 4
    flip = jnp.where(upper, 1.0, -1.0).astype(jnp.float32)

    def swap_half(values):
        return pltpu.roll(values, 4, 0)

    def halves(low, high):
        return low if low == high else jnp.where(upper, low, high)

    def lane_turn(s, v, paired):
        angle = [2.0 * np.pi * ((k * v) % grid_len) / grid_len for k in (s, s + half)]
        cos_val, sin_val = [float(np.cos(a)) for a in angle], [float(np.sin(a)) for a in angle]
        if paired:
            return halves(*cos_val), halves(*sin_val)
        return cos_val[0], sin_val[0]

    def twist(item, s, v, paired, direction):
        if v == 0 or (s == 0 and not paired):
            return item
        cos_val, sin_val = lane_turn(s, v, paired)
        return c_mul(item, cos_val, sin_val if direction > 0 else -sin_val)

    def z_turn(tiles, which):
        stacked = jnp.concatenate([jnp.concatenate(list(t), axis=1) for t in tiles], axis=0)
        high, low = two_parts(stacked)
        out = bdot(high, zed_ref[which]) + bdot(low, zed_ref[which]) + bdot(high, zed_ref[which + 1])
        return [(out[8 * k:8 * k + 8, :128], out[8 * k:8 * k + 8, 128:]) for k in range(len(tiles))]

    def keep(slot, v, item):
        work_ref[0, v, slot] = item[0]
        work_ref[1, v, slot] = item[1]

    def kept(slot, v):
        return work_ref[0, v, slot], work_ref[1, v, slot]

    def own_row(ref, turn, part):
        return ref[turn, part, pl.ds(me, 1), :]

    def put(turn, src):
        v_re, v_im = in_vec[turn, 0, src:src + 1, :], in_vec[turn, 1, src:src + 1, :]
        both = split_rows(ta_ref[src] * v_re + tb_ref[src] * v_im)
        pieces = []
        for k in range(folds):
            for at in range(0, 2 * slab, 16):
                pieces.append(both[at:at + 16] * mask_ref[src, k])
        out = bdot_t(jnp.concatenate(pieces, axis=0), hot_ref[src])
        tiles = []
        for k in range(folds):
            base = k * 2 * slab
            block = out[base:base + slab] + out[base + slab:base + 2 * slab]
            for at in (0, 128):
                tiles.append([block[8 * t:8 * t + 8, at:at + 128] for t in range(3)])
        return tiles

    def forward_pair(turn, s):
        low, high = put(turn, s), put(turn, s + half)
        rest = [(
            jnp.where(upper, a[1], swap_half(b[1])), jnp.where(upper, swap_half(a[1]), b[1]),
        ) for a, b in zip(low, high)]
        turned = z_turn([(a[0], a[2]) for a in low] + [(b[0], b[2]) for b in high] + rest, 0)
        for k, (slot, first, paired) in enumerate(((s, s, False), (s + half, s + half, False), (group + s, s, True))):
            for v, item in enumerate(twelve_point(turned[k * planes:(k + 1) * planes], 1)):
                keep(slot, v, twist(item, first, v, paired, 1))

    def cross(item):
        return tuple(swap_half(x) + x * flip for x in item)

    def half_turn(item, s, direction):
        if s == 0:
            return item
        angle = 2.0 * np.pi * s / group
        return c_mul(item, halves(1.0, float(np.cos(angle))), direction * halves(0.0, float(np.sin(angle))))

    def middle(v):
        items = eight_point([kept(s, v) for s in range(group)], 1)
        items = [c_scale(item, pot_ref[v, u]) for u, item in enumerate(items)]
        for s, item in enumerate(eight_point(items, -1)):
            keep(s, v, twist(item, s, v, False, -1))
        items = four_point([half_turn(cross(kept(group + s, v)), s, 1) for s in range(half)], 1)
        items = [c_scale(item, pot_ref[v, group + t]) for t, item in enumerate(items)]
        for s, item in enumerate(four_point(items, -1)):
            keep(group + s, v, twist(cross(half_turn(item, s, -1)), s, v, True, -1))

    def backward_pair(s):
        spread = []
        for slot in (s, s + half, group + s):
            spread += twelve_point([kept(slot, v) for v in range(planes)], -1)
        turned = z_turn(spread, 2)
        low, high, rest = [turned[k * planes:(k + 1) * planes] for k in range(3)]
        low = [(a[0], jnp.where(upper, r[0], swap_half(r[1])), a[1]) for a, r in zip(low, rest)]
        high = [(b[0], jnp.where(upper, swap_half(r[0]), r[1]), b[1]) for b, r in zip(high, rest)]
        for dest, tiles in ((s, low), (s + half, high)):
            for k in range(folds):
                block = jnp.concatenate([jnp.concatenate(tiles[2 * k + m], axis=0) for m in range(2)], axis=1)
                left_ref[dest, k * 2 * slab:(k + 1) * 2 * slab, :] = split_rows(block)

    def partial_copy(turn, mask):
        return pltpu.make_async_remote_copy(
            src_ref=rsend.at[turn, mask], dst_ref=rrecv.at[turn, mask],
            send_sem=rs_sem.at[turn, mask - 1], recv_sem=rr_sem.at[turn, mask - 1],
            device_id={"ga": peer_of(mask)}, device_id_type=MESH)

    def take_tile(mask, at):
        return bdot(left_ref[peer_of(mask)], hot_ref[peer_of(mask), :, at:at + WIDE])

    def take_sum(turn, mask, at, out):
        dest = peer_of(mask)
        span = slice(at, at + WIDE)
        fold = group_ref[dest, :, span]
        chosen = out[:2 * slab]
        for k in range(1, folds):
            chosen = jnp.where(fold == float(k), out[k * 2 * slab:(k + 1) * 2 * slab], chosen)
        value = chosen[:slab] + chosen[slab:]
        for part, table in enumerate((ta_ref, tb_ref)):
            rsend[turn, mask, part:part + 1, span] = jnp.sum(table[dest, :, span] * value, axis=0, keepdims=True)

    def take_all(turn):
        order = ((6, 7), (2, 3), (4, 5), (1, 0))
        units = [(masks, mask, at) for masks in order for mask in masks for at in range(0, pw, WIDE)]
        lag = 3
        pending = []
        for unit in units + [None] * lag:
            if unit:
                pending.append((unit, take_tile(*unit[1:])))
            if len(pending) > lag or not unit:
                (masks, mask, at), out = pending.pop(0)
                take_sum(turn, mask, at, out)
                if mask == masks[-1] and at + WIDE == pw:
                    for ready in masks:
                        if ready:
                            partial_copy(turn, ready).start()

    def sum_copy(off, send, recv, send_sem, recv_sem, incoming):
        source = lax.rem(me + group - off, group) if incoming else me
        return pltpu.make_async_remote_copy(
            src_ref=send, dst_ref=recv.at[source],
            send_sem=send_sem.at[off - 1], recv_sem=recv_sem.at[off - 1],
            device_id={"ga": lax.rem(me + off, group)}, device_id_type=MESH)

    def all_sum(local, send, recv, send_sem, recv_sem):
        send[...] = local
        recv[me] = local
        for off in range(1, group):
            sum_copy(off, send, recv, send_sem, recv_sem, False).start()

    def all_sum_end(send, recv, send_sem, recv_sem):
        for off in range(1, group):
            sum_copy(off, send, recv, send_sem, recv_sem, True).wait()
        running = recv[0]
        for dev in range(1, group):
            running = running + recv[dev]
        return running

    def project(turn):
        found = []
        for part in range(2):
            row = own_row(in_vec, turn, part)
            running = proj_ref[:, :128] * row[:, :128]
            for at in range(128, pw, 128):
                running = running + proj_ref[:, at:at + 128] * row[:, at:at + 128]
            found.append(jnp.sum(jnp.transpose(running), axis=0, keepdims=True))
        return jnp.concatenate(found, axis=0)

    def nonlocal_rows(sums):
        half = sums.shape[1] // 2
        pair = jnp.concatenate([
            sums[0:1, :half] + sums[1:2, half:], sums[1:2, :half] - sums[0:1, half:]], axis=0)
        mixed = jnp.dot(pair, couple_ref[...], precision=top_precision, preferred_element_type=jnp.float32)
        m_re, m_im = mixed[0:1], mixed[1:2]
        found = []
        for row in (jnp.concatenate([m_re, -m_im], axis=1), jnp.concatenate([m_im, m_re], axis=1)):
            column = jnp.transpose(jnp.broadcast_to(row, (2 * half, 128)))
            found.append(jnp.concatenate([
                jnp.sum(proj_ref[:, at:at + 128] * column, axis=0, keepdims=True) for at in range(0, pw, 128)], axis=1))
        return jnp.concatenate(found, axis=0)

    def apply_h(turn):
        sums = (psend.at[turn], precv.at[turn], ps_sem.at[turn], pr_sem.at[turn])
        all_sum(project(turn), *sums)
        for s in range(half):
            forward_pair(turn, s)
        for v in range(planes):
            middle(v)
        for s in range(half):
            backward_pair(s)
        take_all(turn)
        start = nonlocal_rows(all_sum_end(*sums) * (1.0 / total_pw))
        own_kin = kin_ref[pl.ds(me, 1), :]
        start = start + own_kin * jnp.concatenate([own_row(in_vec, turn, 0), own_row(in_vec, turn, 1)], axis=0)
        running = start + rsend[turn, 0]
        for mask in range(1, group):
            partial_copy(turn, mask).wait()
            running = running + rrecv[turn, mask]
        hsend[turn] = running
        return running

    def share_h(turn):
        out = (hsend.at[turn], hrecv.at[turn], hs_sem.at[turn], hr_sem.at[turn])
        spread_start(*out)
        hrecv[turn, me] = hsend[turn]
        spread_wait(*out)
        for part in range(2):
            out_vec[turn, part] = stack_rows([hrecv[turn, s, part:part + 1] for s in range(group)])

    def vector(index):
        ref = out_vec if index % 2 else in_vec
        return ref[index // 2]

    def gram_sums(pair_list):
        found = {}
        for one, two, use_kin in pair_list:
            left, right = vector(one), vector(two)
            product = left[0] * right[0] + left[1] * right[1]
            value = total_of(product * kin_ref[...] if use_kin else product) * (1.0 / total_pw)
            found[use_kin, one, two] = value
            found[use_kin, two, one] = value
        return found

    def realize(coef_map, basis):
        running = 0.0
        for index, coef in coef_map.items():
            running = running + (basis(index) if isinstance(coef, float) and coef == 1.0 else coef * basis(index))
        return running

    def smooth(residual, level):
        kin = kin_ref[...]
        ratio = kin / (1.5 * level + 1.0)
        poly = 27.0 + ratio * (18.0 + ratio * (12.0 + 8.0 * ratio))
        square = ratio * ratio
        return residual * (poly / (poly + 16.0 * square * square))

    def save(names, slot):
        for k, value in enumerate(names):
            save_ref[slot + k:slot + k + 1, :] = jnp.broadcast_to(value, (1, 128))

    def load_saved(slot):
        return save_ref[slot:slot + 1, 0:1]

    def first_step(gram):
        psi, ham = {0: 1.0}, {1: 1.0}
        eps_zero = gram_form(gram, psi, ham, False) / (gram_form(gram, psi, psi, False) + small_eps)
        return psi, ham, eps_zero, combine([(1.0, ham), (-eps_zero, psi)])

    def second_step(gram):
        psi, ham, eps_zero, r_map = first_step(gram)
        q_map = combine([(1.0, {3: 1.0}), (-eps_zero, {2: 1.0})])
        lam_zero = -gram_form(gram, r_map, q_map, False) / (gram_form(gram, q_map, q_map, False) + small_eps)
        psi_one = combine([(1.0, psi), (lam_zero, {2: 1.0})])
        h_one = combine([(1.0, ham), (lam_zero, {3: 1.0})])
        eps_one = gram_form(gram, psi_one, h_one, False) / (gram_form(gram, psi_one, psi_one, False) + small_eps)
        r_one = combine([(1.0, h_one), (-eps_one, psi_one)])
        change = combine([(1.0, r_map), (-1.0, r_one)])
        weight = gram_form(gram, r_map, change, False) / (gram_form(gram, change, change, False) + small_eps)
        step = weight * lam_zero
        psi_mid = combine([(1.0, psi), (step, {2: 1.0})])
        h_mid = combine([(1.0, ham), (step, {3: 1.0})])
        r_mid = combine([(1.0, r_map), (-weight, change)])
        eps_mid = gram_form(gram, psi_mid, h_mid, False) / (gram_form(gram, psi_mid, psi_mid, False) + small_eps)
        return psi_mid, h_mid, r_mid, eps_mid, step

    first_pairs = new_pairs(0, 2, (False, True))
    second_pairs = new_pairs(2, 4, (False, True))
    gram_pairs = first_pairs + second_pairs

    def swap(which, send, recv, off, incoming):
        source = lax.rem(band + bands - off, bands) if incoming else band
        return pltpu.make_async_remote_copy(
            src_ref=send, dst_ref=recv.at[source],
            send_sem=ns_sem.at[which, off - 1], recv_sem=nr_sem.at[which, off - 1],
            device_id={"band": lax.rem(band + off, bands)}, device_id_type=MESH)

    def share(which, send, recv, values):
        send[...] = values
        recv[band] = values
        for off in range(1, bands):
            swap(which, send, recv, off, False).start()

    def share_end(which, send, recv):
        for off in range(1, bands):
            swap(which, send, recv, off, True).wait()

    def own(index):
        ref = out_vec if index % 2 else in_vec
        return jnp.concatenate([own_row(ref, index // 2, 0), own_row(ref, index // 2, 1)], axis=0)

    def turn_step(turn, carry):
        apply_h(turn)

        @pl.when(turn == 0)
        def _():
            share_h(0)
            gram = gram_sums(first_pairs)
            save([gram[kind, one, two] for one, two, kind in first_pairs], 0)
            r_map = first_step(gram)[3]
            level = gram_form(gram, r_map, r_map, True) / (gram_form(gram, r_map, r_map, False) + small_eps)
            p_zero = smooth(realize(r_map, vector), level)
            in_vec[1] = p_zero

        @pl.when(turn == 1)
        def _():
            share_h(1)
            gram = gram_sums(second_pairs)
            save([gram[kind, one, two] for one, two, kind in second_pairs], len(first_pairs))
            for k, (one, two, kind) in enumerate(first_pairs):
                gram[kind, one, two] = gram[kind, two, one] = load_saved(k)
            psi_mid, h_mid, r_mid, eps_mid, step = second_step(gram)
            level = gram_form(gram, r_mid, r_mid, True) / (gram_form(gram, r_mid, r_mid, False) + small_eps)
            p_one = smooth(realize(r_mid, vector), level)
            in_vec[2] = p_one
            share(0, nsend, nrecv, jnp.stack([realize(psi_mid, own), own(4), realize(h_mid, own)]))

        return carry

    lax.fori_loop(0, 3, turn_step, 0)

    g_own = hsend[2]
    share(1, isend, irecv, g_own)
    last_pairs = new_pairs(4, 6, (False,))

    def own_last(index):
        return g_own if index == 5 else own(index)

    lane_id = lax.broadcasted_iota(jnp.int32, (1, 128), 1)
    local = jnp.zeros((1, 128), jnp.float32)
    held = [own_last(index) for index in range(6)]
    for k, (one, two, kind) in enumerate(last_pairs):
        local = jnp.where(lane_id == k, total_of(held[one] * held[two]), local)
    sums = (gsend, grecv, gs_sem, gr_sem)
    all_sum(local, *sums)
    gram = {}
    for k, (one, two, kind) in enumerate(gram_pairs):
        gram[kind, one, two] = gram[kind, two, one] = load_saved(k)
    psi_mid, h_mid, r_mid, eps_mid, step = second_step(gram)
    summed = all_sum_end(*sums) * (1.0 / total_pw)
    for k, (one, two, kind) in enumerate(last_pairs):
        gram[kind, one, two] = gram[kind, two, one] = summed[:, k:k + 1]
    q_one = combine([(1.0, {5: 1.0}), (-eps_mid, {4: 1.0})])
    lam_one = -gram_form(gram, r_mid, q_one, False) / (gram_form(gram, q_one, q_one, False) + small_eps)
    share(2, lsend, lrecv, jnp.broadcast_to(lam_one, (1, 128)))
    share_end(0, nsend, nrecv)
    share_end(1, isend, irecv)

    pairs = [
        [stack_rows([nrecv[o, 0, part:part + 1] for o in range(bands)] + [nrecv[o, 1, part:part + 1] for o in range(bands)]) for part in range(2)],
        [stack_rows([nrecv[o, 2, part:part + 1] for o in range(bands)] + [irecv[o, part:part + 1] for o in range(bands)]) for part in range(2)],
    ]
    column_id = lax.broadcasted_iota(jnp.int32, (2 * bands, 128), 1)
    local = jnp.zeros((2 * bands, 128), jnp.float32)
    slot = 0
    for o_re, o_im in pairs:
        for mine in (0, 1):
            m_re, m_im = nsend[mine, 0:1], nsend[mine, 1:2]
            for product in (m_re * o_re + m_im * o_im, m_re * o_im - m_im * o_re):
                local = jnp.where(column_id == slot, jnp.sum(product, axis=1, keepdims=True), local)
                slot += 1
    crossed = (csend, crecv, cs_sem, cr_sem)
    all_sum(local, *crossed)

    new_map = combine([(1.0, psi_mid), (lam_one, {4: 1.0})])
    ham_new = combine([(1.0, h_mid), (lam_one, {5: 1.0})])
    norm_new = gram_form(gram, new_map, new_map, False) + small_eps
    energy = gram_form(gram, new_map, ham_new, False) / norm_new
    resid = combine([(1.0, ham_new), (-energy, new_map)])
    resid_norm = gram_form(gram, resid, resid, False) / norm_new
    new_ref[...] = nsend[0] + lam_one * nsend[1]
    stores = [pltpu.make_async_copy(new_ref, new_hbm, in_sem.at[0]), pltpu.make_async_copy(scal_ref, scal_hbm, in_sem.at[1])]
    stores[0].start()
    share_end(2, lsend, lrecv)
    summed = all_sum_end(*crossed) * (1.0 / total_pw)
    lam_rows = stack_rows([lrecv[o] for o in range(bands)])
    mixed = summed[:bands] + lam_rows * summed[bands:]
    result = mixed + lam_one * pltpu.roll(mixed, 126, 1)
    scal_ref[...] = jnp.concatenate([
        result, jnp.broadcast_to(energy, (1, 128)), jnp.broadcast_to(resid_norm, (1, 128)),
        jnp.zeros((scal_ref.shape[0] - bands - 2, 128), jnp.float32)], axis=0)
    stores[1].start()
    for store in stores:
        store.wait()


def finish_kernel(bands, new_ref, scal_ref, bands_ref, energy_ref, norm_ref, corr_ref, sub_ref):
    bands_ref[:, 0, :] = new_ref[...]
    lane = lax.broadcasted_iota(jnp.int32, (1, bands), 1)
    for ref, base in ((corr_ref, 0), (sub_ref, 4)):
        for part in range(2):
            row = jnp.zeros((1, bands), jnp.float32)
            for other in range(bands):
                at = base + part
                row = jnp.where(lane == other, scal_ref[other:other + 1, at:at + 1], row)
            ref[part] = row
    energy_ref[0] = scal_ref[bands, 0]
    norm_ref[0] = scal_ref[bands + 1, 0]


def kernel_body(coeffs, cell_map, potential, projectors, strengths, proj_atom, proj_chan):
    group = lax.axis_size("ga")
    bands = lax.axis_size("band")
    grid_len = potential.shape[0]
    planes = grid_len // group
    pw = coeffs.shape[2]
    total_pw = pw * group
    slab = 2 * planes
    folds = planes // 2
    tile_count = group + group // 2
    proj_rows = 2 * projectors.shape[1]
    tables = [jnp.asarray(t) for t in const_tables(grid_len, group)]
    dma = pltpu.SemaphoreType.DMA
    vmem = pl.BlockSpec(memory_space=pltpu.VMEM)
    far = pl.BlockSpec(memory_space=pl.ANY)
    f32, b16 = jnp.float32, jnp.bfloat16
    scal_rows = 8 * (-(-(bands + 2) // 8))
    peers = group - 1
    new, scal = pl.pallas_call(
        functools.partial(sweep_kernel, (group, bands, planes, grid_len, total_pw, pw)),
        out_shape=(
            jax.ShapeDtypeStruct((2, pw), f32),
            jax.ShapeDtypeStruct((scal_rows, 128), f32),
        ),
        in_specs=[far] * 9,
        out_specs=(far, far),
        scratch_shapes=[
            pltpu.VMEM((group, WIDE, pw), b16),
            pltpu.VMEM((group, folds, 16, pw), b16),
            pltpu.VMEM((group, 1, pw), f32),
            pltpu.VMEM((group, slab, pw), f32),
            pltpu.VMEM((group, slab, pw), f32),
            pltpu.VMEM((group, pw), f32),
            pltpu.VMEM((2, planes, tile_count, 8, 128), f32),
            pltpu.VMEM((group, folds * 2 * slab, WIDE), b16),
            pltpu.VMEM((planes, tile_count, 8, 128), f32),
            pltpu.VMEM((planes * grid_len, grid_len), f32),
            pltpu.VMEM((proj_rows, pw), f32),
            pltpu.VMEM((proj_rows // 2, proj_rows // 2), f32),
            pltpu.VMEM((3, 2, group, pw), f32),
            pltpu.VMEM((2, 2, group, pw), f32),
            pltpu.VMEM((24, 128), f32),
            pltpu.VMEM((strengths.shape[0] * strengths.shape[1], strengths.shape[2]), f32),
            pltpu.VMEM((1, proj_atom.shape[0]), jnp.int32), pltpu.VMEM((1, proj_chan.shape[0]), jnp.int32),
            pltpu.VMEM(tables[0].shape[1:], b16), pltpu.VMEM(tables[1].shape, b16),
            pltpu.VMEM((2, pw), f32), pltpu.VMEM((scal_rows, 128), f32),
            dma((9,)),
            pltpu.VMEM((pw // 128, 128), jnp.int32), pltpu.VMEM((group, pw // 128, 128), jnp.int32),
            pltpu.VMEM((2, 1, pw), f32), pltpu.VMEM((group, 2, 1, pw), f32),
            pltpu.VMEM((3, group, 2, pw), f32), pltpu.VMEM((3, group, 2, pw), f32),
            pltpu.VMEM((3, 2, pw), f32), pltpu.VMEM((2, group, 2, pw), f32),
            pltpu.VMEM((3, 2, proj_rows), f32), pltpu.VMEM((3, group, 2, proj_rows), f32),
            pltpu.VMEM((1, 128), f32), pltpu.VMEM((group, 1, 128), f32),
            pltpu.VMEM((3, 2, pw), f32), pltpu.VMEM((bands, 3, 2, pw), f32),
            pltpu.VMEM((2, pw), f32), pltpu.VMEM((bands, 2, pw), f32),
            pltpu.VMEM((1, 128), f32), pltpu.VMEM((bands, 1, 128), f32),
            pltpu.VMEM((2 * bands, 128), f32), pltpu.VMEM((group, 2 * bands, 128), f32),
            dma((peers,)), dma((peers,)), dma((peers,)), dma((peers,)),
            dma((3, peers)), dma((3, peers)), dma((2, peers)), dma((2, peers)),
            dma((3, peers)), dma((3, peers)), dma((peers,)), dma((peers,)),
            dma((3, bands - 1)), dma((3, bands - 1)), dma((peers,)), dma((peers,)),
        ],
        compiler_params=pltpu.CompilerParams(
            collective_id=0, has_side_effects=True, vmem_limit_bytes=60 * 1024 * 1024
        ),
        name="sweeps",
    )(
        coeffs, cell_map.reshape(-1, 128), jnp.swapaxes(potential, 0, 1).reshape(planes * grid_len, grid_len),
        projectors.reshape(proj_rows, pw), strengths.reshape(-1, strengths.shape[2]),
        proj_atom.reshape(1, -1), proj_chan.reshape(1, -1), *tables,
    )

    smem = pl.BlockSpec(memory_space=pltpu.SMEM)
    return pl.pallas_call(
        functools.partial(finish_kernel, bands),
        out_shape=(
            jax.ShapeDtypeStruct((2, 1, pw), f32),
            jax.ShapeDtypeStruct((1,), f32),
            jax.ShapeDtypeStruct((1,), f32),
            jax.ShapeDtypeStruct((2, 1, bands), f32),
            jax.ShapeDtypeStruct((2, 1, bands), f32),
        ),
        in_specs=[vmem, vmem],
        out_specs=(vmem, smem, smem, vmem, vmem),
        name="finish",
    )(new, scal)


def body(coeffs, cell_map, potential, projectors, strengths, proj_atom, proj_chan):
    group = lax.axis_size("ga")
    grid_len = potential.shape[0]
    planes = grid_len // group
    fits = (
        group == 8
        and planes == 12
        and coeffs.shape[1] == 1
        and coeffs.shape[2] % 256 == 0
        and 2 * projectors.shape[1] == 128
    )
    chosen = kernel_body if fits else plain_body
    return chosen(coeffs, cell_map, potential, projectors, strengths, proj_atom, proj_chan)


def solution(mesh):
    placed = (
        P(None, "band", "ga"),
        P("ga"),
        P(None, "ga", None),
        P(None, None, "ga"),
        P(),
        P(),
        P(),
    )
    return jax.shard_map(
        body,
        mesh=mesh,
        in_specs=placed,
        out_specs=(
            P(None, "band", "ga"),
            P("band"),
            P("band"),
            P(None, "band", None),
            P(None, "band", None),
        ),
        check_vma=False,
    )
```

```python
import functools

import jax
import jax.numpy as jnp
import numpy as np
from jax import lax
from jax.experimental import pallas as pl
from jax.experimental.pallas import tpu as pltpu
from jax.sharding import PartitionSpec as P

top_precision = lax.Precision.HIGHEST
kin_unit = 0.02
small_eps = 1e-06


def signed_freq(index_arr, grid_len):
    return jnp.where(index_arr < grid_len // 2, index_arr, index_arr - grid_len)


def wave_tables(grid_len, row_freq, col_freq, sign_val, factor):
    phase = row_freq[:, None] * col_freq[None, :] % grid_len
    angle = 2.0 * jnp.pi / grid_len * phase.astype(jnp.float32)
    return (jnp.cos(angle) * factor, jnp.sin(angle) * (sign_val * factor))


def block_table(cos_table, sin_table):
    upper = jnp.concatenate([cos_table, sin_table], axis=1)
    lower = jnp.concatenate([-sin_table, cos_table], axis=1)
    return jnp.concatenate([upper, lower], axis=0)


def quarter_turn(grid_vals):
    half_len = grid_vals.shape[-1] // 2
    return jnp.concatenate([-grid_vals[..., half_len:], grid_vals[..., :half_len]], axis=-1)


def mix_dim(grid_vals, cos_table, sin_table, pattern):
    direct = jnp.einsum(pattern, cos_table, grid_vals, precision=top_precision)
    turned = jnp.einsum(pattern, sin_table, quarter_turn(grid_vals), precision=top_precision)
    return direct + turned


def mix_last(grid_vals, table_full):
    row_width = grid_vals.shape[-1]
    product = jnp.dot(
        grid_vals.reshape(-1, row_width),
        table_full,
        precision=top_precision,
        preferred_element_type=jnp.float32,
    )
    return product.reshape(grid_vals.shape)


def band_dot(left_vec, right_vec, weight):
    return jnp.sum(left_vec * right_vec * weight, axis=(0, 2))


def per_band(values):
    return values[None, :, None]


def pair_products(left_vec, right_vec):

    def contract(first_part, second_part):
        return jnp.einsum("bg,cg->bc", first_part, second_part, precision=top_precision)

    real_part = contract(left_vec[0], right_vec[0]) + contract(left_vec[1], right_vec[1])
    imag_part = contract(left_vec[0], right_vec[1]) - contract(left_vec[1], right_vec[0])
    return jnp.stack([real_part, imag_part])


def precondition(residual, kinetic, kin_level):
    x_ratio = kinetic[None, :] / (1.5 * kin_level[:, None] + 1.0)
    numer_poly = 27.0 + x_ratio * (18.0 + x_ratio * (12.0 + 8.0 * x_ratio))
    square = x_ratio * x_ratio
    return residual * (numer_poly / (numer_poly + 16.0 * square * square))[None]


def coupling_matrix(proj_atom, proj_chan, strengths):
    atom_count = strengths.shape[0]
    chan_count = strengths.shape[1]
    symmetric = 0.5 * (strengths + jnp.swapaxes(strengths, 1, 2))
    atom_hot = (proj_atom[:, None] == jnp.arange(atom_count, dtype=jnp.int32)[None, :]).astype(
        jnp.float32
    )
    chan_hot = (proj_chan[:, None] == jnp.arange(chan_count, dtype=jnp.int32)[None, :]).astype(
        jnp.float32
    )
    rows_d = jnp.einsum("pa,pc,acd->pd", atom_hot, chan_hot, symmetric, precision=top_precision)
    same_atom = jnp.dot(
        atom_hot, atom_hot.T, precision=top_precision, preferred_element_type=jnp.float32
    )
    return same_atom * jnp.dot(
        rows_d, chan_hot.T, precision=top_precision, preferred_element_type=jnp.float32
    )


def combine(term_list):
    merged = {}
    for scalar, coef_map in term_list:
        for index_one, coef_a in coef_map.items():
            merged[index_one] = merged.get(index_one, 0.0) + scalar * coef_a
    return merged


def gram_form(gram_table, left_map, right_map, use_kin):
    running = 0.0
    for index_one, coef_a in left_map.items():
        for index_two, coef_b in right_map.items():
            running = running + coef_a * coef_b * gram_table[use_kin, index_one, index_two]
    return running


def new_pairs(first_new, last_new, kinds):
    pair_list = []
    for use_kin in kinds:
        for index_two in range(first_new, last_new):
            for index_one in range(index_two + 1):
                pair_list.append((index_one, index_two, use_kin))
    return pair_list


def plain_body(coeffs, cell_map, potential, projectors, strengths, proj_atom, proj_chan):
    ga_count = lax.axis_size("ga")
    grid_len = potential.shape[0]
    planes = grid_len // ga_count
    band_local = coeffs.shape[1]
    total_pw = coeffs.shape[2] * ga_count
    device = lax.axis_index("ga")
    plane_num = cell_map // (grid_len * grid_len)
    y_index = cell_map // grid_len % grid_len
    z_index = cell_map % grid_len
    freq_x = signed_freq(device + ga_count * plane_num, grid_len)
    freq_y = signed_freq(y_index, grid_len)
    freq_z = signed_freq(z_index, grid_len)
    kinetic = kin_unit * (freq_x * freq_x + freq_y * freq_y + freq_z * freq_z).astype(jnp.float32)
    kin_weight = kinetic[None, None, :]
    slot_re = (plane_num * grid_len + y_index) * (2 * grid_len) + z_index
    slot_im = slot_re + grid_len
    cell_count = planes * grid_len * 2 * grid_len
    natural = jnp.arange(grid_len, dtype=jnp.int32)
    cyclic = natural % planes * ga_count + natural // planes
    cos_fwd, sin_fwd = wave_tables(grid_len, natural, natural, 1.0, 1.0)
    cos_back, sin_back = wave_tables(grid_len, natural, natural, -1.0, 1.0 / grid_len)
    z_forward = block_table(cos_fwd, sin_fwd)
    z_backward = block_table(cos_back, sin_back)
    xcos_fwd, xsin_fwd = wave_tables(grid_len, natural, cyclic, 1.0, 1.0)
    xcos_back, xsin_back = wave_tables(grid_len, cyclic, natural, -1.0, 1.0 / grid_len)
    doubled = jnp.concatenate([potential, potential], axis=-1)
    coupling = coupling_matrix(proj_atom, proj_chan, strengths)

    def real_space(grid_vals):
        grid_vals = mix_dim(grid_vals, xcos_fwd, xsin_fwd, "kj,bjyw->bkyw")
        grid_vals = grid_vals * doubled[None]
        grid_vals = mix_dim(grid_vals, xcos_back, xsin_back, "jk,bkyw->bjyw")
        return lax.all_to_all(grid_vals, "ga", split_axis=1, concat_axis=2, tiled=True)

    def local_part(vectors):
        item_count = vectors.shape[1]
        flat_grid = jnp.zeros((item_count, cell_count), jnp.float32)
        flat_grid = flat_grid.at[:, slot_re].set(vectors[0]).at[:, slot_im].set(vectors[1])
        grid_vals = mix_last(
            flat_grid.reshape(item_count, planes, grid_len, 2 * grid_len), z_forward
        )
        grid_vals = mix_dim(grid_vals, cos_fwd, sin_fwd, "ky,bpyw->bpkw")
        grid_vals = real_space(
            lax.all_to_all(grid_vals, "ga", split_axis=2, concat_axis=1, tiled=True)
        )
        grid_vals = mix_dim(grid_vals, cos_back, sin_back, "ky,bpyw->bpkw")
        flat_grid = mix_last(grid_vals, z_backward).reshape(item_count, cell_count)
        return jnp.stack([flat_grid[:, slot_re], flat_grid[:, slot_im]])

    def contract(first_part, second_part):
        return jnp.einsum("pg,bg->pb", first_part, second_part, precision=top_precision)

    def spread(weights, proj_table):
        return jnp.einsum("pb,pg->bg", weights, proj_table, precision=top_precision)

    def projected_part(vectors):
        proj_re = contract(projectors[0], vectors[0]) + contract(projectors[1], vectors[1])
        proj_im = contract(projectors[0], vectors[1]) - contract(projectors[1], vectors[0])
        proj_re, proj_im = lax.psum((proj_re, proj_im), "ga")
        mixed_re = jnp.dot(
            coupling,
            proj_re / total_pw,
            precision=top_precision,
            preferred_element_type=jnp.float32,
        )
        mixed_im = jnp.dot(
            coupling,
            proj_im / total_pw,
            precision=top_precision,
            preferred_element_type=jnp.float32,
        )
        out_re = spread(mixed_re, projectors[0]) - spread(mixed_im, projectors[1])
        out_im = spread(mixed_re, projectors[1]) + spread(mixed_im, projectors[0])
        return jnp.stack([out_re, out_im])

    def apply_h(vectors):
        return kin_weight * vectors + local_part(vectors) + projected_part(vectors)

    def gram_sums(basis, pair_list):
        stacked = []
        for index_one, index_two, use_kin in pair_list:
            stacked.append(
                band_dot(basis[index_one], basis[index_two], kin_weight if use_kin else 1.0)
            )
        summed = lax.psum(jnp.stack(stacked), "ga") / total_pw
        found = {}
        for slot_num, entry in enumerate(pair_list):
            index_one, index_two, use_kin = entry
            found[use_kin, index_one, index_two] = summed[slot_num]
            found[use_kin, index_two, index_one] = summed[slot_num]
        return found

    def realize(coef_map, basis):
        running = jnp.zeros_like(basis[0])
        for index_one, coef_a in coef_map.items():
            running = (
                running
                + per_band(jnp.zeros((band_local,), jnp.float32) + coef_a) * basis[index_one]
            )
        return running

    h_zero = apply_h(coeffs)
    basis = [coeffs, h_zero]
    gram_table = gram_sums(basis, new_pairs(0, 2, (False, True)))
    psi_map = {0: 1.0}
    ham_map = {1: 1.0}
    eps_zero = gram_form(gram_table, psi_map, ham_map, False) / (
        gram_form(gram_table, psi_map, psi_map, False) + small_eps
    )
    r_map = combine([(1.0, ham_map), (-eps_zero, psi_map)])
    level_zero = gram_form(gram_table, r_map, r_map, True) / (
        gram_form(gram_table, r_map, r_map, False) + small_eps
    )
    p_zero = precondition(realize(r_map, basis), kinetic, level_zero)
    g_zero = apply_h(p_zero)
    basis = [coeffs, h_zero, p_zero, g_zero]
    gram_table.update(gram_sums(basis, new_pairs(2, 4, (False, True))))
    q_map = combine([(1.0, {3: 1.0}), (-eps_zero, {2: 1.0})])
    lam_zero = -gram_form(gram_table, r_map, q_map, False) / (
        gram_form(gram_table, q_map, q_map, False) + small_eps
    )
    psi_one_map = combine([(1.0, psi_map), (lam_zero, {2: 1.0})])
    h_one_map = combine([(1.0, ham_map), (lam_zero, {3: 1.0})])
    eps_one = gram_form(gram_table, psi_one_map, h_one_map, False) / (
        gram_form(gram_table, psi_one_map, psi_one_map, False) + small_eps
    )
    r_one_map = combine([(1.0, h_one_map), (-eps_one, psi_one_map)])
    change_map = combine([(1.0, r_map), (-1.0, r_one_map)])
    weight_one = gram_form(gram_table, r_map, change_map, False) / (
        gram_form(gram_table, change_map, change_map, False) + small_eps
    )
    step_mid = weight_one * lam_zero
    psi_mid_map = combine([(1.0, psi_map), (step_mid, {2: 1.0})])
    h_mid_map = combine([(1.0, ham_map), (step_mid, {3: 1.0})])
    r_mid_map = combine([(1.0, r_map), (-weight_one, change_map)])
    eps_mid = gram_form(gram_table, psi_mid_map, h_mid_map, False) / (
        gram_form(gram_table, psi_mid_map, psi_mid_map, False) + small_eps
    )
    level_mid = gram_form(gram_table, r_mid_map, r_mid_map, True) / (
        gram_form(gram_table, r_mid_map, r_mid_map, False) + small_eps
    )
    p_one = precondition(realize(r_mid_map, basis), kinetic, level_mid)
    g_one = apply_h(p_one)
    basis = [coeffs, h_zero, p_zero, g_zero, p_one, g_one]
    gram_table.update(gram_sums(basis, new_pairs(4, 6, (False,))))
    q_one_map = combine([(1.0, {5: 1.0}), (-eps_mid, {4: 1.0})])
    lam_one = -gram_form(gram_table, r_mid_map, q_one_map, False) / (
        gram_form(gram_table, q_one_map, q_one_map, False) + small_eps
    )
    new_map = combine([(1.0, psi_mid_map), (lam_one, {4: 1.0})])
    ham_new_map = combine([(1.0, h_mid_map), (lam_one, {5: 1.0})])
    norm_new = gram_form(gram_table, new_map, new_map, False) + small_eps
    energy = gram_form(gram_table, new_map, ham_new_map, False) / norm_new
    resid_map = combine([(1.0, ham_new_map), (-energy, new_map)])
    residual_norm = gram_form(gram_table, resid_map, resid_map, False) / norm_new
    new_bands = realize(new_map, basis)
    new_ham = realize(ham_new_map, basis)
    blank_rows = jnp.zeros((2, band_local, band_local * lax.axis_size("band")), jnp.float32)
    first_row = jnp.int32(0)
    over_rows = blank_rows
    ham_rows = blank_rows
    piece_bands = lax.all_gather(new_bands, "band", axis=1, tiled=True)
    piece_ham = lax.all_gather(new_ham, "band", axis=1, tiled=True)
    over_rows = lax.dynamic_update_slice_in_dim(
        over_rows, pair_products(new_bands, piece_bands), first_row, 2
    )
    ham_rows = lax.dynamic_update_slice_in_dim(
        ham_rows, pair_products(new_bands, piece_ham), first_row, 2
    )
    over_rows, ham_rows = (over_rows, ham_rows)
    over_rows, ham_rows = lax.psum((over_rows, ham_rows), "ga")
    correlation = over_rows / total_pw
    subspace = ham_rows / total_pw
    return (new_bands, energy, residual_norm, correlation, subspace)


WIDE = 256
MESH = pl.DeviceIdType.MESH


def split_const(values):
    high = np.asarray(values, np.float32).astype(jnp.bfloat16)
    low = (values - high.astype(np.float64)).astype(np.float32).astype(jnp.bfloat16)
    return np.stack([high, low])


def const_tables(grid_len, group):
    planes = grid_len // group
    unit = 2.0 * np.pi / grid_len
    freq = np.arange(grid_len)
    y_real = np.arange(group)[:, None] * planes + np.arange(planes)[None, :]
    phase = unit * ((y_real[..., None] * freq) % grid_len)
    cos_y, sin_y = np.cos(phase), np.sin(phase)
    high, low = split_const(np.concatenate([
        cos_y[:, :8], sin_y[:, :8], cos_y[:, 8:], sin_y[:, 8:], -sin_y[:, 8:], cos_y[:, 8:]], axis=1))
    wave = np.concatenate([high, low], axis=2)
    theta = unit * (np.outer(freq, freq) % grid_len)
    turn = np.zeros((2, 128, 2, 128))
    turn[0, :grid_len, 0, :grid_len] = np.cos(theta)
    turn[0, :grid_len, 1, :grid_len] = np.sin(theta)
    turn[1, :grid_len, 0, :grid_len] = -np.sin(theta)
    turn[1, :grid_len, 1, :grid_len] = np.cos(theta)
    turn = turn.reshape(256, 256)
    zed = np.concatenate([split_const(turn), split_const(turn.T)], axis=0)
    return wave, zed


def two_parts(values):
    high = values.astype(jnp.bfloat16)
    low = (values - high.astype(jnp.float32)).astype(jnp.bfloat16)
    return high, low


def split_rows(values):
    high = values.astype(jnp.bfloat16).astype(jnp.float32)
    return jnp.concatenate([high, values - high], axis=0).astype(jnp.bfloat16)


def bdot(left, right):
    return jnp.dot(left, right, preferred_element_type=jnp.float32)


def bdot_t(left, right):
    return lax.dot_general(left, right, (((1,), (1,)), ((), ())), preferred_element_type=jnp.float32)


def total_of(values):
    return jnp.sum(jnp.sum(values, axis=0, keepdims=True), axis=1, keepdims=True)


def c_add(one, two):
    return one[0] + two[0], one[1] + two[1]


def c_sub(one, two):
    return one[0] - two[0], one[1] - two[1]


def c_turn(one, direction):
    return (-one[1], one[0]) if direction > 0 else (one[1], -one[0])


def c_mul(one, cos_val, sin_val):
    return one[0] * cos_val - one[1] * sin_val, one[0] * sin_val + one[1] * cos_val


def c_scale(one, factor):
    return one[0] * factor, one[1] * factor


def three_point(items, direction):
    total = c_add(items[1], items[2])
    side = c_scale(c_turn(c_sub(items[1], items[2]), direction), 0.8660254037844386)
    base = c_sub(items[0], c_scale(total, 0.5))
    return [c_add(items[0], total), c_add(base, side), c_sub(base, side)]


def four_point(items, direction):
    even, odd = c_add(items[0], items[2]), c_add(items[1], items[3])
    low, high = c_sub(items[0], items[2]), c_turn(c_sub(items[1], items[3]), direction)
    return [c_add(even, odd), c_add(low, high), c_sub(even, odd), c_sub(low, high)]


def eight_point(items, direction):
    even = four_point(items[0::2], direction)
    odd = four_point(items[1::2], direction)
    root = 0.7071067811865476
    turned = [
        odd[0],
        c_scale(c_add(odd[1], c_turn(odd[1], direction)), root),
        c_turn(odd[2], direction),
        c_scale(c_sub(c_turn(odd[3], direction), odd[3]), root),
    ]
    return [c_add(e, o) for e, o in zip(even, turned)] + [c_sub(e, o) for e, o in zip(even, turned)]


def twelve_point(items, direction):
    fours = [four_point([items[(4 * a + 3 * b) % 12] for b in range(4)], direction) for a in range(3)]
    threes = [three_point([fours[a][v] for a in range(3)], direction) for v in range(4)]
    return [threes[v % 4][v % 3] for v in range(12)]


def sweep_kernel(
    dims,
    coeffs_hbm, cell_hbm, potential_hbm, proj_hbm, strength_hbm, atom_hbm, chan_hbm,
    wave_hbm, zed_hbm,
    new_hbm, scal_hbm,
    hot_ref, fold_ref, group_ref, phase_ref, kin_ref, work_ref, left_ref,
    pot_ref, potential_ref, proj_ref, couple_ref, in_vec, out_vec, save_ref,
    strength_ref, atom_ref, chan_ref, wave_ref, zed_ref, new_ref, scal_ref, in_sem,
    ksend, krecv, xsend, xrecv, rsend, rrecv, hsend, hrecv, psend, precv,
    gsend, grecv, nsend, nrecv, isend, irecv, lsend, lrecv, csend, crecv,
    ks_sem, kr_sem, xs_sem, xr_sem, rs_sem, rr_sem, hs_sem, hr_sem, ps_sem, pr_sem,
    gs_sem, gr_sem, ns_sem, nr_sem, cs_sem, cr_sem,
):
    group, bands, planes, grid_len, total_pw, pw = dims
    slab = 2 * planes
    folds = planes // 2 - 1
    half = group // 2
    gap = 128 - grid_len
    splits = grid_len // gap
    tiles = pw // 128
    me = lax.axis_index("ga")
    band = lax.axis_index("band")
    sides = [1 - 2 * lax.rem(me // (1 << bit), 2) for bit in range(3)]

    def peer_of(mask):
        return me + sum(sides[bit] * ((mask // (1 << bit)) % 2) * (1 << bit) for bit in range(3))

    loads = [
        pltpu.make_async_copy(source, target, in_sem.at[k])
        for k, (source, target) in enumerate((
            (cell_hbm, ksend), (coeffs_hbm, xsend), (wave_hbm.at[me], wave_ref), (strength_hbm, strength_ref),
            (atom_hbm, atom_ref), (chan_hbm, chan_ref), (potential_hbm, potential_ref), (proj_hbm, proj_ref),
            (zed_hbm, zed_ref)))
    ]
    barrier = pltpu.get_barrier_semaphore()
    for mask in range(1, group):
        pl.semaphore_signal(barrier, inc=1, device_id={"ga": peer_of(mask)}, device_id_type=MESH)
    for off in range(1, bands):
        pl.semaphore_signal(barrier, inc=1, device_id={"band": lax.rem(band + off, bands)}, device_id_type=MESH)
    for load in loads:
        load.start()
    for load in loads[:2]:
        load.wait()

    far_first = (6, 7, 4, 5, 2, 3, 1)
    near_first = (2, 4, 3, 5, 6, 7, 1)

    def spread_copy(mask, send, recv, send_sem, recv_sem, incoming):
        peer = peer_of(mask)
        return pltpu.make_async_remote_copy(
            src_ref=send, dst_ref=recv.at[peer if incoming else me],
            send_sem=send_sem.at[mask - 1], recv_sem=recv_sem.at[mask - 1],
            device_id={"ga": peer}, device_id_type=MESH)

    def spread_start(order, send, recv, send_sem, recv_sem):
        for mask in order:
            spread_copy(mask, send, recv, send_sem, recv_sem, False).start()

    def spread_wait(send, recv, send_sem, recv_sem):
        for mask in range(1, group):
            spread_copy(mask, send, recv, send_sem, recv_sem, True).wait()

    keys = (ksend, krecv, ks_sem, kr_sem)
    firsts = (xsend, xrecv, xs_sem, xr_sem)
    pl.semaphore_wait(barrier, group + bands - 2)
    spread_start(near_first, *keys)
    spread_start(near_first, *firsts)
    krecv[me] = ksend[...]
    xrecv[me] = xsend[...]

    def whole(values):
        return jnp.floor(values)

    def signed(values):
        return jnp.where(2.0 * values < grid_len, values, values - grid_len)

    def numbers(cells):
        plane = whole((cells + 0.5) * (1.0 / (grid_len * grid_len)))
        in_plane = cells - plane * (grid_len * grid_len)
        y_num = whole((in_plane + 0.5) * (1.0 / grid_len))
        return plane, y_num, in_plane - y_num * grid_len

    def cell_row(src):
        cell = krecv[src].astype(jnp.float32)
        return jnp.concatenate([cell[k:k + 1] for k in range(tiles)], axis=1)

    def kinetic(plane, y_num, z_num, device):
        f_x = signed(plane * group + device)
        f_y, f_z = signed(y_num), signed(z_num)
        return kin_unit * (f_x * f_x + f_y * f_y + f_z * f_z)

    def marks(numbers_row, count):
        wide_row = jnp.broadcast_to(numbers_row, (16, pw)).astype(jnp.bfloat16)
        row_id = lax.broadcasted_iota(jnp.int32, (16, pw), 0).astype(jnp.float32).astype(jnp.bfloat16)
        one, zero = jnp.ones((16, pw), jnp.bfloat16), jnp.zeros((16, pw), jnp.bfloat16)
        return [jnp.where(row_id + 16.0 * k == wide_row, one, zero) for k in range(count)]

    def build_source(src):
        plane, y_num, z_num = numbers(cell_row(src))
        pair = whole((plane + 0.5) * 0.5)
        piece = whole((z_num + 0.5) * (1.0 / gap))
        hole = (plane - 2.0 * folds) * splits + piece
        hole_pair = whole((hole + 0.5) * 0.5)
        main = plane < 2.0 * folds
        fold = jnp.where(main, pair, hole_pair)
        lane = jnp.where(
            main, (plane - 2.0 * pair) * 128.0 + z_num,
            (hole - 2.0 * hole_pair) * 128.0 + grid_len + z_num - gap * piece)
        group_ref[src] = fold
        fold_ref[src] = jnp.broadcast_to(fold, (16, pw)).astype(jnp.bfloat16)
        for k, rows in enumerate(marks(lane, WIDE // 16)):
            hot_ref[src, 16 * k:16 * (k + 1), :] = rows
        y_hot = marks(y_num, grid_len // 16)
        phase_ref[src] = bdot(wave_ref[...], jnp.concatenate(y_hot + y_hot, axis=0))

    def build_potential():
        pad = jnp.zeros((8, 128 - grid_len), jnp.float32)

        def put_tile(v, slot, block):
            pot_ref[v, slot] = jnp.concatenate([block * (1.0 / grid_len**3), pad], axis=1)

        def lines(x_real, first, count):
            return potential_ref[pl.ds(first * grid_len + x_real, count, stride=grid_len), :]

        for v in range(planes):
            for u in range(group):
                put_tile(v, u, lines(v + planes * u, 0, 8))
            for t in range(half):
                put_tile(v, group + t, jnp.concatenate([
                    lines(v + planes * 2 * t, 8, planes - 8), lines(v + planes * (2 * t + 1), 8, planes - 8)], axis=0))

    def build_coupling():
        atoms, chans = strength_ref.shape[0] // strength_ref.shape[1], strength_ref.shape[1]
        size = atoms * chans
        ident = atom_ref[...] * chans + chan_ref[...]
        hot = (lax.broadcasted_iota(jnp.int32, (size, ident.shape[1]), 0) == ident).astype(jnp.float32)
        row_at = lax.broadcasted_iota(jnp.int32, (size, size), 0)
        col_at = lax.broadcasted_iota(jnp.int32, (size, size), 1)
        tiled = jnp.concatenate([strength_ref[...]] * atoms, axis=1)
        same = (row_at // chans == col_at // chans).astype(jnp.float32)
        block = tiled * same
        block = 0.5 * (block + jnp.transpose(block))
        half = lax.dot_general(hot, block, (((0,), (0,)), ((), ())), precision=top_precision, preferred_element_type=jnp.float32)
        couple_ref[...] = jnp.dot(half, hot, precision=top_precision, preferred_element_type=jnp.float32)

    loads[2].wait()
    build_source(me)
    for load in loads[3:6]:
        load.wait()
    build_coupling()
    loads[6].wait()
    build_potential()
    loads[7].wait()
    loads[8].wait()
    for mask in range(1, group):
        spread_copy(mask, *keys, True).wait()
        build_source(peer_of(mask))

    def stack_rows(pieces):
        return jnp.concatenate(pieces, axis=0)

    cells = stack_rows([cell_row(s) for s in range(group)])
    owner = lax.broadcasted_iota(jnp.int32, (group, pw), 0).astype(jnp.float32)
    kin_ref[...] = kinetic(*numbers(cells), owner)
    spread_wait(*firsts)
    for part in range(2):
        in_vec[0, part] = stack_rows([xrecv[s, part] for s in range(group)])

    upper = lax.broadcasted_iota(jnp.int32, (8, 128), 0) < 4
    lane_at = lax.broadcasted_iota(jnp.int32, (8, 128), 1)
    flip = jnp.where(upper, 1.0, -1.0).astype(jnp.float32)

    def swap_half(values):
        return pltpu.roll(values, 4, 0)

    def halves(low, high):
        return low if low == high else jnp.where(upper, low, high)

    def lane_turn(s, v, paired):
        angle = [2.0 * np.pi * ((k * v) % grid_len) / grid_len for k in (s, s + half)]
        cos_val, sin_val = [float(np.cos(a)) for a in angle], [float(np.sin(a)) for a in angle]
        if paired:
            return halves(*cos_val), halves(*sin_val)
        return cos_val[0], sin_val[0]

    def twist(item, s, v, paired, direction):
        if v == 0 or (s == 0 and not paired):
            return item
        cos_val, sin_val = lane_turn(s, v, paired)
        return c_mul(item, cos_val, sin_val if direction > 0 else -sin_val)

    def z_turn(tiles, which):
        stacked = jnp.concatenate([jnp.concatenate(list(t), axis=1) for t in tiles], axis=0)
        high, low = two_parts(stacked)
        out = bdot(high, zed_ref[which]) + bdot(low, zed_ref[which]) + bdot(high, zed_ref[which + 1])
        return [(out[8 * k:8 * k + 8, :128], out[8 * k:8 * k + 8, 128:]) for k in range(len(tiles))]

    def keep(slot, v, item):
        work_ref[0, v, slot] = item[0]
        work_ref[1, v, slot] = item[1]

    def kept(slot, v):
        return work_ref[0, v, slot], work_ref[1, v, slot]

    def own_row(ref, turn, part):
        return ref[turn, part, pl.ds(me, 1), :]

    def put(turn, src):
        v_re, v_im = in_vec[turn, 0, src:src + 1, :], in_vec[turn, 1, src:src + 1, :]
        cos_y, sin_y, mix_re, mix_im = [phase_ref[src, 8 * k:8 * k + 8, :] for k in range(4)]
        both = split_rows(jnp.concatenate([
            cos_y * v_re - sin_y * v_im, mix_re * v_re + mix_im * v_im, sin_y * v_re + cos_y * v_im], axis=0))
        pieces = []
        fold = fold_ref[src]
        blank = jnp.zeros((16, pw), jnp.bfloat16)
        for k in range(folds):
            hit = fold == float(k)
            for at in range(0, 2 * slab, 16):
                pieces.append(jnp.where(hit, both[at:at + 16], blank))
        out = bdot_t(jnp.concatenate(pieces, axis=0), hot_ref[src])
        tiles = []
        for k in range(folds):
            base = k * 2 * slab
            block = out[base:base + slab] + out[base + slab:base + 2 * slab]
            for at in (0, 128):
                tiles.append([block[8 * t:8 * t + 8, at:at + 128] for t in range(3)])
        for extra in range(planes - 2 * folds):
            joined = []
            for t in range(3):
                run = None
                for q in reversed(range(splits)):
                    moved = pltpu.roll(tiles[extra * splits + q][t], (q + 1) * gap, 1)
                    run = moved if run is None else jnp.where(lane_at < (q + 1) * gap, moved, run)
                joined.append(run)
            tiles.append(joined)
        return tiles

    def forward_pair(turn, s):
        low, high = put(turn, s), put(turn, s + half)
        rest = [(
            jnp.where(upper, a[1], swap_half(b[1])), jnp.where(upper, swap_half(a[1]), b[1]),
        ) for a, b in zip(low, high)]
        turned = z_turn([(a[0], a[2]) for a in low] + [(b[0], b[2]) for b in high] + rest, 0)
        for k, (slot, first, paired) in enumerate(((s, s, False), (s + half, s + half, False), (group + s, s, True))):
            for v, item in enumerate(twelve_point(turned[k * planes:(k + 1) * planes], 1)):
                keep(slot, v, twist(item, first, v, paired, 1))

    def cross(item):
        return tuple(swap_half(x) + x * flip for x in item)

    def half_turn(item, s, direction):
        if s == 0:
            return item
        angle = 2.0 * np.pi * s / group
        return c_mul(item, halves(1.0, float(np.cos(angle))), direction * halves(0.0, float(np.sin(angle))))

    def middle(v):
        items = eight_point([kept(s, v) for s in range(group)], 1)
        items = [c_scale(item, pot_ref[v, u]) for u, item in enumerate(items)]
        for s, item in enumerate(eight_point(items, -1)):
            keep(s, v, twist(item, s, v, False, -1))
        items = four_point([half_turn(cross(kept(group + s, v)), s, 1) for s in range(half)], 1)
        items = [c_scale(item, pot_ref[v, group + t]) for t, item in enumerate(items)]
        for s, item in enumerate(four_point(items, -1)):
            keep(group + s, v, twist(cross(half_turn(item, s, -1)), s, v, True, -1))

    def backward_pair(s):
        spread = []
        for slot in (s, s + half, group + s):
            spread += twelve_point([kept(slot, v) for v in range(planes)], -1)
        turned = z_turn(spread, 2)
        low, high, rest = [turned[k * planes:(k + 1) * planes] for k in range(3)]
        low = [(a[0], jnp.where(upper, r[0], swap_half(r[1])), a[1]) for a, r in zip(low, rest)]
        high = [(b[0], jnp.where(upper, swap_half(r[0]), r[1]), b[1]) for b, r in zip(high, rest)]
        for dest, tiles in ((s, low), (s + half, high)):
            for hole in range((planes - 2 * folds) * splits):
                extra, q = 2 * folds + hole // splits, hole % splits
                tiles[hole] = tuple(
                    jnp.where(lane_at >= grid_len, pltpu.roll(tiles[extra][t], grid_len - q * gap, 1), tiles[hole][t])
                    for t in range(3))
            for k in range(folds):
                block = jnp.concatenate([jnp.concatenate(tiles[2 * k + m], axis=0) for m in range(2)], axis=1)
                left_ref[dest, k * 2 * slab:(k + 1) * 2 * slab, :] = split_rows(block)

    def partial_copy(turn, mask):
        return pltpu.make_async_remote_copy(
            src_ref=rsend.at[turn, mask], dst_ref=rrecv.at[turn, mask],
            send_sem=rs_sem.at[turn, mask - 1], recv_sem=rr_sem.at[turn, mask - 1],
            device_id={"ga": peer_of(mask)}, device_id_type=MESH)

    def take_tile(mask, at):
        return bdot(left_ref[peer_of(mask)], hot_ref[peer_of(mask), :, at:at + WIDE])

    def take_sum(turn, mask, at, out):
        dest = peer_of(mask)
        span = slice(at, at + WIDE)
        fold = group_ref[dest, :, span]
        chosen = out[:2 * slab]
        for k in range(1, folds):
            chosen = jnp.where(fold == float(k), out[k * 2 * slab:(k + 1) * 2 * slab], chosen)
        value = chosen[:slab] + chosen[slab:]
        first, mixed, last = [value[8 * k:8 * k + 8] for k in range(3)]
        cos_y, sin_y, mix_re, mix_im = [phase_ref[dest, 8 * k:8 * k + 8, span] for k in range(4)]
        back_re = cos_y * first + sin_y * last + mix_re * mixed
        back_im = cos_y * last - sin_y * first + mix_im * mixed
        for part, back in enumerate((back_re, back_im)):
            rsend[turn, mask, part:part + 1, span] = jnp.sum(back, axis=0, keepdims=True)

    def take_all(turn):
        order = ((6, 7), (2, 3), (4, 5), (1, 0))
        units = [(masks, mask, at) for masks in order for mask in masks for at in range(0, pw, WIDE)]
        lag = 3
        pending = []
        for unit in units + [None] * lag:
            if unit:
                pending.append((unit, take_tile(*unit[1:])))
            if len(pending) > lag or not unit:
                (masks, mask, at), out = pending.pop(0)
                take_sum(turn, mask, at, out)
                if mask == masks[-1] and at + WIDE == pw:
                    for ready in masks:
                        if ready:
                            partial_copy(turn, ready).start()

    def sum_copy(off, send, recv, send_sem, recv_sem, incoming):
        source = lax.rem(me + group - off, group) if incoming else me
        return pltpu.make_async_remote_copy(
            src_ref=send, dst_ref=recv.at[source],
            send_sem=send_sem.at[off - 1], recv_sem=recv_sem.at[off - 1],
            device_id={"ga": lax.rem(me + off, group)}, device_id_type=MESH)

    def all_sum(local, send, recv, send_sem, recv_sem):
        send[...] = local
        recv[me] = local
        for off in range(1, group):
            sum_copy(off, send, recv, send_sem, recv_sem, False).start()

    def all_sum_end(send, recv, send_sem, recv_sem):
        for off in range(1, group):
            sum_copy(off, send, recv, send_sem, recv_sem, True).wait()
        running = recv[0]
        for dev in range(1, group):
            running = running + recv[dev]
        return running

    def project(turn):
        found = []
        for part in range(2):
            row = own_row(in_vec, turn, part)
            running = proj_ref[:, :128] * row[:, :128]
            for at in range(128, pw, 128):
                running = running + proj_ref[:, at:at + 128] * row[:, at:at + 128]
            found.append(jnp.sum(jnp.transpose(running), axis=0, keepdims=True))
        return jnp.concatenate(found, axis=0)

    def nonlocal_rows(sums):
        half = sums.shape[1] // 2
        pair = jnp.concatenate([
            sums[0:1, :half] + sums[1:2, half:], sums[1:2, :half] - sums[0:1, half:]], axis=0)
        mixed = jnp.dot(pair, couple_ref[...], precision=top_precision, preferred_element_type=jnp.float32)
        m_re, m_im = mixed[0:1], mixed[1:2]
        found = []
        for row in (jnp.concatenate([m_re, -m_im], axis=1), jnp.concatenate([m_im, m_re], axis=1)):
            column = jnp.transpose(jnp.broadcast_to(row, (2 * half, 128)))
            found.append(jnp.concatenate([
                jnp.sum(proj_ref[:, at:at + 128] * column, axis=0, keepdims=True) for at in range(0, pw, 128)], axis=1))
        return jnp.concatenate(found, axis=0)

    def apply_h(turn):
        sums = (psend.at[turn], precv.at[turn], ps_sem.at[turn], pr_sem.at[turn])
        for s in range(half):
            forward_pair(turn, s)
        for v in range(planes):
            middle(v)
        for s in range(half):
            backward_pair(s)
        all_sum(project(turn), *sums)
        take_all(turn)
        start = nonlocal_rows(all_sum_end(*sums) * (1.0 / total_pw))
        own_kin = kin_ref[pl.ds(me, 1), :]
        start = start + own_kin * jnp.concatenate([own_row(in_vec, turn, 0), own_row(in_vec, turn, 1)], axis=0)
        running = start + rsend[turn, 0]
        for mask in range(1, group):
            partial_copy(turn, mask).wait()
            running = running + rrecv[turn, mask]
        hsend[turn] = running
        return running

    def share_h(turn):
        out = (hsend.at[turn], hrecv.at[turn], hs_sem.at[turn], hr_sem.at[turn])
        spread_start(far_first, *out)
        hrecv[turn, me] = hsend[turn]
        spread_wait(*out)
        for part in range(2):
            out_vec[turn, part] = stack_rows([hrecv[turn, s, part:part + 1] for s in range(group)])

    def vector(index):
        ref = out_vec if index % 2 else in_vec
        return ref[index // 2]

    def gram_sums(pair_list):
        found = {}
        for one, two, use_kin in pair_list:
            left, right = vector(one), vector(two)
            product = left[0] * right[0] + left[1] * right[1]
            value = total_of(product * kin_ref[...] if use_kin else product) * (1.0 / total_pw)
            found[use_kin, one, two] = value
            found[use_kin, two, one] = value
        return found

    def realize(coef_map, basis):
        running = 0.0
        for index, coef in coef_map.items():
            running = running + (basis(index) if isinstance(coef, float) and coef == 1.0 else coef * basis(index))
        return running

    def smooth(residual, level):
        kin = kin_ref[...]
        ratio = kin / (1.5 * level + 1.0)
        poly = 27.0 + ratio * (18.0 + ratio * (12.0 + 8.0 * ratio))
        square = ratio * ratio
        return residual * (poly / (poly + 16.0 * square * square))

    def save(names, slot):
        for k, value in enumerate(names):
            save_ref[slot + k:slot + k + 1, :] = jnp.broadcast_to(value, (1, 128))

    def load_saved(slot):
        return save_ref[slot:slot + 1, 0:1]

    def first_step(gram):
        psi, ham = {0: 1.0}, {1: 1.0}
        eps_zero = gram_form(gram, psi, ham, False) / (gram_form(gram, psi, psi, False) + small_eps)
        return psi, ham, eps_zero, combine([(1.0, ham), (-eps_zero, psi)])

    def second_step(gram):
        psi, ham, eps_zero, r_map = first_step(gram)
        q_map = combine([(1.0, {3: 1.0}), (-eps_zero, {2: 1.0})])
        lam_zero = -gram_form(gram, r_map, q_map, False) / (gram_form(gram, q_map, q_map, False) + small_eps)
        psi_one = combine([(1.0, psi), (lam_zero, {2: 1.0})])
        h_one = combine([(1.0, ham), (lam_zero, {3: 1.0})])
        eps_one = gram_form(gram, psi_one, h_one, False) / (gram_form(gram, psi_one, psi_one, False) + small_eps)
        r_one = combine([(1.0, h_one), (-eps_one, psi_one)])
        change = combine([(1.0, r_map), (-1.0, r_one)])
        weight = gram_form(gram, r_map, change, False) / (gram_form(gram, change, change, False) + small_eps)
        step = weight * lam_zero
        psi_mid = combine([(1.0, psi), (step, {2: 1.0})])
        h_mid = combine([(1.0, ham), (step, {3: 1.0})])
        r_mid = combine([(1.0, r_map), (-weight, change)])
        eps_mid = gram_form(gram, psi_mid, h_mid, False) / (gram_form(gram, psi_mid, psi_mid, False) + small_eps)
        return psi_mid, h_mid, r_mid, eps_mid, step

    first_pairs = new_pairs(0, 2, (False, True))
    second_pairs = new_pairs(2, 4, (False, True))
    gram_pairs = first_pairs + second_pairs

    def swap(which, send, recv, off, incoming):
        source = lax.rem(band + bands - off, bands) if incoming else band
        return pltpu.make_async_remote_copy(
            src_ref=send, dst_ref=recv.at[source],
            send_sem=ns_sem.at[which, off - 1], recv_sem=nr_sem.at[which, off - 1],
            device_id={"band": lax.rem(band + off, bands)}, device_id_type=MESH)

    def share(which, send, recv, values):
        send[...] = values
        recv[band] = values
        for off in range(1, bands):
            swap(which, send, recv, off, False).start()

    def share_end(which, send, recv):
        for off in range(1, bands):
            swap(which, send, recv, off, True).wait()

    def own(index):
        ref = out_vec if index % 2 else in_vec
        return jnp.concatenate([own_row(ref, index // 2, 0), own_row(ref, index // 2, 1)], axis=0)

    def turn_step(turn, carry):
        apply_h(turn)

        @pl.when(turn == 0)
        def _():
            share_h(0)
            gram = gram_sums(first_pairs)
            save([gram[kind, one, two] for one, two, kind in first_pairs], 0)
            r_map = first_step(gram)[3]
            level = gram_form(gram, r_map, r_map, True) / (gram_form(gram, r_map, r_map, False) + small_eps)
            p_zero = smooth(realize(r_map, vector), level)
            in_vec[1] = p_zero

        @pl.when(turn == 1)
        def _():
            share_h(1)
            gram = gram_sums(second_pairs)
            save([gram[kind, one, two] for one, two, kind in second_pairs], len(first_pairs))
            for k, (one, two, kind) in enumerate(first_pairs):
                gram[kind, one, two] = gram[kind, two, one] = load_saved(k)
            psi_mid, h_mid, r_mid, eps_mid, step = second_step(gram)
            level = gram_form(gram, r_mid, r_mid, True) / (gram_form(gram, r_mid, r_mid, False) + small_eps)
            p_one = smooth(realize(r_mid, vector), level)
            in_vec[2] = p_one
            share(0, nsend, nrecv, jnp.stack([realize(psi_mid, own), own(4), realize(h_mid, own)]))

        return carry

    lax.fori_loop(0, 3, turn_step, 0)

    g_own = hsend[2]
    share(1, isend, irecv, g_own)
    last_pairs = new_pairs(4, 6, (False,))

    def own_last(index):
        return g_own if index == 5 else own(index)

    lane_id = lax.broadcasted_iota(jnp.int32, (1, 128), 1)
    local = jnp.zeros((1, 128), jnp.float32)
    held = [own_last(index) for index in range(6)]
    for k, (one, two, kind) in enumerate(last_pairs):
        local = jnp.where(lane_id == k, total_of(held[one] * held[two]), local)
    sums = (gsend, grecv, gs_sem, gr_sem)
    all_sum(local, *sums)
    gram = {}
    for k, (one, two, kind) in enumerate(gram_pairs):
        gram[kind, one, two] = gram[kind, two, one] = load_saved(k)
    psi_mid, h_mid, r_mid, eps_mid, step = second_step(gram)
    summed = all_sum_end(*sums) * (1.0 / total_pw)
    for k, (one, two, kind) in enumerate(last_pairs):
        gram[kind, one, two] = gram[kind, two, one] = summed[:, k:k + 1]
    q_one = combine([(1.0, {5: 1.0}), (-eps_mid, {4: 1.0})])
    lam_one = -gram_form(gram, r_mid, q_one, False) / (gram_form(gram, q_one, q_one, False) + small_eps)
    share(2, lsend, lrecv, jnp.broadcast_to(lam_one, (1, 128)))
    share_end(0, nsend, nrecv)
    share_end(1, isend, irecv)

    pairs = [
        [stack_rows([nrecv[o, 0, part:part + 1] for o in range(bands)] + [nrecv[o, 1, part:part + 1] for o in range(bands)]) for part in range(2)],
        [stack_rows([nrecv[o, 2, part:part + 1] for o in range(bands)] + [irecv[o, part:part + 1] for o in range(bands)]) for part in range(2)],
    ]
    column_id = lax.broadcasted_iota(jnp.int32, (2 * bands, 128), 1)
    local = jnp.zeros((2 * bands, 128), jnp.float32)
    slot = 0
    for o_re, o_im in pairs:
        for mine in (0, 1):
            m_re, m_im = nsend[mine, 0:1], nsend[mine, 1:2]
            for product in (m_re * o_re + m_im * o_im, m_re * o_im - m_im * o_re):
                local = jnp.where(column_id == slot, jnp.sum(product, axis=1, keepdims=True), local)
                slot += 1
    crossed = (csend, crecv, cs_sem, cr_sem)
    all_sum(local, *crossed)

    new_map = combine([(1.0, psi_mid), (lam_one, {4: 1.0})])
    ham_new = combine([(1.0, h_mid), (lam_one, {5: 1.0})])
    norm_new = gram_form(gram, new_map, new_map, False) + small_eps
    energy = gram_form(gram, new_map, ham_new, False) / norm_new
    resid = combine([(1.0, ham_new), (-energy, new_map)])
    resid_norm = gram_form(gram, resid, resid, False) / norm_new
    new_ref[...] = nsend[0] + lam_one * nsend[1]
    stores = [pltpu.make_async_copy(new_ref, new_hbm, in_sem.at[0]), pltpu.make_async_copy(scal_ref, scal_hbm, in_sem.at[1])]
    stores[0].start()
    share_end(2, lsend, lrecv)
    summed = all_sum_end(*crossed) * (1.0 / total_pw)
    lam_rows = stack_rows([lrecv[o] for o in range(bands)])
    mixed = summed[:bands] + lam_rows * summed[bands:]
    result = mixed + lam_one * pltpu.roll(mixed, 126, 1)
    scal_ref[...] = jnp.concatenate([
        result, jnp.broadcast_to(energy, (1, 128)), jnp.broadcast_to(resid_norm, (1, 128)),
        jnp.zeros((scal_ref.shape[0] - bands - 2, 128), jnp.float32)], axis=0)
    stores[1].start()
    for store in stores:
        store.wait()


def finish_kernel(bands, new_ref, scal_ref, bands_ref, energy_ref, norm_ref, corr_ref, sub_ref):
    bands_ref[:, 0, :] = new_ref[...]
    lane = lax.broadcasted_iota(jnp.int32, (1, bands), 1)
    for ref, base in ((corr_ref, 0), (sub_ref, 4)):
        for part in range(2):
            row = jnp.zeros((1, bands), jnp.float32)
            for other in range(bands):
                at = base + part
                row = jnp.where(lane == other, scal_ref[other:other + 1, at:at + 1], row)
            ref[part] = row
    energy_ref[0] = scal_ref[bands, 0]
    norm_ref[0] = scal_ref[bands + 1, 0]


def kernel_body(coeffs, cell_map, potential, projectors, strengths, proj_atom, proj_chan):
    group = lax.axis_size("ga")
    bands = lax.axis_size("band")
    grid_len = potential.shape[0]
    planes = grid_len // group
    pw = coeffs.shape[2]
    total_pw = pw * group
    slab = 2 * planes
    folds = planes // 2 - 1
    tile_count = group + group // 2
    proj_rows = 2 * projectors.shape[1]
    tables = [jnp.asarray(t) for t in const_tables(grid_len, group)]
    dma = pltpu.SemaphoreType.DMA
    vmem = pl.BlockSpec(memory_space=pltpu.VMEM)
    far = pl.BlockSpec(memory_space=pl.ANY)
    f32, b16 = jnp.float32, jnp.bfloat16
    scal_rows = 8 * (-(-(bands + 2) // 8))
    peers = group - 1
    new, scal = pl.pallas_call(
        functools.partial(sweep_kernel, (group, bands, planes, grid_len, total_pw, pw)),
        out_shape=(
            jax.ShapeDtypeStruct((2, pw), f32),
            jax.ShapeDtypeStruct((scal_rows, 128), f32),
        ),
        in_specs=[far] * 9,
        out_specs=(far, far),
        scratch_shapes=[
            pltpu.VMEM((group, WIDE, pw), b16),
            pltpu.VMEM((group, 16, pw), b16),
            pltpu.VMEM((group, 1, pw), f32),
            pltpu.VMEM((group, 32, pw), f32),
            pltpu.VMEM((group, pw), f32),
            pltpu.VMEM((2, planes, tile_count, 8, 128), f32),
            pltpu.VMEM((group, folds * 2 * slab, WIDE), b16),
            pltpu.VMEM((planes, tile_count, 8, 128), f32),
            pltpu.VMEM((planes * grid_len, grid_len), f32),
            pltpu.VMEM((proj_rows, pw), f32),
            pltpu.VMEM((proj_rows // 2, proj_rows // 2), f32),
            pltpu.VMEM((3, 2, group, pw), f32),
            pltpu.VMEM((2, 2, group, pw), f32),
            pltpu.VMEM((24, 128), f32),
            pltpu.VMEM((strengths.shape[0] * strengths.shape[1], strengths.shape[2]), f32),
            pltpu.VMEM((1, proj_atom.shape[0]), jnp.int32), pltpu.VMEM((1, proj_chan.shape[0]), jnp.int32),
            pltpu.VMEM(tables[0].shape[1:], b16), pltpu.VMEM(tables[1].shape, b16),
            pltpu.VMEM((2, pw), f32), pltpu.VMEM((scal_rows, 128), f32),
            dma((9,)),
            pltpu.VMEM((pw // 128, 128), jnp.int32), pltpu.VMEM((group, pw // 128, 128), jnp.int32),
            pltpu.VMEM((2, 1, pw), f32), pltpu.VMEM((group, 2, 1, pw), f32),
            pltpu.VMEM((3, group, 2, pw), f32), pltpu.VMEM((3, group, 2, pw), f32),
            pltpu.VMEM((3, 2, pw), f32), pltpu.VMEM((2, group, 2, pw), f32),
            pltpu.VMEM((3, 2, proj_rows), f32), pltpu.VMEM((3, group, 2, proj_rows), f32),
            pltpu.VMEM((1, 128), f32), pltpu.VMEM((group, 1, 128), f32),
            pltpu.VMEM((3, 2, pw), f32), pltpu.VMEM((bands, 3, 2, pw), f32),
            pltpu.VMEM((2, pw), f32), pltpu.VMEM((bands, 2, pw), f32),
            pltpu.VMEM((1, 128), f32), pltpu.VMEM((bands, 1, 128), f32),
            pltpu.VMEM((2 * bands, 128), f32), pltpu.VMEM((group, 2 * bands, 128), f32),
            dma((peers,)), dma((peers,)), dma((peers,)), dma((peers,)),
            dma((3, peers)), dma((3, peers)), dma((2, peers)), dma((2, peers)),
            dma((3, peers)), dma((3, peers)), dma((peers,)), dma((peers,)),
            dma((3, bands - 1)), dma((3, bands - 1)), dma((peers,)), dma((peers,)),
        ],
        compiler_params=pltpu.CompilerParams(
            collective_id=0, has_side_effects=True, vmem_limit_bytes=60 * 1024 * 1024
        ),
        name="sweeps",
    )(
        coeffs, cell_map.reshape(-1, 128), jnp.swapaxes(potential, 0, 1).reshape(planes * grid_len, grid_len),
        projectors.reshape(proj_rows, pw), strengths.reshape(-1, strengths.shape[2]),
        proj_atom.reshape(1, -1), proj_chan.reshape(1, -1), *tables,
    )

    smem = pl.BlockSpec(memory_space=pltpu.SMEM)
    return pl.pallas_call(
        functools.partial(finish_kernel, bands),
        out_shape=(
            jax.ShapeDtypeStruct((2, 1, pw), f32),
            jax.ShapeDtypeStruct((1,), f32),
            jax.ShapeDtypeStruct((1,), f32),
            jax.ShapeDtypeStruct((2, 1, bands), f32),
            jax.ShapeDtypeStruct((2, 1, bands), f32),
        ),
        in_specs=[vmem, vmem],
        out_specs=(vmem, smem, smem, vmem, vmem),
        name="finish",
    )(new, scal)


def body(coeffs, cell_map, potential, projectors, strengths, proj_atom, proj_chan):
    group = lax.axis_size("ga")
    grid_len = potential.shape[0]
    planes = grid_len // group
    fits = (
        group == 8
        and planes == 12
        and coeffs.shape[1] == 1
        and coeffs.shape[2] % 256 == 0
        and 2 * projectors.shape[1] == 128
    )
    chosen = kernel_body if fits else plain_body
    return chosen(coeffs, cell_map, potential, projectors, strengths, proj_atom, proj_chan)


def solution(mesh):
    placed = (
        P(None, "band", "ga"),
        P("ga"),
        P(None, "ga", None),
        P(None, None, "ga"),
        P(),
        P(),
        P(),
    )
    return jax.shard_map(
        body,
        mesh=mesh,
        in_specs=placed,
        out_specs=(
            P(None, "band", "ga"),
            P("band"),
            P("band"),
            P(None, "band", None),
            P(None, "band", None),
        ),
        check_vma=False,
    )
```

```python
import functools

import jax
import jax.numpy as jnp
import numpy as np
from jax import lax
from jax.experimental import pallas as pl
from jax.experimental.pallas import tpu as pltpu
from jax.sharding import PartitionSpec as P

top_precision = lax.Precision.HIGHEST
kin_unit = 0.02
small_eps = 1e-06


def signed_freq(index_arr, grid_len):
    return jnp.where(index_arr < grid_len // 2, index_arr, index_arr - grid_len)


def wave_tables(grid_len, row_freq, col_freq, sign_val, factor):
    phase = row_freq[:, None] * col_freq[None, :] % grid_len
    angle = 2.0 * jnp.pi / grid_len * phase.astype(jnp.float32)
    return (jnp.cos(angle) * factor, jnp.sin(angle) * (sign_val * factor))


def block_table(cos_table, sin_table):
    upper = jnp.concatenate([cos_table, sin_table], axis=1)
    lower = jnp.concatenate([-sin_table, cos_table], axis=1)
    return jnp.concatenate([upper, lower], axis=0)


def quarter_turn(grid_vals):
    half_len = grid_vals.shape[-1] // 2
    return jnp.concatenate([-grid_vals[..., half_len:], grid_vals[..., :half_len]], axis=-1)


def mix_dim(grid_vals, cos_table, sin_table, pattern):
    direct = jnp.einsum(pattern, cos_table, grid_vals, precision=top_precision)
    turned = jnp.einsum(pattern, sin_table, quarter_turn(grid_vals), precision=top_precision)
    return direct + turned


def mix_last(grid_vals, table_full):
    row_width = grid_vals.shape[-1]
    product = jnp.dot(
        grid_vals.reshape(-1, row_width),
        table_full,
        precision=top_precision,
        preferred_element_type=jnp.float32,
    )
    return product.reshape(grid_vals.shape)


def band_dot(left_vec, right_vec, weight):
    return jnp.sum(left_vec * right_vec * weight, axis=(0, 2))


def per_band(values):
    return values[None, :, None]


def pair_products(left_vec, right_vec):

    def contract(first_part, second_part):
        return jnp.einsum("bg,cg->bc", first_part, second_part, precision=top_precision)

    real_part = contract(left_vec[0], right_vec[0]) + contract(left_vec[1], right_vec[1])
    imag_part = contract(left_vec[0], right_vec[1]) - contract(left_vec[1], right_vec[0])
    return jnp.stack([real_part, imag_part])


def precondition(residual, kinetic, kin_level):
    x_ratio = kinetic[None, :] / (1.5 * kin_level[:, None] + 1.0)
    numer_poly = 27.0 + x_ratio * (18.0 + x_ratio * (12.0 + 8.0 * x_ratio))
    square = x_ratio * x_ratio
    return residual * (numer_poly / (numer_poly + 16.0 * square * square))[None]


def coupling_matrix(proj_atom, proj_chan, strengths):
    atom_count = strengths.shape[0]
    chan_count = strengths.shape[1]
    symmetric = 0.5 * (strengths + jnp.swapaxes(strengths, 1, 2))
    atom_hot = (proj_atom[:, None] == jnp.arange(atom_count, dtype=jnp.int32)[None, :]).astype(
        jnp.float32
    )
    chan_hot = (proj_chan[:, None] == jnp.arange(chan_count, dtype=jnp.int32)[None, :]).astype(
        jnp.float32
    )
    rows_d = jnp.einsum("pa,pc,acd->pd", atom_hot, chan_hot, symmetric, precision=top_precision)
    same_atom = jnp.dot(
        atom_hot, atom_hot.T, precision=top_precision, preferred_element_type=jnp.float32
    )
    return same_atom * jnp.dot(
        rows_d, chan_hot.T, precision=top_precision, preferred_element_type=jnp.float32
    )


def combine(term_list):
    merged = {}
    for scalar, coef_map in term_list:
        for index_one, coef_a in coef_map.items():
            merged[index_one] = merged.get(index_one, 0.0) + scalar * coef_a
    return merged


def gram_form(gram_table, left_map, right_map, use_kin):
    running = 0.0
    for index_one, coef_a in left_map.items():
        for index_two, coef_b in right_map.items():
            running = running + coef_a * coef_b * gram_table[use_kin, index_one, index_two]
    return running


def new_pairs(first_new, last_new, kinds):
    pair_list = []
    for use_kin in kinds:
        for index_two in range(first_new, last_new):
            for index_one in range(index_two + 1):
                pair_list.append((index_one, index_two, use_kin))
    return pair_list


def plain_body(coeffs, cell_map, potential, projectors, strengths, proj_atom, proj_chan):
    ga_count = lax.axis_size("ga")
    grid_len = potential.shape[0]
    planes = grid_len // ga_count
    band_local = coeffs.shape[1]
    total_pw = coeffs.shape[2] * ga_count
    device = lax.axis_index("ga")
    plane_num = cell_map // (grid_len * grid_len)
    y_index = cell_map // grid_len % grid_len
    z_index = cell_map % grid_len
    freq_x = signed_freq(device + ga_count * plane_num, grid_len)
    freq_y = signed_freq(y_index, grid_len)
    freq_z = signed_freq(z_index, grid_len)
    kinetic = kin_unit * (freq_x * freq_x + freq_y * freq_y + freq_z * freq_z).astype(jnp.float32)
    kin_weight = kinetic[None, None, :]
    slot_re = (plane_num * grid_len + y_index) * (2 * grid_len) + z_index
    slot_im = slot_re + grid_len
    cell_count = planes * grid_len * 2 * grid_len
    natural = jnp.arange(grid_len, dtype=jnp.int32)
    cyclic = natural % planes * ga_count + natural // planes
    cos_fwd, sin_fwd = wave_tables(grid_len, natural, natural, 1.0, 1.0)
    cos_back, sin_back = wave_tables(grid_len, natural, natural, -1.0, 1.0 / grid_len)
    z_forward = block_table(cos_fwd, sin_fwd)
    z_backward = block_table(cos_back, sin_back)
    xcos_fwd, xsin_fwd = wave_tables(grid_len, natural, cyclic, 1.0, 1.0)
    xcos_back, xsin_back = wave_tables(grid_len, cyclic, natural, -1.0, 1.0 / grid_len)
    doubled = jnp.concatenate([potential, potential], axis=-1)
    coupling = coupling_matrix(proj_atom, proj_chan, strengths)

    def real_space(grid_vals):
        grid_vals = mix_dim(grid_vals, xcos_fwd, xsin_fwd, "kj,bjyw->bkyw")
        grid_vals = grid_vals * doubled[None]
        grid_vals = mix_dim(grid_vals, xcos_back, xsin_back, "jk,bkyw->bjyw")
        return lax.all_to_all(grid_vals, "ga", split_axis=1, concat_axis=2, tiled=True)

    def local_part(vectors):
        item_count = vectors.shape[1]
        flat_grid = jnp.zeros((item_count, cell_count), jnp.float32)
        flat_grid = flat_grid.at[:, slot_re].set(vectors[0]).at[:, slot_im].set(vectors[1])
        grid_vals = mix_last(
            flat_grid.reshape(item_count, planes, grid_len, 2 * grid_len), z_forward
        )
        grid_vals = mix_dim(grid_vals, cos_fwd, sin_fwd, "ky,bpyw->bpkw")
        grid_vals = real_space(
            lax.all_to_all(grid_vals, "ga", split_axis=2, concat_axis=1, tiled=True)
        )
        grid_vals = mix_dim(grid_vals, cos_back, sin_back, "ky,bpyw->bpkw")
        flat_grid = mix_last(grid_vals, z_backward).reshape(item_count, cell_count)
        return jnp.stack([flat_grid[:, slot_re], flat_grid[:, slot_im]])

    def contract(first_part, second_part):
        return jnp.einsum("pg,bg->pb", first_part, second_part, precision=top_precision)

    def spread(weights, proj_table):
        return jnp.einsum("pb,pg->bg", weights, proj_table, precision=top_precision)

    def projected_part(vectors):
        proj_re = contract(projectors[0], vectors[0]) + contract(projectors[1], vectors[1])
        proj_im = contract(projectors[0], vectors[1]) - contract(projectors[1], vectors[0])
        proj_re, proj_im = lax.psum((proj_re, proj_im), "ga")
        mixed_re = jnp.dot(
            coupling,
            proj_re / total_pw,
            precision=top_precision,
            preferred_element_type=jnp.float32,
        )
        mixed_im = jnp.dot(
            coupling,
            proj_im / total_pw,
            precision=top_precision,
            preferred_element_type=jnp.float32,
        )
        out_re = spread(mixed_re, projectors[0]) - spread(mixed_im, projectors[1])
        out_im = spread(mixed_re, projectors[1]) + spread(mixed_im, projectors[0])
        return jnp.stack([out_re, out_im])

    def apply_h(vectors):
        return kin_weight * vectors + local_part(vectors) + projected_part(vectors)

    def gram_sums(basis, pair_list):
        stacked = []
        for index_one, index_two, use_kin in pair_list:
            stacked.append(
                band_dot(basis[index_one], basis[index_two], kin_weight if use_kin else 1.0)
            )
        summed = lax.psum(jnp.stack(stacked), "ga") / total_pw
        found = {}
        for slot_num, entry in enumerate(pair_list):
            index_one, index_two, use_kin = entry
            found[use_kin, index_one, index_two] = summed[slot_num]
            found[use_kin, index_two, index_one] = summed[slot_num]
        return found

    def realize(coef_map, basis):
        running = jnp.zeros_like(basis[0])
        for index_one, coef_a in coef_map.items():
            running = (
                running
                + per_band(jnp.zeros((band_local,), jnp.float32) + coef_a) * basis[index_one]
            )
        return running

    h_zero = apply_h(coeffs)
    basis = [coeffs, h_zero]
    gram_table = gram_sums(basis, new_pairs(0, 2, (False, True)))
    psi_map = {0: 1.0}
    ham_map = {1: 1.0}
    eps_zero = gram_form(gram_table, psi_map, ham_map, False) / (
        gram_form(gram_table, psi_map, psi_map, False) + small_eps
    )
    r_map = combine([(1.0, ham_map), (-eps_zero, psi_map)])
    level_zero = gram_form(gram_table, r_map, r_map, True) / (
        gram_form(gram_table, r_map, r_map, False) + small_eps
    )
    p_zero = precondition(realize(r_map, basis), kinetic, level_zero)
    g_zero = apply_h(p_zero)
    basis = [coeffs, h_zero, p_zero, g_zero]
    gram_table.update(gram_sums(basis, new_pairs(2, 4, (False, True))))
    q_map = combine([(1.0, {3: 1.0}), (-eps_zero, {2: 1.0})])
    lam_zero = -gram_form(gram_table, r_map, q_map, False) / (
        gram_form(gram_table, q_map, q_map, False) + small_eps
    )
    psi_one_map = combine([(1.0, psi_map), (lam_zero, {2: 1.0})])
    h_one_map = combine([(1.0, ham_map), (lam_zero, {3: 1.0})])
    eps_one = gram_form(gram_table, psi_one_map, h_one_map, False) / (
        gram_form(gram_table, psi_one_map, psi_one_map, False) + small_eps
    )
    r_one_map = combine([(1.0, h_one_map), (-eps_one, psi_one_map)])
    change_map = combine([(1.0, r_map), (-1.0, r_one_map)])
    weight_one = gram_form(gram_table, r_map, change_map, False) / (
        gram_form(gram_table, change_map, change_map, False) + small_eps
    )
    step_mid = weight_one * lam_zero
    psi_mid_map = combine([(1.0, psi_map), (step_mid, {2: 1.0})])
    h_mid_map = combine([(1.0, ham_map), (step_mid, {3: 1.0})])
    r_mid_map = combine([(1.0, r_map), (-weight_one, change_map)])
    eps_mid = gram_form(gram_table, psi_mid_map, h_mid_map, False) / (
        gram_form(gram_table, psi_mid_map, psi_mid_map, False) + small_eps
    )
    level_mid = gram_form(gram_table, r_mid_map, r_mid_map, True) / (
        gram_form(gram_table, r_mid_map, r_mid_map, False) + small_eps
    )
    p_one = precondition(realize(r_mid_map, basis), kinetic, level_mid)
    g_one = apply_h(p_one)
    basis = [coeffs, h_zero, p_zero, g_zero, p_one, g_one]
    gram_table.update(gram_sums(basis, new_pairs(4, 6, (False,))))
    q_one_map = combine([(1.0, {5: 1.0}), (-eps_mid, {4: 1.0})])
    lam_one = -gram_form(gram_table, r_mid_map, q_one_map, False) / (
        gram_form(gram_table, q_one_map, q_one_map, False) + small_eps
    )
    new_map = combine([(1.0, psi_mid_map), (lam_one, {4: 1.0})])
    ham_new_map = combine([(1.0, h_mid_map), (lam_one, {5: 1.0})])
    norm_new = gram_form(gram_table, new_map, new_map, False) + small_eps
    energy = gram_form(gram_table, new_map, ham_new_map, False) / norm_new
    resid_map = combine([(1.0, ham_new_map), (-energy, new_map)])
    residual_norm = gram_form(gram_table, resid_map, resid_map, False) / norm_new
    new_bands = realize(new_map, basis)
    new_ham = realize(ham_new_map, basis)
    blank_rows = jnp.zeros((2, band_local, band_local * lax.axis_size("band")), jnp.float32)
    first_row = jnp.int32(0)
    over_rows = blank_rows
    ham_rows = blank_rows
    piece_bands = lax.all_gather(new_bands, "band", axis=1, tiled=True)
    piece_ham = lax.all_gather(new_ham, "band", axis=1, tiled=True)
    over_rows = lax.dynamic_update_slice_in_dim(
        over_rows, pair_products(new_bands, piece_bands), first_row, 2
    )
    ham_rows = lax.dynamic_update_slice_in_dim(
        ham_rows, pair_products(new_bands, piece_ham), first_row, 2
    )
    over_rows, ham_rows = (over_rows, ham_rows)
    over_rows, ham_rows = lax.psum((over_rows, ham_rows), "ga")
    correlation = over_rows / total_pw
    subspace = ham_rows / total_pw
    return (new_bands, energy, residual_norm, correlation, subspace)


WIDE = 256
MESH = pl.DeviceIdType.MESH


def split_const(values):
    high = np.asarray(values, np.float32).astype(jnp.bfloat16)
    low = (values - high.astype(np.float64)).astype(np.float32).astype(jnp.bfloat16)
    return np.stack([high, low])


def const_tables(grid_len, group):
    planes = grid_len // group
    unit = 2.0 * np.pi / grid_len
    freq = np.arange(grid_len)
    y_real = np.arange(group)[:, None] * planes + np.arange(planes)[None, :]
    phase = unit * ((y_real[..., None] * freq) % grid_len)
    cos_y, sin_y = np.cos(phase), np.sin(phase)
    high, low = split_const(np.concatenate([
        cos_y[:, :8], sin_y[:, :8], cos_y[:, 8:], sin_y[:, 8:], -sin_y[:, 8:], cos_y[:, 8:]], axis=1))
    wave = np.concatenate([high, low], axis=2)
    theta = unit * (np.outer(freq, freq) % grid_len)
    turn = np.zeros((2, 128, 2, 128))
    turn[0, :grid_len, 0, :grid_len] = np.cos(theta)
    turn[0, :grid_len, 1, :grid_len] = np.sin(theta)
    turn[1, :grid_len, 0, :grid_len] = -np.sin(theta)
    turn[1, :grid_len, 1, :grid_len] = np.cos(theta)
    turn = turn.reshape(256, 256)
    zed = np.concatenate([split_const(turn), split_const(turn.T)], axis=0)
    return wave, zed


def two_parts(values):
    high = values.astype(jnp.bfloat16)
    low = (values - high.astype(jnp.float32)).astype(jnp.bfloat16)
    return high, low


def split_rows(values):
    high = values.astype(jnp.bfloat16).astype(jnp.float32)
    return jnp.concatenate([high, values - high], axis=0).astype(jnp.bfloat16)


def bdot(left, right):
    return jnp.dot(left, right, preferred_element_type=jnp.float32)


def bdot_t(left, right):
    return lax.dot_general(left, right, (((1,), (1,)), ((), ())), preferred_element_type=jnp.float32)


def total_of(values):
    return jnp.sum(jnp.sum(values, axis=0, keepdims=True), axis=1, keepdims=True)


def c_add(one, two):
    return one[0] + two[0], one[1] + two[1]


def c_sub(one, two):
    return one[0] - two[0], one[1] - two[1]


def c_turn(one, direction):
    return (-one[1], one[0]) if direction > 0 else (one[1], -one[0])


def c_mul(one, cos_val, sin_val):
    return one[0] * cos_val - one[1] * sin_val, one[0] * sin_val + one[1] * cos_val


def c_scale(one, factor):
    return one[0] * factor, one[1] * factor


def three_point(items, direction):
    total = c_add(items[1], items[2])
    side = c_scale(c_turn(c_sub(items[1], items[2]), direction), 0.8660254037844386)
    base = c_sub(items[0], c_scale(total, 0.5))
    return [c_add(items[0], total), c_add(base, side), c_sub(base, side)]


def four_point(items, direction):
    even, odd = c_add(items[0], items[2]), c_add(items[1], items[3])
    low, high = c_sub(items[0], items[2]), c_turn(c_sub(items[1], items[3]), direction)
    return [c_add(even, odd), c_add(low, high), c_sub(even, odd), c_sub(low, high)]


def eight_point(items, direction):
    even = four_point(items[0::2], direction)
    odd = four_point(items[1::2], direction)
    root = 0.7071067811865476
    turned = [
        odd[0],
        c_scale(c_add(odd[1], c_turn(odd[1], direction)), root),
        c_turn(odd[2], direction),
        c_scale(c_sub(c_turn(odd[3], direction), odd[3]), root),
    ]
    return [c_add(e, o) for e, o in zip(even, turned)] + [c_sub(e, o) for e, o in zip(even, turned)]


def twelve_point(items, direction):
    fours = [four_point([items[(4 * a + 3 * b) % 12] for b in range(4)], direction) for a in range(3)]
    threes = [three_point([fours[a][v] for a in range(3)], direction) for v in range(4)]
    return [threes[v % 4][v % 3] for v in range(12)]


def sweep_kernel(
    dims,
    coeffs_hbm, cell_hbm, potential_hbm, proj_hbm, strength_hbm, atom_hbm, chan_hbm,
    wave_hbm, zed_hbm,
    new_hbm, scal_hbm,
    hot_ref, fold_ref, group_ref, phase_ref, kin_ref, work_ref, left_ref,
    pot_ref, potential_ref, proj_ref, couple_ref, in_vec, out_vec, save_ref,
    strength_ref, atom_ref, chan_ref, wave_ref, zed_ref, new_ref, scal_ref, in_sem,
    ksend, krecv, xsend, xrecv, rsend, rrecv, hsend, hrecv, psend, precv,
    wsend, wrecv, nsend, nrecv, lsend, lrecv, csend, crecv,
    ks_sem, kr_sem, xs_sem, xr_sem, rs_sem, rr_sem, hs_sem, hr_sem, ps_sem, pr_sem,
    ws_sem, wr_sem, ns_sem, nr_sem, cs_sem, cr_sem,
):
    group, bands, planes, grid_len, total_pw, pw = dims
    slab = 2 * planes
    folds = planes // 2 - 1
    half = group // 2
    gap = 128 - grid_len
    splits = grid_len // gap
    tiles = pw // 128
    me = lax.axis_index("ga")
    band = lax.axis_index("band")
    sides = [1 - 2 * lax.rem(me // (1 << bit), 2) for bit in range(3)]

    def peer_of(mask):
        return me + sum(sides[bit] * ((mask // (1 << bit)) % 2) * (1 << bit) for bit in range(3))

    loads = [
        pltpu.make_async_copy(source, target, in_sem.at[k])
        for k, (source, target) in enumerate((
            (cell_hbm, ksend), (coeffs_hbm, xsend), (wave_hbm.at[me], wave_ref), (strength_hbm, strength_ref),
            (atom_hbm, atom_ref), (chan_hbm, chan_ref), (potential_hbm, potential_ref), (proj_hbm, proj_ref),
            (zed_hbm, zed_ref)))
    ]
    barrier = pltpu.get_barrier_semaphore()
    world = [(off, mask) for off in (2, 3, 1, 0) for mask in (7, 6, 5, 4, 3, 2, 1, 0) if off or mask]
    for off, mask in world:
        pl.semaphore_signal(barrier, inc=1, device_id={"band": lax.rem(band + off, bands), "ga": peer_of(mask)}, device_id_type=MESH)
    for load in loads:
        load.start()
    for load in loads[:2]:
        load.wait()

    far_first = (6, 7, 4, 5, 2, 3, 1)
    near_first = (2, 4, 3, 5, 6, 7, 1)

    def spread_copy(mask, send, recv, send_sem, recv_sem, incoming):
        peer = peer_of(mask)
        return pltpu.make_async_remote_copy(
            src_ref=send, dst_ref=recv.at[peer if incoming else me],
            send_sem=send_sem.at[mask - 1], recv_sem=recv_sem.at[mask - 1],
            device_id={"ga": peer}, device_id_type=MESH)

    def spread_start(order, send, recv, send_sem, recv_sem):
        for mask in order:
            spread_copy(mask, send, recv, send_sem, recv_sem, False).start()

    def spread_wait(send, recv, send_sem, recv_sem):
        for mask in range(1, group):
            spread_copy(mask, send, recv, send_sem, recv_sem, True).wait()

    keys = (ksend, krecv, ks_sem, kr_sem)
    firsts = (xsend, xrecv, xs_sem, xr_sem)
    pl.semaphore_wait(barrier, group * bands - 1)
    spread_start(near_first, *keys)
    spread_start(near_first, *firsts)
    krecv[me] = ksend[...]
    xrecv[me] = xsend[...]

    def whole(values):
        return jnp.floor(values)

    def signed(values):
        return jnp.where(2.0 * values < grid_len, values, values - grid_len)

    def numbers(cells):
        plane = whole((cells + 0.5) * (1.0 / (grid_len * grid_len)))
        in_plane = cells - plane * (grid_len * grid_len)
        y_num = whole((in_plane + 0.5) * (1.0 / grid_len))
        return plane, y_num, in_plane - y_num * grid_len

    def cell_row(src):
        cell = krecv[src].astype(jnp.float32)
        return jnp.concatenate([cell[k:k + 1] for k in range(tiles)], axis=1)

    def kinetic(plane, y_num, z_num, device):
        f_x = signed(plane * group + device)
        f_y, f_z = signed(y_num), signed(z_num)
        return kin_unit * (f_x * f_x + f_y * f_y + f_z * f_z)

    def marks(numbers_row, count):
        wide_row = jnp.broadcast_to(numbers_row, (16, pw)).astype(jnp.bfloat16)
        row_id = lax.broadcasted_iota(jnp.int32, (16, pw), 0).astype(jnp.float32).astype(jnp.bfloat16)
        one, zero = jnp.ones((16, pw), jnp.bfloat16), jnp.zeros((16, pw), jnp.bfloat16)
        return [jnp.where(row_id + 16.0 * k == wide_row, one, zero) for k in range(count)]

    def build_source(src):
        plane, y_num, z_num = numbers(cell_row(src))
        pair = whole((plane + 0.5) * 0.5)
        piece = whole((z_num + 0.5) * (1.0 / gap))
        hole = (plane - 2.0 * folds) * splits + piece
        hole_pair = whole((hole + 0.5) * 0.5)
        main = plane < 2.0 * folds
        fold = jnp.where(main, pair, hole_pair)
        lane = jnp.where(
            main, (plane - 2.0 * pair) * 128.0 + z_num,
            (hole - 2.0 * hole_pair) * 128.0 + grid_len + z_num - gap * piece)
        group_ref[src] = fold
        fold_ref[src] = jnp.broadcast_to(fold, (16, pw)).astype(jnp.bfloat16)
        for k, rows in enumerate(marks(lane, WIDE // 16)):
            hot_ref[src, 16 * k:16 * (k + 1), :] = rows
        y_hot = marks(y_num, grid_len // 16)
        phase_ref[src] = bdot(wave_ref[...], jnp.concatenate(y_hot + y_hot, axis=0))

    def build_potential():
        pad = jnp.zeros((8, 128 - grid_len), jnp.float32)

        def put_tile(v, slot, block):
            pot_ref[v, slot] = jnp.concatenate([block * (1.0 / grid_len**3), pad], axis=1)

        def lines(x_real, first, count):
            return potential_ref[pl.ds(first * grid_len + x_real, count, stride=grid_len), :]

        for v in range(planes):
            for u in range(group):
                put_tile(v, u, lines(v + planes * u, 0, 8))
            for t in range(half):
                put_tile(v, group + t, jnp.concatenate([
                    lines(v + planes * 2 * t, 8, planes - 8), lines(v + planes * (2 * t + 1), 8, planes - 8)], axis=0))

    def build_coupling():
        atoms, chans = strength_ref.shape[0] // strength_ref.shape[1], strength_ref.shape[1]
        size = atoms * chans
        ident = atom_ref[...] * chans + chan_ref[...]
        hot = (lax.broadcasted_iota(jnp.int32, (size, ident.shape[1]), 0) == ident).astype(jnp.float32)
        row_at = lax.broadcasted_iota(jnp.int32, (size, size), 0)
        col_at = lax.broadcasted_iota(jnp.int32, (size, size), 1)
        tiled = jnp.concatenate([strength_ref[...]] * atoms, axis=1)
        same = (row_at // chans == col_at // chans).astype(jnp.float32)
        block = tiled * same
        block = 0.5 * (block + jnp.transpose(block))
        half = lax.dot_general(hot, block, (((0,), (0,)), ((), ())), precision=top_precision, preferred_element_type=jnp.float32)
        couple_ref[...] = jnp.dot(half, hot, precision=top_precision, preferred_element_type=jnp.float32)

    loads[2].wait()
    build_source(me)
    for load in loads[3:6]:
        load.wait()
    build_coupling()
    loads[6].wait()
    build_potential()
    loads[7].wait()
    loads[8].wait()
    for mask in range(1, group):
        spread_copy(mask, *keys, True).wait()
        build_source(peer_of(mask))

    def stack_rows(pieces):
        return jnp.concatenate(pieces, axis=0)

    cells = stack_rows([cell_row(s) for s in range(group)])
    owner = lax.broadcasted_iota(jnp.int32, (group, pw), 0).astype(jnp.float32)
    kin_ref[...] = kinetic(*numbers(cells), owner)
    spread_wait(*firsts)
    for part in range(2):
        in_vec[0, part] = stack_rows([xrecv[s, part] for s in range(group)])

    upper = lax.broadcasted_iota(jnp.int32, (8, 128), 0) < 4
    lane_at = lax.broadcasted_iota(jnp.int32, (8, 128), 1)
    flip = jnp.where(upper, 1.0, -1.0).astype(jnp.float32)

    def swap_half(values):
        return pltpu.roll(values, 4, 0)

    def halves(low, high):
        return low if low == high else jnp.where(upper, low, high)

    def lane_turn(s, v, paired):
        angle = [2.0 * np.pi * ((k * v) % grid_len) / grid_len for k in (s, s + half)]
        cos_val, sin_val = [float(np.cos(a)) for a in angle], [float(np.sin(a)) for a in angle]
        if paired:
            return halves(*cos_val), halves(*sin_val)
        return cos_val[0], sin_val[0]

    def twist(item, s, v, paired, direction):
        if v == 0 or (s == 0 and not paired):
            return item
        cos_val, sin_val = lane_turn(s, v, paired)
        return c_mul(item, cos_val, sin_val if direction > 0 else -sin_val)

    def z_turn(tiles, which):
        stacked = jnp.concatenate([jnp.concatenate(list(t), axis=1) for t in tiles], axis=0)
        high, low = two_parts(stacked)
        out = bdot(high, zed_ref[which]) + bdot(low, zed_ref[which]) + bdot(high, zed_ref[which + 1])
        return [(out[8 * k:8 * k + 8, :128], out[8 * k:8 * k + 8, 128:]) for k in range(len(tiles))]

    def keep(slot, v, item):
        work_ref[0, v, slot] = item[0]
        work_ref[1, v, slot] = item[1]

    def kept(slot, v):
        return work_ref[0, v, slot], work_ref[1, v, slot]

    def own_row(ref, turn, part):
        return ref[turn, part, pl.ds(me, 1), :]

    def put(turn, src):
        v_re, v_im = in_vec[turn, 0, src:src + 1, :], in_vec[turn, 1, src:src + 1, :]
        cos_y, sin_y, mix_re, mix_im = [phase_ref[src, 8 * k:8 * k + 8, :] for k in range(4)]
        both = split_rows(jnp.concatenate([
            cos_y * v_re - sin_y * v_im, mix_re * v_re + mix_im * v_im, sin_y * v_re + cos_y * v_im], axis=0))
        pieces = []
        fold = fold_ref[src]
        blank = jnp.zeros((16, pw), jnp.bfloat16)
        for k in range(folds):
            hit = fold == float(k)
            for at in range(0, 2 * slab, 16):
                pieces.append(jnp.where(hit, both[at:at + 16], blank))
        out = bdot_t(jnp.concatenate(pieces, axis=0), hot_ref[src])
        tiles = []
        for k in range(folds):
            base = k * 2 * slab
            block = out[base:base + slab] + out[base + slab:base + 2 * slab]
            for at in (0, 128):
                tiles.append([block[8 * t:8 * t + 8, at:at + 128] for t in range(3)])
        for extra in range(planes - 2 * folds):
            joined = []
            for t in range(3):
                run = None
                for q in reversed(range(splits)):
                    moved = pltpu.roll(tiles[extra * splits + q][t], (q + 1) * gap, 1)
                    run = moved if run is None else jnp.where(lane_at < (q + 1) * gap, moved, run)
                joined.append(run)
            tiles.append(joined)
        return tiles

    def forward_pair(turn, s):
        low, high = put(turn, s), put(turn, s + half)
        rest = [(
            jnp.where(upper, a[1], swap_half(b[1])), jnp.where(upper, swap_half(a[1]), b[1]),
        ) for a, b in zip(low, high)]
        turned = z_turn([(a[0], a[2]) for a in low] + [(b[0], b[2]) for b in high] + rest, 0)
        for k, (slot, first, paired) in enumerate(((s, s, False), (s + half, s + half, False), (group + s, s, True))):
            for v, item in enumerate(twelve_point(turned[k * planes:(k + 1) * planes], 1)):
                keep(slot, v, twist(item, first, v, paired, 1))

    def cross(item):
        return tuple(swap_half(x) + x * flip for x in item)

    def half_turn(item, s, direction):
        if s == 0:
            return item
        angle = 2.0 * np.pi * s / group
        return c_mul(item, halves(1.0, float(np.cos(angle))), direction * halves(0.0, float(np.sin(angle))))

    def middle(v):
        items = eight_point([kept(s, v) for s in range(group)], 1)
        items = [c_scale(item, pot_ref[v, u]) for u, item in enumerate(items)]
        for s, item in enumerate(eight_point(items, -1)):
            keep(s, v, twist(item, s, v, False, -1))
        items = four_point([half_turn(cross(kept(group + s, v)), s, 1) for s in range(half)], 1)
        items = [c_scale(item, pot_ref[v, group + t]) for t, item in enumerate(items)]
        for s, item in enumerate(four_point(items, -1)):
            keep(group + s, v, twist(cross(half_turn(item, s, -1)), s, v, True, -1))

    def backward_pair(s):
        spread = []
        for slot in (s, s + half, group + s):
            spread += twelve_point([kept(slot, v) for v in range(planes)], -1)
        turned = z_turn(spread, 2)
        low, high, rest = [turned[k * planes:(k + 1) * planes] for k in range(3)]
        low = [(a[0], jnp.where(upper, r[0], swap_half(r[1])), a[1]) for a, r in zip(low, rest)]
        high = [(b[0], jnp.where(upper, swap_half(r[0]), r[1]), b[1]) for b, r in zip(high, rest)]
        for dest, tiles in ((s, low), (s + half, high)):
            for hole in range((planes - 2 * folds) * splits):
                extra, q = 2 * folds + hole // splits, hole % splits
                tiles[hole] = tuple(
                    jnp.where(lane_at >= grid_len, pltpu.roll(tiles[extra][t], grid_len - q * gap, 1), tiles[hole][t])
                    for t in range(3))
            for k in range(folds):
                block = jnp.concatenate([jnp.concatenate(tiles[2 * k + m], axis=0) for m in range(2)], axis=1)
                left_ref[dest, k * 2 * slab:(k + 1) * 2 * slab, :] = split_rows(block)

    def partial_copy(turn, mask):
        return pltpu.make_async_remote_copy(
            src_ref=rsend.at[turn, mask], dst_ref=rrecv.at[turn, mask],
            send_sem=rs_sem.at[turn, mask - 1], recv_sem=rr_sem.at[turn, mask - 1],
            device_id={"ga": peer_of(mask)}, device_id_type=MESH)

    def take_tile(mask, at):
        return bdot(left_ref[peer_of(mask)], hot_ref[peer_of(mask), :, at:at + WIDE])

    def take_sum(turn, mask, at, out):
        dest = peer_of(mask)
        span = slice(at, at + WIDE)
        fold = group_ref[dest, :, span]
        chosen = out[:2 * slab]
        for k in range(1, folds):
            chosen = jnp.where(fold == float(k), out[k * 2 * slab:(k + 1) * 2 * slab], chosen)
        value = chosen[:slab] + chosen[slab:]
        first, mixed, last = [value[8 * k:8 * k + 8] for k in range(3)]
        cos_y, sin_y, mix_re, mix_im = [phase_ref[dest, 8 * k:8 * k + 8, span] for k in range(4)]
        back_re = cos_y * first + sin_y * last + mix_re * mixed
        back_im = cos_y * last - sin_y * first + mix_im * mixed
        for part, back in enumerate((back_re, back_im)):
            rsend[turn, mask, part:part + 1, span] = jnp.sum(back, axis=0, keepdims=True)

    def take_all(turn):
        order = ((6, 7), (2, 3), (4, 5), (1, 0))
        units = [(masks, mask, at) for masks in order for mask in masks for at in range(0, pw, WIDE)]
        lag = 3
        pending = []
        for unit in units + [None] * lag:
            if unit:
                pending.append((unit, take_tile(*unit[1:])))
            if len(pending) > lag or not unit:
                (masks, mask, at), out = pending.pop(0)
                take_sum(turn, mask, at, out)
                if mask == masks[-1] and at + WIDE == pw:
                    for ready in masks:
                        if ready:
                            partial_copy(turn, ready).start()

    def sum_copy(off, send, recv, send_sem, recv_sem, incoming):
        source = lax.rem(me + group - off, group) if incoming else me
        return pltpu.make_async_remote_copy(
            src_ref=send, dst_ref=recv.at[source],
            send_sem=send_sem.at[off - 1], recv_sem=recv_sem.at[off - 1],
            device_id={"ga": lax.rem(me + off, group)}, device_id_type=MESH)

    def all_sum(local, send, recv, send_sem, recv_sem):
        send[...] = local
        recv[me] = local
        for off in range(1, group):
            sum_copy(off, send, recv, send_sem, recv_sem, False).start()

    def all_sum_end(send, recv, send_sem, recv_sem):
        for off in range(1, group):
            sum_copy(off, send, recv, send_sem, recv_sem, True).wait()
        running = recv[0]
        for dev in range(1, group):
            running = running + recv[dev]
        return running

    def project(turn):
        found = []
        for part in range(2):
            row = own_row(in_vec, turn, part)
            running = proj_ref[:, :128] * row[:, :128]
            for at in range(128, pw, 128):
                running = running + proj_ref[:, at:at + 128] * row[:, at:at + 128]
            found.append(jnp.sum(jnp.transpose(running), axis=0, keepdims=True))
        return jnp.concatenate(found, axis=0)

    def nonlocal_rows(sums):
        half = sums.shape[1] // 2
        pair = jnp.concatenate([
            sums[0:1, :half] + sums[1:2, half:], sums[1:2, :half] - sums[0:1, half:]], axis=0)
        mixed = jnp.dot(pair, couple_ref[...], precision=top_precision, preferred_element_type=jnp.float32)
        m_re, m_im = mixed[0:1], mixed[1:2]
        found = []
        for row in (jnp.concatenate([m_re, -m_im], axis=1), jnp.concatenate([m_im, m_re], axis=1)):
            column = jnp.transpose(jnp.broadcast_to(row, (2 * half, 128)))
            found.append(jnp.concatenate([
                jnp.sum(proj_ref[:, at:at + 128] * column, axis=0, keepdims=True) for at in range(0, pw, 128)], axis=1))
        return jnp.concatenate(found, axis=0)

    def apply_h(turn):
        sums = (psend.at[turn], precv.at[turn], ps_sem.at[turn], pr_sem.at[turn])
        for s in range(half):
            forward_pair(turn, s)
        for v in range(planes):
            middle(v)
        for s in range(half):
            backward_pair(s)
        all_sum(project(turn), *sums)
        take_all(turn)
        start = nonlocal_rows(all_sum_end(*sums) * (1.0 / total_pw))
        own_kin = kin_ref[pl.ds(me, 1), :]
        start = start + own_kin * jnp.concatenate([own_row(in_vec, turn, 0), own_row(in_vec, turn, 1)], axis=0)
        running = start + rsend[turn, 0]
        for mask in range(1, group):
            partial_copy(turn, mask).wait()
            running = running + rrecv[turn, mask]
        hsend[turn] = running
        return running

    def share_h(turn):
        out = (hsend.at[turn], hrecv.at[turn], hs_sem.at[turn], hr_sem.at[turn])
        spread_start(far_first, *out)
        hrecv[turn, me] = hsend[turn]
        spread_wait(*out)
        for part in range(2):
            out_vec[turn, part] = stack_rows([hrecv[turn, s, part:part + 1] for s in range(group)])

    def vector(index):
        ref = out_vec if index % 2 else in_vec
        return ref[index // 2]

    def gram_sums(pair_list):
        found = {}
        for one, two, use_kin in pair_list:
            left, right = vector(one), vector(two)
            product = left[0] * right[0] + left[1] * right[1]
            value = total_of(product * kin_ref[...] if use_kin else product) * (1.0 / total_pw)
            found[use_kin, one, two] = value
            found[use_kin, two, one] = value
        return found

    def realize(coef_map, basis):
        running = 0.0
        for index, coef in coef_map.items():
            running = running + (basis(index) if isinstance(coef, float) and coef == 1.0 else coef * basis(index))
        return running

    def smooth(residual, level):
        kin = kin_ref[...]
        ratio = kin / (1.5 * level + 1.0)
        poly = 27.0 + ratio * (18.0 + ratio * (12.0 + 8.0 * ratio))
        square = ratio * ratio
        return residual * (poly / (poly + 16.0 * square * square))

    def save(names, slot):
        for k, value in enumerate(names):
            save_ref[slot + k:slot + k + 1, :] = jnp.broadcast_to(value, (1, 128))

    def load_saved(slot):
        return save_ref[slot:slot + 1, 0:1]

    def first_step(gram):
        psi, ham = {0: 1.0}, {1: 1.0}
        eps_zero = gram_form(gram, psi, ham, False) / (gram_form(gram, psi, psi, False) + small_eps)
        return psi, ham, eps_zero, combine([(1.0, ham), (-eps_zero, psi)])

    def second_step(gram):
        psi, ham, eps_zero, r_map = first_step(gram)
        q_map = combine([(1.0, {3: 1.0}), (-eps_zero, {2: 1.0})])
        lam_zero = -gram_form(gram, r_map, q_map, False) / (gram_form(gram, q_map, q_map, False) + small_eps)
        psi_one = combine([(1.0, psi), (lam_zero, {2: 1.0})])
        h_one = combine([(1.0, ham), (lam_zero, {3: 1.0})])
        eps_one = gram_form(gram, psi_one, h_one, False) / (gram_form(gram, psi_one, psi_one, False) + small_eps)
        r_one = combine([(1.0, h_one), (-eps_one, psi_one)])
        change = combine([(1.0, r_map), (-1.0, r_one)])
        weight = gram_form(gram, r_map, change, False) / (gram_form(gram, change, change, False) + small_eps)
        step = weight * lam_zero
        psi_mid = combine([(1.0, psi), (step, {2: 1.0})])
        h_mid = combine([(1.0, ham), (step, {3: 1.0})])
        r_mid = combine([(1.0, r_map), (-weight, change)])
        eps_mid = gram_form(gram, psi_mid, h_mid, False) / (gram_form(gram, psi_mid, psi_mid, False) + small_eps)
        return psi_mid, h_mid, r_mid, eps_mid, step

    first_pairs = new_pairs(0, 2, (False, True))
    second_pairs = new_pairs(2, 4, (False, True))
    third_pairs = new_pairs(4, 5, (False,))
    last_pairs = new_pairs(5, 6, (False,))
    gram_pairs = first_pairs + second_pairs + third_pairs
    lane_id = lax.broadcasted_iota(jnp.int32, (1, 128), 1)

    def swap(which, send, recv, off, incoming):
        source = lax.rem(band + bands - off, bands) if incoming else band
        return pltpu.make_async_remote_copy(
            src_ref=send, dst_ref=recv.at[source],
            send_sem=ns_sem.at[which, off - 1], recv_sem=nr_sem.at[which, off - 1],
            device_id={"band": lax.rem(band + off, bands)}, device_id_type=MESH)

    def share(which, send, recv, values):
        send[...] = values
        recv[band] = values
        for off in range(1, bands):
            swap(which, send, recv, off, False).start()

    def share_end(which, send, recv):
        for off in range(1, bands):
            swap(which, send, recv, off, True).wait()

    def own(index):
        ref = out_vec if index % 2 else in_vec
        return jnp.concatenate([own_row(ref, index // 2, 0), own_row(ref, index // 2, 1)], axis=0)

    def turn_step(turn, carry):
        apply_h(turn)

        @pl.when(turn == 0)
        def _():
            share_h(0)
            gram = gram_sums(first_pairs)
            save([gram[kind, one, two] for one, two, kind in first_pairs], 0)
            r_map = first_step(gram)[3]
            level = gram_form(gram, r_map, r_map, True) / (gram_form(gram, r_map, r_map, False) + small_eps)
            p_zero = smooth(realize(r_map, vector), level)
            in_vec[1] = p_zero

        @pl.when(turn == 1)
        def _():
            share_h(1)
            gram = gram_sums(second_pairs)
            for k, (one, two, kind) in enumerate(first_pairs):
                gram[kind, one, two] = gram[kind, two, one] = load_saved(k)
            psi_mid, h_mid, r_mid, eps_mid, step = second_step(gram)
            level = gram_form(gram, r_mid, r_mid, True) / (gram_form(gram, r_mid, r_mid, False) + small_eps)
            p_one = smooth(realize(r_mid, vector), level)
            in_vec[2] = p_one
            share(0, nsend, nrecv, jnp.stack([realize(psi_mid, own), own(4), realize(h_mid, own)]))
            gram.update(gram_sums(third_pairs))
            packed = jnp.zeros((1, 128), jnp.float32)
            for k, (one, two, kind) in enumerate(gram_pairs):
                packed = jnp.where(lane_id == k, gram[kind, one, two], packed)
            share(1, lsend, lrecv, packed)

        return carry

    lax.fori_loop(0, 3, turn_step, 0)

    g_own = hsend[2]

    def own_last(index):
        return g_own if index == 5 else own(index)

    def world_copy(off, mask, incoming):
        source = (lax.rem(band + bands - off, bands) * group + peer_of(mask)) if incoming else band * group + me
        return pltpu.make_async_remote_copy(
            src_ref=wsend, dst_ref=wrecv.at[source],
            send_sem=ws_sem.at[off * group + mask - 1], recv_sem=wr_sem.at[off * group + mask - 1],
            device_id={"band": lax.rem(band + off, bands), "ga": peer_of(mask)}, device_id_type=MESH)

    local = jnp.zeros((1, 128), jnp.float32)
    for k, (one, two, kind) in enumerate(last_pairs):
        local = jnp.where(lane_id == k, total_of(own_last(one) * g_own), local)
    wsend[...] = local
    for off, mask in world:
        world_copy(off, mask, False).start()
    wrecv[band * group + me] = local

    share_end(0, nsend, nrecv)
    others = [[stack_rows([nrecv[o, which, part:part + 1] for o in range(bands)]) for part in range(2)] for which in range(3)]
    mine = [[nsend[which, part:part + 1] for part in range(2)] for which in range(3)] + [[g_own[0:1], g_own[1:2]]]

    def joined(first, second):
        return [jnp.concatenate([first[part], second[part]], axis=0) for part in range(2)]

    def twice(first, second):
        return [jnp.concatenate([jnp.broadcast_to(first[part], (bands, pw)), jnp.broadcast_to(second[part], (bands, pw))], axis=0) for part in range(2)]

    column_id = lax.broadcasted_iota(jnp.int32, (2 * bands, 128), 1)
    local = jnp.zeros((2 * bands, 128), jnp.float32)
    slot = 0
    for o_row, m_rows in (
        (joined(others[0], others[1]), (twice(mine[0], mine[0]), twice(mine[1], mine[1]))),
        (joined(others[2], others[1]), (twice(mine[0], mine[2]), twice(mine[1], mine[3]))),
    ):
        for m_re, m_im in m_rows:
            for product in (m_re * o_row[0] + m_im * o_row[1], m_re * o_row[1] - m_im * o_row[0]):
                local = jnp.where(column_id == slot, jnp.sum(product, axis=1, keepdims=True), local)
                slot += 1
    crossed = (csend, crecv, cs_sem, cr_sem)
    all_sum(local, *crossed)

    share_end(1, lsend, lrecv)
    early = stack_rows([lrecv[o] for o in range(bands)])
    gram = {}
    for k, (one, two, kind) in enumerate(gram_pairs):
        gram[kind, one, two] = gram[kind, two, one] = early[:, k:k + 1]
    psi_mid, h_mid, r_mid, eps_mid, step = second_step(gram)
    for off, mask in world:
        world_copy(off, mask, True).wait_recv()
    late = []
    for other in range(bands):
        running = wrecv[other * group]
        for dev in range(1, group):
            running = running + wrecv[other * group + dev]
        late.append(running)
    late = stack_rows(late) * (1.0 / total_pw)
    for k, (one, two, kind) in enumerate(last_pairs):
        gram[kind, one, two] = gram[kind, two, one] = late[:, k:k + 1]
    q_one = combine([(1.0, {5: 1.0}), (-eps_mid, {4: 1.0})])
    lam_one = -gram_form(gram, r_mid, q_one, False) / (gram_form(gram, q_one, q_one, False) + small_eps)
    own_band = lax.broadcasted_iota(jnp.int32, (bands, 1), 0) == band

    def pick(column):
        return jnp.sum(jnp.where(own_band, column, 0.0), axis=0, keepdims=True)

    own_lam = pick(lam_one)
    new_ref[...] = nsend[0] + own_lam * nsend[1]
    stores = [pltpu.make_async_copy(new_ref, new_hbm, in_sem.at[0]), pltpu.make_async_copy(scal_ref, scal_hbm, in_sem.at[1])]
    stores[0].start()
    new_map = combine([(1.0, psi_mid), (lam_one, {4: 1.0})])
    ham_new = combine([(1.0, h_mid), (lam_one, {5: 1.0})])
    norm_new = gram_form(gram, new_map, new_map, False) + small_eps
    energy = gram_form(gram, new_map, ham_new, False) / norm_new
    resid = combine([(1.0, ham_new), (-energy, new_map)])
    resid_norm = gram_form(gram, resid, resid, False) / norm_new
    summed = all_sum_end(*crossed) * (1.0 / total_pw)
    mixed = summed[:bands] + lam_one * summed[bands:]
    result = mixed + own_lam * pltpu.roll(mixed, 126, 1)
    scal_ref[...] = jnp.concatenate([
        result, jnp.broadcast_to(pick(energy), (1, 128)), jnp.broadcast_to(pick(resid_norm), (1, 128)),
        jnp.zeros((scal_ref.shape[0] - bands - 2, 128), jnp.float32)], axis=0)
    stores[1].start()
    for off, mask in world:
        world_copy(off, mask, True).wait_send()
    for store in stores:
        store.wait()


def finish_kernel(bands, new_ref, scal_ref, bands_ref, energy_ref, norm_ref, corr_ref, sub_ref):
    bands_ref[:, 0, :] = new_ref[...]
    lane = lax.broadcasted_iota(jnp.int32, (1, bands), 1)
    for ref, base in ((corr_ref, 0), (sub_ref, 4)):
        for part in range(2):
            row = jnp.zeros((1, bands), jnp.float32)
            for other in range(bands):
                at = base + part
                row = jnp.where(lane == other, scal_ref[other:other + 1, at:at + 1], row)
            ref[part] = row
    energy_ref[0] = scal_ref[bands, 0]
    norm_ref[0] = scal_ref[bands + 1, 0]


def kernel_body(coeffs, cell_map, potential, projectors, strengths, proj_atom, proj_chan):
    group = lax.axis_size("ga")
    bands = lax.axis_size("band")
    grid_len = potential.shape[0]
    planes = grid_len // group
    pw = coeffs.shape[2]
    total_pw = pw * group
    slab = 2 * planes
    folds = planes // 2 - 1
    tile_count = group + group // 2
    proj_rows = 2 * projectors.shape[1]
    tables = [jnp.asarray(t) for t in const_tables(grid_len, group)]
    dma = pltpu.SemaphoreType.DMA
    vmem = pl.BlockSpec(memory_space=pltpu.VMEM)
    far = pl.BlockSpec(memory_space=pl.ANY)
    f32, b16 = jnp.float32, jnp.bfloat16
    scal_rows = 8 * (-(-(bands + 2) // 8))
    peers = group - 1
    new, scal = pl.pallas_call(
        functools.partial(sweep_kernel, (group, bands, planes, grid_len, total_pw, pw)),
        out_shape=(
            jax.ShapeDtypeStruct((2, pw), f32),
            jax.ShapeDtypeStruct((scal_rows, 128), f32),
        ),
        in_specs=[far] * 9,
        out_specs=(far, far),
        scratch_shapes=[
            pltpu.VMEM((group, WIDE, pw), b16),
            pltpu.VMEM((group, 16, pw), b16),
            pltpu.VMEM((group, 1, pw), f32),
            pltpu.VMEM((group, 32, pw), f32),
            pltpu.VMEM((group, pw), f32),
            pltpu.VMEM((2, planes, tile_count, 8, 128), f32),
            pltpu.VMEM((group, folds * 2 * slab, WIDE), b16),
            pltpu.VMEM((planes, tile_count, 8, 128), f32),
            pltpu.VMEM((planes * grid_len, grid_len), f32),
            pltpu.VMEM((proj_rows, pw), f32),
            pltpu.VMEM((proj_rows // 2, proj_rows // 2), f32),
            pltpu.VMEM((3, 2, group, pw), f32),
            pltpu.VMEM((2, 2, group, pw), f32),
            pltpu.VMEM((24, 128), f32),
            pltpu.VMEM((strengths.shape[0] * strengths.shape[1], strengths.shape[2]), f32),
            pltpu.VMEM((1, proj_atom.shape[0]), jnp.int32), pltpu.VMEM((1, proj_chan.shape[0]), jnp.int32),
            pltpu.VMEM(tables[0].shape[1:], b16), pltpu.VMEM(tables[1].shape, b16),
            pltpu.VMEM((2, pw), f32), pltpu.VMEM((scal_rows, 128), f32),
            dma((9,)),
            pltpu.VMEM((pw // 128, 128), jnp.int32), pltpu.VMEM((group, pw // 128, 128), jnp.int32),
            pltpu.VMEM((2, 1, pw), f32), pltpu.VMEM((group, 2, 1, pw), f32),
            pltpu.VMEM((3, group, 2, pw), f32), pltpu.VMEM((3, group, 2, pw), f32),
            pltpu.VMEM((3, 2, pw), f32), pltpu.VMEM((2, group, 2, pw), f32),
            pltpu.VMEM((3, 2, proj_rows), f32), pltpu.VMEM((3, group, 2, proj_rows), f32),
            pltpu.VMEM((1, 128), f32), pltpu.VMEM((bands * group, 1, 128), f32),
            pltpu.VMEM((3, 2, pw), f32), pltpu.VMEM((bands, 3, 2, pw), f32),
            pltpu.VMEM((1, 128), f32), pltpu.VMEM((bands, 1, 128), f32),
            pltpu.VMEM((2 * bands, 128), f32), pltpu.VMEM((group, 2 * bands, 128), f32),
            dma((peers,)), dma((peers,)), dma((peers,)), dma((peers,)),
            dma((3, peers)), dma((3, peers)), dma((2, peers)), dma((2, peers)),
            dma((3, peers)), dma((3, peers)), dma((bands * group - 1,)), dma((bands * group - 1,)),
            dma((2, bands - 1)), dma((2, bands - 1)), dma((peers,)), dma((peers,)),
        ],
        compiler_params=pltpu.CompilerParams(
            collective_id=0, has_side_effects=True, vmem_limit_bytes=60 * 1024 * 1024
        ),
        name="sweeps",
    )(
        coeffs, cell_map.reshape(-1, 128), jnp.swapaxes(potential, 0, 1).reshape(planes * grid_len, grid_len),
        projectors.reshape(proj_rows, pw), strengths.reshape(-1, strengths.shape[2]),
        proj_atom.reshape(1, -1), proj_chan.reshape(1, -1), *tables,
    )

    smem = pl.BlockSpec(memory_space=pltpu.SMEM)
    return pl.pallas_call(
        functools.partial(finish_kernel, bands),
        out_shape=(
            jax.ShapeDtypeStruct((2, 1, pw), f32),
            jax.ShapeDtypeStruct((1,), f32),
            jax.ShapeDtypeStruct((1,), f32),
            jax.ShapeDtypeStruct((2, 1, bands), f32),
            jax.ShapeDtypeStruct((2, 1, bands), f32),
        ),
        in_specs=[vmem, vmem],
        out_specs=(vmem, smem, smem, vmem, vmem),
        name="finish",
    )(new, scal)


def body(coeffs, cell_map, potential, projectors, strengths, proj_atom, proj_chan):
    group = lax.axis_size("ga")
    grid_len = potential.shape[0]
    planes = grid_len // group
    fits = (
        group == 8
        and planes == 12
        and coeffs.shape[1] == 1
        and coeffs.shape[2] % 256 == 0
        and 2 * projectors.shape[1] == 128
    )
    chosen = kernel_body if fits else plain_body
    return chosen(coeffs, cell_map, potential, projectors, strengths, proj_atom, proj_chan)


def solution(mesh):
    placed = (
        P(None, "band", "ga"),
        P("ga"),
        P(None, "ga", None),
        P(None, None, "ga"),
        P(),
        P(),
        P(),
    )
    return jax.shard_map(
        body,
        mesh=mesh,
        in_specs=placed,
        out_specs=(
            P(None, "band", "ga"),
            P("band"),
            P("band"),
            P(None, "band", None),
            P(None, "band", None),
        ),
        check_vma=False,
    )
```

```python
import functools

import jax
import jax.numpy as jnp
import numpy as np
from jax import lax
from jax.experimental import pallas as pl
from jax.experimental.pallas import tpu as pltpu
from jax.sharding import PartitionSpec as P

top_precision = lax.Precision.HIGHEST
kin_unit = 0.02
small_eps = 1e-06


def signed_freq(index_arr, grid_len):
    return jnp.where(index_arr < grid_len // 2, index_arr, index_arr - grid_len)


def wave_tables(grid_len, row_freq, col_freq, sign_val, factor):
    phase = row_freq[:, None] * col_freq[None, :] % grid_len
    angle = 2.0 * jnp.pi / grid_len * phase.astype(jnp.float32)
    return (jnp.cos(angle) * factor, jnp.sin(angle) * (sign_val * factor))


def block_table(cos_table, sin_table):
    upper = jnp.concatenate([cos_table, sin_table], axis=1)
    lower = jnp.concatenate([-sin_table, cos_table], axis=1)
    return jnp.concatenate([upper, lower], axis=0)


def quarter_turn(grid_vals):
    half_len = grid_vals.shape[-1] // 2
    return jnp.concatenate([-grid_vals[..., half_len:], grid_vals[..., :half_len]], axis=-1)


def mix_dim(grid_vals, cos_table, sin_table, pattern):
    direct = jnp.einsum(pattern, cos_table, grid_vals, precision=top_precision)
    turned = jnp.einsum(pattern, sin_table, quarter_turn(grid_vals), precision=top_precision)
    return direct + turned


def mix_last(grid_vals, table_full):
    row_width = grid_vals.shape[-1]
    product = jnp.dot(
        grid_vals.reshape(-1, row_width),
        table_full,
        precision=top_precision,
        preferred_element_type=jnp.float32,
    )
    return product.reshape(grid_vals.shape)


def band_dot(left_vec, right_vec, weight):
    return jnp.sum(left_vec * right_vec * weight, axis=(0, 2))


def per_band(values):
    return values[None, :, None]


def pair_products(left_vec, right_vec):

    def contract(first_part, second_part):
        return jnp.einsum("bg,cg->bc", first_part, second_part, precision=top_precision)

    real_part = contract(left_vec[0], right_vec[0]) + contract(left_vec[1], right_vec[1])
    imag_part = contract(left_vec[0], right_vec[1]) - contract(left_vec[1], right_vec[0])
    return jnp.stack([real_part, imag_part])


def precondition(residual, kinetic, kin_level):
    x_ratio = kinetic[None, :] / (1.5 * kin_level[:, None] + 1.0)
    numer_poly = 27.0 + x_ratio * (18.0 + x_ratio * (12.0 + 8.0 * x_ratio))
    square = x_ratio * x_ratio
    return residual * (numer_poly / (numer_poly + 16.0 * square * square))[None]


def coupling_matrix(proj_atom, proj_chan, strengths):
    atom_count = strengths.shape[0]
    chan_count = strengths.shape[1]
    symmetric = 0.5 * (strengths + jnp.swapaxes(strengths, 1, 2))
    atom_hot = (proj_atom[:, None] == jnp.arange(atom_count, dtype=jnp.int32)[None, :]).astype(
        jnp.float32
    )
    chan_hot = (proj_chan[:, None] == jnp.arange(chan_count, dtype=jnp.int32)[None, :]).astype(
        jnp.float32
    )
    rows_d = jnp.einsum("pa,pc,acd->pd", atom_hot, chan_hot, symmetric, precision=top_precision)
    same_atom = jnp.dot(
        atom_hot, atom_hot.T, precision=top_precision, preferred_element_type=jnp.float32
    )
    return same_atom * jnp.dot(
        rows_d, chan_hot.T, precision=top_precision, preferred_element_type=jnp.float32
    )


def combine(term_list):
    merged = {}
    for scalar, coef_map in term_list:
        for index_one, coef_a in coef_map.items():
            merged[index_one] = merged.get(index_one, 0.0) + scalar * coef_a
    return merged


def gram_form(gram_table, left_map, right_map, use_kin):
    running = 0.0
    for index_one, coef_a in left_map.items():
        for index_two, coef_b in right_map.items():
            running = running + coef_a * coef_b * gram_table[use_kin, index_one, index_two]
    return running


def new_pairs(first_new, last_new, kinds):
    pair_list = []
    for use_kin in kinds:
        for index_two in range(first_new, last_new):
            for index_one in range(index_two + 1):
                pair_list.append((index_one, index_two, use_kin))
    return pair_list


def plain_body(coeffs, cell_map, potential, projectors, strengths, proj_atom, proj_chan):
    ga_count = lax.axis_size("ga")
    grid_len = potential.shape[0]
    planes = grid_len // ga_count
    band_local = coeffs.shape[1]
    total_pw = coeffs.shape[2] * ga_count
    device = lax.axis_index("ga")
    plane_num = cell_map // (grid_len * grid_len)
    y_index = cell_map // grid_len % grid_len
    z_index = cell_map % grid_len
    freq_x = signed_freq(device + ga_count * plane_num, grid_len)
    freq_y = signed_freq(y_index, grid_len)
    freq_z = signed_freq(z_index, grid_len)
    kinetic = kin_unit * (freq_x * freq_x + freq_y * freq_y + freq_z * freq_z).astype(jnp.float32)
    kin_weight = kinetic[None, None, :]
    slot_re = (plane_num * grid_len + y_index) * (2 * grid_len) + z_index
    slot_im = slot_re + grid_len
    cell_count = planes * grid_len * 2 * grid_len
    natural = jnp.arange(grid_len, dtype=jnp.int32)
    cyclic = natural % planes * ga_count + natural // planes
    cos_fwd, sin_fwd = wave_tables(grid_len, natural, natural, 1.0, 1.0)
    cos_back, sin_back = wave_tables(grid_len, natural, natural, -1.0, 1.0 / grid_len)
    z_forward = block_table(cos_fwd, sin_fwd)
    z_backward = block_table(cos_back, sin_back)
    xcos_fwd, xsin_fwd = wave_tables(grid_len, natural, cyclic, 1.0, 1.0)
    xcos_back, xsin_back = wave_tables(grid_len, cyclic, natural, -1.0, 1.0 / grid_len)
    doubled = jnp.concatenate([potential, potential], axis=-1)
    coupling = coupling_matrix(proj_atom, proj_chan, strengths)

    def real_space(grid_vals):
        grid_vals = mix_dim(grid_vals, xcos_fwd, xsin_fwd, "kj,bjyw->bkyw")
        grid_vals = grid_vals * doubled[None]
        grid_vals = mix_dim(grid_vals, xcos_back, xsin_back, "jk,bkyw->bjyw")
        return lax.all_to_all(grid_vals, "ga", split_axis=1, concat_axis=2, tiled=True)

    def local_part(vectors):
        item_count = vectors.shape[1]
        flat_grid = jnp.zeros((item_count, cell_count), jnp.float32)
        flat_grid = flat_grid.at[:, slot_re].set(vectors[0]).at[:, slot_im].set(vectors[1])
        grid_vals = mix_last(
            flat_grid.reshape(item_count, planes, grid_len, 2 * grid_len), z_forward
        )
        grid_vals = mix_dim(grid_vals, cos_fwd, sin_fwd, "ky,bpyw->bpkw")
        grid_vals = real_space(
            lax.all_to_all(grid_vals, "ga", split_axis=2, concat_axis=1, tiled=True)
        )
        grid_vals = mix_dim(grid_vals, cos_back, sin_back, "ky,bpyw->bpkw")
        flat_grid = mix_last(grid_vals, z_backward).reshape(item_count, cell_count)
        return jnp.stack([flat_grid[:, slot_re], flat_grid[:, slot_im]])

    def contract(first_part, second_part):
        return jnp.einsum("pg,bg->pb", first_part, second_part, precision=top_precision)

    def spread(weights, proj_table):
        return jnp.einsum("pb,pg->bg", weights, proj_table, precision=top_precision)

    def projected_part(vectors):
        proj_re = contract(projectors[0], vectors[0]) + contract(projectors[1], vectors[1])
        proj_im = contract(projectors[0], vectors[1]) - contract(projectors[1], vectors[0])
        proj_re, proj_im = lax.psum((proj_re, proj_im), "ga")
        mixed_re = jnp.dot(
            coupling,
            proj_re / total_pw,
            precision=top_precision,
            preferred_element_type=jnp.float32,
        )
        mixed_im = jnp.dot(
            coupling,
            proj_im / total_pw,
            precision=top_precision,
            preferred_element_type=jnp.float32,
        )
        out_re = spread(mixed_re, projectors[0]) - spread(mixed_im, projectors[1])
        out_im = spread(mixed_re, projectors[1]) + spread(mixed_im, projectors[0])
        return jnp.stack([out_re, out_im])

    def apply_h(vectors):
        return kin_weight * vectors + local_part(vectors) + projected_part(vectors)

    def gram_sums(basis, pair_list):
        stacked = []
        for index_one, index_two, use_kin in pair_list:
            stacked.append(
                band_dot(basis[index_one], basis[index_two], kin_weight if use_kin else 1.0)
            )
        summed = lax.psum(jnp.stack(stacked), "ga") / total_pw
        found = {}
        for slot_num, entry in enumerate(pair_list):
            index_one, index_two, use_kin = entry
            found[use_kin, index_one, index_two] = summed[slot_num]
            found[use_kin, index_two, index_one] = summed[slot_num]
        return found

    def realize(coef_map, basis):
        running = jnp.zeros_like(basis[0])
        for index_one, coef_a in coef_map.items():
            running = (
                running
                + per_band(jnp.zeros((band_local,), jnp.float32) + coef_a) * basis[index_one]
            )
        return running

    h_zero = apply_h(coeffs)
    basis = [coeffs, h_zero]
    gram_table = gram_sums(basis, new_pairs(0, 2, (False, True)))
    psi_map = {0: 1.0}
    ham_map = {1: 1.0}
    eps_zero = gram_form(gram_table, psi_map, ham_map, False) / (
        gram_form(gram_table, psi_map, psi_map, False) + small_eps
    )
    r_map = combine([(1.0, ham_map), (-eps_zero, psi_map)])
    level_zero = gram_form(gram_table, r_map, r_map, True) / (
        gram_form(gram_table, r_map, r_map, False) + small_eps
    )
    p_zero = precondition(realize(r_map, basis), kinetic, level_zero)
    g_zero = apply_h(p_zero)
    basis = [coeffs, h_zero, p_zero, g_zero]
    gram_table.update(gram_sums(basis, new_pairs(2, 4, (False, True))))
    q_map = combine([(1.0, {3: 1.0}), (-eps_zero, {2: 1.0})])
    lam_zero = -gram_form(gram_table, r_map, q_map, False) / (
        gram_form(gram_table, q_map, q_map, False) + small_eps
    )
    psi_one_map = combine([(1.0, psi_map), (lam_zero, {2: 1.0})])
    h_one_map = combine([(1.0, ham_map), (lam_zero, {3: 1.0})])
    eps_one = gram_form(gram_table, psi_one_map, h_one_map, False) / (
        gram_form(gram_table, psi_one_map, psi_one_map, False) + small_eps
    )
    r_one_map = combine([(1.0, h_one_map), (-eps_one, psi_one_map)])
    change_map = combine([(1.0, r_map), (-1.0, r_one_map)])
    weight_one = gram_form(gram_table, r_map, change_map, False) / (
        gram_form(gram_table, change_map, change_map, False) + small_eps
    )
    step_mid = weight_one * lam_zero
    psi_mid_map = combine([(1.0, psi_map), (step_mid, {2: 1.0})])
    h_mid_map = combine([(1.0, ham_map), (step_mid, {3: 1.0})])
    r_mid_map = combine([(1.0, r_map), (-weight_one, change_map)])
    eps_mid = gram_form(gram_table, psi_mid_map, h_mid_map, False) / (
        gram_form(gram_table, psi_mid_map, psi_mid_map, False) + small_eps
    )
    level_mid = gram_form(gram_table, r_mid_map, r_mid_map, True) / (
        gram_form(gram_table, r_mid_map, r_mid_map, False) + small_eps
    )
    p_one = precondition(realize(r_mid_map, basis), kinetic, level_mid)
    g_one = apply_h(p_one)
    basis = [coeffs, h_zero, p_zero, g_zero, p_one, g_one]
    gram_table.update(gram_sums(basis, new_pairs(4, 6, (False,))))
    q_one_map = combine([(1.0, {5: 1.0}), (-eps_mid, {4: 1.0})])
    lam_one = -gram_form(gram_table, r_mid_map, q_one_map, False) / (
        gram_form(gram_table, q_one_map, q_one_map, False) + small_eps
    )
    new_map = combine([(1.0, psi_mid_map), (lam_one, {4: 1.0})])
    ham_new_map = combine([(1.0, h_mid_map), (lam_one, {5: 1.0})])
    norm_new = gram_form(gram_table, new_map, new_map, False) + small_eps
    energy = gram_form(gram_table, new_map, ham_new_map, False) / norm_new
    resid_map = combine([(1.0, ham_new_map), (-energy, new_map)])
    residual_norm = gram_form(gram_table, resid_map, resid_map, False) / norm_new
    new_bands = realize(new_map, basis)
    new_ham = realize(ham_new_map, basis)
    blank_rows = jnp.zeros((2, band_local, band_local * lax.axis_size("band")), jnp.float32)
    first_row = jnp.int32(0)
    over_rows = blank_rows
    ham_rows = blank_rows
    piece_bands = lax.all_gather(new_bands, "band", axis=1, tiled=True)
    piece_ham = lax.all_gather(new_ham, "band", axis=1, tiled=True)
    over_rows = lax.dynamic_update_slice_in_dim(
        over_rows, pair_products(new_bands, piece_bands), first_row, 2
    )
    ham_rows = lax.dynamic_update_slice_in_dim(
        ham_rows, pair_products(new_bands, piece_ham), first_row, 2
    )
    over_rows, ham_rows = (over_rows, ham_rows)
    over_rows, ham_rows = lax.psum((over_rows, ham_rows), "ga")
    correlation = over_rows / total_pw
    subspace = ham_rows / total_pw
    return (new_bands, energy, residual_norm, correlation, subspace)


WIDE = 256
MESH = pl.DeviceIdType.MESH


def split_const(values):
    high = np.asarray(values, np.float32).astype(jnp.bfloat16)
    low = (values - high.astype(np.float64)).astype(np.float32).astype(jnp.bfloat16)
    return np.stack([high, low])


def const_tables(grid_len, group):
    planes = grid_len // group
    unit = 2.0 * np.pi / grid_len
    freq = np.arange(grid_len)
    y_real = np.arange(group)[:, None] * planes + np.arange(planes)[None, :]
    phase = unit * ((y_real[..., None] * freq) % grid_len)
    cos_y, sin_y = np.cos(phase), np.sin(phase)
    high, low = split_const(np.concatenate([
        cos_y[:, :8], sin_y[:, :8], cos_y[:, 8:], sin_y[:, 8:], -sin_y[:, 8:], cos_y[:, 8:]], axis=1))
    wave = np.concatenate([high, low], axis=2)
    theta = unit * (np.outer(freq, freq) % grid_len)
    turn = np.zeros((2, 128, 2, 128))
    turn[0, :grid_len, 0, :grid_len] = np.cos(theta)
    turn[0, :grid_len, 1, :grid_len] = np.sin(theta)
    turn[1, :grid_len, 0, :grid_len] = -np.sin(theta)
    turn[1, :grid_len, 1, :grid_len] = np.cos(theta)
    turn = turn.reshape(256, 256)
    zed = np.concatenate([split_const(turn), split_const(turn.T)], axis=0)
    return wave, zed


def two_parts(values):
    high = values.astype(jnp.bfloat16)
    low = (values - high.astype(jnp.float32)).astype(jnp.bfloat16)
    return high, low


def split_rows(values):
    high = values.astype(jnp.bfloat16).astype(jnp.float32)
    return jnp.concatenate([high, values - high], axis=0).astype(jnp.bfloat16)


def bdot(left, right):
    return jnp.dot(left, right, preferred_element_type=jnp.float32)


def bdot_t(left, right):
    return lax.dot_general(left, right, (((1,), (1,)), ((), ())), preferred_element_type=jnp.float32)


def total_of(values):
    return jnp.sum(jnp.sum(values, axis=0, keepdims=True), axis=1, keepdims=True)


def c_add(one, two):
    return one[0] + two[0], one[1] + two[1]


def c_sub(one, two):
    return one[0] - two[0], one[1] - two[1]


def c_turn(one, direction):
    return (-one[1], one[0]) if direction > 0 else (one[1], -one[0])


def c_mul(one, cos_val, sin_val):
    return one[0] * cos_val - one[1] * sin_val, one[0] * sin_val + one[1] * cos_val


def c_scale(one, factor):
    return one[0] * factor, one[1] * factor


def three_point(items, direction):
    total = c_add(items[1], items[2])
    side = c_scale(c_turn(c_sub(items[1], items[2]), direction), 0.8660254037844386)
    base = c_sub(items[0], c_scale(total, 0.5))
    return [c_add(items[0], total), c_add(base, side), c_sub(base, side)]


def four_point(items, direction):
    even, odd = c_add(items[0], items[2]), c_add(items[1], items[3])
    low, high = c_sub(items[0], items[2]), c_turn(c_sub(items[1], items[3]), direction)
    return [c_add(even, odd), c_add(low, high), c_sub(even, odd), c_sub(low, high)]


def eight_point(items, direction):
    even = four_point(items[0::2], direction)
    odd = four_point(items[1::2], direction)
    root = 0.7071067811865476
    turned = [
        odd[0],
        c_scale(c_add(odd[1], c_turn(odd[1], direction)), root),
        c_turn(odd[2], direction),
        c_scale(c_sub(c_turn(odd[3], direction), odd[3]), root),
    ]
    return [c_add(e, o) for e, o in zip(even, turned)] + [c_sub(e, o) for e, o in zip(even, turned)]


def twelve_point(items, direction):
    fours = [four_point([items[(4 * a + 3 * b) % 12] for b in range(4)], direction) for a in range(3)]
    threes = [three_point([fours[a][v] for a in range(3)], direction) for v in range(4)]
    return [threes[v % 4][v % 3] for v in range(12)]


def sweep_kernel(
    dims,
    coeffs_hbm, cell_hbm, potential_hbm, proj_hbm, strength_hbm, atom_hbm, chan_hbm,
    wave_hbm, zed_hbm,
    new_hbm, scal_hbm,
    hot_ref, fold_ref, group_ref, phase_ref, kin_ref, work_ref, left_ref,
    pot_ref, potential_ref, proj_ref, couple_ref, in_vec, out_vec, save_ref,
    strength_ref, atom_ref, chan_ref, wave_ref, zed_ref, new_ref, scal_ref, in_sem,
    ksend, krecv, xsend, xrecv, rsend, rrecv, hsend, hrecv, psend, precv,
    wsend, wrecv, nsend, nrecv, lsend, lrecv, csend, crecv,
    ks_sem, kr_sem, xs_sem, xr_sem, rs_sem, rr_sem, hs_sem, hr_sem, ps_sem, pr_sem,
    ws_sem, wr_sem, ns_sem, nr_sem, cs_sem, cr_sem,
):
    group, bands, planes, grid_len, total_pw, pw = dims
    slab = 2 * planes
    folds = planes // 2 - 1
    half = group // 2
    gap = 128 - grid_len
    splits = grid_len // gap
    tiles = pw // 128
    me = lax.axis_index("ga")
    band = lax.axis_index("band")
    sides = [1 - 2 * lax.rem(me // (1 << bit), 2) for bit in range(3)]

    def peer_of(mask):
        return me + sum(sides[bit] * ((mask // (1 << bit)) % 2) * (1 << bit) for bit in range(3))

    loads = [
        pltpu.make_async_copy(source, target, in_sem.at[k])
        for k, (source, target) in enumerate((
            (cell_hbm, ksend), (coeffs_hbm, xsend), (wave_hbm.at[me], wave_ref), (strength_hbm, strength_ref),
            (atom_hbm, atom_ref), (chan_hbm, chan_ref), (potential_hbm, potential_ref), (proj_hbm, proj_ref),
            (zed_hbm, zed_ref)))
    ]
    barrier = pltpu.get_barrier_semaphore()
    world = [(off, mask) for off in (2, 3, 1, 0) for mask in (7, 6, 5, 4, 3, 2, 1, 0) if off or mask]
    for off, mask in world:
        pl.semaphore_signal(barrier, inc=1, device_id={"band": lax.rem(band + off, bands), "ga": peer_of(mask)}, device_id_type=MESH)
    for load in loads:
        load.start()
    for load in loads[:2]:
        load.wait()

    far_first = (6, 7, 4, 5, 2, 3, 1)
    near_first = (2, 4, 3, 5, 6, 7, 1)

    def wait_bytes(ref, sem):
        pltpu.make_async_copy(ref, ref, sem).wait()

    def spread_copy(mask, send, recv, send_sem, recv_sem):
        peer = peer_of(mask)
        return pltpu.make_async_remote_copy(
            src_ref=send, dst_ref=recv.at[me],
            send_sem=send_sem.at[0], recv_sem=recv_sem.at[0 if mask > 1 else recv_sem.shape[0] - 1],
            device_id={"ga": peer}, device_id_type=MESH)

    def spread_start(order, send, recv, send_sem, recv_sem):
        for mask in order:
            spread_copy(mask, send, recv, send_sem, recv_sem).start()

    def spread_wait(send, recv, send_sem, recv_sem):
        wait_bytes(recv.at[pl.ds(0, group - 1)], recv_sem.at[0])
        wait_bytes(recv.at[pl.ds(0, group - 1)], send_sem.at[0])

    keys = (ksend, krecv, ks_sem, kr_sem)
    firsts = (xsend, xrecv, xs_sem, xr_sem)
    pl.semaphore_wait(barrier, group * bands - 1)
    spread_start(near_first, *keys)
    spread_start(near_first, *firsts)
    krecv[me] = ksend[...]
    xrecv[me] = xsend[...]

    def whole(values):
        return jnp.floor(values)

    def signed(values):
        return jnp.where(2.0 * values < grid_len, values, values - grid_len)

    def numbers(cells):
        plane = whole((cells + 0.5) * (1.0 / (grid_len * grid_len)))
        in_plane = cells - plane * (grid_len * grid_len)
        y_num = whole((in_plane + 0.5) * (1.0 / grid_len))
        return plane, y_num, in_plane - y_num * grid_len

    def cell_row(src):
        cell = krecv[src].astype(jnp.float32)
        return jnp.concatenate([cell[k:k + 1] for k in range(tiles)], axis=1)

    def kinetic(plane, y_num, z_num, device):
        f_x = signed(plane * group + device)
        f_y, f_z = signed(y_num), signed(z_num)
        return kin_unit * (f_x * f_x + f_y * f_y + f_z * f_z)

    def marks(numbers_row, count):
        wide_row = jnp.broadcast_to(numbers_row, (16, pw)).astype(jnp.bfloat16)
        row_id = lax.broadcasted_iota(jnp.int32, (16, pw), 0).astype(jnp.float32).astype(jnp.bfloat16)
        one, zero = jnp.ones((16, pw), jnp.bfloat16), jnp.zeros((16, pw), jnp.bfloat16)
        return [jnp.where(row_id + 16.0 * k == wide_row, one, zero) for k in range(count)]

    def build_source(src):
        plane, y_num, z_num = numbers(cell_row(src))
        pair = whole((plane + 0.5) * 0.5)
        piece = whole((z_num + 0.5) * (1.0 / gap))
        hole = (plane - 2.0 * folds) * splits + piece
        hole_pair = whole((hole + 0.5) * 0.5)
        main = plane < 2.0 * folds
        fold = jnp.where(main, pair, hole_pair)
        lane = jnp.where(
            main, (plane - 2.0 * pair) * 128.0 + z_num,
            (hole - 2.0 * hole_pair) * 128.0 + grid_len + z_num - gap * piece)
        group_ref[src] = fold
        fold_ref[src] = jnp.broadcast_to(fold, (16, pw)).astype(jnp.bfloat16)
        for k, rows in enumerate(marks(lane, WIDE // 16)):
            hot_ref[src, 16 * k:16 * (k + 1), :] = rows
        y_hot = marks(y_num, grid_len // 16)
        phase_ref[src] = bdot(wave_ref[...], jnp.concatenate(y_hot + y_hot, axis=0))

    def build_potential():
        pad = jnp.zeros((8, 128 - grid_len), jnp.float32)

        def put_tile(v, slot, block):
            pot_ref[v, slot] = jnp.concatenate([block * (1.0 / grid_len**3), pad], axis=1)

        def lines(x_real, first, count):
            return potential_ref[pl.ds(first * grid_len + x_real, count, stride=grid_len), :]

        for v in range(planes):
            for u in range(group):
                put_tile(v, u, lines(v + planes * u, 0, 8))
            for t in range(half):
                put_tile(v, group + t, jnp.concatenate([
                    lines(v + planes * 2 * t, 8, planes - 8), lines(v + planes * (2 * t + 1), 8, planes - 8)], axis=0))

    def build_coupling():
        atoms, chans = strength_ref.shape[0] // strength_ref.shape[1], strength_ref.shape[1]
        size = atoms * chans
        ident = atom_ref[...] * chans + chan_ref[...]
        hot = (lax.broadcasted_iota(jnp.int32, (size, ident.shape[1]), 0) == ident).astype(jnp.float32)
        row_at = lax.broadcasted_iota(jnp.int32, (size, size), 0)
        col_at = lax.broadcasted_iota(jnp.int32, (size, size), 1)
        tiled = jnp.concatenate([strength_ref[...]] * atoms, axis=1)
        same = (row_at // chans == col_at // chans).astype(jnp.float32)
        block = tiled * same
        block = 0.5 * (block + jnp.transpose(block))
        half = lax.dot_general(hot, block, (((0,), (0,)), ((), ())), precision=top_precision, preferred_element_type=jnp.float32)
        couple_ref[...] = jnp.dot(half, hot, precision=top_precision, preferred_element_type=jnp.float32)

    loads[2].wait()
    build_source(me)
    for load in loads[3:6]:
        load.wait()
    build_coupling()
    loads[6].wait()
    build_potential()
    loads[7].wait()
    loads[8].wait()
    wait_bytes(krecv.at[pl.ds(0, 1)], kr_sem.at[1])
    build_source(peer_of(1))
    wait_bytes(krecv.at[pl.ds(0, group - 2)], kr_sem.at[0])
    for mask in range(2, group):
        build_source(peer_of(mask))
    wait_bytes(krecv.at[pl.ds(0, group - 1)], ks_sem.at[0])

    def stack_rows(pieces):
        return jnp.concatenate(pieces, axis=0)

    cells = stack_rows([cell_row(s) for s in range(group)])
    owner = lax.broadcasted_iota(jnp.int32, (group, pw), 0).astype(jnp.float32)
    kin_ref[...] = kinetic(*numbers(cells), owner)
    spread_wait(*firsts)
    for part in range(2):
        in_vec[0, part] = stack_rows([xrecv[s, part] for s in range(group)])

    upper = lax.broadcasted_iota(jnp.int32, (8, 128), 0) < 4
    lane_at = lax.broadcasted_iota(jnp.int32, (8, 128), 1)
    flip = jnp.where(upper, 1.0, -1.0).astype(jnp.float32)

    def swap_half(values):
        return pltpu.roll(values, 4, 0)

    def halves(low, high):
        return low if low == high else jnp.where(upper, low, high)

    def lane_turn(s, v, paired):
        angle = [2.0 * np.pi * ((k * v) % grid_len) / grid_len for k in (s, s + half)]
        cos_val, sin_val = [float(np.cos(a)) for a in angle], [float(np.sin(a)) for a in angle]
        if paired:
            return halves(*cos_val), halves(*sin_val)
        return cos_val[0], sin_val[0]

    def twist(item, s, v, paired, direction):
        if v == 0 or (s == 0 and not paired):
            return item
        cos_val, sin_val = lane_turn(s, v, paired)
        return c_mul(item, cos_val, sin_val if direction > 0 else -sin_val)

    def z_turn(tiles, which):
        stacked = jnp.concatenate([jnp.concatenate(list(t), axis=1) for t in tiles], axis=0)
        high, low = two_parts(stacked)
        out = bdot(high, zed_ref[which]) + bdot(low, zed_ref[which]) + bdot(high, zed_ref[which + 1])
        return [(out[8 * k:8 * k + 8, :128], out[8 * k:8 * k + 8, 128:]) for k in range(len(tiles))]

    def keep(slot, v, item):
        work_ref[0, v, slot] = item[0]
        work_ref[1, v, slot] = item[1]

    def kept(slot, v):
        return work_ref[0, v, slot], work_ref[1, v, slot]

    def own_row(ref, turn, part):
        return ref[turn, part, pl.ds(me, 1), :]

    def put(turn, src):
        v_re, v_im = in_vec[turn, 0, src:src + 1, :], in_vec[turn, 1, src:src + 1, :]
        cos_y, sin_y, mix_re, mix_im = [phase_ref[src, 8 * k:8 * k + 8, :] for k in range(4)]
        both = split_rows(jnp.concatenate([
            cos_y * v_re - sin_y * v_im, mix_re * v_re + mix_im * v_im, sin_y * v_re + cos_y * v_im], axis=0))
        pieces = []
        fold = fold_ref[src]
        blank = jnp.zeros((16, pw), jnp.bfloat16)
        for k in range(folds):
            hit = fold == float(k)
            for at in range(0, 2 * slab, 16):
                pieces.append(jnp.where(hit, both[at:at + 16], blank))
        out = bdot_t(jnp.concatenate(pieces, axis=0), hot_ref[src])
        tiles = []
        for k in range(folds):
            base = k * 2 * slab
            block = out[base:base + slab] + out[base + slab:base + 2 * slab]
            for at in (0, 128):
                tiles.append([block[8 * t:8 * t + 8, at:at + 128] for t in range(3)])
        for extra in range(planes - 2 * folds):
            joined = []
            for t in range(3):
                run = None
                for q in reversed(range(splits)):
                    moved = pltpu.roll(tiles[extra * splits + q][t], (q + 1) * gap, 1)
                    run = moved if run is None else jnp.where(lane_at < (q + 1) * gap, moved, run)
                joined.append(run)
            tiles.append(joined)
        return tiles

    def forward_turn(s, low, high):
        rest = [(
            jnp.where(upper, a[1], swap_half(b[1])), jnp.where(upper, swap_half(a[1]), b[1]),
        ) for a, b in zip(low, high)]
        turned = z_turn([(a[0], a[2]) for a in low] + [(b[0], b[2]) for b in high] + rest, 0)
        for k, (slot, first, paired) in enumerate(((s, s, False), (s + half, s + half, False), (group + s, s, True))):
            for v, item in enumerate(twelve_point(turned[k * planes:(k + 1) * planes], 1)):
                keep(slot, v, twist(item, first, v, paired, 1))

    def cross(item):
        return tuple(swap_half(x) + x * flip for x in item)

    def half_turn(item, s, direction):
        if s == 0:
            return item
        angle = 2.0 * np.pi * s / group
        return c_mul(item, halves(1.0, float(np.cos(angle))), direction * halves(0.0, float(np.sin(angle))))

    def middle(v):
        items = eight_point([kept(s, v) for s in range(group)], 1)
        items = [c_scale(item, pot_ref[v, u]) for u, item in enumerate(items)]
        for s, item in enumerate(eight_point(items, -1)):
            keep(s, v, twist(item, s, v, False, -1))
        items = four_point([half_turn(cross(kept(group + s, v)), s, 1) for s in range(half)], 1)
        items = [c_scale(item, pot_ref[v, group + t]) for t, item in enumerate(items)]
        for s, item in enumerate(four_point(items, -1)):
            keep(group + s, v, twist(cross(half_turn(item, s, -1)), s, v, True, -1))

    def backward_pair(s):
        spread = []
        for slot in (s, s + half, group + s):
            spread += twelve_point([kept(slot, v) for v in range(planes)], -1)
        turned = z_turn(spread, 2)
        low, high, rest = [turned[k * planes:(k + 1) * planes] for k in range(3)]
        low = [(a[0], jnp.where(upper, r[0], swap_half(r[1])), a[1]) for a, r in zip(low, rest)]
        high = [(b[0], jnp.where(upper, swap_half(r[0]), r[1]), b[1]) for b, r in zip(high, rest)]
        for dest, tiles in ((s, low), (s + half, high)):
            for hole in range((planes - 2 * folds) * splits):
                extra, q = 2 * folds + hole // splits, hole % splits
                tiles[hole] = tuple(
                    jnp.where(lane_at >= grid_len, pltpu.roll(tiles[extra][t], grid_len - q * gap, 1), tiles[hole][t])
                    for t in range(3))
            for k in range(folds):
                block = jnp.concatenate([jnp.concatenate(tiles[2 * k + m], axis=0) for m in range(2)], axis=1)
                left_ref[dest, k * 2 * slab:(k + 1) * 2 * slab, :] = split_rows(block)

    def partial_copy(turn, mask):
        return pltpu.make_async_remote_copy(
            src_ref=rsend.at[turn, mask], dst_ref=rrecv.at[turn, mask],
            send_sem=rs_sem.at[0], recv_sem=rr_sem.at[0],
            device_id={"ga": peer_of(mask)}, device_id_type=MESH)

    def take_tile(mask, at):
        return bdot(left_ref[peer_of(mask)], hot_ref[peer_of(mask), :, at:at + WIDE])

    def take_sum(turn, mask, at, out):
        dest = peer_of(mask)
        span = slice(at, at + WIDE)
        fold = group_ref[dest, :, span]
        chosen = out[:2 * slab]
        for k in range(1, folds):
            chosen = jnp.where(fold == float(k), out[k * 2 * slab:(k + 1) * 2 * slab], chosen)
        value = chosen[:slab] + chosen[slab:]
        first, mixed, last = [value[8 * k:8 * k + 8] for k in range(3)]
        cos_y, sin_y, mix_re, mix_im = [phase_ref[dest, 8 * k:8 * k + 8, span] for k in range(4)]
        back_re = cos_y * first + sin_y * last + mix_re * mixed
        back_im = cos_y * last - sin_y * first + mix_im * mixed
        for part, back in enumerate((back_re, back_im)):
            rsend[turn, mask, part:part + 1, span] = jnp.sum(back, axis=0, keepdims=True)

    def take_all(turn):
        order = ((6, 7), (2, 3), (4, 5), (1, 0))
        units = [(masks, mask, at) for masks in order for mask in masks for at in range(0, pw, WIDE)]
        lag = 3
        pending = []
        for unit in units + [None] * lag:
            if unit:
                pending.append((unit, take_tile(*unit[1:])))
            if len(pending) > lag or not unit:
                (masks, mask, at), out = pending.pop(0)
                take_sum(turn, mask, at, out)
                if mask == masks[-1] and at + WIDE == pw:
                    for ready in masks:
                        if ready:
                            partial_copy(turn, ready).start()

    def all_sum(local, send, recv, send_sem, recv_sem):
        send[...] = local
        recv[me] = local
        spread_start(far_first, send, recv, send_sem, recv_sem)

    def all_sum_end(send, recv, send_sem, recv_sem):
        spread_wait(send, recv, send_sem, recv_sem)
        running = recv[0]
        for dev in range(1, group):
            running = running + recv[dev]
        return running

    def project(turn):
        found = []
        for part in range(2):
            row = own_row(in_vec, turn, part)
            running = proj_ref[:, :128] * row[:, :128]
            for at in range(128, pw, 128):
                running = running + proj_ref[:, at:at + 128] * row[:, at:at + 128]
            found.append(jnp.sum(jnp.transpose(running), axis=0, keepdims=True))
        return jnp.concatenate(found, axis=0)

    def nonlocal_rows(sums):
        half = sums.shape[1] // 2
        pair = jnp.concatenate([
            sums[0:1, :half] + sums[1:2, half:], sums[1:2, :half] - sums[0:1, half:]], axis=0)
        mixed = jnp.dot(pair, couple_ref[...], precision=top_precision, preferred_element_type=jnp.float32)
        m_re, m_im = mixed[0:1], mixed[1:2]
        found = []
        for row in (jnp.concatenate([m_re, -m_im], axis=1), jnp.concatenate([m_im, m_re], axis=1)):
            column = jnp.transpose(jnp.broadcast_to(row, (2 * half, 128)))
            found.append(jnp.concatenate([
                jnp.sum(proj_ref[:, at:at + 128] * column, axis=0, keepdims=True) for at in range(0, pw, 128)], axis=1))
        return jnp.concatenate(found, axis=0)

    def apply_h(turn):
        sums = (psend.at[turn], precv.at[turn], ps_sem, pr_sem)
        placed = []
        for s in range(half):
            placed.append((s, put(turn, s), put(turn, s + half)))
            if s:
                forward_turn(*placed.pop(0))
        forward_turn(*placed.pop(0))
        for v in range(planes):
            middle(v)
        for s in range(half):
            backward_pair(s)
        all_sum(project(turn), *sums)
        take_all(turn)
        start = nonlocal_rows(all_sum_end(*sums) * (1.0 / total_pw))
        own_kin = kin_ref[pl.ds(me, 1), :]
        start = start + own_kin * jnp.concatenate([own_row(in_vec, turn, 0), own_row(in_vec, turn, 1)], axis=0)
        running = start + rsend[turn, 0]
        wait_bytes(rrecv.at[turn, pl.ds(1, group - 1)], rr_sem.at[0])
        wait_bytes(rrecv.at[turn, pl.ds(1, group - 1)], rs_sem.at[0])
        for mask in range(1, group):
            running = running + rrecv[turn, mask]
        hsend[turn] = running
        return running

    def share_h(turn):
        out = (hsend.at[turn], hrecv.at[turn], hs_sem, hr_sem)
        spread_start(far_first, *out)
        hrecv[turn, me] = hsend[turn]
        spread_wait(*out)
        for part in range(2):
            out_vec[turn, part] = stack_rows([hrecv[turn, s, part:part + 1] for s in range(group)])

    def vector(index):
        ref = out_vec if index % 2 else in_vec
        return ref[index // 2]

    def gram_sums(pair_list):
        found = {}
        for one, two, use_kin in pair_list:
            left, right = vector(one), vector(two)
            product = left[0] * right[0] + left[1] * right[1]
            value = total_of(product * kin_ref[...] if use_kin else product) * (1.0 / total_pw)
            found[use_kin, one, two] = value
            found[use_kin, two, one] = value
        return found

    def realize(coef_map, basis):
        running = 0.0
        for index, coef in coef_map.items():
            running = running + (basis(index) if isinstance(coef, float) and coef == 1.0 else coef * basis(index))
        return running

    def smooth(residual, level):
        kin = kin_ref[...]
        ratio = kin / (1.5 * level + 1.0)
        poly = 27.0 + ratio * (18.0 + ratio * (12.0 + 8.0 * ratio))
        square = ratio * ratio
        return residual * (poly / (poly + 16.0 * square * square))

    def save(names, slot):
        for k, value in enumerate(names):
            save_ref[slot + k:slot + k + 1, :] = jnp.broadcast_to(value, (1, 128))

    def load_saved(slot):
        return save_ref[slot:slot + 1, 0:1]

    def first_step(gram):
        psi, ham = {0: 1.0}, {1: 1.0}
        eps_zero = gram_form(gram, psi, ham, False) / (gram_form(gram, psi, psi, False) + small_eps)
        return psi, ham, eps_zero, combine([(1.0, ham), (-eps_zero, psi)])

    def second_step(gram):
        psi, ham, eps_zero, r_map = first_step(gram)
        q_map = combine([(1.0, {3: 1.0}), (-eps_zero, {2: 1.0})])
        lam_zero = -gram_form(gram, r_map, q_map, False) / (gram_form(gram, q_map, q_map, False) + small_eps)
        psi_one = combine([(1.0, psi), (lam_zero, {2: 1.0})])
        h_one = combine([(1.0, ham), (lam_zero, {3: 1.0})])
        eps_one = gram_form(gram, psi_one, h_one, False) / (gram_form(gram, psi_one, psi_one, False) + small_eps)
        r_one = combine([(1.0, h_one), (-eps_one, psi_one)])
        change = combine([(1.0, r_map), (-1.0, r_one)])
        weight = gram_form(gram, r_map, change, False) / (gram_form(gram, change, change, False) + small_eps)
        step = weight * lam_zero
        psi_mid = combine([(1.0, psi), (step, {2: 1.0})])
        h_mid = combine([(1.0, ham), (step, {3: 1.0})])
        r_mid = combine([(1.0, r_map), (-weight, change)])
        eps_mid = gram_form(gram, psi_mid, h_mid, False) / (gram_form(gram, psi_mid, psi_mid, False) + small_eps)
        return psi_mid, h_mid, r_mid, eps_mid, step

    first_pairs = new_pairs(0, 2, (False, True))
    second_pairs = new_pairs(2, 4, (False, True))
    third_pairs = new_pairs(4, 5, (False,))
    last_pairs = new_pairs(5, 6, (False,))
    gram_pairs = first_pairs + second_pairs + third_pairs
    lane_id = lax.broadcasted_iota(jnp.int32, (1, 128), 1)

    def swap(which, send, recv, off):
        return pltpu.make_async_remote_copy(
            src_ref=send, dst_ref=recv.at[band],
            send_sem=ns_sem.at[which], recv_sem=nr_sem.at[which],
            device_id={"band": lax.rem(band + off, bands)}, device_id_type=MESH)

    def share(which, send, recv, values):
        send[...] = values
        recv[band] = values
        for off in range(1, bands):
            swap(which, send, recv, off).start()

    def share_end(which, send, recv):
        wait_bytes(recv.at[pl.ds(0, bands - 1)], nr_sem.at[which])
        wait_bytes(recv.at[pl.ds(0, bands - 1)], ns_sem.at[which])

    def own(index):
        ref = out_vec if index % 2 else in_vec
        return jnp.concatenate([own_row(ref, index // 2, 0), own_row(ref, index // 2, 1)], axis=0)

    def turn_step(turn, carry):
        apply_h(turn)

        @pl.when(turn == 0)
        def _():
            share_h(0)
            gram = gram_sums(first_pairs)
            save([gram[kind, one, two] for one, two, kind in first_pairs], 0)
            r_map = first_step(gram)[3]
            level = gram_form(gram, r_map, r_map, True) / (gram_form(gram, r_map, r_map, False) + small_eps)
            p_zero = smooth(realize(r_map, vector), level)
            in_vec[1] = p_zero

        @pl.when(turn == 1)
        def _():
            share_h(1)
            gram = gram_sums(second_pairs)
            for k, (one, two, kind) in enumerate(first_pairs):
                gram[kind, one, two] = gram[kind, two, one] = load_saved(k)
            psi_mid, h_mid, r_mid, eps_mid, step = second_step(gram)
            level = gram_form(gram, r_mid, r_mid, True) / (gram_form(gram, r_mid, r_mid, False) + small_eps)
            p_one = smooth(realize(r_mid, vector), level)
            in_vec[2] = p_one
            share(0, nsend, nrecv, jnp.stack([realize(psi_mid, own), own(4), realize(h_mid, own)]))
            gram.update(gram_sums(third_pairs))
            packed = jnp.zeros((1, 128), jnp.float32)
            for k, (one, two, kind) in enumerate(gram_pairs):
                packed = jnp.where(lane_id == k, gram[kind, one, two], packed)
            share(1, lsend, lrecv, packed)

        return carry

    lax.fori_loop(0, 3, turn_step, 0)

    g_own = hsend[2]

    def own_last(index):
        return g_own if index == 5 else own(index)

    def world_copy(off, mask):
        return pltpu.make_async_remote_copy(
            src_ref=wsend, dst_ref=wrecv.at[band * group + me],
            send_sem=ws_sem.at[0], recv_sem=wr_sem.at[0],
            device_id={"band": lax.rem(band + off, bands), "ga": peer_of(mask)}, device_id_type=MESH)

    local = jnp.zeros((1, 128), jnp.float32)
    for k, (one, two, kind) in enumerate(last_pairs):
        local = jnp.where(lane_id == k, total_of(own_last(one) * g_own), local)
    wsend[...] = local
    for off, mask in world:
        world_copy(off, mask).start()
    wrecv[band * group + me] = local

    share_end(0, nsend, nrecv)
    others = [[stack_rows([nrecv[o, which, part:part + 1] for o in range(bands)]) for part in range(2)] for which in range(3)]
    mine = [[nsend[which, part:part + 1] for part in range(2)] for which in range(3)] + [[g_own[0:1], g_own[1:2]]]

    def joined(first, second):
        return [jnp.concatenate([first[part], second[part]], axis=0) for part in range(2)]

    def twice(first, second):
        return [jnp.concatenate([jnp.broadcast_to(first[part], (bands, pw)), jnp.broadcast_to(second[part], (bands, pw))], axis=0) for part in range(2)]

    column_id = lax.broadcasted_iota(jnp.int32, (2 * bands, 128), 1)
    local = jnp.zeros((2 * bands, 128), jnp.float32)
    slot = 0
    for o_row, m_rows in (
        (joined(others[0], others[1]), (twice(mine[0], mine[0]), twice(mine[1], mine[1]))),
        (joined(others[2], others[1]), (twice(mine[0], mine[2]), twice(mine[1], mine[3]))),
    ):
        for m_re, m_im in m_rows:
            for product in (m_re * o_row[0] + m_im * o_row[1], m_re * o_row[1] - m_im * o_row[0]):
                local = jnp.where(column_id == slot, jnp.sum(product, axis=1, keepdims=True), local)
                slot += 1
    crossed = (csend, crecv, cs_sem, cr_sem)
    all_sum(local, *crossed)

    share_end(1, lsend, lrecv)
    early = stack_rows([lrecv[o] for o in range(bands)])
    gram = {}
    for k, (one, two, kind) in enumerate(gram_pairs):
        gram[kind, one, two] = gram[kind, two, one] = early[:, k:k + 1]
    psi_mid, h_mid, r_mid, eps_mid, step = second_step(gram)
    wait_bytes(wrecv.at[pl.ds(0, group * bands - 1)], wr_sem.at[0])
    late = []
    for other in range(bands):
        running = wrecv[other * group]
        for dev in range(1, group):
            running = running + wrecv[other * group + dev]
        late.append(running)
    late = stack_rows(late) * (1.0 / total_pw)
    for k, (one, two, kind) in enumerate(last_pairs):
        gram[kind, one, two] = gram[kind, two, one] = late[:, k:k + 1]
    q_one = combine([(1.0, {5: 1.0}), (-eps_mid, {4: 1.0})])
    lam_one = -gram_form(gram, r_mid, q_one, False) / (gram_form(gram, q_one, q_one, False) + small_eps)
    own_band = lax.broadcasted_iota(jnp.int32, (bands, 1), 0) == band

    def pick(column):
        return jnp.sum(jnp.where(own_band, column, 0.0), axis=0, keepdims=True)

    own_lam = pick(lam_one)
    new_ref[...] = nsend[0] + own_lam * nsend[1]
    stores = [pltpu.make_async_copy(new_ref, new_hbm, in_sem.at[0]), pltpu.make_async_copy(scal_ref, scal_hbm, in_sem.at[1])]
    stores[0].start()
    new_map = combine([(1.0, psi_mid), (lam_one, {4: 1.0})])
    ham_new = combine([(1.0, h_mid), (lam_one, {5: 1.0})])
    norm_new = gram_form(gram, new_map, new_map, False) + small_eps
    energy = gram_form(gram, new_map, ham_new, False) / norm_new
    resid = combine([(1.0, ham_new), (-energy, new_map)])
    resid_norm = gram_form(gram, resid, resid, False) / norm_new
    summed = all_sum_end(*crossed) * (1.0 / total_pw)
    mixed = summed[:bands] + lam_one * summed[bands:]
    result = mixed + own_lam * pltpu.roll(mixed, 126, 1)
    scal_ref[...] = jnp.concatenate([
        result, jnp.broadcast_to(pick(energy), (1, 128)), jnp.broadcast_to(pick(resid_norm), (1, 128)),
        jnp.zeros((scal_ref.shape[0] - bands - 2, 128), jnp.float32)], axis=0)
    stores[1].start()
    wait_bytes(wrecv.at[pl.ds(0, group * bands - 1)], ws_sem.at[0])
    for store in stores:
        store.wait()


def finish_kernel(bands, new_ref, scal_ref, bands_ref, energy_ref, norm_ref, corr_ref, sub_ref):
    bands_ref[:, 0, :] = new_ref[...]
    lane = lax.broadcasted_iota(jnp.int32, (1, bands), 1)
    for ref, base in ((corr_ref, 0), (sub_ref, 4)):
        for part in range(2):
            row = jnp.zeros((1, bands), jnp.float32)
            for other in range(bands):
                at = base + part
                row = jnp.where(lane == other, scal_ref[other:other + 1, at:at + 1], row)
            ref[part] = row
    energy_ref[0] = scal_ref[bands, 0]
    norm_ref[0] = scal_ref[bands + 1, 0]


def kernel_body(coeffs, cell_map, potential, projectors, strengths, proj_atom, proj_chan):
    group = lax.axis_size("ga")
    bands = lax.axis_size("band")
    grid_len = potential.shape[0]
    planes = grid_len // group
    pw = coeffs.shape[2]
    total_pw = pw * group
    slab = 2 * planes
    folds = planes // 2 - 1
    tile_count = group + group // 2
    proj_rows = 2 * projectors.shape[1]
    tables = [jnp.asarray(t) for t in const_tables(grid_len, group)]
    dma = pltpu.SemaphoreType.DMA
    vmem = pl.BlockSpec(memory_space=pltpu.VMEM)
    far = pl.BlockSpec(memory_space=pl.ANY)
    f32, b16 = jnp.float32, jnp.bfloat16
    scal_rows = 8 * (-(-(bands + 2) // 8))
    new, scal = pl.pallas_call(
        functools.partial(sweep_kernel, (group, bands, planes, grid_len, total_pw, pw)),
        out_shape=(
            jax.ShapeDtypeStruct((2, pw), f32),
            jax.ShapeDtypeStruct((scal_rows, 128), f32),
        ),
        in_specs=[far] * 9,
        out_specs=(far, far),
        scratch_shapes=[
            pltpu.VMEM((group, WIDE, pw), b16),
            pltpu.VMEM((group, 16, pw), b16),
            pltpu.VMEM((group, 1, pw), f32),
            pltpu.VMEM((group, 32, pw), f32),
            pltpu.VMEM((group, pw), f32),
            pltpu.VMEM((2, planes, tile_count, 8, 128), f32),
            pltpu.VMEM((group, folds * 2 * slab, WIDE), b16),
            pltpu.VMEM((planes, tile_count, 8, 128), f32),
            pltpu.VMEM((planes * grid_len, grid_len), f32),
            pltpu.VMEM((proj_rows, pw), f32),
            pltpu.VMEM((proj_rows // 2, proj_rows // 2), f32),
            pltpu.VMEM((3, 2, group, pw), f32),
            pltpu.VMEM((2, 2, group, pw), f32),
            pltpu.VMEM((24, 128), f32),
            pltpu.VMEM((strengths.shape[0] * strengths.shape[1], strengths.shape[2]), f32),
            pltpu.VMEM((1, proj_atom.shape[0]), jnp.int32), pltpu.VMEM((1, proj_chan.shape[0]), jnp.int32),
            pltpu.VMEM(tables[0].shape[1:], b16), pltpu.VMEM(tables[1].shape, b16),
            pltpu.VMEM((2, pw), f32), pltpu.VMEM((scal_rows, 128), f32),
            dma((9,)),
            pltpu.VMEM((pw // 128, 128), jnp.int32), pltpu.VMEM((group, pw // 128, 128), jnp.int32),
            pltpu.VMEM((2, 1, pw), f32), pltpu.VMEM((group, 2, 1, pw), f32),
            pltpu.VMEM((3, group, 2, pw), f32), pltpu.VMEM((3, group, 2, pw), f32),
            pltpu.VMEM((3, 2, pw), f32), pltpu.VMEM((2, group, 2, pw), f32),
            pltpu.VMEM((3, 2, proj_rows), f32), pltpu.VMEM((3, group, 2, proj_rows), f32),
            pltpu.VMEM((1, 128), f32), pltpu.VMEM((bands * group, 1, 128), f32),
            pltpu.VMEM((3, 2, pw), f32), pltpu.VMEM((bands, 3, 2, pw), f32),
            pltpu.VMEM((1, 128), f32), pltpu.VMEM((bands, 1, 128), f32),
            pltpu.VMEM((2 * bands, 128), f32), pltpu.VMEM((group, 2 * bands, 128), f32),
            dma((1,)), dma((2,)), dma((1,)), dma((1,)), dma((1,)), dma((1,)), dma((1,)), dma((1,)),
            dma((1,)), dma((1,)), dma((1,)), dma((1,)), dma((2,)), dma((2,)), dma((1,)), dma((1,)),
        ],
        compiler_params=pltpu.CompilerParams(
            collective_id=0, has_side_effects=True, vmem_limit_bytes=60 * 1024 * 1024
        ),
        name="sweeps",
    )(
        coeffs, cell_map.reshape(-1, 128), jnp.swapaxes(potential, 0, 1).reshape(planes * grid_len, grid_len),
        projectors.reshape(proj_rows, pw), strengths.reshape(-1, strengths.shape[2]),
        proj_atom.reshape(1, -1), proj_chan.reshape(1, -1), *tables,
    )

    smem = pl.BlockSpec(memory_space=pltpu.SMEM)
    return pl.pallas_call(
        functools.partial(finish_kernel, bands),
        out_shape=(
            jax.ShapeDtypeStruct((2, 1, pw), f32),
            jax.ShapeDtypeStruct((1,), f32),
            jax.ShapeDtypeStruct((1,), f32),
            jax.ShapeDtypeStruct((2, 1, bands), f32),
            jax.ShapeDtypeStruct((2, 1, bands), f32),
        ),
        in_specs=[vmem, vmem],
        out_specs=(vmem, smem, smem, vmem, vmem),
        name="finish",
    )(new, scal)


def body(coeffs, cell_map, potential, projectors, strengths, proj_atom, proj_chan):
    group = lax.axis_size("ga")
    grid_len = potential.shape[0]
    planes = grid_len // group
    fits = (
        group == 8
        and planes == 12
        and coeffs.shape[1] == 1
        and coeffs.shape[2] % 256 == 0
        and 2 * projectors.shape[1] == 128
    )
    chosen = kernel_body if fits else plain_body
    return chosen(coeffs, cell_map, potential, projectors, strengths, proj_atom, proj_chan)


def solution(mesh):
    placed = (
        P(None, "band", "ga"),
        P("ga"),
        P(None, "ga", None),
        P(None, None, "ga"),
        P(),
        P(),
        P(),
    )
    return jax.shard_map(
        body,
        mesh=mesh,
        in_specs=placed,
        out_specs=(
            P(None, "band", "ga"),
            P("band"),
            P("band"),
            P(None, "band", None),
            P(None, "band", None),
        ),
        check_vma=False,
    )
```

```python
import functools

import jax
import jax.numpy as jnp
import numpy as np
from jax import lax
from jax.experimental import pallas as pl
from jax.experimental.pallas import tpu as pltpu
from jax.sharding import PartitionSpec as P

top_precision = lax.Precision.HIGHEST
kin_unit = 0.02
small_eps = 1e-06


def signed_freq(index_arr, grid_len):
    return jnp.where(index_arr < grid_len // 2, index_arr, index_arr - grid_len)


def wave_tables(grid_len, row_freq, col_freq, sign_val, factor):
    phase = row_freq[:, None] * col_freq[None, :] % grid_len
    angle = 2.0 * jnp.pi / grid_len * phase.astype(jnp.float32)
    return (jnp.cos(angle) * factor, jnp.sin(angle) * (sign_val * factor))


def block_table(cos_table, sin_table):
    upper = jnp.concatenate([cos_table, sin_table], axis=1)
    lower = jnp.concatenate([-sin_table, cos_table], axis=1)
    return jnp.concatenate([upper, lower], axis=0)


def quarter_turn(grid_vals):
    half_len = grid_vals.shape[-1] // 2
    return jnp.concatenate([-grid_vals[..., half_len:], grid_vals[..., :half_len]], axis=-1)


def mix_dim(grid_vals, cos_table, sin_table, pattern):
    direct = jnp.einsum(pattern, cos_table, grid_vals, precision=top_precision)
    turned = jnp.einsum(pattern, sin_table, quarter_turn(grid_vals), precision=top_precision)
    return direct + turned


def mix_last(grid_vals, table_full):
    row_width = grid_vals.shape[-1]
    product = jnp.dot(
        grid_vals.reshape(-1, row_width),
        table_full,
        precision=top_precision,
        preferred_element_type=jnp.float32,
    )
    return product.reshape(grid_vals.shape)


def band_dot(left_vec, right_vec, weight):
    return jnp.sum(left_vec * right_vec * weight, axis=(0, 2))


def per_band(values):
    return values[None, :, None]


def pair_products(left_vec, right_vec):

    def contract(first_part, second_part):
        return jnp.einsum("bg,cg->bc", first_part, second_part, precision=top_precision)

    real_part = contract(left_vec[0], right_vec[0]) + contract(left_vec[1], right_vec[1])
    imag_part = contract(left_vec[0], right_vec[1]) - contract(left_vec[1], right_vec[0])
    return jnp.stack([real_part, imag_part])


def precondition(residual, kinetic, kin_level):
    x_ratio = kinetic[None, :] / (1.5 * kin_level[:, None] + 1.0)
    numer_poly = 27.0 + x_ratio * (18.0 + x_ratio * (12.0 + 8.0 * x_ratio))
    square = x_ratio * x_ratio
    return residual * (numer_poly / (numer_poly + 16.0 * square * square))[None]


def coupling_matrix(proj_atom, proj_chan, strengths):
    atom_count = strengths.shape[0]
    chan_count = strengths.shape[1]
    symmetric = 0.5 * (strengths + jnp.swapaxes(strengths, 1, 2))
    atom_hot = (proj_atom[:, None] == jnp.arange(atom_count, dtype=jnp.int32)[None, :]).astype(
        jnp.float32
    )
    chan_hot = (proj_chan[:, None] == jnp.arange(chan_count, dtype=jnp.int32)[None, :]).astype(
        jnp.float32
    )
    rows_d = jnp.einsum("pa,pc,acd->pd", atom_hot, chan_hot, symmetric, precision=top_precision)
    same_atom = jnp.dot(
        atom_hot, atom_hot.T, precision=top_precision, preferred_element_type=jnp.float32
    )
    return same_atom * jnp.dot(
        rows_d, chan_hot.T, precision=top_precision, preferred_element_type=jnp.float32
    )


def combine(term_list):
    merged = {}
    for scalar, coef_map in term_list:
        for index_one, coef_a in coef_map.items():
            merged[index_one] = merged.get(index_one, 0.0) + scalar * coef_a
    return merged


def gram_form(gram_table, left_map, right_map, use_kin):
    running = 0.0
    for index_one, coef_a in left_map.items():
        for index_two, coef_b in right_map.items():
            running = running + coef_a * coef_b * gram_table[use_kin, index_one, index_two]
    return running


def new_pairs(first_new, last_new, kinds):
    pair_list = []
    for use_kin in kinds:
        for index_two in range(first_new, last_new):
            for index_one in range(index_two + 1):
                pair_list.append((index_one, index_two, use_kin))
    return pair_list


def plain_body(coeffs, cell_map, potential, projectors, strengths, proj_atom, proj_chan):
    ga_count = lax.axis_size("ga")
    grid_len = potential.shape[0]
    planes = grid_len // ga_count
    band_local = coeffs.shape[1]
    total_pw = coeffs.shape[2] * ga_count
    device = lax.axis_index("ga")
    plane_num = cell_map // (grid_len * grid_len)
    y_index = cell_map // grid_len % grid_len
    z_index = cell_map % grid_len
    freq_x = signed_freq(device + ga_count * plane_num, grid_len)
    freq_y = signed_freq(y_index, grid_len)
    freq_z = signed_freq(z_index, grid_len)
    kinetic = kin_unit * (freq_x * freq_x + freq_y * freq_y + freq_z * freq_z).astype(jnp.float32)
    kin_weight = kinetic[None, None, :]
    slot_re = (plane_num * grid_len + y_index) * (2 * grid_len) + z_index
    slot_im = slot_re + grid_len
    cell_count = planes * grid_len * 2 * grid_len
    natural = jnp.arange(grid_len, dtype=jnp.int32)
    cyclic = natural % planes * ga_count + natural // planes
    cos_fwd, sin_fwd = wave_tables(grid_len, natural, natural, 1.0, 1.0)
    cos_back, sin_back = wave_tables(grid_len, natural, natural, -1.0, 1.0 / grid_len)
    z_forward = block_table(cos_fwd, sin_fwd)
    z_backward = block_table(cos_back, sin_back)
    xcos_fwd, xsin_fwd = wave_tables(grid_len, natural, cyclic, 1.0, 1.0)
    xcos_back, xsin_back = wave_tables(grid_len, cyclic, natural, -1.0, 1.0 / grid_len)
    doubled = jnp.concatenate([potential, potential], axis=-1)
    coupling = coupling_matrix(proj_atom, proj_chan, strengths)

    def real_space(grid_vals):
        grid_vals = mix_dim(grid_vals, xcos_fwd, xsin_fwd, "kj,bjyw->bkyw")
        grid_vals = grid_vals * doubled[None]
        grid_vals = mix_dim(grid_vals, xcos_back, xsin_back, "jk,bkyw->bjyw")
        return lax.all_to_all(grid_vals, "ga", split_axis=1, concat_axis=2, tiled=True)

    def local_part(vectors):
        item_count = vectors.shape[1]
        flat_grid = jnp.zeros((item_count, cell_count), jnp.float32)
        flat_grid = flat_grid.at[:, slot_re].set(vectors[0]).at[:, slot_im].set(vectors[1])
        grid_vals = mix_last(
            flat_grid.reshape(item_count, planes, grid_len, 2 * grid_len), z_forward
        )
        grid_vals = mix_dim(grid_vals, cos_fwd, sin_fwd, "ky,bpyw->bpkw")
        grid_vals = real_space(
            lax.all_to_all(grid_vals, "ga", split_axis=2, concat_axis=1, tiled=True)
        )
        grid_vals = mix_dim(grid_vals, cos_back, sin_back, "ky,bpyw->bpkw")
        flat_grid = mix_last(grid_vals, z_backward).reshape(item_count, cell_count)
        return jnp.stack([flat_grid[:, slot_re], flat_grid[:, slot_im]])

    def contract(first_part, second_part):
        return jnp.einsum("pg,bg->pb", first_part, second_part, precision=top_precision)

    def spread(weights, proj_table):
        return jnp.einsum("pb,pg->bg", weights, proj_table, precision=top_precision)

    def projected_part(vectors):
        proj_re = contract(projectors[0], vectors[0]) + contract(projectors[1], vectors[1])
        proj_im = contract(projectors[0], vectors[1]) - contract(projectors[1], vectors[0])
        proj_re, proj_im = lax.psum((proj_re, proj_im), "ga")
        mixed_re = jnp.dot(
            coupling,
            proj_re / total_pw,
            precision=top_precision,
            preferred_element_type=jnp.float32,
        )
        mixed_im = jnp.dot(
            coupling,
            proj_im / total_pw,
            precision=top_precision,
            preferred_element_type=jnp.float32,
        )
        out_re = spread(mixed_re, projectors[0]) - spread(mixed_im, projectors[1])
        out_im = spread(mixed_re, projectors[1]) + spread(mixed_im, projectors[0])
        return jnp.stack([out_re, out_im])

    def apply_h(vectors):
        return kin_weight * vectors + local_part(vectors) + projected_part(vectors)

    def gram_sums(basis, pair_list):
        stacked = []
        for index_one, index_two, use_kin in pair_list:
            stacked.append(
                band_dot(basis[index_one], basis[index_two], kin_weight if use_kin else 1.0)
            )
        summed = lax.psum(jnp.stack(stacked), "ga") / total_pw
        found = {}
        for slot_num, entry in enumerate(pair_list):
            index_one, index_two, use_kin = entry
            found[use_kin, index_one, index_two] = summed[slot_num]
            found[use_kin, index_two, index_one] = summed[slot_num]
        return found

    def realize(coef_map, basis):
        running = jnp.zeros_like(basis[0])
        for index_one, coef_a in coef_map.items():
            running = (
                running
                + per_band(jnp.zeros((band_local,), jnp.float32) + coef_a) * basis[index_one]
            )
        return running

    h_zero = apply_h(coeffs)
    basis = [coeffs, h_zero]
    gram_table = gram_sums(basis, new_pairs(0, 2, (False, True)))
    psi_map = {0: 1.0}
    ham_map = {1: 1.0}
    eps_zero = gram_form(gram_table, psi_map, ham_map, False) / (
        gram_form(gram_table, psi_map, psi_map, False) + small_eps
    )
    r_map = combine([(1.0, ham_map), (-eps_zero, psi_map)])
    level_zero = gram_form(gram_table, r_map, r_map, True) / (
        gram_form(gram_table, r_map, r_map, False) + small_eps
    )
    p_zero = precondition(realize(r_map, basis), kinetic, level_zero)
    g_zero = apply_h(p_zero)
    basis = [coeffs, h_zero, p_zero, g_zero]
    gram_table.update(gram_sums(basis, new_pairs(2, 4, (False, True))))
    q_map = combine([(1.0, {3: 1.0}), (-eps_zero, {2: 1.0})])
    lam_zero = -gram_form(gram_table, r_map, q_map, False) / (
        gram_form(gram_table, q_map, q_map, False) + small_eps
    )
    psi_one_map = combine([(1.0, psi_map), (lam_zero, {2: 1.0})])
    h_one_map = combine([(1.0, ham_map), (lam_zero, {3: 1.0})])
    eps_one = gram_form(gram_table, psi_one_map, h_one_map, False) / (
        gram_form(gram_table, psi_one_map, psi_one_map, False) + small_eps
    )
    r_one_map = combine([(1.0, h_one_map), (-eps_one, psi_one_map)])
    change_map = combine([(1.0, r_map), (-1.0, r_one_map)])
    weight_one = gram_form(gram_table, r_map, change_map, False) / (
        gram_form(gram_table, change_map, change_map, False) + small_eps
    )
    step_mid = weight_one * lam_zero
    psi_mid_map = combine([(1.0, psi_map), (step_mid, {2: 1.0})])
    h_mid_map = combine([(1.0, ham_map), (step_mid, {3: 1.0})])
    r_mid_map = combine([(1.0, r_map), (-weight_one, change_map)])
    eps_mid = gram_form(gram_table, psi_mid_map, h_mid_map, False) / (
        gram_form(gram_table, psi_mid_map, psi_mid_map, False) + small_eps
    )
    level_mid = gram_form(gram_table, r_mid_map, r_mid_map, True) / (
        gram_form(gram_table, r_mid_map, r_mid_map, False) + small_eps
    )
    p_one = precondition(realize(r_mid_map, basis), kinetic, level_mid)
    g_one = apply_h(p_one)
    basis = [coeffs, h_zero, p_zero, g_zero, p_one, g_one]
    gram_table.update(gram_sums(basis, new_pairs(4, 6, (False,))))
    q_one_map = combine([(1.0, {5: 1.0}), (-eps_mid, {4: 1.0})])
    lam_one = -gram_form(gram_table, r_mid_map, q_one_map, False) / (
        gram_form(gram_table, q_one_map, q_one_map, False) + small_eps
    )
    new_map = combine([(1.0, psi_mid_map), (lam_one, {4: 1.0})])
    ham_new_map = combine([(1.0, h_mid_map), (lam_one, {5: 1.0})])
    norm_new = gram_form(gram_table, new_map, new_map, False) + small_eps
    energy = gram_form(gram_table, new_map, ham_new_map, False) / norm_new
    resid_map = combine([(1.0, ham_new_map), (-energy, new_map)])
    residual_norm = gram_form(gram_table, resid_map, resid_map, False) / norm_new
    new_bands = realize(new_map, basis)
    new_ham = realize(ham_new_map, basis)
    blank_rows = jnp.zeros((2, band_local, band_local * lax.axis_size("band")), jnp.float32)
    first_row = jnp.int32(0)
    over_rows = blank_rows
    ham_rows = blank_rows
    piece_bands = lax.all_gather(new_bands, "band", axis=1, tiled=True)
    piece_ham = lax.all_gather(new_ham, "band", axis=1, tiled=True)
    over_rows = lax.dynamic_update_slice_in_dim(
        over_rows, pair_products(new_bands, piece_bands), first_row, 2
    )
    ham_rows = lax.dynamic_update_slice_in_dim(
        ham_rows, pair_products(new_bands, piece_ham), first_row, 2
    )
    over_rows, ham_rows = (over_rows, ham_rows)
    over_rows, ham_rows = lax.psum((over_rows, ham_rows), "ga")
    correlation = over_rows / total_pw
    subspace = ham_rows / total_pw
    return (new_bands, energy, residual_norm, correlation, subspace)


WIDE = 256
MESH = pl.DeviceIdType.MESH


def split_const(values):
    high = np.asarray(values, np.float32).astype(jnp.bfloat16)
    low = (values - high.astype(np.float64)).astype(np.float32).astype(jnp.bfloat16)
    return np.stack([high, low])


def const_tables(grid_len, group):
    planes = grid_len // group
    unit = 2.0 * np.pi / grid_len
    freq = np.arange(grid_len)
    y_real = np.arange(group)[:, None] * planes + np.arange(planes)[None, :]
    phase = unit * ((y_real[..., None] * freq) % grid_len)
    cos_y, sin_y = np.cos(phase), np.sin(phase)
    high, low = split_const(np.concatenate([
        cos_y[:, :8], sin_y[:, :8], cos_y[:, 8:], sin_y[:, 8:], -sin_y[:, 8:], cos_y[:, 8:]], axis=1))
    wave = np.concatenate([high, low], axis=2)
    theta = unit * (np.outer(freq, freq) % grid_len)
    turn = np.zeros((2, 128, 2, 128))
    turn[0, :grid_len, 0, :grid_len] = np.cos(theta)
    turn[0, :grid_len, 1, :grid_len] = np.sin(theta)
    turn[1, :grid_len, 0, :grid_len] = -np.sin(theta)
    turn[1, :grid_len, 1, :grid_len] = np.cos(theta)
    turn = turn.reshape(256, 256)
    zed = np.concatenate([split_const(turn), split_const(turn.T)], axis=0)
    return wave, zed


def two_parts(values):
    high = values.astype(jnp.bfloat16)
    low = (values - high.astype(jnp.float32)).astype(jnp.bfloat16)
    return high, low


def split_rows(values):
    high = values.astype(jnp.bfloat16).astype(jnp.float32)
    return jnp.concatenate([high, values - high], axis=0).astype(jnp.bfloat16)


def bdot(left, right):
    return jnp.dot(left, right, preferred_element_type=jnp.float32)


def bdot_t(left, right):
    return lax.dot_general(left, right, (((1,), (1,)), ((), ())), preferred_element_type=jnp.float32)


def total_of(values):
    return jnp.sum(jnp.sum(values, axis=0, keepdims=True), axis=1, keepdims=True)


def c_add(one, two):
    return one[0] + two[0], one[1] + two[1]


def c_sub(one, two):
    return one[0] - two[0], one[1] - two[1]


def c_turn(one, direction):
    return (-one[1], one[0]) if direction > 0 else (one[1], -one[0])


def c_mul(one, cos_val, sin_val):
    return one[0] * cos_val - one[1] * sin_val, one[0] * sin_val + one[1] * cos_val


def c_scale(one, factor):
    return one[0] * factor, one[1] * factor


def three_point(items, direction):
    total = c_add(items[1], items[2])
    side = c_scale(c_turn(c_sub(items[1], items[2]), direction), 0.8660254037844386)
    base = c_sub(items[0], c_scale(total, 0.5))
    return [c_add(items[0], total), c_add(base, side), c_sub(base, side)]


def four_point(items, direction):
    even, odd = c_add(items[0], items[2]), c_add(items[1], items[3])
    low, high = c_sub(items[0], items[2]), c_turn(c_sub(items[1], items[3]), direction)
    return [c_add(even, odd), c_add(low, high), c_sub(even, odd), c_sub(low, high)]


def eight_point(items, direction):
    even = four_point(items[0::2], direction)
    odd = four_point(items[1::2], direction)
    root = 0.7071067811865476
    turned = [
        odd[0],
        c_scale(c_add(odd[1], c_turn(odd[1], direction)), root),
        c_turn(odd[2], direction),
        c_scale(c_sub(c_turn(odd[3], direction), odd[3]), root),
    ]
    return [c_add(e, o) for e, o in zip(even, turned)] + [c_sub(e, o) for e, o in zip(even, turned)]


def twelve_point(items, direction):
    fours = [four_point([items[(4 * a + 3 * b) % 12] for b in range(4)], direction) for a in range(3)]
    threes = [three_point([fours[a][v] for a in range(3)], direction) for v in range(4)]
    return [threes[v % 4][v % 3] for v in range(12)]


def sweep_kernel(
    dims,
    coeffs_hbm, cell_hbm, potential_hbm, proj_hbm, strength_hbm, atom_hbm, chan_hbm,
    wave_hbm, zed_hbm,
    new_hbm, scal_hbm,
    hot_ref, fold_ref, group_ref, phase_ref, kin_ref, work_ref, left_ref,
    pot_ref, potential_ref, proj_ref, couple_ref, in_vec, out_vec, save_ref,
    strength_ref, atom_ref, chan_ref, wave_ref, zed_ref, new_ref, scal_ref, in_sem,
    ksend, krecv, xsend, xrecv, rsend, rrecv, hsend, hrecv, psend, precv,
    wsend, wrecv, nsend, nrecv, lsend, lrecv, csend, crecv,
    ks_sem, kr_sem, xs_sem, xr_sem, rs_sem, rr_sem, hs_sem, hr_sem, ps_sem, pr_sem,
    ws_sem, wr_sem, ns_sem, nr_sem, cs_sem, cr_sem,
):
    group, bands, planes, grid_len, total_pw, pw = dims
    slab = 2 * planes
    folds = planes // 2 - 1
    half = group // 2
    gap = 128 - grid_len
    splits = grid_len // gap
    tiles = pw // 128
    me = lax.axis_index("ga")
    band = lax.axis_index("band")
    sides = [1 - 2 * lax.rem(me // (1 << bit), 2) for bit in range(3)]

    def peer_of(mask):
        return me + sum(sides[bit] * ((mask // (1 << bit)) % 2) * (1 << bit) for bit in range(3))

    loads = [
        pltpu.make_async_copy(source, target, in_sem.at[k])
        for k, (source, target) in enumerate((
            (cell_hbm, ksend), (coeffs_hbm, xsend), (wave_hbm.at[me], wave_ref), (strength_hbm, strength_ref),
            (atom_hbm, atom_ref), (chan_hbm, chan_ref), (potential_hbm, potential_ref), (proj_hbm, proj_ref),
            (zed_hbm, zed_ref)))
    ]
    barrier = pltpu.get_barrier_semaphore()
    world = [(off, mask) for off in (2, 3, 1, 0) for mask in (7, 6, 5, 4, 3, 2, 1, 0) if off or mask]
    for off, mask in world:
        pl.semaphore_signal(barrier, inc=1, device_id={"band": lax.rem(band + off, bands), "ga": peer_of(mask)}, device_id_type=MESH)
    for load in loads:
        load.start()
    for load in loads[:2]:
        load.wait()

    far_first = (6, 7, 4, 5, 2, 3, 1)
    near_first = (2, 4, 3, 5, 6, 7, 1)

    def stage_of(mask):
        return (mask > 1) + (mask > 5)

    def wait_bytes(ref, sem):
        pltpu.make_async_copy(ref, ref, sem).wait()

    def spread_copy(mask, send, recv, send_sem, recv_sem):
        peer = peer_of(mask)
        return pltpu.make_async_remote_copy(
            src_ref=send, dst_ref=recv.at[me],
            send_sem=send_sem.at[0], recv_sem=recv_sem.at[0 if recv_sem.shape[0] == 1 else stage_of(mask)],
            device_id={"ga": peer}, device_id_type=MESH)

    def spread_start(order, send, recv, send_sem, recv_sem):
        for mask in order:
            spread_copy(mask, send, recv, send_sem, recv_sem).start()

    def spread_wait(send, recv, send_sem, recv_sem):
        wait_bytes(recv.at[pl.ds(0, group - 1)], recv_sem.at[0])
        wait_bytes(recv.at[pl.ds(0, group - 1)], send_sem.at[0])

    keys = (ksend, krecv, ks_sem, kr_sem)
    firsts = (xsend, xrecv, xs_sem, xr_sem)
    pl.semaphore_wait(barrier, group * bands - 1)
    spread_start(near_first, *keys)
    spread_start(near_first, *firsts)
    krecv[me] = ksend[...]
    xrecv[me] = xsend[...]

    def whole(values):
        return jnp.floor(values)

    def signed(values):
        return jnp.where(2.0 * values < grid_len, values, values - grid_len)

    def numbers(cells):
        plane = whole((cells + 0.5) * (1.0 / (grid_len * grid_len)))
        in_plane = cells - plane * (grid_len * grid_len)
        y_num = whole((in_plane + 0.5) * (1.0 / grid_len))
        return plane, y_num, in_plane - y_num * grid_len

    def cell_row(src):
        cell = krecv[src].astype(jnp.float32)
        return jnp.concatenate([cell[k:k + 1] for k in range(tiles)], axis=1)

    def kinetic(plane, y_num, z_num, device):
        f_x = signed(plane * group + device)
        f_y, f_z = signed(y_num), signed(z_num)
        return kin_unit * (f_x * f_x + f_y * f_y + f_z * f_z)

    def marks(numbers_row, count):
        wide_row = jnp.broadcast_to(numbers_row, (16, pw)).astype(jnp.bfloat16)
        row_id = lax.broadcasted_iota(jnp.int32, (16, pw), 0).astype(jnp.float32).astype(jnp.bfloat16)
        one, zero = jnp.ones((16, pw), jnp.bfloat16), jnp.zeros((16, pw), jnp.bfloat16)
        return [jnp.where(row_id + 16.0 * k == wide_row, one, zero) for k in range(count)]

    def build_source(src):
        plane, y_num, z_num = numbers(cell_row(src))
        pair = whole((plane + 0.5) * 0.5)
        piece = whole((z_num + 0.5) * (1.0 / gap))
        hole = (plane - 2.0 * folds) * splits + piece
        hole_pair = whole((hole + 0.5) * 0.5)
        main = plane < 2.0 * folds
        fold = jnp.where(main, pair, hole_pair)
        lane = jnp.where(
            main, (plane - 2.0 * pair) * 128.0 + z_num,
            (hole - 2.0 * hole_pair) * 128.0 + grid_len + z_num - gap * piece)
        group_ref[src] = fold
        fold_ref[src] = jnp.broadcast_to(fold, (16, pw)).astype(jnp.bfloat16)
        for k, rows in enumerate(marks(lane, WIDE // 16)):
            hot_ref[src, 16 * k:16 * (k + 1), :] = rows
        y_hot = marks(y_num, grid_len // 16)
        phase_ref[src] = bdot(wave_ref[...], jnp.concatenate(y_hot + y_hot, axis=0))

    def build_potential():
        pad = jnp.zeros((8, 128 - grid_len), jnp.float32)

        def put_tile(v, slot, block):
            pot_ref[v, slot] = jnp.concatenate([block * (1.0 / grid_len**3), pad], axis=1)

        def lines(x_real, first, count):
            return potential_ref[pl.ds(first * grid_len + x_real, count, stride=grid_len), :]

        for v in range(planes):
            for u in range(group):
                put_tile(v, u, lines(v + planes * u, 0, 8))
            for t in range(half):
                put_tile(v, group + t, jnp.concatenate([
                    lines(v + planes * 2 * t, 8, planes - 8), lines(v + planes * (2 * t + 1), 8, planes - 8)], axis=0))

    def build_coupling():
        atoms, chans = strength_ref.shape[0] // strength_ref.shape[1], strength_ref.shape[1]
        size = atoms * chans
        ident = atom_ref[...] * chans + chan_ref[...]
        hot = (lax.broadcasted_iota(jnp.int32, (size, ident.shape[1]), 0) == ident).astype(jnp.float32)
        row_at = lax.broadcasted_iota(jnp.int32, (size, size), 0)
        col_at = lax.broadcasted_iota(jnp.int32, (size, size), 1)
        tiled = jnp.concatenate([strength_ref[...]] * atoms, axis=1)
        same = (row_at // chans == col_at // chans).astype(jnp.float32)
        block = tiled * same
        block = 0.5 * (block + jnp.transpose(block))
        half = lax.dot_general(hot, block, (((0,), (0,)), ((), ())), precision=top_precision, preferred_element_type=jnp.float32)
        couple_ref[...] = jnp.dot(half, hot, precision=top_precision, preferred_element_type=jnp.float32)

    loads[2].wait()
    build_source(me)
    for load in loads[3:6]:
        load.wait()
    build_coupling()
    loads[6].wait()
    build_potential()
    loads[7].wait()
    loads[8].wait()
    for stage, masks in enumerate(((1,), (2, 3, 4, 5), (6, 7))):
        wait_bytes(krecv.at[pl.ds(0, len(masks))], kr_sem.at[stage])
        for mask in masks:
            build_source(peer_of(mask))
    wait_bytes(krecv.at[pl.ds(0, group - 1)], ks_sem.at[0])

    def stack_rows(pieces):
        return jnp.concatenate(pieces, axis=0)

    cells = stack_rows([cell_row(s) for s in range(group)])
    owner = lax.broadcasted_iota(jnp.int32, (group, pw), 0).astype(jnp.float32)
    kin_ref[...] = kinetic(*numbers(cells), owner)
    spread_wait(*firsts)
    for part in range(2):
        in_vec[0, part] = stack_rows([xrecv[s, part] for s in range(group)])

    upper = lax.broadcasted_iota(jnp.int32, (8, 128), 0) < 4
    lane_at = lax.broadcasted_iota(jnp.int32, (8, 128), 1)
    flip = jnp.where(upper, 1.0, -1.0).astype(jnp.float32)

    def swap_half(values):
        return pltpu.roll(values, 4, 0)

    def halves(low, high):
        return low if low == high else jnp.where(upper, low, high)

    def lane_turn(s, v, paired):
        angle = [2.0 * np.pi * ((k * v) % grid_len) / grid_len for k in (s, s + half)]
        cos_val, sin_val = [float(np.cos(a)) for a in angle], [float(np.sin(a)) for a in angle]
        if paired:
            return halves(*cos_val), halves(*sin_val)
        return cos_val[0], sin_val[0]

    def twist(item, s, v, paired, direction):
        if v == 0 or (s == 0 and not paired):
            return item
        cos_val, sin_val = lane_turn(s, v, paired)
        return c_mul(item, cos_val, sin_val if direction > 0 else -sin_val)

    def z_turn(tiles, which):
        stacked = jnp.concatenate([jnp.concatenate(list(t), axis=1) for t in tiles], axis=0)
        high, low = two_parts(stacked)
        out = bdot(high, zed_ref[which]) + bdot(low, zed_ref[which]) + bdot(high, zed_ref[which + 1])
        return [(out[8 * k:8 * k + 8, :128], out[8 * k:8 * k + 8, 128:]) for k in range(len(tiles))]

    def keep(slot, v, item):
        work_ref[0, v, slot] = item[0]
        work_ref[1, v, slot] = item[1]

    def kept(slot, v):
        return work_ref[0, v, slot], work_ref[1, v, slot]

    def own_row(ref, turn, part):
        return ref[turn, part, pl.ds(me, 1), :]

    def put(turn, src):
        v_re, v_im = in_vec[turn, 0, src:src + 1, :], in_vec[turn, 1, src:src + 1, :]
        cos_y, sin_y, mix_re, mix_im = [phase_ref[src, 8 * k:8 * k + 8, :] for k in range(4)]
        both = split_rows(jnp.concatenate([
            cos_y * v_re - sin_y * v_im, mix_re * v_re + mix_im * v_im, sin_y * v_re + cos_y * v_im], axis=0))
        pieces = []
        fold = fold_ref[src]
        blank = jnp.zeros((16, pw), jnp.bfloat16)
        for k in range(folds):
            hit = fold == float(k)
            for at in range(0, 2 * slab, 16):
                pieces.append(jnp.where(hit, both[at:at + 16], blank))
        out = bdot_t(jnp.concatenate(pieces, axis=0), hot_ref[src])
        tiles = []
        for k in range(folds):
            base = k * 2 * slab
            block = out[base:base + slab] + out[base + slab:base + 2 * slab]
            for at in (0, 128):
                tiles.append([block[8 * t:8 * t + 8, at:at + 128] for t in range(3)])
        for extra in range(planes - 2 * folds):
            joined = []
            for t in range(3):
                run = None
                for q in reversed(range(splits)):
                    moved = pltpu.roll(tiles[extra * splits + q][t], (q + 1) * gap, 1)
                    run = moved if run is None else jnp.where(lane_at < (q + 1) * gap, moved, run)
                joined.append(run)
            tiles.append(joined)
        return tiles

    def forward_turn(s, low, high):
        rest = [(
            jnp.where(upper, a[1], swap_half(b[1])), jnp.where(upper, swap_half(a[1]), b[1]),
        ) for a, b in zip(low, high)]
        turned = z_turn([(a[0], a[2]) for a in low] + [(b[0], b[2]) for b in high] + rest, 0)
        for k, (slot, first, paired) in enumerate(((s, s, False), (s + half, s + half, False), (group + s, s, True))):
            for v, item in enumerate(twelve_point(turned[k * planes:(k + 1) * planes], 1)):
                keep(slot, v, twist(item, first, v, paired, 1))

    def cross(item):
        return tuple(swap_half(x) + x * flip for x in item)

    def half_turn(item, s, direction):
        if s == 0:
            return item
        angle = 2.0 * np.pi * s / group
        return c_mul(item, halves(1.0, float(np.cos(angle))), direction * halves(0.0, float(np.sin(angle))))

    def middle(v):
        items = eight_point([kept(s, v) for s in range(group)], 1)
        items = [c_scale(item, pot_ref[v, u]) for u, item in enumerate(items)]
        for s, item in enumerate(eight_point(items, -1)):
            keep(s, v, twist(item, s, v, False, -1))
        items = four_point([half_turn(cross(kept(group + s, v)), s, 1) for s in range(half)], 1)
        items = [c_scale(item, pot_ref[v, group + t]) for t, item in enumerate(items)]
        for s, item in enumerate(four_point(items, -1)):
            keep(group + s, v, twist(cross(half_turn(item, s, -1)), s, v, True, -1))

    def backward_pair(s):
        spread = []
        for slot in (s, s + half, group + s):
            spread += twelve_point([kept(slot, v) for v in range(planes)], -1)
        turned = z_turn(spread, 2)
        low, high, rest = [turned[k * planes:(k + 1) * planes] for k in range(3)]
        low = [(a[0], jnp.where(upper, r[0], swap_half(r[1])), a[1]) for a, r in zip(low, rest)]
        high = [(b[0], jnp.where(upper, swap_half(r[0]), r[1]), b[1]) for b, r in zip(high, rest)]
        for dest, tiles in ((s, low), (s + half, high)):
            for hole in range((planes - 2 * folds) * splits):
                extra, q = 2 * folds + hole // splits, hole % splits
                tiles[hole] = tuple(
                    jnp.where(lane_at >= grid_len, pltpu.roll(tiles[extra][t], grid_len - q * gap, 1), tiles[hole][t])
                    for t in range(3))
            for k in range(folds):
                block = jnp.concatenate([jnp.concatenate(tiles[2 * k + m], axis=0) for m in range(2)], axis=1)
                left_ref[dest, k * 2 * slab:(k + 1) * 2 * slab, :] = split_rows(block)

    def partial_copy(turn, mask):
        return pltpu.make_async_remote_copy(
            src_ref=rsend.at[turn, mask], dst_ref=rrecv.at[turn, mask],
            send_sem=rs_sem.at[0], recv_sem=rr_sem.at[0],
            device_id={"ga": peer_of(mask)}, device_id_type=MESH)

    def take_tile(mask, at):
        return bdot(left_ref[peer_of(mask)], hot_ref[peer_of(mask), :, at:at + WIDE])

    def take_sum(turn, mask, at, out):
        dest = peer_of(mask)
        span = slice(at, at + WIDE)
        fold = group_ref[dest, :, span]
        chosen = out[:2 * slab]
        for k in range(1, folds):
            chosen = jnp.where(fold == float(k), out[k * 2 * slab:(k + 1) * 2 * slab], chosen)
        value = chosen[:slab] + chosen[slab:]
        first, mixed, last = [value[8 * k:8 * k + 8] for k in range(3)]
        cos_y, sin_y, mix_re, mix_im = [phase_ref[dest, 8 * k:8 * k + 8, span] for k in range(4)]
        back_re = cos_y * first + sin_y * last + mix_re * mixed
        back_im = cos_y * last - sin_y * first + mix_im * mixed
        for part, back in enumerate((back_re, back_im)):
            rsend[turn, mask, part:part + 1, span] = jnp.sum(back, axis=0, keepdims=True)

    def take_all(turn):
        order = ((6, 7), (4, 5), (2, 3), (1, 0))
        units = [(masks, mask, at) for masks in order for mask in masks for at in range(0, pw, WIDE)]
        lag = 6
        pending = []
        for unit in units + [None] * lag:
            if unit:
                pending.append((unit, take_tile(*unit[1:])))
            if len(pending) > lag or not unit:
                (masks, mask, at), out = pending.pop(0)
                take_sum(turn, mask, at, out)
                if mask == masks[-1] and at + WIDE == pw:
                    for ready in masks:
                        if ready:
                            partial_copy(turn, ready).start()

    def all_sum(local, send, recv, send_sem, recv_sem):
        send[...] = local
        recv[me] = local
        spread_start(far_first, send, recv, send_sem, recv_sem)

    def all_sum_end(send, recv, send_sem, recv_sem):
        spread_wait(send, recv, send_sem, recv_sem)
        running = recv[0]
        for dev in range(1, group):
            running = running + recv[dev]
        return running

    def project(turn):
        found = []
        for part in range(2):
            row = own_row(in_vec, turn, part)
            running = proj_ref[:, :128] * row[:, :128]
            for at in range(128, pw, 128):
                running = running + proj_ref[:, at:at + 128] * row[:, at:at + 128]
            found.append(jnp.sum(jnp.transpose(running), axis=0, keepdims=True))
        return jnp.concatenate(found, axis=0)

    def nonlocal_rows(sums):
        half = sums.shape[1] // 2
        pair = jnp.concatenate([
            sums[0:1, :half] + sums[1:2, half:], sums[1:2, :half] - sums[0:1, half:]], axis=0)
        mixed = jnp.dot(pair, couple_ref[...], precision=top_precision, preferred_element_type=jnp.float32)
        m_re, m_im = mixed[0:1], mixed[1:2]
        found = []
        for row in (jnp.concatenate([m_re, -m_im], axis=1), jnp.concatenate([m_im, m_re], axis=1)):
            column = jnp.transpose(jnp.broadcast_to(row, (2 * half, 128)))
            found.append(jnp.concatenate([
                jnp.sum(proj_ref[:, at:at + 128] * column, axis=0, keepdims=True) for at in range(0, pw, 128)], axis=1))
        return jnp.concatenate(found, axis=0)

    def apply_h(turn):
        sums = (psend.at[turn], precv.at[turn], ps_sem, pr_sem)
        placed = []
        for s in range(half):
            placed.append((s, put(turn, s), put(turn, s + half)))
            if s:
                forward_turn(*placed.pop(0))
        forward_turn(*placed.pop(0))
        for v in range(planes):
            middle(v)
        for s in range(half):
            backward_pair(s)
        all_sum(project(turn), *sums)
        take_all(turn)
        start = nonlocal_rows(all_sum_end(*sums) * (1.0 / total_pw))
        own_kin = kin_ref[pl.ds(me, 1), :]
        start = start + own_kin * jnp.concatenate([own_row(in_vec, turn, 0), own_row(in_vec, turn, 1)], axis=0)
        running = start + rsend[turn, 0]
        wait_bytes(rrecv.at[turn, pl.ds(1, group - 1)], rr_sem.at[0])
        wait_bytes(rrecv.at[turn, pl.ds(1, group - 1)], rs_sem.at[0])
        for mask in range(1, group):
            running = running + rrecv[turn, mask]
        hsend[turn] = running
        return running

    def share_h(turn):
        out = (hsend.at[turn], hrecv.at[turn], hs_sem, hr_sem)
        spread_start(far_first, *out)
        hrecv[turn, me] = hsend[turn]
        spread_wait(*out)
        for part in range(2):
            out_vec[turn, part] = stack_rows([hrecv[turn, s, part:part + 1] for s in range(group)])

    def vector(index):
        ref = out_vec if index % 2 else in_vec
        return ref[index // 2]

    def gram_sums(pair_list):
        found = {}
        for one, two, use_kin in pair_list:
            left, right = vector(one), vector(two)
            product = left[0] * right[0] + left[1] * right[1]
            value = total_of(product * kin_ref[...] if use_kin else product) * (1.0 / total_pw)
            found[use_kin, one, two] = value
            found[use_kin, two, one] = value
        return found

    def realize(coef_map, basis):
        running = 0.0
        for index, coef in coef_map.items():
            running = running + (basis(index) if isinstance(coef, float) and coef == 1.0 else coef * basis(index))
        return running

    def smooth(residual, level):
        kin = kin_ref[...]
        ratio = kin / (1.5 * level + 1.0)
        poly = 27.0 + ratio * (18.0 + ratio * (12.0 + 8.0 * ratio))
        square = ratio * ratio
        return residual * (poly / (poly + 16.0 * square * square))

    def save(names, slot):
        for k, value in enumerate(names):
            save_ref[slot + k:slot + k + 1, :] = jnp.broadcast_to(value, (1, 128))

    def load_saved(slot):
        return save_ref[slot:slot + 1, 0:1]

    def first_step(gram):
        psi, ham = {0: 1.0}, {1: 1.0}
        eps_zero = gram_form(gram, psi, ham, False) / (gram_form(gram, psi, psi, False) + small_eps)
        return psi, ham, eps_zero, combine([(1.0, ham), (-eps_zero, psi)])

    def second_step(gram):
        psi, ham, eps_zero, r_map = first_step(gram)
        q_map = combine([(1.0, {3: 1.0}), (-eps_zero, {2: 1.0})])
        lam_zero = -gram_form(gram, r_map, q_map, False) / (gram_form(gram, q_map, q_map, False) + small_eps)
        psi_one = combine([(1.0, psi), (lam_zero, {2: 1.0})])
        h_one = combine([(1.0, ham), (lam_zero, {3: 1.0})])
        eps_one = gram_form(gram, psi_one, h_one, False) / (gram_form(gram, psi_one, psi_one, False) + small_eps)
        r_one = combine([(1.0, h_one), (-eps_one, psi_one)])
        change = combine([(1.0, r_map), (-1.0, r_one)])
        weight = gram_form(gram, r_map, change, False) / (gram_form(gram, change, change, False) + small_eps)
        step = weight * lam_zero
        psi_mid = combine([(1.0, psi), (step, {2: 1.0})])
        h_mid = combine([(1.0, ham), (step, {3: 1.0})])
        r_mid = combine([(1.0, r_map), (-weight, change)])
        eps_mid = gram_form(gram, psi_mid, h_mid, False) / (gram_form(gram, psi_mid, psi_mid, False) + small_eps)
        return psi_mid, h_mid, r_mid, eps_mid, step

    first_pairs = new_pairs(0, 2, (False, True))
    second_pairs = new_pairs(2, 4, (False, True))
    third_pairs = new_pairs(4, 5, (False,))
    last_pairs = new_pairs(5, 6, (False,))
    gram_pairs = first_pairs + second_pairs + third_pairs
    lane_id = lax.broadcasted_iota(jnp.int32, (1, 128), 1)

    def swap(which, send, recv, off):
        return pltpu.make_async_remote_copy(
            src_ref=send, dst_ref=recv.at[band],
            send_sem=ns_sem.at[which], recv_sem=nr_sem.at[which],
            device_id={"band": lax.rem(band + off, bands)}, device_id_type=MESH)

    def share(which, send, recv, values):
        send[...] = values
        recv[band] = values
        for off in range(1, bands):
            swap(which, send, recv, off).start()

    def share_end(which, send, recv):
        wait_bytes(recv.at[pl.ds(0, bands - 1)], nr_sem.at[which])
        wait_bytes(recv.at[pl.ds(0, bands - 1)], ns_sem.at[which])

    def own(index):
        ref = out_vec if index % 2 else in_vec
        return jnp.concatenate([own_row(ref, index // 2, 0), own_row(ref, index // 2, 1)], axis=0)

    def turn_step(turn, carry):
        apply_h(turn)

        @pl.when(turn == 0)
        def _():
            share_h(0)
            gram = gram_sums(first_pairs)
            save([gram[kind, one, two] for one, two, kind in first_pairs], 0)
            r_map = first_step(gram)[3]
            level = gram_form(gram, r_map, r_map, True) / (gram_form(gram, r_map, r_map, False) + small_eps)
            p_zero = smooth(realize(r_map, vector), level)
            in_vec[1] = p_zero

        @pl.when(turn == 1)
        def _():
            share_h(1)
            gram = gram_sums(second_pairs)
            for k, (one, two, kind) in enumerate(first_pairs):
                gram[kind, one, two] = gram[kind, two, one] = load_saved(k)
            psi_mid, h_mid, r_mid, eps_mid, step = second_step(gram)
            level = gram_form(gram, r_mid, r_mid, True) / (gram_form(gram, r_mid, r_mid, False) + small_eps)
            p_one = smooth(realize(r_mid, vector), level)
            in_vec[2] = p_one
            share(0, nsend, nrecv, jnp.stack([realize(psi_mid, own), own(4), realize(h_mid, own)]))
            gram.update(gram_sums(third_pairs))
            packed = jnp.zeros((1, 128), jnp.float32)
            for k, (one, two, kind) in enumerate(gram_pairs):
                packed = jnp.where(lane_id == k, gram[kind, one, two], packed)
            share(1, lsend, lrecv, packed)

        return carry

    lax.fori_loop(0, 3, turn_step, 0)

    g_own = hsend[2]

    def own_last(index):
        return g_own if index == 5 else own(index)

    def world_copy(off, mask):
        return pltpu.make_async_remote_copy(
            src_ref=wsend, dst_ref=wrecv.at[band * group + me],
            send_sem=ws_sem.at[0], recv_sem=wr_sem.at[0],
            device_id={"band": lax.rem(band + off, bands), "ga": peer_of(mask)}, device_id_type=MESH)

    local = jnp.zeros((1, 128), jnp.float32)
    for k, (one, two, kind) in enumerate(last_pairs):
        local = jnp.where(lane_id == k, total_of(own_last(one) * g_own), local)
    wsend[...] = local
    for off, mask in world:
        world_copy(off, mask).start()
    wrecv[band * group + me] = local

    share_end(0, nsend, nrecv)
    others = [[stack_rows([nrecv[o, which, part:part + 1] for o in range(bands)]) for part in range(2)] for which in range(3)]
    mine = [[nsend[which, part:part + 1] for part in range(2)] for which in range(3)] + [[g_own[0:1], g_own[1:2]]]

    def joined(first, second):
        return [jnp.concatenate([first[part], second[part]], axis=0) for part in range(2)]

    def twice(first, second):
        return [jnp.concatenate([jnp.broadcast_to(first[part], (bands, pw)), jnp.broadcast_to(second[part], (bands, pw))], axis=0) for part in range(2)]

    column_id = lax.broadcasted_iota(jnp.int32, (2 * bands, 128), 1)
    local = jnp.zeros((2 * bands, 128), jnp.float32)
    slot = 0
    for o_row, m_rows in (
        (joined(others[0], others[1]), (twice(mine[0], mine[0]), twice(mine[1], mine[1]))),
        (joined(others[2], others[1]), (twice(mine[0], mine[2]), twice(mine[1], mine[3]))),
    ):
        for m_re, m_im in m_rows:
            for product in (m_re * o_row[0] + m_im * o_row[1], m_re * o_row[1] - m_im * o_row[0]):
                local = jnp.where(column_id == slot, jnp.sum(product, axis=1, keepdims=True), local)
                slot += 1
    crossed = (csend, crecv, cs_sem, cr_sem)
    all_sum(local, *crossed)

    share_end(1, lsend, lrecv)
    early = stack_rows([lrecv[o] for o in range(bands)])
    gram = {}
    for k, (one, two, kind) in enumerate(gram_pairs):
        gram[kind, one, two] = gram[kind, two, one] = early[:, k:k + 1]
    psi_mid, h_mid, r_mid, eps_mid, step = second_step(gram)
    wait_bytes(wrecv.at[pl.ds(0, group * bands - 1)], wr_sem.at[0])
    late = []
    for other in range(bands):
        running = wrecv[other * group]
        for dev in range(1, group):
            running = running + wrecv[other * group + dev]
        late.append(running)
    late = stack_rows(late) * (1.0 / total_pw)
    for k, (one, two, kind) in enumerate(last_pairs):
        gram[kind, one, two] = gram[kind, two, one] = late[:, k:k + 1]
    q_one = combine([(1.0, {5: 1.0}), (-eps_mid, {4: 1.0})])
    lam_one = -gram_form(gram, r_mid, q_one, False) / (gram_form(gram, q_one, q_one, False) + small_eps)
    own_band = lax.broadcasted_iota(jnp.int32, (bands, 1), 0) == band

    def pick(column):
        return jnp.sum(jnp.where(own_band, column, 0.0), axis=0, keepdims=True)

    own_lam = pick(lam_one)
    new_ref[...] = nsend[0] + own_lam * nsend[1]
    stores = [pltpu.make_async_copy(new_ref, new_hbm, in_sem.at[0]), pltpu.make_async_copy(scal_ref, scal_hbm, in_sem.at[1])]
    stores[0].start()
    new_map = combine([(1.0, psi_mid), (lam_one, {4: 1.0})])
    ham_new = combine([(1.0, h_mid), (lam_one, {5: 1.0})])
    norm_new = gram_form(gram, new_map, new_map, False) + small_eps
    energy = gram_form(gram, new_map, ham_new, False) / norm_new
    resid = combine([(1.0, ham_new), (-energy, new_map)])
    resid_norm = gram_form(gram, resid, resid, False) / norm_new
    summed = all_sum_end(*crossed) * (1.0 / total_pw)
    mixed = summed[:bands] + lam_one * summed[bands:]
    result = mixed + own_lam * pltpu.roll(mixed, 126, 1)
    scal_ref[...] = jnp.concatenate([
        result, jnp.broadcast_to(pick(energy), (1, 128)), jnp.broadcast_to(pick(resid_norm), (1, 128)),
        jnp.zeros((scal_ref.shape[0] - bands - 2, 128), jnp.float32)], axis=0)
    stores[1].start()
    wait_bytes(wrecv.at[pl.ds(0, group * bands - 1)], ws_sem.at[0])
    for store in stores:
        store.wait()


def finish_kernel(bands, new_ref, scal_ref, bands_ref, energy_ref, norm_ref, corr_ref, sub_ref):
    bands_ref[:, 0, :] = new_ref[...]
    lane = lax.broadcasted_iota(jnp.int32, (1, bands), 1)
    for ref, base in ((corr_ref, 0), (sub_ref, 4)):
        for part in range(2):
            row = jnp.zeros((1, bands), jnp.float32)
            for other in range(bands):
                at = base + part
                row = jnp.where(lane == other, scal_ref[other:other + 1, at:at + 1], row)
            ref[part] = row
    energy_ref[0] = scal_ref[bands, 0]
    norm_ref[0] = scal_ref[bands + 1, 0]


def kernel_body(coeffs, cell_map, potential, projectors, strengths, proj_atom, proj_chan):
    group = lax.axis_size("ga")
    bands = lax.axis_size("band")
    grid_len = potential.shape[0]
    planes = grid_len // group
    pw = coeffs.shape[2]
    total_pw = pw * group
    slab = 2 * planes
    folds = planes // 2 - 1
    tile_count = group + group // 2
    proj_rows = 2 * projectors.shape[1]
    tables = [jnp.asarray(t) for t in const_tables(grid_len, group)]
    dma = pltpu.SemaphoreType.DMA
    vmem = pl.BlockSpec(memory_space=pltpu.VMEM)
    far = pl.BlockSpec(memory_space=pl.ANY)
    f32, b16 = jnp.float32, jnp.bfloat16
    scal_rows = 8 * (-(-(bands + 2) // 8))
    new, scal = pl.pallas_call(
        functools.partial(sweep_kernel, (group, bands, planes, grid_len, total_pw, pw)),
        out_shape=(
            jax.ShapeDtypeStruct((2, pw), f32),
            jax.ShapeDtypeStruct((scal_rows, 128), f32),
        ),
        in_specs=[far] * 9,
        out_specs=(far, far),
        scratch_shapes=[
            pltpu.VMEM((group, WIDE, pw), b16),
            pltpu.VMEM((group, 16, pw), b16),
            pltpu.VMEM((group, 1, pw), f32),
            pltpu.VMEM((group, 32, pw), f32),
            pltpu.VMEM((group, pw), f32),
            pltpu.VMEM((2, planes, tile_count, 8, 128), f32),
            pltpu.VMEM((group, folds * 2 * slab, WIDE), b16),
            pltpu.VMEM((planes, tile_count, 8, 128), f32),
            pltpu.VMEM((planes * grid_len, grid_len), f32),
            pltpu.VMEM((proj_rows, pw), f32),
            pltpu.VMEM((proj_rows // 2, proj_rows // 2), f32),
            pltpu.VMEM((3, 2, group, pw), f32),
            pltpu.VMEM((2, 2, group, pw), f32),
            pltpu.VMEM((24, 128), f32),
            pltpu.VMEM((strengths.shape[0] * strengths.shape[1], strengths.shape[2]), f32),
            pltpu.VMEM((1, proj_atom.shape[0]), jnp.int32), pltpu.VMEM((1, proj_chan.shape[0]), jnp.int32),
            pltpu.VMEM(tables[0].shape[1:], b16), pltpu.VMEM(tables[1].shape, b16),
            pltpu.VMEM((2, pw), f32), pltpu.VMEM((scal_rows, 128), f32),
            dma((9,)),
            pltpu.VMEM((pw // 128, 128), jnp.int32), pltpu.VMEM((group, pw // 128, 128), jnp.int32),
            pltpu.VMEM((2, 1, pw), f32), pltpu.VMEM((group, 2, 1, pw), f32),
            pltpu.VMEM((3, group, 2, pw), f32), pltpu.VMEM((3, group, 2, pw), f32),
            pltpu.VMEM((3, 2, pw), f32), pltpu.VMEM((2, group, 2, pw), f32),
            pltpu.VMEM((3, 2, proj_rows), f32), pltpu.VMEM((3, group, 2, proj_rows), f32),
            pltpu.VMEM((1, 128), f32), pltpu.VMEM((bands * group, 1, 128), f32),
            pltpu.VMEM((3, 2, pw), f32), pltpu.VMEM((bands, 3, 2, pw), f32),
            pltpu.VMEM((1, 128), f32), pltpu.VMEM((bands, 1, 128), f32),
            pltpu.VMEM((2 * bands, 128), f32), pltpu.VMEM((group, 2 * bands, 128), f32),
            dma((1,)), dma((3,)), dma((1,)), dma((1,)), dma((1,)), dma((1,)), dma((1,)), dma((1,)),
            dma((1,)), dma((1,)), dma((1,)), dma((1,)), dma((2,)), dma((2,)), dma((1,)), dma((1,)),
        ],
        compiler_params=pltpu.CompilerParams(
            collective_id=0, has_side_effects=True, vmem_limit_bytes=60 * 1024 * 1024
        ),
        name="sweeps",
    )(
        coeffs, cell_map.reshape(-1, 128), jnp.swapaxes(potential, 0, 1).reshape(planes * grid_len, grid_len),
        projectors.reshape(proj_rows, pw), strengths.reshape(-1, strengths.shape[2]),
        proj_atom.reshape(1, -1), proj_chan.reshape(1, -1), *tables,
    )

    smem = pl.BlockSpec(memory_space=pltpu.SMEM)
    return pl.pallas_call(
        functools.partial(finish_kernel, bands),
        out_shape=(
            jax.ShapeDtypeStruct((2, 1, pw), f32),
            jax.ShapeDtypeStruct((1,), f32),
            jax.ShapeDtypeStruct((1,), f32),
            jax.ShapeDtypeStruct((2, 1, bands), f32),
            jax.ShapeDtypeStruct((2, 1, bands), f32),
        ),
        in_specs=[vmem, vmem],
        out_specs=(vmem, smem, smem, vmem, vmem),
        name="finish",
    )(new, scal)


def body(coeffs, cell_map, potential, projectors, strengths, proj_atom, proj_chan):
    group = lax.axis_size("ga")
    grid_len = potential.shape[0]
    planes = grid_len // group
    fits = (
        group == 8
        and planes == 12
        and coeffs.shape[1] == 1
        and coeffs.shape[2] % 256 == 0
        and 2 * projectors.shape[1] == 128
    )
    chosen = kernel_body if fits else plain_body
    return chosen(coeffs, cell_map, potential, projectors, strengths, proj_atom, proj_chan)


def solution(mesh):
    placed = (
        P(None, "band", "ga"),
        P("ga"),
        P(None, "ga", None),
        P(None, None, "ga"),
        P(),
        P(),
        P(),
    )
    return jax.shard_map(
        body,
        mesh=mesh,
        in_specs=placed,
        out_specs=(
            P(None, "band", "ga"),
            P("band"),
            P("band"),
            P(None, "band", None),
            P(None, "band", None),
        ),
        check_vma=False,
    )
```

```python
import functools

import jax
import jax.numpy as jnp
import numpy as np
from jax import lax
from jax.experimental import pallas as pl
from jax.experimental.pallas import tpu as pltpu
from jax.sharding import PartitionSpec as P

top_precision = lax.Precision.HIGHEST
kin_unit = 0.02
small_eps = 1e-06


def signed_freq(index_arr, grid_len):
    return jnp.where(index_arr < grid_len // 2, index_arr, index_arr - grid_len)


def wave_tables(grid_len, row_freq, col_freq, sign_val, factor):
    phase = row_freq[:, None] * col_freq[None, :] % grid_len
    angle = 2.0 * jnp.pi / grid_len * phase.astype(jnp.float32)
    return (jnp.cos(angle) * factor, jnp.sin(angle) * (sign_val * factor))


def block_table(cos_table, sin_table):
    upper = jnp.concatenate([cos_table, sin_table], axis=1)
    lower = jnp.concatenate([-sin_table, cos_table], axis=1)
    return jnp.concatenate([upper, lower], axis=0)


def quarter_turn(grid_vals):
    half_len = grid_vals.shape[-1] // 2
    return jnp.concatenate([-grid_vals[..., half_len:], grid_vals[..., :half_len]], axis=-1)


def mix_dim(grid_vals, cos_table, sin_table, pattern):
    direct = jnp.einsum(pattern, cos_table, grid_vals, precision=top_precision)
    turned = jnp.einsum(pattern, sin_table, quarter_turn(grid_vals), precision=top_precision)
    return direct + turned


def mix_last(grid_vals, table_full):
    row_width = grid_vals.shape[-1]
    product = jnp.dot(
        grid_vals.reshape(-1, row_width),
        table_full,
        precision=top_precision,
        preferred_element_type=jnp.float32,
    )
    return product.reshape(grid_vals.shape)


def band_dot(left_vec, right_vec, weight):
    return jnp.sum(left_vec * right_vec * weight, axis=(0, 2))


def per_band(values):
    return values[None, :, None]


def pair_products(left_vec, right_vec):

    def contract(first_part, second_part):
        return jnp.einsum("bg,cg->bc", first_part, second_part, precision=top_precision)

    real_part = contract(left_vec[0], right_vec[0]) + contract(left_vec[1], right_vec[1])
    imag_part = contract(left_vec[0], right_vec[1]) - contract(left_vec[1], right_vec[0])
    return jnp.stack([real_part, imag_part])


def precondition(residual, kinetic, kin_level):
    x_ratio = kinetic[None, :] / (1.5 * kin_level[:, None] + 1.0)
    numer_poly = 27.0 + x_ratio * (18.0 + x_ratio * (12.0 + 8.0 * x_ratio))
    square = x_ratio * x_ratio
    return residual * (numer_poly / (numer_poly + 16.0 * square * square))[None]


def coupling_matrix(proj_atom, proj_chan, strengths):
    atom_count = strengths.shape[0]
    chan_count = strengths.shape[1]
    symmetric = 0.5 * (strengths + jnp.swapaxes(strengths, 1, 2))
    atom_hot = (proj_atom[:, None] == jnp.arange(atom_count, dtype=jnp.int32)[None, :]).astype(
        jnp.float32
    )
    chan_hot = (proj_chan[:, None] == jnp.arange(chan_count, dtype=jnp.int32)[None, :]).astype(
        jnp.float32
    )
    rows_d = jnp.einsum("pa,pc,acd->pd", atom_hot, chan_hot, symmetric, precision=top_precision)
    same_atom = jnp.dot(
        atom_hot, atom_hot.T, precision=top_precision, preferred_element_type=jnp.float32
    )
    return same_atom * jnp.dot(
        rows_d, chan_hot.T, precision=top_precision, preferred_element_type=jnp.float32
    )


def combine(term_list):
    merged = {}
    for scalar, coef_map in term_list:
        for index_one, coef_a in coef_map.items():
            merged[index_one] = merged.get(index_one, 0.0) + scalar * coef_a
    return merged


def gram_form(gram_table, left_map, right_map, use_kin):
    running = 0.0
    for index_one, coef_a in left_map.items():
        for index_two, coef_b in right_map.items():
            running = running + coef_a * coef_b * gram_table[use_kin, index_one, index_two]
    return running


def new_pairs(first_new, last_new, kinds):
    pair_list = []
    for use_kin in kinds:
        for index_two in range(first_new, last_new):
            for index_one in range(index_two + 1):
                pair_list.append((index_one, index_two, use_kin))
    return pair_list


def plain_body(coeffs, cell_map, potential, projectors, strengths, proj_atom, proj_chan):
    ga_count = lax.axis_size("ga")
    grid_len = potential.shape[0]
    planes = grid_len // ga_count
    band_local = coeffs.shape[1]
    total_pw = coeffs.shape[2] * ga_count
    device = lax.axis_index("ga")
    plane_num = cell_map // (grid_len * grid_len)
    y_index = cell_map // grid_len % grid_len
    z_index = cell_map % grid_len
    freq_x = signed_freq(device + ga_count * plane_num, grid_len)
    freq_y = signed_freq(y_index, grid_len)
    freq_z = signed_freq(z_index, grid_len)
    kinetic = kin_unit * (freq_x * freq_x + freq_y * freq_y + freq_z * freq_z).astype(jnp.float32)
    kin_weight = kinetic[None, None, :]
    slot_re = (plane_num * grid_len + y_index) * (2 * grid_len) + z_index
    slot_im = slot_re + grid_len
    cell_count = planes * grid_len * 2 * grid_len
    natural = jnp.arange(grid_len, dtype=jnp.int32)
    cyclic = natural % planes * ga_count + natural // planes
    cos_fwd, sin_fwd = wave_tables(grid_len, natural, natural, 1.0, 1.0)
    cos_back, sin_back = wave_tables(grid_len, natural, natural, -1.0, 1.0 / grid_len)
    z_forward = block_table(cos_fwd, sin_fwd)
    z_backward = block_table(cos_back, sin_back)
    xcos_fwd, xsin_fwd = wave_tables(grid_len, natural, cyclic, 1.0, 1.0)
    xcos_back, xsin_back = wave_tables(grid_len, cyclic, natural, -1.0, 1.0 / grid_len)
    doubled = jnp.concatenate([potential, potential], axis=-1)
    coupling = coupling_matrix(proj_atom, proj_chan, strengths)

    def real_space(grid_vals):
        grid_vals = mix_dim(grid_vals, xcos_fwd, xsin_fwd, "kj,bjyw->bkyw")
        grid_vals = grid_vals * doubled[None]
        grid_vals = mix_dim(grid_vals, xcos_back, xsin_back, "jk,bkyw->bjyw")
        return lax.all_to_all(grid_vals, "ga", split_axis=1, concat_axis=2, tiled=True)

    def local_part(vectors):
        item_count = vectors.shape[1]
        flat_grid = jnp.zeros((item_count, cell_count), jnp.float32)
        flat_grid = flat_grid.at[:, slot_re].set(vectors[0]).at[:, slot_im].set(vectors[1])
        grid_vals = mix_last(
            flat_grid.reshape(item_count, planes, grid_len, 2 * grid_len), z_forward
        )
        grid_vals = mix_dim(grid_vals, cos_fwd, sin_fwd, "ky,bpyw->bpkw")
        grid_vals = real_space(
            lax.all_to_all(grid_vals, "ga", split_axis=2, concat_axis=1, tiled=True)
        )
        grid_vals = mix_dim(grid_vals, cos_back, sin_back, "ky,bpyw->bpkw")
        flat_grid = mix_last(grid_vals, z_backward).reshape(item_count, cell_count)
        return jnp.stack([flat_grid[:, slot_re], flat_grid[:, slot_im]])

    def contract(first_part, second_part):
        return jnp.einsum("pg,bg->pb", first_part, second_part, precision=top_precision)

    def spread(weights, proj_table):
        return jnp.einsum("pb,pg->bg", weights, proj_table, precision=top_precision)

    def projected_part(vectors):
        proj_re = contract(projectors[0], vectors[0]) + contract(projectors[1], vectors[1])
        proj_im = contract(projectors[0], vectors[1]) - contract(projectors[1], vectors[0])
        proj_re, proj_im = lax.psum((proj_re, proj_im), "ga")
        mixed_re = jnp.dot(
            coupling,
            proj_re / total_pw,
            precision=top_precision,
            preferred_element_type=jnp.float32,
        )
        mixed_im = jnp.dot(
            coupling,
            proj_im / total_pw,
            precision=top_precision,
            preferred_element_type=jnp.float32,
        )
        out_re = spread(mixed_re, projectors[0]) - spread(mixed_im, projectors[1])
        out_im = spread(mixed_re, projectors[1]) + spread(mixed_im, projectors[0])
        return jnp.stack([out_re, out_im])

    def apply_h(vectors):
        return kin_weight * vectors + local_part(vectors) + projected_part(vectors)

    def gram_sums(basis, pair_list):
        stacked = []
        for index_one, index_two, use_kin in pair_list:
            stacked.append(
                band_dot(basis[index_one], basis[index_two], kin_weight if use_kin else 1.0)
            )
        summed = lax.psum(jnp.stack(stacked), "ga") / total_pw
        found = {}
        for slot_num, entry in enumerate(pair_list):
            index_one, index_two, use_kin = entry
            found[use_kin, index_one, index_two] = summed[slot_num]
            found[use_kin, index_two, index_one] = summed[slot_num]
        return found

    def realize(coef_map, basis):
        running = jnp.zeros_like(basis[0])
        for index_one, coef_a in coef_map.items():
            running = (
                running
                + per_band(jnp.zeros((band_local,), jnp.float32) + coef_a) * basis[index_one]
            )
        return running

    h_zero = apply_h(coeffs)
    basis = [coeffs, h_zero]
    gram_table = gram_sums(basis, new_pairs(0, 2, (False, True)))
    psi_map = {0: 1.0}
    ham_map = {1: 1.0}
    eps_zero = gram_form(gram_table, psi_map, ham_map, False) / (
        gram_form(gram_table, psi_map, psi_map, False) + small_eps
    )
    r_map = combine([(1.0, ham_map), (-eps_zero, psi_map)])
    level_zero = gram_form(gram_table, r_map, r_map, True) / (
        gram_form(gram_table, r_map, r_map, False) + small_eps
    )
    p_zero = precondition(realize(r_map, basis), kinetic, level_zero)
    g_zero = apply_h(p_zero)
    basis = [coeffs, h_zero, p_zero, g_zero]
    gram_table.update(gram_sums(basis, new_pairs(2, 4, (False, True))))
    q_map = combine([(1.0, {3: 1.0}), (-eps_zero, {2: 1.0})])
    lam_zero = -gram_form(gram_table, r_map, q_map, False) / (
        gram_form(gram_table, q_map, q_map, False) + small_eps
    )
    psi_one_map = combine([(1.0, psi_map), (lam_zero, {2: 1.0})])
    h_one_map = combine([(1.0, ham_map), (lam_zero, {3: 1.0})])
    eps_one = gram_form(gram_table, psi_one_map, h_one_map, False) / (
        gram_form(gram_table, psi_one_map, psi_one_map, False) + small_eps
    )
    r_one_map = combine([(1.0, h_one_map), (-eps_one, psi_one_map)])
    change_map = combine([(1.0, r_map), (-1.0, r_one_map)])
    weight_one = gram_form(gram_table, r_map, change_map, False) / (
        gram_form(gram_table, change_map, change_map, False) + small_eps
    )
    step_mid = weight_one * lam_zero
    psi_mid_map = combine([(1.0, psi_map), (step_mid, {2: 1.0})])
    h_mid_map = combine([(1.0, ham_map), (step_mid, {3: 1.0})])
    r_mid_map = combine([(1.0, r_map), (-weight_one, change_map)])
    eps_mid = gram_form(gram_table, psi_mid_map, h_mid_map, False) / (
        gram_form(gram_table, psi_mid_map, psi_mid_map, False) + small_eps
    )
    level_mid = gram_form(gram_table, r_mid_map, r_mid_map, True) / (
        gram_form(gram_table, r_mid_map, r_mid_map, False) + small_eps
    )
    p_one = precondition(realize(r_mid_map, basis), kinetic, level_mid)
    g_one = apply_h(p_one)
    basis = [coeffs, h_zero, p_zero, g_zero, p_one, g_one]
    gram_table.update(gram_sums(basis, new_pairs(4, 6, (False,))))
    q_one_map = combine([(1.0, {5: 1.0}), (-eps_mid, {4: 1.0})])
    lam_one = -gram_form(gram_table, r_mid_map, q_one_map, False) / (
        gram_form(gram_table, q_one_map, q_one_map, False) + small_eps
    )
    new_map = combine([(1.0, psi_mid_map), (lam_one, {4: 1.0})])
    ham_new_map = combine([(1.0, h_mid_map), (lam_one, {5: 1.0})])
    norm_new = gram_form(gram_table, new_map, new_map, False) + small_eps
    energy = gram_form(gram_table, new_map, ham_new_map, False) / norm_new
    resid_map = combine([(1.0, ham_new_map), (-energy, new_map)])
    residual_norm = gram_form(gram_table, resid_map, resid_map, False) / norm_new
    new_bands = realize(new_map, basis)
    new_ham = realize(ham_new_map, basis)
    blank_rows = jnp.zeros((2, band_local, band_local * lax.axis_size("band")), jnp.float32)
    first_row = jnp.int32(0)
    over_rows = blank_rows
    ham_rows = blank_rows
    piece_bands = lax.all_gather(new_bands, "band", axis=1, tiled=True)
    piece_ham = lax.all_gather(new_ham, "band", axis=1, tiled=True)
    over_rows = lax.dynamic_update_slice_in_dim(
        over_rows, pair_products(new_bands, piece_bands), first_row, 2
    )
    ham_rows = lax.dynamic_update_slice_in_dim(
        ham_rows, pair_products(new_bands, piece_ham), first_row, 2
    )
    over_rows, ham_rows = (over_rows, ham_rows)
    over_rows, ham_rows = lax.psum((over_rows, ham_rows), "ga")
    correlation = over_rows / total_pw
    subspace = ham_rows / total_pw
    return (new_bands, energy, residual_norm, correlation, subspace)


WIDE = 256
MESH = pl.DeviceIdType.MESH


def split_const(values):
    high = np.asarray(values, np.float32).astype(jnp.bfloat16)
    low = (values - high.astype(np.float64)).astype(np.float32).astype(jnp.bfloat16)
    return np.stack([high, low])


def const_tables(grid_len, group):
    planes = grid_len // group
    unit = 2.0 * np.pi / grid_len
    freq = np.arange(grid_len)
    y_real = np.arange(group)[:, None] * planes + np.arange(planes)[None, :]
    phase = unit * ((y_real[..., None] * freq) % grid_len)
    cos_y, sin_y = np.cos(phase), np.sin(phase)
    high, low = split_const(np.concatenate([
        cos_y[:, :8], sin_y[:, :8], cos_y[:, 8:], sin_y[:, 8:], -sin_y[:, 8:], cos_y[:, 8:]], axis=1))
    wave = np.concatenate([high, low], axis=2)
    theta = unit * (np.outer(freq, freq) % grid_len)
    turn = np.zeros((2, 128, 2, 128))
    turn[0, :grid_len, 0, :grid_len] = np.cos(theta)
    turn[0, :grid_len, 1, :grid_len] = np.sin(theta)
    turn[1, :grid_len, 0, :grid_len] = -np.sin(theta)
    turn[1, :grid_len, 1, :grid_len] = np.cos(theta)
    turn = turn.reshape(256, 256)
    zed = np.concatenate([split_const(turn), split_const(turn.T)], axis=0)
    return wave, zed


def two_parts(values):
    high = values.astype(jnp.bfloat16)
    low = (values - high.astype(jnp.float32)).astype(jnp.bfloat16)
    return high, low


def split_rows(values):
    high = values.astype(jnp.bfloat16).astype(jnp.float32)
    return jnp.concatenate([high, values - high], axis=0).astype(jnp.bfloat16)


def bdot(left, right):
    return jnp.dot(left, right, preferred_element_type=jnp.float32)


def bdot_t(left, right):
    return lax.dot_general(left, right, (((1,), (1,)), ((), ())), preferred_element_type=jnp.float32)


def total_of(values):
    return jnp.sum(jnp.sum(values, axis=0, keepdims=True), axis=1, keepdims=True)


def c_add(one, two):
    return one[0] + two[0], one[1] + two[1]


def c_sub(one, two):
    return one[0] - two[0], one[1] - two[1]


def c_turn(one, direction):
    return (-one[1], one[0]) if direction > 0 else (one[1], -one[0])


def c_mul(one, cos_val, sin_val):
    return one[0] * cos_val - one[1] * sin_val, one[0] * sin_val + one[1] * cos_val


def c_scale(one, factor):
    return one[0] * factor, one[1] * factor


def three_point(items, direction):
    total = c_add(items[1], items[2])
    side = c_scale(c_turn(c_sub(items[1], items[2]), direction), 0.8660254037844386)
    base = c_sub(items[0], c_scale(total, 0.5))
    return [c_add(items[0], total), c_add(base, side), c_sub(base, side)]


def four_point(items, direction):
    even, odd = c_add(items[0], items[2]), c_add(items[1], items[3])
    low, high = c_sub(items[0], items[2]), c_turn(c_sub(items[1], items[3]), direction)
    return [c_add(even, odd), c_add(low, high), c_sub(even, odd), c_sub(low, high)]


def eight_point(items, direction):
    even = four_point(items[0::2], direction)
    odd = four_point(items[1::2], direction)
    root = 0.7071067811865476
    turned = [
        odd[0],
        c_scale(c_add(odd[1], c_turn(odd[1], direction)), root),
        c_turn(odd[2], direction),
        c_scale(c_sub(c_turn(odd[3], direction), odd[3]), root),
    ]
    return [c_add(e, o) for e, o in zip(even, turned)] + [c_sub(e, o) for e, o in zip(even, turned)]


def twelve_point(items, direction):
    fours = [four_point([items[(4 * a + 3 * b) % 12] for b in range(4)], direction) for a in range(3)]
    threes = [three_point([fours[a][v] for a in range(3)], direction) for v in range(4)]
    return [threes[v % 4][v % 3] for v in range(12)]


def sweep_kernel(
    dims,
    coeffs_hbm, cell_hbm, potential_hbm, proj_hbm, strength_hbm, atom_hbm, chan_hbm,
    wave_hbm, zed_hbm,
    new_hbm, scal_hbm,
    hot_ref, fold_ref, group_ref, phase_ref, kin_ref, work_ref, left_ref,
    pot_ref, potential_ref, proj_ref, couple_ref, in_vec, out_vec, save_ref,
    strength_ref, atom_ref, chan_ref, wave_ref, zed_ref, new_ref, scal_ref, in_sem,
    ksend, krecv, xsend, xrecv, rsend, rrecv, hsend, hrecv, psend, precv,
    wsend, wrecv, nsend, nrecv, lsend, lrecv, csend, crecv,
    ks_sem, kr_sem, xs_sem, xr_sem, rs_sem, rr_sem, hs_sem, hr_sem, ps_sem, pr_sem,
    ws_sem, wr_sem, ns_sem, nr_sem, cs_sem, cr_sem,
):
    group, bands, planes, grid_len, total_pw, pw = dims
    slab = 2 * planes
    folds = planes // 2 - 1
    half = group // 2
    gap = 128 - grid_len
    splits = grid_len // gap
    tiles = pw // 128
    me = lax.axis_index("ga")
    band = lax.axis_index("band")
    sides = [1 - 2 * lax.rem(me // (1 << bit), 2) for bit in range(3)]

    def peer_of(mask):
        return me + sum(sides[bit] * ((mask // (1 << bit)) % 2) * (1 << bit) for bit in range(3))

    loads = [
        pltpu.make_async_copy(source, target, in_sem.at[k])
        for k, (source, target) in enumerate((
            (cell_hbm, ksend), (coeffs_hbm, xsend), (wave_hbm.at[me], wave_ref), (strength_hbm, strength_ref),
            (atom_hbm, atom_ref), (chan_hbm, chan_ref), (potential_hbm, potential_ref), (proj_hbm, proj_ref),
            (zed_hbm, zed_ref)))
    ]
    for load in loads[:2]:
        load.start()
    barrier = pltpu.get_barrier_semaphore()
    world = [(off, mask) for off in (2, 3, 1, 0) for mask in (7, 6, 5, 4, 3, 2, 1, 0) if off or mask]
    for off, mask in world:
        pl.semaphore_signal(barrier, inc=1, device_id={"band": lax.rem(band + off, bands), "ga": peer_of(mask)}, device_id_type=MESH)
    for load in loads[2:]:
        load.start()
    for load in loads[:2]:
        load.wait()

    far_first = (6, 7, 4, 5, 2, 3, 1)
    near_first = (2, 4, 3, 5, 6, 7, 1)

    def stage_of(mask):
        return (mask > 1) + (mask > 5)

    def wait_bytes(ref, sem):
        pltpu.make_async_copy(ref, ref, sem).wait()

    def spread_copy(mask, send, recv, send_sem, recv_sem):
        peer = peer_of(mask)
        return pltpu.make_async_remote_copy(
            src_ref=send, dst_ref=recv.at[me],
            send_sem=send_sem.at[0], recv_sem=recv_sem.at[0 if recv_sem.shape[0] == 1 else stage_of(mask)],
            device_id={"ga": peer}, device_id_type=MESH)

    def spread_start(order, send, recv, send_sem, recv_sem):
        for mask in order:
            spread_copy(mask, send, recv, send_sem, recv_sem).start()

    def spread_wait(send, recv, send_sem, recv_sem):
        wait_bytes(recv.at[pl.ds(0, group - 1)], recv_sem.at[0])
        wait_bytes(recv.at[pl.ds(0, group - 1)], send_sem.at[0])

    keys = (ksend, krecv, ks_sem, kr_sem)
    firsts = (xsend, xrecv, xs_sem, xr_sem)
    pl.semaphore_wait(barrier, group * bands - 1)
    spread_start(near_first, *keys)
    spread_start(near_first, *firsts)
    krecv[me] = ksend[...]
    xrecv[me] = xsend[...]

    def whole(values):
        return jnp.floor(values)

    def signed(values):
        return jnp.where(2.0 * values < grid_len, values, values - grid_len)

    def numbers(cells):
        plane = whole((cells + 0.5) * (1.0 / (grid_len * grid_len)))
        in_plane = cells - plane * (grid_len * grid_len)
        y_num = whole((in_plane + 0.5) * (1.0 / grid_len))
        return plane, y_num, in_plane - y_num * grid_len

    def cell_row(src):
        cell = krecv[src].astype(jnp.float32)
        return jnp.concatenate([cell[k:k + 1] for k in range(tiles)], axis=1)

    def kinetic(plane, y_num, z_num, device):
        f_x = signed(plane * group + device)
        f_y, f_z = signed(y_num), signed(z_num)
        return kin_unit * (f_x * f_x + f_y * f_y + f_z * f_z)

    def marks(numbers_row, count):
        wide_row = jnp.broadcast_to(numbers_row, (16, pw)).astype(jnp.bfloat16)
        row_id = lax.broadcasted_iota(jnp.int32, (16, pw), 0).astype(jnp.float32).astype(jnp.bfloat16)
        one, zero = jnp.ones((16, pw), jnp.bfloat16), jnp.zeros((16, pw), jnp.bfloat16)
        return [jnp.where(row_id + 16.0 * k == wide_row, one, zero) for k in range(count)]

    def build_source(src):
        plane, y_num, z_num = numbers(cell_row(src))
        pair = whole((plane + 0.5) * 0.5)
        piece = whole((z_num + 0.5) * (1.0 / gap))
        hole = (plane - 2.0 * folds) * splits + piece
        hole_pair = whole((hole + 0.5) * 0.5)
        main = plane < 2.0 * folds
        fold = jnp.where(main, pair, hole_pair)
        lane = jnp.where(
            main, (plane - 2.0 * pair) * 128.0 + z_num,
            (hole - 2.0 * hole_pair) * 128.0 + grid_len + z_num - gap * piece)
        group_ref[src] = fold
        fold_ref[src] = jnp.broadcast_to(fold, (16, pw)).astype(jnp.bfloat16)
        for k, rows in enumerate(marks(lane, WIDE // 16)):
            hot_ref[src, 16 * k:16 * (k + 1), :] = rows
        y_hot = marks(y_num, grid_len // 16)
        phase_ref[src] = bdot(wave_ref[...], jnp.concatenate(y_hot + y_hot, axis=0))

    def build_potential():
        pad = jnp.zeros((8, 128 - grid_len), jnp.float32)

        def put_tile(v, slot, block):
            pot_ref[v, slot] = jnp.concatenate([block * (1.0 / grid_len**3), pad], axis=1)

        def lines(x_real, first, count):
            return potential_ref[pl.ds(first * grid_len + x_real, count, stride=grid_len), :]

        for v in range(planes):
            for u in range(group):
                put_tile(v, u, lines(v + planes * u, 0, 8))
            for t in range(half):
                put_tile(v, group + t, jnp.concatenate([
                    lines(v + planes * 2 * t, 8, planes - 8), lines(v + planes * (2 * t + 1), 8, planes - 8)], axis=0))

    def build_coupling():
        atoms, chans = strength_ref.shape[0] // strength_ref.shape[1], strength_ref.shape[1]
        size = atoms * chans
        ident = atom_ref[...] * chans + chan_ref[...]
        hot = (lax.broadcasted_iota(jnp.int32, (size, ident.shape[1]), 0) == ident).astype(jnp.float32)
        row_at = lax.broadcasted_iota(jnp.int32, (size, size), 0)
        col_at = lax.broadcasted_iota(jnp.int32, (size, size), 1)
        tiled = jnp.concatenate([strength_ref[...]] * atoms, axis=1)
        same = (row_at // chans == col_at // chans).astype(jnp.float32)
        block = tiled * same
        block = 0.5 * (block + jnp.transpose(block))
        half = lax.dot_general(hot, block, (((0,), (0,)), ((), ())), precision=top_precision, preferred_element_type=jnp.float32)
        couple_ref[...] = jnp.dot(half, hot, precision=top_precision, preferred_element_type=jnp.float32)

    loads[2].wait()
    build_source(me)
    for load in loads[3:6]:
        load.wait()
    build_coupling()
    loads[6].wait()
    build_potential()
    loads[7].wait()
    loads[8].wait()
    for stage, masks in enumerate(((1,), (2, 3, 4, 5), (6, 7))):
        wait_bytes(krecv.at[pl.ds(0, len(masks))], kr_sem.at[stage])
        for mask in masks:
            build_source(peer_of(mask))
    wait_bytes(krecv.at[pl.ds(0, group - 1)], ks_sem.at[0])

    def stack_rows(pieces):
        return jnp.concatenate(pieces, axis=0)

    cells = stack_rows([cell_row(s) for s in range(group)])
    owner = lax.broadcasted_iota(jnp.int32, (group, pw), 0).astype(jnp.float32)
    kin_ref[...] = kinetic(*numbers(cells), owner)
    spread_wait(*firsts)
    for part in range(2):
        in_vec[0, part] = stack_rows([xrecv[s, part] for s in range(group)])

    upper = lax.broadcasted_iota(jnp.int32, (8, 128), 0) < 4
    lane_at = lax.broadcasted_iota(jnp.int32, (8, 128), 1)
    flip = jnp.where(upper, 1.0, -1.0).astype(jnp.float32)

    def swap_half(values):
        return pltpu.roll(values, 4, 0)

    def halves(low, high):
        return low if low == high else jnp.where(upper, low, high)

    def lane_turn(s, v, paired):
        angle = [2.0 * np.pi * ((k * v) % grid_len) / grid_len for k in (s, s + half)]
        cos_val, sin_val = [float(np.cos(a)) for a in angle], [float(np.sin(a)) for a in angle]
        if paired:
            return halves(*cos_val), halves(*sin_val)
        return cos_val[0], sin_val[0]

    def twist(item, s, v, paired, direction):
        if v == 0 or (s == 0 and not paired):
            return item
        cos_val, sin_val = lane_turn(s, v, paired)
        return c_mul(item, cos_val, sin_val if direction > 0 else -sin_val)

    def z_turn(tiles, which):
        stacked = jnp.concatenate([jnp.concatenate(list(t), axis=1) for t in tiles], axis=0)
        high, low = two_parts(stacked)
        out = bdot(high, zed_ref[which]) + bdot(low, zed_ref[which]) + bdot(high, zed_ref[which + 1])
        return [(out[8 * k:8 * k + 8, :128], out[8 * k:8 * k + 8, 128:]) for k in range(len(tiles))]

    def keep(slot, v, item):
        work_ref[0, v, slot] = item[0]
        work_ref[1, v, slot] = item[1]

    def kept(slot, v):
        return work_ref[0, v, slot], work_ref[1, v, slot]

    def own_row(ref, turn, part):
        return ref[turn, part, pl.ds(me, 1), :]

    def put(turn, src):
        v_re, v_im = in_vec[turn, 0, src:src + 1, :], in_vec[turn, 1, src:src + 1, :]
        cos_y, sin_y, mix_re, mix_im = [phase_ref[src, 8 * k:8 * k + 8, :] for k in range(4)]
        both = split_rows(jnp.concatenate([
            cos_y * v_re - sin_y * v_im, mix_re * v_re + mix_im * v_im, sin_y * v_re + cos_y * v_im], axis=0))
        pieces = []
        fold = fold_ref[src]
        blank = jnp.zeros((16, pw), jnp.bfloat16)
        for k in range(folds):
            hit = fold == float(k)
            for at in range(0, 2 * slab, 16):
                pieces.append(jnp.where(hit, both[at:at + 16], blank))
        out = bdot_t(jnp.concatenate(pieces, axis=0), hot_ref[src])
        tiles = []
        for k in range(folds):
            base = k * 2 * slab
            block = out[base:base + slab] + out[base + slab:base + 2 * slab]
            for at in (0, 128):
                tiles.append([block[8 * t:8 * t + 8, at:at + 128] for t in range(3)])
        for extra in range(planes - 2 * folds):
            joined = []
            for t in range(3):
                run = None
                for q in reversed(range(splits)):
                    moved = pltpu.roll(tiles[extra * splits + q][t], (q + 1) * gap, 1)
                    run = moved if run is None else jnp.where(lane_at < (q + 1) * gap, moved, run)
                joined.append(run)
            tiles.append(joined)
        return tiles

    def forward_turn(s, low, high):
        rest = [(
            jnp.where(upper, a[1], swap_half(b[1])), jnp.where(upper, swap_half(a[1]), b[1]),
        ) for a, b in zip(low, high)]
        turned = z_turn([(a[0], a[2]) for a in low] + [(b[0], b[2]) for b in high] + rest, 0)
        for k, (slot, first, paired) in enumerate(((s, s, False), (s + half, s + half, False), (group + s, s, True))):
            for v, item in enumerate(twelve_point(turned[k * planes:(k + 1) * planes], 1)):
                keep(slot, v, twist(item, first, v, paired, 1))

    def cross(item):
        return tuple(swap_half(x) + x * flip for x in item)

    def half_turn(item, s, direction):
        if s == 0:
            return item
        angle = 2.0 * np.pi * s / group
        return c_mul(item, halves(1.0, float(np.cos(angle))), direction * halves(0.0, float(np.sin(angle))))

    def middle(v):
        items = eight_point([kept(s, v) for s in range(group)], 1)
        items = [c_scale(item, pot_ref[v, u]) for u, item in enumerate(items)]
        for s, item in enumerate(eight_point(items, -1)):
            keep(s, v, twist(item, s, v, False, -1))
        items = four_point([half_turn(cross(kept(group + s, v)), s, 1) for s in range(half)], 1)
        items = [c_scale(item, pot_ref[v, group + t]) for t, item in enumerate(items)]
        for s, item in enumerate(four_point(items, -1)):
            keep(group + s, v, twist(cross(half_turn(item, s, -1)), s, v, True, -1))

    def backward_pair(s):
        spread = []
        for slot in (s, s + half, group + s):
            spread += twelve_point([kept(slot, v) for v in range(planes)], -1)
        turned = z_turn(spread, 2)
        low, high, rest = [turned[k * planes:(k + 1) * planes] for k in range(3)]
        low = [(a[0], jnp.where(upper, r[0], swap_half(r[1])), a[1]) for a, r in zip(low, rest)]
        high = [(b[0], jnp.where(upper, swap_half(r[0]), r[1]), b[1]) for b, r in zip(high, rest)]
        for dest, tiles in ((s, low), (s + half, high)):
            for hole in range((planes - 2 * folds) * splits):
                extra, q = 2 * folds + hole // splits, hole % splits
                tiles[hole] = tuple(
                    jnp.where(lane_at >= grid_len, pltpu.roll(tiles[extra][t], grid_len - q * gap, 1), tiles[hole][t])
                    for t in range(3))
            for k in range(folds):
                block = jnp.concatenate([jnp.concatenate(tiles[2 * k + m], axis=0) for m in range(2)], axis=1)
                left_ref[dest, k * 2 * slab:(k + 1) * 2 * slab, :] = split_rows(block)

    def partial_copy(turn, mask):
        return pltpu.make_async_remote_copy(
            src_ref=rsend.at[turn, mask], dst_ref=rrecv.at[turn, mask],
            send_sem=rs_sem.at[0], recv_sem=rr_sem.at[0],
            device_id={"ga": peer_of(mask)}, device_id_type=MESH)

    def take_tile(mask, at):
        return bdot(left_ref[peer_of(mask)], hot_ref[peer_of(mask), :, at:at + WIDE])

    def take_sum(turn, mask, at, out):
        dest = peer_of(mask)
        span = slice(at, at + WIDE)
        fold = group_ref[dest, :, span]
        chosen = out[:2 * slab]
        for k in range(1, folds):
            chosen = jnp.where(fold == float(k), out[k * 2 * slab:(k + 1) * 2 * slab], chosen)
        value = chosen[:slab] + chosen[slab:]
        first, mixed, last = [value[8 * k:8 * k + 8] for k in range(3)]
        cos_y, sin_y, mix_re, mix_im = [phase_ref[dest, 8 * k:8 * k + 8, span] for k in range(4)]
        back_re = cos_y * first + sin_y * last + mix_re * mixed
        back_im = cos_y * last - sin_y * first + mix_im * mixed
        for part, back in enumerate((back_re, back_im)):
            rsend[turn, mask, part:part + 1, span] = jnp.sum(back, axis=0, keepdims=True)

    def take_all(turn):
        order = ((6, 7), (4, 5), (2, 3), (1, 0))
        units = [(masks, mask, at) for masks in order for mask in masks for at in range(0, pw, WIDE)]
        lag = 6
        pending = []
        for unit in units + [None] * lag:
            if unit:
                pending.append((unit, take_tile(*unit[1:])))
            if len(pending) > lag or not unit:
                (masks, mask, at), out = pending.pop(0)
                take_sum(turn, mask, at, out)
                if mask == masks[-1] and at + WIDE == pw:
                    for ready in masks:
                        if ready:
                            partial_copy(turn, ready).start()

    def all_sum(local, send, recv, send_sem, recv_sem):
        send[...] = local
        recv[me] = local
        spread_start(far_first, send, recv, send_sem, recv_sem)

    def all_sum_end(send, recv, send_sem, recv_sem):
        spread_wait(send, recv, send_sem, recv_sem)
        running = recv[0]
        for dev in range(1, group):
            running = running + recv[dev]
        return running

    def project(turn):
        found = []
        for part in range(2):
            row = own_row(in_vec, turn, part)
            running = proj_ref[:, :128] * row[:, :128]
            for at in range(128, pw, 128):
                running = running + proj_ref[:, at:at + 128] * row[:, at:at + 128]
            found.append(jnp.sum(jnp.transpose(running), axis=0, keepdims=True))
        return jnp.concatenate(found, axis=0)

    def nonlocal_rows(sums):
        half = sums.shape[1] // 2
        pair = jnp.concatenate([
            sums[0:1, :half] + sums[1:2, half:], sums[1:2, :half] - sums[0:1, half:]], axis=0)
        mixed = jnp.dot(pair, couple_ref[...], precision=top_precision, preferred_element_type=jnp.float32)
        m_re, m_im = mixed[0:1], mixed[1:2]
        found = []
        for row in (jnp.concatenate([m_re, -m_im], axis=1), jnp.concatenate([m_im, m_re], axis=1)):
            column = jnp.transpose(jnp.broadcast_to(row, (2 * half, 128)))
            found.append(jnp.concatenate([
                jnp.sum(proj_ref[:, at:at + 128] * column, axis=0, keepdims=True) for at in range(0, pw, 128)], axis=1))
        return jnp.concatenate(found, axis=0)

    def apply_h(turn):
        sums = (psend.at[turn], precv.at[turn], ps_sem, pr_sem)
        placed = []
        for s in range(half):
            placed.append((s, put(turn, s), put(turn, s + half)))
            if s:
                forward_turn(*placed.pop(0))
        forward_turn(*placed.pop(0))
        for v in range(planes):
            middle(v)
        for s in range(half):
            backward_pair(s)
        all_sum(project(turn), *sums)
        take_all(turn)
        start = nonlocal_rows(all_sum_end(*sums) * (1.0 / total_pw))
        own_kin = kin_ref[pl.ds(me, 1), :]
        start = start + own_kin * jnp.concatenate([own_row(in_vec, turn, 0), own_row(in_vec, turn, 1)], axis=0)
        running = start + rsend[turn, 0]
        @pl.when(turn == 2)
        def _():
            gram = gram_sums(third_pairs)
            packed = save_ref[8:9, :]
            for k, (one, two, kind) in enumerate(third_pairs):
                packed = jnp.where(lane_id == k + len(first_pairs + second_pairs), gram[kind, one, two], packed)
            share(1, lsend, lrecv, packed)

        wait_bytes(rrecv.at[turn, pl.ds(1, group - 1)], rr_sem.at[0])
        wait_bytes(rrecv.at[turn, pl.ds(1, group - 1)], rs_sem.at[0])
        for mask in range(1, group):
            running = running + rrecv[turn, mask]
        hsend[turn] = running
        return running

    def share_h(turn):
        out = (hsend.at[turn], hrecv.at[turn], hs_sem, hr_sem)
        spread_start(far_first, *out)
        hrecv[turn, me] = hsend[turn]
        spread_wait(*out)
        for part in range(2):
            out_vec[turn, part] = stack_rows([hrecv[turn, s, part:part + 1] for s in range(group)])

    def vector(index):
        ref = out_vec if index % 2 else in_vec
        return ref[index // 2]

    def gram_sums(pair_list):
        found = {}
        for one, two, use_kin in pair_list:
            left, right = vector(one), vector(two)
            product = left[0] * right[0] + left[1] * right[1]
            value = total_of(product * kin_ref[...] if use_kin else product) * (1.0 / total_pw)
            found[use_kin, one, two] = value
            found[use_kin, two, one] = value
        return found

    def realize(coef_map, basis):
        running = 0.0
        for index, coef in coef_map.items():
            running = running + (basis(index) if isinstance(coef, float) and coef == 1.0 else coef * basis(index))
        return running

    def smooth(residual, level):
        kin = kin_ref[...]
        ratio = kin / (1.5 * level + 1.0)
        poly = 27.0 + ratio * (18.0 + ratio * (12.0 + 8.0 * ratio))
        square = ratio * ratio
        return residual * (poly / (poly + 16.0 * square * square))

    def save(names, slot):
        for k, value in enumerate(names):
            save_ref[slot + k:slot + k + 1, :] = jnp.broadcast_to(value, (1, 128))

    def load_saved(slot):
        return save_ref[slot:slot + 1, 0:1]

    def first_step(gram):
        psi, ham = {0: 1.0}, {1: 1.0}
        eps_zero = gram_form(gram, psi, ham, False) / (gram_form(gram, psi, psi, False) + small_eps)
        return psi, ham, eps_zero, combine([(1.0, ham), (-eps_zero, psi)])

    def second_step(gram):
        psi, ham, eps_zero, r_map = first_step(gram)
        q_map = combine([(1.0, {3: 1.0}), (-eps_zero, {2: 1.0})])
        lam_zero = -gram_form(gram, r_map, q_map, False) / (gram_form(gram, q_map, q_map, False) + small_eps)
        psi_one = combine([(1.0, psi), (lam_zero, {2: 1.0})])
        h_one = combine([(1.0, ham), (lam_zero, {3: 1.0})])
        eps_one = gram_form(gram, psi_one, h_one, False) / (gram_form(gram, psi_one, psi_one, False) + small_eps)
        r_one = combine([(1.0, h_one), (-eps_one, psi_one)])
        change = combine([(1.0, r_map), (-1.0, r_one)])
        weight = gram_form(gram, r_map, change, False) / (gram_form(gram, change, change, False) + small_eps)
        step = weight * lam_zero
        psi_mid = combine([(1.0, psi), (step, {2: 1.0})])
        h_mid = combine([(1.0, ham), (step, {3: 1.0})])
        r_mid = combine([(1.0, r_map), (-weight, change)])
        eps_mid = gram_form(gram, psi_mid, h_mid, False) / (gram_form(gram, psi_mid, psi_mid, False) + small_eps)
        return psi_mid, h_mid, r_mid, eps_mid, step

    first_pairs = new_pairs(0, 2, (False, True))
    second_pairs = new_pairs(2, 4, (False, True))
    third_pairs = new_pairs(4, 5, (False,))
    last_pairs = new_pairs(5, 6, (False,))
    gram_pairs = first_pairs + second_pairs + third_pairs
    lane_id = lax.broadcasted_iota(jnp.int32, (1, 128), 1)

    def swap(which, send, recv, off):
        return pltpu.make_async_remote_copy(
            src_ref=send, dst_ref=recv.at[band],
            send_sem=ns_sem.at[which], recv_sem=nr_sem.at[which],
            device_id={"band": lax.rem(band + off, bands)}, device_id_type=MESH)

    def share(which, send, recv, values):
        send[...] = values
        recv[band] = values
        for off in range(1, bands):
            swap(which, send, recv, off).start()

    def share_end(which, send, recv):
        wait_bytes(recv.at[pl.ds(0, bands - 1)], nr_sem.at[which])
        wait_bytes(recv.at[pl.ds(0, bands - 1)], ns_sem.at[which])

    def own(index):
        ref = out_vec if index % 2 else in_vec
        return jnp.concatenate([own_row(ref, index // 2, 0), own_row(ref, index // 2, 1)], axis=0)

    def turn_step(turn, carry):
        apply_h(turn)

        @pl.when(turn == 0)
        def _():
            share_h(0)
            gram = gram_sums(first_pairs)
            save([gram[kind, one, two] for one, two, kind in first_pairs], 0)
            r_map = first_step(gram)[3]
            level = gram_form(gram, r_map, r_map, True) / (gram_form(gram, r_map, r_map, False) + small_eps)
            p_zero = smooth(realize(r_map, vector), level)
            in_vec[1] = p_zero

        @pl.when(turn == 1)
        def _():
            share_h(1)
            gram = gram_sums(second_pairs)
            for k, (one, two, kind) in enumerate(first_pairs):
                gram[kind, one, two] = gram[kind, two, one] = load_saved(k)
            psi_mid, h_mid, r_mid, eps_mid, step = second_step(gram)
            level = gram_form(gram, r_mid, r_mid, True) / (gram_form(gram, r_mid, r_mid, False) + small_eps)
            p_one = smooth(realize(r_mid, vector), level)
            in_vec[2] = p_one
            share(0, nsend, nrecv, jnp.stack([realize(psi_mid, own), own(4), realize(h_mid, own)]))
            packed = jnp.zeros((1, 128), jnp.float32)
            for k, (one, two, kind) in enumerate(first_pairs + second_pairs):
                packed = jnp.where(lane_id == k, gram[kind, one, two], packed)
            save_ref[8:9, :] = packed

        return carry

    lax.fori_loop(0, 3, turn_step, 0)

    g_own = hsend[2]

    def own_last(index):
        return g_own if index == 5 else own(index)

    def world_copy(off, mask):
        return pltpu.make_async_remote_copy(
            src_ref=wsend, dst_ref=wrecv.at[band * group + me],
            send_sem=ws_sem.at[0], recv_sem=wr_sem.at[0],
            device_id={"band": lax.rem(band + off, bands), "ga": peer_of(mask)}, device_id_type=MESH)

    local = jnp.zeros((1, 128), jnp.float32)
    for k, (one, two, kind) in enumerate(last_pairs):
        local = jnp.where(lane_id == k, total_of(own_last(one) * g_own), local)
    wsend[...] = local
    for off, mask in world:
        world_copy(off, mask).start()
    wrecv[band * group + me] = local

    share_end(0, nsend, nrecv)
    others = [[stack_rows([nrecv[o, which, part:part + 1] for o in range(bands)]) for part in range(2)] for which in range(3)]
    mine = [[nsend[which, part:part + 1] for part in range(2)] for which in range(3)] + [[g_own[0:1], g_own[1:2]]]

    def joined(first, second):
        return [jnp.concatenate([first[part], second[part]], axis=0) for part in range(2)]

    def twice(first, second):
        return [jnp.concatenate([jnp.broadcast_to(first[part], (bands, pw)), jnp.broadcast_to(second[part], (bands, pw))], axis=0) for part in range(2)]

    column_id = lax.broadcasted_iota(jnp.int32, (2 * bands, 128), 1)
    local = jnp.zeros((2 * bands, 128), jnp.float32)
    slot = 0
    for o_row, m_rows in (
        (joined(others[0], others[1]), (twice(mine[0], mine[0]), twice(mine[1], mine[1]))),
        (joined(others[2], others[1]), (twice(mine[0], mine[2]), twice(mine[1], mine[3]))),
    ):
        for m_re, m_im in m_rows:
            for product in (m_re * o_row[0] + m_im * o_row[1], m_re * o_row[1] - m_im * o_row[0]):
                local = jnp.where(column_id == slot, jnp.sum(product, axis=1, keepdims=True), local)
                slot += 1
    crossed = (csend, crecv, cs_sem, cr_sem)
    all_sum(local, *crossed)

    share_end(1, lsend, lrecv)
    early = stack_rows([lrecv[o] for o in range(bands)])
    gram = {}
    for k, (one, two, kind) in enumerate(gram_pairs):
        gram[kind, one, two] = gram[kind, two, one] = early[:, k:k + 1]
    psi_mid, h_mid, r_mid, eps_mid, step = second_step(gram)
    wait_bytes(wrecv.at[pl.ds(0, group * bands - 1)], wr_sem.at[0])
    late = []
    for other in range(bands):
        running = wrecv[other * group]
        for dev in range(1, group):
            running = running + wrecv[other * group + dev]
        late.append(running)
    late = stack_rows(late) * (1.0 / total_pw)
    for k, (one, two, kind) in enumerate(last_pairs):
        gram[kind, one, two] = gram[kind, two, one] = late[:, k:k + 1]
    q_one = combine([(1.0, {5: 1.0}), (-eps_mid, {4: 1.0})])
    lam_one = -gram_form(gram, r_mid, q_one, False) / (gram_form(gram, q_one, q_one, False) + small_eps)
    own_band = lax.broadcasted_iota(jnp.int32, (bands, 1), 0) == band

    def pick(column):
        return jnp.sum(jnp.where(own_band, column, 0.0), axis=0, keepdims=True)

    own_lam = pick(lam_one)
    new_ref[...] = nsend[0] + own_lam * nsend[1]
    stores = [pltpu.make_async_copy(new_ref, new_hbm, in_sem.at[0]), pltpu.make_async_copy(scal_ref, scal_hbm, in_sem.at[1])]
    stores[0].start()
    new_map = combine([(1.0, psi_mid), (lam_one, {4: 1.0})])
    ham_new = combine([(1.0, h_mid), (lam_one, {5: 1.0})])
    norm_new = gram_form(gram, new_map, new_map, False) + small_eps
    energy = gram_form(gram, new_map, ham_new, False) / norm_new
    resid = combine([(1.0, ham_new), (-energy, new_map)])
    resid_norm = gram_form(gram, resid, resid, False) / norm_new
    summed = all_sum_end(*crossed) * (1.0 / total_pw)
    mixed = summed[:bands] + lam_one * summed[bands:]
    result = mixed + own_lam * pltpu.roll(mixed, 126, 1)
    scal_ref[...] = jnp.concatenate([
        result, jnp.broadcast_to(pick(energy), (1, 128)), jnp.broadcast_to(pick(resid_norm), (1, 128)),
        jnp.zeros((scal_ref.shape[0] - bands - 2, 128), jnp.float32)], axis=0)
    stores[1].start()
    wait_bytes(wrecv.at[pl.ds(0, group * bands - 1)], ws_sem.at[0])
    for store in stores:
        store.wait()


def finish_kernel(bands, new_ref, scal_ref, bands_ref, energy_ref, norm_ref, corr_ref, sub_ref):
    bands_ref[:, 0, :] = new_ref[...]
    lane = lax.broadcasted_iota(jnp.int32, (1, bands), 1)
    for ref, base in ((corr_ref, 0), (sub_ref, 4)):
        for part in range(2):
            row = jnp.zeros((1, bands), jnp.float32)
            for other in range(bands):
                at = base + part
                row = jnp.where(lane == other, scal_ref[other:other + 1, at:at + 1], row)
            ref[part] = row
    energy_ref[0] = scal_ref[bands, 0]
    norm_ref[0] = scal_ref[bands + 1, 0]


def kernel_body(coeffs, cell_map, potential, projectors, strengths, proj_atom, proj_chan):
    group = lax.axis_size("ga")
    bands = lax.axis_size("band")
    grid_len = potential.shape[0]
    planes = grid_len // group
    pw = coeffs.shape[2]
    total_pw = pw * group
    slab = 2 * planes
    folds = planes // 2 - 1
    tile_count = group + group // 2
    proj_rows = 2 * projectors.shape[1]
    tables = [jnp.asarray(t) for t in const_tables(grid_len, group)]
    dma = pltpu.SemaphoreType.DMA
    vmem = pl.BlockSpec(memory_space=pltpu.VMEM)
    far = pl.BlockSpec(memory_space=pl.ANY)
    f32, b16 = jnp.float32, jnp.bfloat16
    scal_rows = 8 * (-(-(bands + 2) // 8))
    new, scal = pl.pallas_call(
        functools.partial(sweep_kernel, (group, bands, planes, grid_len, total_pw, pw)),
        out_shape=(
            jax.ShapeDtypeStruct((2, pw), f32),
            jax.ShapeDtypeStruct((scal_rows, 128), f32),
        ),
        in_specs=[far] * 9,
        out_specs=(far, far),
        scratch_shapes=[
            pltpu.VMEM((group, WIDE, pw), b16),
            pltpu.VMEM((group, 16, pw), b16),
            pltpu.VMEM((group, 1, pw), f32),
            pltpu.VMEM((group, 32, pw), f32),
            pltpu.VMEM((group, pw), f32),
            pltpu.VMEM((2, planes, tile_count, 8, 128), f32),
            pltpu.VMEM((group, folds * 2 * slab, WIDE), b16),
            pltpu.VMEM((planes, tile_count, 8, 128), f32),
            pltpu.VMEM((planes * grid_len, grid_len), f32),
            pltpu.VMEM((proj_rows, pw), f32),
            pltpu.VMEM((proj_rows // 2, proj_rows // 2), f32),
            pltpu.VMEM((3, 2, group, pw), f32),
            pltpu.VMEM((2, 2, group, pw), f32),
            pltpu.VMEM((24, 128), f32),
            pltpu.VMEM((strengths.shape[0] * strengths.shape[1], strengths.shape[2]), f32),
            pltpu.VMEM((1, proj_atom.shape[0]), jnp.int32), pltpu.VMEM((1, proj_chan.shape[0]), jnp.int32),
            pltpu.VMEM(tables[0].shape[1:], b16), pltpu.VMEM(tables[1].shape, b16),
            pltpu.VMEM((2, pw), f32), pltpu.VMEM((scal_rows, 128), f32),
            dma((9,)),
            pltpu.VMEM((pw // 128, 128), jnp.int32), pltpu.VMEM((group, pw // 128, 128), jnp.int32),
            pltpu.VMEM((2, 1, pw), f32), pltpu.VMEM((group, 2, 1, pw), f32),
            pltpu.VMEM((3, group, 2, pw), f32), pltpu.VMEM((3, group, 2, pw), f32),
            pltpu.VMEM((3, 2, pw), f32), pltpu.VMEM((2, group, 2, pw), f32),
            pltpu.VMEM((3, 2, proj_rows), f32), pltpu.VMEM((3, group, 2, proj_rows), f32),
            pltpu.VMEM((1, 128), f32), pltpu.VMEM((bands * group, 1, 128), f32),
            pltpu.VMEM((3, 2, pw), f32), pltpu.VMEM((bands, 3, 2, pw), f32),
            pltpu.VMEM((1, 128), f32), pltpu.VMEM((bands, 1, 128), f32),
            pltpu.VMEM((2 * bands, 128), f32), pltpu.VMEM((group, 2 * bands, 128), f32),
            dma((1,)), dma((3,)), dma((1,)), dma((1,)), dma((1,)), dma((1,)), dma((1,)), dma((1,)),
            dma((1,)), dma((1,)), dma((1,)), dma((1,)), dma((2,)), dma((2,)), dma((1,)), dma((1,)),
        ],
        compiler_params=pltpu.CompilerParams(
            collective_id=0, has_side_effects=True, vmem_limit_bytes=60 * 1024 * 1024
        ),
        name="sweeps",
    )(
        coeffs, cell_map.reshape(-1, 128), jnp.swapaxes(potential, 0, 1).reshape(planes * grid_len, grid_len),
        projectors.reshape(proj_rows, pw), strengths.reshape(-1, strengths.shape[2]),
        proj_atom.reshape(1, -1), proj_chan.reshape(1, -1), *tables,
    )

    smem = pl.BlockSpec(memory_space=pltpu.SMEM)
    return pl.pallas_call(
        functools.partial(finish_kernel, bands),
        out_shape=(
            jax.ShapeDtypeStruct((2, 1, pw), f32),
            jax.ShapeDtypeStruct((1,), f32),
            jax.ShapeDtypeStruct((1,), f32),
            jax.ShapeDtypeStruct((2, 1, bands), f32),
            jax.ShapeDtypeStruct((2, 1, bands), f32),
        ),
        in_specs=[vmem, vmem],
        out_specs=(vmem, smem, smem, vmem, vmem),
        name="finish",
    )(new, scal)


def body(coeffs, cell_map, potential, projectors, strengths, proj_atom, proj_chan):
    group = lax.axis_size("ga")
    grid_len = potential.shape[0]
    planes = grid_len // group
    fits = (
        group == 8
        and planes == 12
        and coeffs.shape[1] == 1
        and coeffs.shape[2] % 256 == 0
        and 2 * projectors.shape[1] == 128
    )
    chosen = kernel_body if fits else plain_body
    return chosen(coeffs, cell_map, potential, projectors, strengths, proj_atom, proj_chan)


def solution(mesh):
    placed = (
        P(None, "band", "ga"),
        P("ga"),
        P(None, "ga", None),
        P(None, None, "ga"),
        P(),
        P(),
        P(),
    )
    return jax.shard_map(
        body,
        mesh=mesh,
        in_specs=placed,
        out_specs=(
            P(None, "band", "ga"),
            P("band"),
            P("band"),
            P(None, "band", None),
            P(None, "band", None),
        ),
        check_vma=False,
    )
```
